16 devices in a mesh: graph: 16 (over z, y, x, core).
Axes of the slice: x: 2, y: 2, z: 2, core: 2. Of those that a mesh axis runs over, the one named last changes fastest.
Arguments:
- node_feats: bfloat16 [32768, 128], P('graph')
- w_one: float32 [128, 256], replicated
- w_two: float32 [256, 172], replicated
- send_idx: int32 [32, 1024], P('graph')
- edge_src: int32 [131072], P('graph')
- edge_dst: int32 [131072], P('graph')
- edge_w: float32 [131072], P('graph')
- labels: int32 [32768], P('graph')
- label_mask: int32 [32768], P('graph')
Outputs:
- output 1: float32 [], replicated
- output 2: float32 [128, 256], replicated
- output 3: float32 [256, 172], replicated
All inputs are finite; a program needn't handle non-finite values.
Results may differ from the reference program's by a relative error of at most 0.001.
Values are sent between devices in bfloat16 or wider.
A program may use at most 1 GiB of HBM per device.

```python
import jax
import jax.numpy as jnp
from jax import lax

GRAPH = 16
N_LOC = 2048
HALO = 1024
EDGES = 8192
F_IN = 128
F_HID = 256
CLASSES = 172


def draw_structure(key):
    sub_keys = jax.random.split(key, 9)
    halo_pct = jax.random.randint(sub_keys[0], (GRAPH, 1), 5, 21, jnp.int32)
    pick_draw = jax.random.randint(sub_keys[1], (GRAPH, EDGES), 0, 100, jnp.int32)
    own_src = jax.random.randint(sub_keys[2], (GRAPH, EDGES), 0, N_LOC, jnp.int32)
    halo_src = jax.random.randint(sub_keys[3], (GRAPH, EDGES), N_LOC, N_LOC + 2 * HALO, jnp.int32)
    edge_src = jnp.where(pick_draw < halo_pct, halo_src, own_src)
    edge_dst = jax.random.randint(sub_keys[4], (GRAPH, EDGES), 0, N_LOC, jnp.int32)
    live_count = jax.random.randint(sub_keys[5], (GRAPH, 1), EDGES // 4, EDGES + 1, jnp.int32)
    is_live = jnp.arange(EDGES)[None, :] < live_count
    send_idx = jax.random.randint(sub_keys[6], (GRAPH * 2, HALO), 0, N_LOC, jnp.int32)
    labels = jax.random.randint(sub_keys[7], (GRAPH * N_LOC,), 0, CLASSES, jnp.int32)
    label_mask = jax.random.randint(sub_keys[8], (GRAPH * N_LOC,), 0, 2, jnp.int32)
    return edge_src, edge_dst, is_live, send_idx, labels, label_mask


def normalise(raw_weight, edge_dst):
    weight_sum = jax.vmap(lambda w_g, dst_g: jax.ops.segment_sum(w_g, dst_g, num_segments=N_LOC))(raw_weight, edge_dst)
    node_sum = jnp.take_along_axis(weight_sum, edge_dst, axis=1)
    return raw_weight / jnp.maximum(node_sum, 1e-6)


def setup_inputs(seed: int = 0) -> dict:
    key_list = jax.random.split(jax.random.key(seed), 5)
    edge_src, edge_dst, is_live, send_idx, labels, label_mask = draw_structure(key_list[0])
    deg_gain = EDGES / N_LOC
    node_feats = jax.random.normal(key_list[1], (GRAPH * N_LOC, F_IN), jnp.float32)
    w_one = jax.random.normal(key_list[2], (F_IN, F_HID), jnp.float32) * (deg_gain / F_IN) ** 0.5
    w_two = jax.random.normal(key_list[3], (F_HID, CLASSES), jnp.float32) * (deg_gain / F_HID) ** 0.5
    raw_weight = jax.random.uniform(key_list[4], (GRAPH, EDGES), jnp.float32, 0.5, 1.5) * is_live
    edge_w = normalise(raw_weight, edge_dst)
    return {"node_feats": node_feats.astype(jnp.bfloat16), "w_one": w_one, "w_two": w_two, "send_idx": send_idx, "edge_src": edge_src.reshape(-1), "edge_dst": edge_dst.reshape(-1), "edge_w": edge_w.reshape(-1), "labels": labels, "label_mask": label_mask}


def halo_extend(node_table, send_rows):
    pick_rows = jax.vmap(lambda table_g, idx_g: table_g[idx_g])
    from_prev = pick_rows(jnp.roll(node_table, 1, axis=0), jnp.roll(send_rows[:, 1], 1, axis=0))
    from_next = pick_rows(jnp.roll(node_table, -1, axis=0), jnp.roll(send_rows[:, 0], -1, axis=0))
    return jnp.concatenate([node_table, from_prev, from_next], axis=1)


def aggregate(ext_table, src_dev, dst_dev, w_dev):
    def one_device(args_g):
        ext_g, src_g, dst_g, w_g = args_g
        return jax.ops.segment_sum(w_g[:, None] * ext_g[src_g].astype(jnp.float32), dst_g, num_segments=N_LOC)
    return lax.map(one_device, (ext_table, src_dev, dst_dev, w_dev))


def scatter_back(grad_rows, send_rows, src_dev, dst_dev, w_dev):
    def one_device(args_g):
        grad_g, src_g, dst_g, w_g = args_g
        return jax.ops.segment_sum(w_g[:, None] * grad_g[dst_g], src_g, num_segments=N_LOC + 2 * HALO)
    ext_grad = lax.map(one_device, (grad_rows, src_dev, dst_dev, w_dev))
    back_prev = jnp.roll(ext_grad[:, N_LOC:N_LOC + HALO], -1, axis=0)
    back_next = jnp.roll(ext_grad[:, N_LOC + HALO:], 1, axis=0)
    row_ids = jnp.concatenate([send_rows[:, 1], send_rows[:, 0]], axis=1)
    ret_vals = jnp.concatenate([back_prev, back_next], axis=1)
    returned = jax.vmap(lambda vals_g, ids_g: jax.ops.segment_sum(vals_g, ids_g, num_segments=N_LOC))(ret_vals, row_ids)
    return ext_grad[:, :N_LOC] + returned


def reference(node_feats, w_one, w_two, send_idx, edge_src, edge_dst, edge_w, labels, label_mask):
    send_rows = send_idx.reshape(GRAPH, 2, HALO)
    src_dev = edge_src.reshape(GRAPH, EDGES)
    dst_dev = edge_dst.reshape(GRAPH, EDGES)
    w_dev = edge_w.reshape(GRAPH, EDGES)
    w_one_b = w_one.astype(jnp.bfloat16)
    w_two_b = w_two.astype(jnp.bfloat16)
    tab_one = jnp.dot(node_feats, w_one_b, preferred_element_type=jnp.float32).astype(jnp.bfloat16)
    pre_one = aggregate(halo_extend(tab_one.reshape(GRAPH, N_LOC, F_HID), send_rows), src_dev, dst_dev, w_dev).reshape(GRAPH * N_LOC, F_HID)
    hidden = jnp.maximum(pre_one, 0.0).astype(jnp.bfloat16)
    tab_two = jnp.dot(hidden, w_two_b, preferred_element_type=jnp.float32).astype(jnp.bfloat16)
    logits = aggregate(halo_extend(tab_two.reshape(GRAPH, N_LOC, CLASSES), send_rows), src_dev, dst_dev, w_dev).reshape(GRAPH * N_LOC, CLASSES)
    mask_f = label_mask.astype(jnp.float32)
    label_count = jnp.maximum(jnp.sum(mask_f), 1.0)
    log_norm = jax.nn.logsumexp(logits, axis=1)
    one_hot = (labels[:, None] == jnp.arange(CLASSES)[None, :]).astype(jnp.float32)
    picked = jnp.sum(logits * one_hot, axis=1)
    mean_loss = jnp.sum(mask_f * (log_norm - picked)) / label_count
    d_logits = (jnp.exp(logits - log_norm[:, None]) - one_hot) * (mask_f / label_count)[:, None]
    d_tab_two = scatter_back(d_logits.reshape(GRAPH, N_LOC, CLASSES), send_rows, src_dev, dst_dev, w_dev).reshape(GRAPH * N_LOC, CLASSES).astype(jnp.bfloat16)
    grad_two = jnp.dot(hidden.T, d_tab_two, preferred_element_type=jnp.float32)
    d_hidden = jnp.dot(d_tab_two, w_two_b.T, preferred_element_type=jnp.float32)
    d_pre = jnp.where(pre_one > 0.0, d_hidden, 0.0)
    d_tab_one = scatter_back(d_pre.reshape(GRAPH, N_LOC, F_HID), send_rows, src_dev, dst_dev, w_dev).reshape(GRAPH * N_LOC, F_HID).astype(jnp.bfloat16)
    grad_one = jnp.dot(node_feats.T, d_tab_one, preferred_element_type=jnp.float32)
    return mean_loss, grad_one, grad_two
```

```python
import functools

import jax
import jax.numpy as jnp
from jax import lax
from jax.experimental import pallas as pl
from jax.experimental.pallas import tpu as pltpu
from jax.sharding import PartitionSpec as P

AXIS = "graph"
LANES = 128
ROWS_A = (((0,), (0,)), ((), ()))
COLS_A = (((1,), (1,)), ((), ()))
F32, BF16 = jnp.float32, jnp.bfloat16
VMEM = pl.BlockSpec(memory_space=pltpu.VMEM)
SMEM = pl.BlockSpec(memory_space=pltpu.SMEM)
STEP = 512


def dot(a, b, dims=(((1,), (0,)), ((), ()))):
    return lax.dot_general(a, b, dims, preferred_element_type=F32)


def fill_zero(ref):
    zero = jnp.zeros((STEP, LANES), F32)

    @pl.loop(0, ref.shape[0], step=STEP)
    def _(i):
        ref[pl.ds(i, STEP), :] = zero


def copy_in(dst, src):
    @pl.loop(0, dst.shape[0], step=STEP)
    def _(i):
        dst[pl.ds(i, STEP), :] = src[pl.ds(i, STEP), :].astype(F32)


def walk_edges(first, last, chunk, from_idx, to_idx, w, table, accs):
    group = len(accs)

    def body(c, _):
        base = c * chunk
        for g in range(0, chunk, group):
            pend = []
            for u in range(group):
                k = base + g + u
                s = pl.multiple_of(from_idx[k], 2)
                d = pl.multiple_of(to_idx[k], 2)
                pend.append((d, accs[u][pl.ds(d, 2), :] + table[pl.ds(s, 2), :] * w[k]))
            for u in range(group):
                accs[u][pl.ds(pend[u][0], 2), :] = pend[u][1]
        return 0

    lax.fori_loop(first, last, body, 0)


def gather_rows(idx, which, table, buf, chunk=32):
    @pl.loop(0, idx.shape[1] // chunk)
    def _(c):
        for u in range(chunk):
            j = c * chunk + u
            s = pl.multiple_of(idx[which, j] * 2, 2)
            buf[pl.ds(pl.multiple_of(j * 2, 2), 2), :] = table[pl.ds(s, 2), :]


def return_rows(idx, which, vals, accs, chunk=32):
    group = len(accs)

    @pl.loop(0, idx.shape[1] // chunk)
    def _(c):
        for g in range(0, chunk, group):
            pend = []
            for u in range(group):
                j = c * chunk + g + u
                d = pl.multiple_of(idx[which, j] * 2, 2)
                pend.append((d, accs[u][pl.ds(d, 2), :] + vals[pl.ds(pl.multiple_of(j * 2, 2), 2), :]))
            for u in range(group):
                accs[u][pl.ds(pend[u][0], 2), :] = pend[u][1]


def send_halo(idx, table, buf, prev_out, next_out):
    gather_rows(idx, 0, table, buf)
    prev_out[...] = buf[...].astype(BF16)
    gather_rows(idx, 1, table, buf)
    next_out[...] = buf[...].astype(BF16)


def halves(accs, i, n):
    even = functools.reduce(jnp.add, [a[pl.ds(2 * i, n, stride=2), :] for a in accs])
    odd = functools.reduce(jnp.add, [a[pl.ds(2 * i + 1, n, stride=2), :] for a in accs])
    return even, odd


def put_halves(table, i, n, even, odd):
    table[pl.ds(2 * i, n, stride=2), :] = even
    table[pl.ds(2 * i + 1, n, stride=2), :] = odd


def first_kernel(x, w1, send, tab, to_prev, to_next, buf):
    rows = x.shape[0]
    w = w1[...].astype(BF16)

    @pl.loop(0, rows, step=256)
    def _(i):
        t = dot(x[pl.ds(i, 256), :], w).astype(BF16).astype(F32)
        put_halves(tab, i, 256, t[:, :LANES], t[:, LANES:])

    send_halo(send, tab, buf, to_prev, to_next)


def local_kernel(chunk, n_acc, counts, from_idx, to_idx, w, table, out, *accs):
    for a in accs:
        fill_zero(a)
    walk_edges(0, (counts[0] + chunk - 1) // chunk, chunk, from_idx, to_idx, w, table, accs)

    @pl.loop(0, out.shape[0], step=STEP)
    def _(i):
        out[pl.ds(i, STEP), :] = functools.reduce(jnp.add, [a[pl.ds(i, STEP), :] for a in accs])


def halo_range(counts, chunk):
    return counts[0] // chunk, (counts[0] + counts[1] + chunk - 1) // chunk


def forward_halo(chunk, counts, src, dst, w, from_prev, from_next, part, htab, accs):
    half = from_prev.shape[0]
    copy_in(htab.at[pl.ds(0, half)], from_prev)
    copy_in(htab.at[pl.ds(half, half)], from_next)
    copy_in(accs[0], part)
    for a in accs[1:]:
        fill_zero(a)
    first, last = halo_range(counts, chunk)
    walk_edges(first, last, chunk, src, dst, w, htab, accs)


def backward_halo(chunk, counts, src, dst, w, grad, back_prev, back_next, accs):
    for a in accs:
        fill_zero(a)
    first, last = halo_range(counts, chunk)
    walk_edges(first, last, chunk, dst, src, w, grad, accs)
    half = back_prev.shape[0]

    @pl.loop(0, half, step=STEP)
    def _(i):
        back_prev[pl.ds(i, STEP), :] = functools.reduce(jnp.add, [a[pl.ds(i, STEP), :] for a in accs])
        back_next[pl.ds(i, STEP), :] = functools.reduce(jnp.add, [a[pl.ds(half + i, STEP), :] for a in accs])


def hidden_kernel(chunk, counts, src, dst, w, send, from_prev, from_next, part, w2, hid, tab, to_prev, to_next, htab, buf, *accs):
    forward_halo(chunk, counts, src, dst, w, from_prev, from_next, part, htab, accs)

    @pl.loop(0, hid.shape[0], step=256)
    def _(i):
        even, odd = halves(accs, i, 256)
        h = jnp.concatenate([jnp.maximum(even, 0.0), jnp.maximum(odd, 0.0)], axis=1).astype(BF16)
        hid[pl.ds(i, 256), :] = h
        t = dot(h, w2[...]).astype(BF16).astype(F32)
        put_halves(tab, i, 256, t[:, :LANES], t[:, LANES:])

    send_halo(send, tab, buf, to_prev, to_next)


def spread(row):
    return jnp.transpose(jnp.broadcast_to(row, (LANES, LANES)))


def loss_kernel(chunk, classes, counts, src, dst, w, inv_count, from_prev, from_next, part, labels, mask, loss, grad, back_prev, back_next, htab, *accs):
    forward_halo(chunk, counts, src, dst, w, from_prev, from_next, part, htab, accs)
    lane = lax.broadcasted_iota(jnp.int32, (LANES, LANES), 1)
    live = lane < classes - LANES
    scale = inv_count[0, 0]
    loss[...] = jnp.zeros_like(loss)

    @pl.loop(0, labels.shape[0])
    def _(b):
        even, odd = halves(accs, b * LANES, LANES)
        label = spread(labels[pl.ds(b, 1), :])
        keep = spread(mask[pl.ds(b, 1), :])
        odd = jnp.where(live, odd, -jnp.inf)
        top = jnp.max(jnp.maximum(even, odd), axis=1, keepdims=True)
        total = jnp.sum(jnp.exp(even - top) + jnp.exp(odd - top), axis=1, keepdims=True)
        norm = top + jnp.log(total)
        hit_even, hit_odd = lane == label, lane + LANES == label
        picked = jnp.where(hit_even, even, 0.0) + jnp.where(hit_odd, odd, 0.0)
        per_row = jnp.where(lane == 0, norm, 0.0) - picked
        loss[...] += jnp.sum((keep * per_row).reshape(LANES // 8, 8, LANES), axis=0)
        d_even = (jnp.exp(even - norm) - hit_even.astype(F32)) * (keep * scale)
        d_odd = (jnp.exp(odd - norm) - hit_odd.astype(F32)) * (keep * scale)
        put_halves(grad, b * LANES, LANES, d_even, d_odd)

    backward_halo(chunk, counts, src, dst, w, grad, back_prev, back_next, accs)


def take_returns(send, part, got_prev, got_next, accs):
    copy_in(accs[0], part)
    for a in accs[1:]:
        fill_zero(a)
    return_rows(send, 1, got_prev, accs)
    return_rows(send, 0, got_next, accs)


def middle_kernel(chunk, counts, src, dst, w, send, got_prev, got_next, part, hid, w2, grad_two, grad, back_prev, back_next, *accs):
    take_returns(send, part, got_prev, got_next, accs)
    grad_two[...] = jnp.zeros_like(grad_two)

    @pl.loop(0, hid.shape[0], step=256)
    def _(i):
        even, odd = halves(accs, i, 256)
        d_tab = jnp.concatenate([even, odd], axis=1).astype(BF16)
        h = hid[pl.ds(i, 256), :]
        grad_two[...] += dot(h, d_tab, ROWS_A)
        d_hid = dot(d_tab, w2[...], COLS_A)
        d_pre = jnp.where(h > 0, d_hid, 0.0)
        put_halves(grad, i, 256, d_pre[:, :LANES], d_pre[:, LANES:])

    backward_halo(chunk, counts, src, dst, w, grad, back_prev, back_next, accs)


def last_kernel(send, got_prev, got_next, part, x, grad_one, *accs):
    take_returns(send, part, got_prev, got_next, accs)
    grad_one[...] = jnp.zeros_like(grad_one)

    @pl.loop(0, x.shape[0], step=256)
    def _(i):
        even, odd = halves(accs, i, 256)
        d_tab = jnp.concatenate([even, odd], axis=1).astype(BF16)
        grad_one[...] += dot(x[pl.ds(i, 256), :], d_tab, ROWS_A)


def call(body, name, outs, ins, scratch, flops=10**9):
    return pl.pallas_call(
        body, name=name, out_shape=outs, in_specs=ins, out_specs=jax.tree.map(lambda _: VMEM, outs),
        scratch_shapes=[pltpu.VMEM(s, F32) for s in scratch],
        compiler_params=pltpu.CompilerParams(vmem_limit_bytes=60 * 2**20),
        cost_estimate=pl.CostEstimate(flops=flops, bytes_accessed=8 * 2**20, transcendentals=0),
    )


def solution(mesh):
    num_dev = mesh.shape[AXIS]
    to_next = [(d, (d + 1) % num_dev) for d in range(num_dev)]
    to_prev = [(d, (d - 1) % num_dev) for d in range(num_dev)]

    def step(x, w_one, w_two, send, edge_src, edge_dst, edge_w, labels, mask):
        rows, halo, edges, classes = x.shape[0], send.shape[1], edge_src.shape[0], w_two.shape[1]
        tab = (2 * rows, LANES)
        half = (2 * halo, LANES)
        sds = jax.ShapeDtypeStruct
        tab_f, half_f, half_b = sds(tab, F32), sds(half, F32), sds(half, BF16)
        chunk_l, chunk_h = 64, 32
        w2 = jnp.pad(w_two, ((0, 0), (0, 2 * LANES - classes))).astype(BF16)
        mask_f = mask.astype(F32)

        tab_one, to_p, to_n = call(first_kernel, "first", [tab_f, half_b, half_b], [VMEM, VMEM, SMEM], [half])(x, w_one, send)
        from_prev = lax.ppermute(to_n, AXIS, to_next)
        from_next = lax.ppermute(to_p, AXIS, to_prev)

        kind = jnp.where(edge_w == 0.0, 2, (edge_src >= rows).astype(jnp.int32))
        key = (kind << 23) | (edge_src << 11) | edge_dst
        key, w = lax.sort((key, edge_w), num_keys=1, is_stable=False)
        kind, src, dst = key >> 23, (key >> 11) & 4095, (key & 2047) * 2
        is_local, is_halo = kind == 0, kind == 1
        src_l, w_l = jnp.where(is_local, src * 2, 0), jnp.where(is_local, w, 0.0)
        src_h, w_h = jnp.where(is_halo, (src - rows) * 2, 0), jnp.where(is_halo, w, 0.0)
        counts = jnp.stack([jnp.sum(is_local.astype(jnp.int32)), jnp.sum(is_halo.astype(jnp.int32))])
        label_count = jnp.maximum(lax.psum(jnp.sum(mask_f), AXIS), 1.0)

        walk_l = [SMEM, SMEM, SMEM, SMEM]
        local = call(functools.partial(local_kernel, chunk_l, 4), "local_edges", tab_f, walk_l + [VMEM], [tab] * 4, 10**10)
        part = local(counts, src_l, dst, w_l, tab_one)
        hid, tab_two, to_p, to_n = call(
            functools.partial(hidden_kernel, chunk_h), "hidden", [sds((rows, 2 * LANES), BF16), tab_f, half_b, half_b],
            walk_l + [SMEM] + [VMEM] * 4, [tab, half] + [tab] * 4,
        )(counts, src_h, dst, w_h, send, from_prev, from_next, part, w2)
        from_prev = lax.ppermute(to_n, AXIS, to_next)
        from_next = lax.ppermute(to_p, AXIS, to_prev)
        part = local(counts, src_l, dst, w_l, tab_two)
        loss, grad, to_p, to_n = call(
            functools.partial(loss_kernel, chunk_h, classes), "loss", [sds((8, LANES), F32), tab_f, half_f, half_f],
            walk_l + [SMEM] + [VMEM] * 5, [tab] + [tab] * 4,
        )(counts, src_h, dst, w_h, (1.0 / label_count).reshape(1, 1), from_prev, from_next, part, labels.reshape(-1, LANES), mask_f.reshape(-1, LANES))
        got_prev = lax.ppermute(to_p, AXIS, to_prev)
        got_next = lax.ppermute(to_n, AXIS, to_next)
        part = local(counts, dst, src_l, w_l, grad)
        grad_two, grad, to_p, to_n = call(
            functools.partial(middle_kernel, chunk_h), "middle", [sds((2 * LANES, 2 * LANES), F32), tab_f, half_f, half_f],
            walk_l + [SMEM] + [VMEM] * 5, [tab] * 4,
        )(counts, src_h, dst, w_h, send, got_prev, got_next, part, hid, w2)
        got_prev = lax.ppermute(to_p, AXIS, to_prev)
        got_next = lax.ppermute(to_n, AXIS, to_next)
        part = local(counts, dst, src_l, w_l, grad)
        grad_one = call(last_kernel, "last", sds((x.shape[1], 2 * LANES), F32), [SMEM] + [VMEM] * 4, [tab] * 4)(send, got_prev, got_next, part, x)
        loss, grad_one, grad_two = lax.psum((jnp.sum(loss), grad_one, grad_two[:, :classes]), AXIS)
        return loss / label_count, grad_one, grad_two

    row = P(AXIS)
    return jax.shard_map(
        step, mesh=mesh, in_specs=(row, P(), P(), row, row, row, row, row, row), out_specs=(P(), P(), P()), check_vma=False
    )
```

```python
import functools

import jax
import jax.numpy as jnp
from jax import lax
from jax.experimental import pallas as pl
from jax.experimental.pallas import tpu as pltpu
from jax.sharding import PartitionSpec as P

AXIS = "graph"
LANES = 128
ROWS_A = (((0,), (0,)), ((), ()))
COLS_A = (((1,), (1,)), ((), ()))
F32, BF16 = jnp.float32, jnp.bfloat16
VMEM = pl.BlockSpec(memory_space=pltpu.VMEM)
SMEM = pl.BlockSpec(memory_space=pltpu.SMEM)
STEP = 512
PREP_CHUNK = 64
MESH = pl.DeviceIdType.MESH


def dot(a, b, dims=(((1,), (0,)), ((), ()))):
    return lax.dot_general(a, b, dims, preferred_element_type=F32)


def fill_zero(ref):
    zero = jnp.zeros((STEP, LANES), F32)

    @pl.loop(0, ref.shape[0], step=STEP)
    def _(i):
        ref[pl.ds(i, STEP), :] = zero


def copy_in(dst, src):
    @pl.loop(0, dst.shape[0], step=STEP)
    def _(i):
        dst[pl.ds(i, STEP), :] = src[pl.ds(i, STEP), :].astype(F32)


def walk_edges(first, last, chunk, from_idx, to_idx, w, table, accs):
    group = len(accs)

    def body(c, _):
        base = c * chunk
        for g in range(0, chunk, group):
            pend = []
            for u in range(group):
                k = base + g + u
                s = pl.multiple_of(from_idx[k], 2)
                d = pl.multiple_of(to_idx[k], 2)
                pend.append((d, accs[u][pl.ds(d, 2), :] + table[pl.ds(s, 2), :] * w[k]))
            for u in range(group):
                accs[u][pl.ds(pend[u][0], 2), :] = pend[u][1]
        return 0

    lax.fori_loop(first, last, body, 0)


def gather_rows(idx, line, table, out):
    lane = lax.broadcasted_iota(jnp.int32, (LANES, LANES), 1) * 2
    groups = table.shape[0] // LANES

    @pl.loop(0, out.shape[0] // 256)
    def _(c):
        hot = []
        for q in range(2):
            want = spread(idx[pl.ds(line + c * 2 + q, 1), :])
            hot.append(jnp.concatenate([jnp.where(want == lane + 2 * LANES * j, 1.0, 0.0).astype(BF16) for j in range(groups)], axis=1))
        out[pl.ds(pl.multiple_of(c * 256, 256), 256), :] = dot(jnp.concatenate(hot, axis=0), table[...]).astype(BF16)


def spread(row):
    return jnp.transpose(jnp.broadcast_to(row, (LANES, LANES)))


def return_rows(idx, start, vals, accs, chunk=32):
    group = len(accs)

    @pl.loop(0, vals.shape[0] // (2 * chunk))
    def _(c):
        block = vals.at[pl.ds(pl.multiple_of(c * 2 * chunk, 2 * chunk), 2 * chunk)]
        for g in range(0, chunk, group):
            pend = []
            for u in range(group):
                d = pl.multiple_of(idx[start + c * chunk + g + u], 2)
                pend.append((d, accs[u][pl.ds(d, 2), :] + block[2 * (g + u) : 2 * (g + u) + 2, :]))
            for u in range(group):
                accs[u][pl.ds(pend[u][0], 2), :] = pend[u][1]


def send_halo(idx, table, prev_out, next_out):
    gather_rows(idx, 0, table, prev_out)
    gather_rows(idx, idx.shape[0] // 2, table, next_out)


def halves(accs, i, n):
    even = functools.reduce(jnp.add, [a[pl.ds(2 * i, n, stride=2), :] for a in accs])
    odd = functools.reduce(jnp.add, [a[pl.ds(2 * i + 1, n, stride=2), :] for a in accs])
    return even, odd


def put_halves(table, i, n, even, odd):
    table[pl.ds(2 * i, n, stride=2), :] = even
    table[pl.ds(2 * i + 1, n, stride=2), :] = odd


def greet(n):
    me = lax.axis_index(AXIS)
    barrier = pltpu.get_barrier_semaphore()
    for o in range(1, n):
        pl.semaphore_signal(barrier, inc=1, device_id=(lax.rem(me + o, n),), device_id_type=MESH)
    return me, lambda: pl.semaphore_wait(barrier, n - 1)


def remote(src, dst, send_sem, recv_sem, peer):
    return pltpu.make_async_remote_copy(
        src_ref=src, dst_ref=dst, send_sem=send_sem, recv_sem=recv_sem, device_id=(peer,), device_id_type=MESH
    )


def first_kernel(n, x, w1, send, mask, tab, to_prev, to_next, count, tab_b, mine, theirs, send_sem, recv_sem):
    me, met = greet(n)
    rows = x.shape[0]
    mask_f = mask[...].astype(F32)
    mine[...] = jnp.sum(mask_f.reshape(-1, 8, LANES), axis=0)
    w = w1[...].astype(BF16)

    @pl.loop(0, rows, step=256)
    def _(i):
        t = dot(x[pl.ds(i, 256), :], w).astype(BF16)
        tab_b[pl.ds(i, 256), :] = t
        t = t.astype(F32)
        put_halves(tab, i, 256, t[:, :LANES], t[:, LANES:])

    met()
    copies = [remote(mine, theirs.at[o - 1], send_sem.at[o - 1], recv_sem.at[o - 1], lax.rem(me + o, n)) for o in range(1, n)]
    for c in copies:
        c.start()
    send_halo(send, tab_b, to_prev, to_next)
    for c in copies:
        c.wait()
    total = mine[...] + jnp.sum(theirs[...], axis=0)
    count[...] = jnp.maximum(jnp.broadcast_to(jnp.sum(total, keepdims=True), count.shape), 1.0)


def reduce_kernel(n, part, *refs):
    if len(refs) == 9:
        extra, count, out, mean, got, full, mine, sems, theirs = refs
    else:
        out, got, full, mine, sems = refs
        extra = None
    me, met = greet(n)
    rows = part.shape[0] // n
    met()
    peers = [lax.rem(me + o, n) for o in range(1, n)]
    scatter = [
        remote(part.at[pl.ds(pl.multiple_of(p * rows, 8), rows)], got.at[o], sems.at[0, o], sems.at[1, o], p) for o, p in enumerate(peers)
    ]
    for c in scatter:
        c.start()
    if extra is not None:
        spread_out = [remote(extra, theirs.at[o], sems.at[4, o], sems.at[5, o], p) for o, p in enumerate(peers)]
        for c in spread_out:
            c.start()
    for c in scatter:
        c.wait_recv()
    own = pl.ds(pl.multiple_of(me * rows, 8), rows)
    mine[...] = part[own, :] + jnp.sum(got[...], axis=0)
    if extra is not None:
        for c in spread_out:
            c.wait()
        total = jnp.sum(extra[...] + jnp.sum(theirs[...], axis=0), keepdims=True)
        mean[...] = jnp.broadcast_to(total, mean.shape) / count[...]
    gather = [remote(mine, full.at[own], sems.at[2, o], sems.at[3, o], p) for o, p in enumerate(peers)]
    for c in gather:
        c.start()
    full[own, :] = mine[...]
    for c in scatter:
        c.wait_send()
    for c in gather:
        c.wait()
    out[...] = full[:, : out.shape[1]]


def prep_kernel(chunk, rows, src, dst, w, src_out, dst_out, w_out, counts, total):
    lines = src.shape[0]
    slots = src_out.shape[0]
    live = w[...] != 0.0
    halo = src[...] >= rows
    at = lambda shape, axis: lax.broadcasted_iota(jnp.int32, shape, axis)
    before = (at((LANES, LANES), 0) < at((LANES, LANES), 1)).astype(BF16)
    above = (at((lines, lines), 1) < at((lines, lines), 0)).astype(BF16)
    ones = jnp.ones((LANES, LANES), BF16)

    def rank(mask):
        m = mask.astype(F32).astype(BF16)
        return dot(m, before) + dot(above, dot(m, ones).astype(BF16))

    is_local, is_halo = jnp.logical_and(live, jnp.logical_not(halo)), jnp.logical_and(live, halo)
    n_local = jnp.sum(is_local.astype(F32)).astype(jnp.int32)
    n_halo = jnp.sum(is_halo.astype(F32)).astype(jnp.int32)
    local_chunks = (n_local + chunk - 1) // chunk
    counts[0] = local_chunks
    counts[1] = local_chunks + (n_halo + chunk - 1) // chunk
    pos = jnp.where(
        is_local, rank(is_local).astype(jnp.int32), jnp.where(is_halo, rank(is_halo).astype(jnp.int32) + local_chunks * chunk, -1)
    )
    line, lane = pos >> 7, pos & (LANES - 1)
    s = jnp.where(halo, src[...] - rows, src[...])
    d = dst[...]
    half_w = w[...] * 0.5
    w_a = half_w.astype(BF16).astype(F32)
    w_b = (half_w - w_a).astype(BF16).astype(F32)
    w_c = half_w - w_a - w_b
    high = ((s >> 8) * 8 + (d >> 8)).astype(F32)
    planes = [(s & 255).astype(F32), (d & 255).astype(F32), high, w_a, w_b, w_c]
    acc = jnp.zeros((len(planes) * slots, LANES), F32)
    for r in range(0, lines, 2):
        lhs, rhs = [], []
        for q in (r, r + 1):
            pick = at((slots, LANES), 0) == line[q : q + 1, :]
            lhs.append(jnp.concatenate([jnp.where(pick, p[q : q + 1, :], 0.0) for p in planes], axis=0))
            rhs.append((at((LANES, LANES), 0) == lane[q : q + 1, :]).astype(F32))
        acc += dot(jnp.concatenate(lhs, axis=1).astype(BF16), jnp.concatenate(rhs, axis=1).astype(BF16), COLS_A)
    total[...] = acc
    plane = lambda i: total[i * slots : (i + 1) * slots, :]
    high = plane(2).astype(jnp.int32)
    src_out[...] = ((high >> 3) * 256 + plane(0).astype(jnp.int32)) * 2
    dst_out[...] = ((high & 7) * 256 + plane(1).astype(jnp.int32)) * 2
    w_out[...] = (plane(3) + plane(4) + plane(5)) * 2.0


def local_kernel(chunk, n_acc, counts, from_idx, to_idx, w, table, out, *accs):
    for a in accs:
        fill_zero(a)
    walk_edges(0, counts[0] * (PREP_CHUNK // chunk), chunk, from_idx, to_idx, w, table, accs)

    @pl.loop(0, out.shape[0], step=STEP)
    def _(i):
        out[pl.ds(i, STEP), :] = functools.reduce(jnp.add, [a[pl.ds(i, STEP), :] for a in accs])


def halo_range(counts, chunk):
    return counts[0] * (PREP_CHUNK // chunk), counts[1] * (PREP_CHUNK // chunk)


def forward_halo(chunk, counts, src, dst, w, from_prev, from_next, part, htab, accs):
    half = from_prev.shape[0]

    @pl.loop(0, half, step=256)
    def _(i):
        for start, got in ((0, from_prev), (half, from_next)):
            t = got[pl.ds(i, 256), :].astype(F32)
            put_halves(htab, start + i, 256, t[:, :LANES], t[:, LANES:])

    copy_in(accs[0], part)
    for a in accs[1:]:
        fill_zero(a)
    first, last = halo_range(counts, chunk)
    walk_edges(first, last, chunk, src, dst, w, htab, accs)


def backward_halo(chunk, counts, src, dst, w, grad, back_prev, back_next, accs):
    for a in accs:
        fill_zero(a)
    first, last = halo_range(counts, chunk)
    walk_edges(first, last, chunk, dst, src, w, grad, accs)
    half = back_prev.shape[0]

    @pl.loop(0, half, step=STEP)
    def _(i):
        back_prev[pl.ds(i, STEP), :] = functools.reduce(jnp.add, [a[pl.ds(i, STEP), :] for a in accs])
        back_next[pl.ds(i, STEP), :] = functools.reduce(jnp.add, [a[pl.ds(half + i, STEP), :] for a in accs])


def hidden_kernel(chunk, counts, src, dst, w, send, from_prev, from_next, part, w2, hid, tab, to_prev, to_next, htab, tab_b, *accs):
    forward_halo(chunk, counts, src, dst, w, from_prev, from_next, part, htab, accs)

    @pl.loop(0, hid.shape[0], step=256)
    def _(i):
        even, odd = halves(accs, i, 256)
        h = jnp.concatenate([jnp.maximum(even, 0.0), jnp.maximum(odd, 0.0)], axis=1).astype(BF16)
        hid[pl.ds(i, 256), :] = h
        t = dot(h, w2[...]).astype(BF16)
        tab_b[pl.ds(i, 256), :] = t
        t = t.astype(F32)
        put_halves(tab, i, 256, t[:, :LANES], t[:, LANES:])

    send_halo(send, tab_b, to_prev, to_next)


def loss_kernel(chunk, classes, counts, src, dst, w, count, from_prev, from_next, part, labels, mask, loss, grad, back_prev, back_next, htab, *accs):
    forward_halo(chunk, counts, src, dst, w, from_prev, from_next, part, htab, accs)
    lane = lax.broadcasted_iota(jnp.int32, (LANES, LANES), 1)
    live = lane < classes - LANES
    scale = 1.0 / count[0:1, :]
    loss[...] = jnp.zeros_like(loss)

    @pl.loop(0, labels.shape[0])
    def _(b):
        even, odd = halves(accs, b * LANES, LANES)
        label = spread(labels[pl.ds(b, 1), :])
        keep = spread(mask[pl.ds(b, 1), :]).astype(F32)
        odd = jnp.where(live, odd, -jnp.inf)
        top = jnp.max(jnp.maximum(even, odd), axis=1, keepdims=True)
        total = jnp.sum(jnp.exp(even - top) + jnp.exp(odd - top), axis=1, keepdims=True)
        norm = top + jnp.log(total)
        hit_even, hit_odd = lane == label, lane + LANES == label
        picked = jnp.where(hit_even, even, 0.0) + jnp.where(hit_odd, odd, 0.0)
        per_row = jnp.where(lane == 0, norm, 0.0) - picked
        loss[...] += jnp.sum((keep * per_row).reshape(LANES // 8, 8, LANES), axis=0)
        d_even = (jnp.exp(even - norm) - hit_even.astype(F32)) * (keep * scale)
        d_odd = (jnp.exp(odd - norm) - hit_odd.astype(F32)) * (keep * scale)
        put_halves(grad, b * LANES, LANES, d_even, d_odd)

    backward_halo(chunk, counts, src, dst, w, grad, back_prev, back_next, accs)


def take_returns(send, part, got_prev, got_next, accs):
    copy_in(accs[0], part)
    for a in accs[1:]:
        fill_zero(a)
    return_rows(send, send.shape[0] // 2, got_prev, accs)
    return_rows(send, 0, got_next, accs)


def middle_kernel(chunk, counts, src, dst, w, send, got_prev, got_next, part, hid, w2, grad_two, grad, back_prev, back_next, *accs):
    take_returns(send, part, got_prev, got_next, accs)
    grad_two[...] = jnp.zeros_like(grad_two)

    @pl.loop(0, hid.shape[0], step=256)
    def _(i):
        even, odd = halves(accs, i, 256)
        d_tab = jnp.concatenate([even, odd], axis=1).astype(BF16)
        h = hid[pl.ds(i, 256), :]
        grad_two[...] += dot(h, d_tab, ROWS_A)
        d_hid = dot(d_tab, w2[...], COLS_A)
        d_pre = jnp.where(h > 0, d_hid, 0.0)
        put_halves(grad, i, 256, d_pre[:, :LANES], d_pre[:, LANES:])

    backward_halo(chunk, counts, src, dst, w, grad, back_prev, back_next, accs)


def last_kernel(send, got_prev, got_next, part, x, grad_one, *accs):
    take_returns(send, part, got_prev, got_next, accs)
    grad_one[...] = jnp.zeros_like(grad_one)

    @pl.loop(0, x.shape[0], step=256)
    def _(i):
        even, odd = halves(accs, i, 256)
        d_tab = jnp.concatenate([even, odd], axis=1).astype(BF16)
        grad_one[...] += dot(x[pl.ds(i, 256), :], d_tab, ROWS_A)


def call(body, name, outs, ins, scratch, flops=10**9, out_specs=None, collective=None):
    extra = {} if collective is None else dict(collective_id=collective, has_side_effects=True)
    return pl.pallas_call(
        body, name=name, out_shape=outs, in_specs=ins, out_specs=out_specs or jax.tree.map(lambda _: VMEM, outs),
        scratch_shapes=[pltpu.VMEM(s, F32) if isinstance(s, tuple) else s for s in scratch],
        compiler_params=pltpu.CompilerParams(vmem_limit_bytes=60 * 2**20, **extra),
        cost_estimate=pl.CostEstimate(flops=flops, bytes_accessed=8 * 2**20, transcendentals=0),
    )


def solution(mesh):
    num_dev = mesh.shape[AXIS]
    to_next = [(d, (d + 1) % num_dev) for d in range(num_dev)]
    to_prev = [(d, (d - 1) % num_dev) for d in range(num_dev)]

    def step(x, w_one, w_two, send, edge_src, edge_dst, edge_w, labels, mask):
        rows, halo, edges, classes = x.shape[0], send.shape[1], edge_src.shape[0], w_two.shape[1]
        tab = (2 * rows, LANES)
        half = (2 * halo, LANES)
        sds = jax.ShapeDtypeStruct
        tab_f, half_f, half_b = sds(tab, F32), sds(half, F32), sds((halo, 2 * LANES), BF16)
        tab_b = pltpu.VMEM((rows, 2 * LANES), BF16)
        one = sds((8, LANES), F32)
        dma = pltpu.SemaphoreType.DMA
        chunk_l, chunk_h = 64, 32
        lines = edges // LANES
        slots = lines + 8
        w2 = jnp.pad(w_two, ((0, 0), (0, 2 * LANES - classes))).astype(BF16)
        mask = mask.reshape(-1, LANES)
        send = send.reshape(-1) * 2

        tab_one, to_p, to_n, count = call(
            functools.partial(first_kernel, num_dev), "first", [tab_f, half_b, half_b, one], [VMEM] * 4,
            [tab_b, (8, LANES), (num_dev - 1, 8, LANES), dma((num_dev - 1,)), dma((num_dev - 1,))], collective=0,
        )(x, w_one, send.reshape(-1, LANES), mask)
        from_prev = lax.ppermute(to_n, AXIS, to_next)
        from_next = lax.ppermute(to_p, AXIS, to_prev)

        lined = lambda a: a.reshape(lines, LANES)
        ints = sds((slots, LANES), jnp.int32)
        src, dst, w, counts = call(
            functools.partial(prep_kernel, PREP_CHUNK, rows), "prep", [ints, ints, sds((slots, LANES), F32), sds((2,), jnp.int32)], [VMEM] * 3,
            [(6 * slots, LANES)], out_specs=[VMEM] * 3 + [SMEM],
        )(lined(edge_src), lined(edge_dst), lined(edge_w))
        src, dst, w = src.reshape(-1), dst.reshape(-1), w.reshape(-1)

        walk = [SMEM] * 4
        local = call(functools.partial(local_kernel, chunk_l, 4), "local_edges", tab_f, walk + [VMEM], [tab] * 4, 10**10)
        part = local(counts, src, dst, w, tab_one)
        hid, tab_two, to_p, to_n = call(
            functools.partial(hidden_kernel, chunk_h), "hidden", [sds((rows, 2 * LANES), BF16), tab_f, half_b, half_b],
            walk + [VMEM] * 5, [tab, tab_b] + [tab] * 4,
        )(counts, src, dst, w, send.reshape(-1, LANES), from_prev, from_next, part, w2)
        from_prev = lax.ppermute(to_n, AXIS, to_next)
        from_next = lax.ppermute(to_p, AXIS, to_prev)
        part = local(counts, src, dst, w, tab_two)
        loss, grad, to_p, to_n = call(
            functools.partial(loss_kernel, chunk_h, classes), "loss", [sds((8, LANES), F32), tab_f, half_f, half_f],
            walk + [VMEM] * 6, [tab] + [tab] * 4,
        )(counts, src, dst, w, count, from_prev, from_next, part, labels.reshape(-1, LANES), mask)
        got_prev = lax.ppermute(to_p, AXIS, to_prev)
        got_next = lax.ppermute(to_n, AXIS, to_next)
        part = local(counts, dst, src, w, grad)
        grad_two, grad, to_p, to_n = call(
            functools.partial(middle_kernel, chunk_h), "middle", [sds((2 * LANES, 2 * LANES), F32), tab_f, half_f, half_f],
            walk + [SMEM] + [VMEM] * 5, [tab] * 4,
        )(counts, src, dst, w, send, got_prev, got_next, part, hid, w2)
        got_prev = lax.ppermute(to_p, AXIS, to_prev)
        got_next = lax.ppermute(to_n, AXIS, to_next)
        part = local(counts, dst, src, w, grad)

        def reducer(shape, out, name, collective, extra):
            n = num_dev
            piece = (shape[0] // n, shape[1])
            outs = [sds(out, F32)] + ([one] if extra else [])
            return call(
                functools.partial(reduce_kernel, n), name, outs, [VMEM] * (3 if extra else 1),
                [(n - 1, *piece), shape, piece, dma((6, n - 1))] + ([(n - 1, 8, LANES)] if extra else []),
                collective=collective, flops=10**10,
            )

        grad_two, mean = reducer(grad_two.shape, (2 * LANES, classes), "reduce_two", 1, True)(grad_two, loss, count)
        grad_one = call(last_kernel, "last", sds((x.shape[1], 2 * LANES), F32), [SMEM] + [VMEM] * 4, [tab] * 4)(send, got_prev, got_next, part, x)
        (grad_one,) = reducer(grad_one.shape, grad_one.shape, "reduce_one", 2, False)(grad_one)
        return mean[0, 0], grad_one, grad_two

    row = P(AXIS)
    return jax.shard_map(
        step, mesh=mesh, in_specs=(row, P(), P(), row, row, row, row, row, row), out_specs=(P(), P(), P()), check_vma=False
    )
```

```python
import functools

import jax
import jax.numpy as jnp
from jax import lax
from jax.experimental import pallas as pl
from jax.experimental.pallas import tpu as pltpu
from jax.sharding import PartitionSpec as P

AXIS = "graph"
LANES = 128
ROWS_A = (((0,), (0,)), ((), ()))
COLS_A = (((1,), (1,)), ((), ()))
F32, BF16 = jnp.float32, jnp.bfloat16
VMEM = pl.BlockSpec(memory_space=pltpu.VMEM)
SMEM = pl.BlockSpec(memory_space=pltpu.SMEM)
STEP = 512
PREP_CHUNK = 64
MESH = pl.DeviceIdType.MESH


def dot(a, b, dims=(((1,), (0,)), ((), ()))):
    return lax.dot_general(a, b, dims, preferred_element_type=F32)


def fill_zero(ref):
    zero = jnp.zeros((STEP, LANES), F32)

    @pl.loop(0, ref.shape[0], step=STEP)
    def _(i):
        ref[pl.ds(i, STEP), :] = zero


def copy_in(dst, src):
    @pl.loop(0, dst.shape[0], step=STEP)
    def _(i):
        dst[pl.ds(i, STEP), :] = src[pl.ds(i, STEP), :].astype(F32)


def walk_edges(first, last, chunk, from_idx, to_idx, w, table, accs):
    group = len(accs)

    def body(c, _):
        base = c * chunk
        for g in range(0, chunk, group):
            pend = []
            for u in range(group):
                k = base + g + u
                s = pl.multiple_of(from_idx[k], 2)
                d = pl.multiple_of(to_idx[k], 2)
                pend.append((d, accs[u][pl.ds(d, 2), :] + table[pl.ds(s, 2), :] * w[k]))
            for u in range(group):
                accs[u][pl.ds(pend[u][0], 2), :] = pend[u][1]
        return 0

    lax.fori_loop(first, last, body, 0)


def one_hot_rows(idx, line, table):
    lane = lax.broadcasted_iota(jnp.int32, (LANES, LANES), 1) * 2
    hot = []
    for q in range(2):
        want = spread(idx[pl.ds(line + q, 1), :])
        hot.append(
            jnp.concatenate([jnp.where(want == lane + 2 * LANES * j, 1.0, 0.0).astype(BF16) for j in range(table.shape[0] // LANES)], axis=1)
        )
    return dot(jnp.concatenate(hot, axis=0), table[...])


def low_lanes(rows):
    return lax.broadcasted_iota(jnp.int32, (rows, LANES), 1) < LANES // 2


def swap_lanes(v):
    return pltpu.roll(v, LANES // 2, 1)


def gather_rows(idx, line, table, out):
    @pl.loop(0, out.shape[0], step=256)
    def _(i):
        out[pl.ds(pl.multiple_of(i, 256), 256), :] = one_hot_rows(idx, line + i // LANES, table).astype(BF16)


def gather_packed(idx, line, table, out):
    halo = out.shape[0] * 2 // 3

    @pl.loop(0, halo // 2, step=256)
    def _(i):
        i = pl.multiple_of(i, 256)
        a = one_hot_rows(idx, line + i // LANES, table)
        b = one_hot_rows(idx, line + (halo // 2 + i) // LANES, table)
        out[pl.ds(i, 256), :] = a[:, :LANES].astype(BF16)
        out[pl.ds(halo // 2 + i, 256), :] = b[:, :LANES].astype(BF16)
        out[pl.ds(halo + i, 256), :] = jnp.where(low_lanes(256), a[:, LANES:], swap_lanes(b[:, LANES:])).astype(BF16)


def unpack_rows(got, table, start):
    halo = got.shape[0] * 2 // 3

    @pl.loop(0, halo // 2, step=256)
    def _(i):
        i = pl.multiple_of(i, 256)
        a, b, both = (got[pl.ds(k + i, 256), :].astype(F32) for k in (0, halo // 2, halo))
        put_halves(table, start + i, 256, a, jnp.where(low_lanes(256), both, 0.0))
        put_halves(table, start + halo // 2 + i, 256, b, jnp.where(low_lanes(256), swap_lanes(both), 0.0))


def unpack_plain(got, table, start):
    @pl.loop(0, got.shape[0], step=256)
    def _(i):
        t = got[pl.ds(i, 256), :].astype(F32)
        put_halves(table, start + i, 256, t[:, :LANES], t[:, LANES:])


def spread(row):
    return jnp.transpose(jnp.broadcast_to(row, (LANES, LANES)))


def return_rows(idx, start, vals, accs, chunk=32):
    group = len(accs)

    @pl.loop(0, vals.shape[0] // (2 * chunk))
    def _(c):
        block = vals.at[pl.ds(pl.multiple_of(c * 2 * chunk, 2 * chunk), 2 * chunk)]
        for g in range(0, chunk, group):
            pend = []
            for u in range(group):
                d = pl.multiple_of(idx[start + c * chunk + g + u], 2)
                pend.append((d, accs[u][pl.ds(d, 2), :] + block[2 * (g + u) : 2 * (g + u) + 2, :]))
            for u in range(group):
                accs[u][pl.ds(pend[u][0], 2), :] = pend[u][1]


def halves(accs, i, n):
    even = functools.reduce(jnp.add, [a[pl.ds(2 * i, n, stride=2), :] for a in accs])
    odd = functools.reduce(jnp.add, [a[pl.ds(2 * i + 1, n, stride=2), :] for a in accs])
    return even, odd


def put_halves(table, i, n, even, odd):
    table[pl.ds(2 * i, n, stride=2), :] = even
    table[pl.ds(2 * i + 1, n, stride=2), :] = odd


def greet(n):
    me = lax.axis_index(AXIS)
    barrier = pltpu.get_barrier_semaphore()
    for o in range(1, n):
        pl.semaphore_signal(barrier, inc=1, device_id=(lax.rem(me + o, n),), device_id_type=MESH)
    return me, lambda: pl.semaphore_wait(barrier, n - 1)


def remote(src, dst, send_sem, recv_sem, peer):
    return pltpu.make_async_remote_copy(
        src_ref=src, dst_ref=dst, send_sem=send_sem, recv_sem=recv_sem, device_id=(peer,), device_id_type=MESH
    )


def first_kernel(n, x, w1, send, mask, tab, to_prev, to_next, count, tab_b, mine, theirs, send_sem, recv_sem):
    me, met = greet(n)
    rows = x.shape[0]
    mask_f = mask[...].astype(F32)
    mine[...] = jnp.sum(mask_f.reshape(-1, 8, LANES), axis=0)
    w = w1[...].astype(BF16)

    @pl.loop(0, rows, step=256)
    def _(i):
        t = dot(x[pl.ds(i, 256), :], w).astype(BF16)
        tab_b[pl.ds(i, 256), :] = t
        t = t.astype(F32)
        put_halves(tab, i, 256, t[:, :LANES], t[:, LANES:])

    met()
    copies = [remote(mine, theirs.at[o - 1], send_sem.at[o - 1], recv_sem.at[o - 1], lax.rem(me + o, n)) for o in range(1, n)]
    for c in copies:
        c.start()
    gather_rows(send, 0, tab_b, to_prev)
    gather_rows(send, send.shape[0] // 2, tab_b, to_next)
    for c in copies:
        c.wait()
    total = mine[...] + jnp.sum(theirs[...], axis=0)
    count[...] = jnp.maximum(jnp.broadcast_to(jnp.sum(total, keepdims=True), count.shape), 1.0)


def reduce_kernel(n, one, two, loss, count, one_out, two_out, mean, work, full, got_pair, got_rest, sems):
    me = lax.axis_index(AXIS)
    chips, core = n // 2, lax.rem(me, 2)
    chip = lax.div(me, 2)
    pair = me + 1 - 2 * core
    others = [lax.rem(chip + o, chips) for o in range(1, chips)]
    barrier = pltpu.get_barrier_semaphore()
    for p in [pair] + [2 * c + core for c in others]:
        pl.semaphore_signal(barrier, inc=1, device_id=(p,), device_id_type=MESH)
    classes = two_out.shape[0]
    lines = -(-classes // 8) * 8
    top, wide = one.shape
    work[0:top, :] = one[:, :LANES]
    work[top : 2 * top, :] = one[:, LANES:]
    work[2 * top : 2 * top + lines, :] = two[:lines, :LANES]
    work[2 * top + lines : 2 * top + 2 * lines, :] = two[:lines, LANES:]
    tail = 2 * top + 2 * lines
    work[tail : tail + 8, :] = loss[...]
    work[tail + 8 :, :] = jnp.zeros((work.shape[0] - tail - 8, LANES), F32)
    pl.semaphore_wait(barrier, chips)

    half = work.shape[0] // 2
    piece = half // chips
    rows = lambda start, size: pl.ds(pl.multiple_of(start, 8), size)
    mine, other = rows(core * half, half), rows((1 - core) * half, half)
    swap = remote(work.at[other], got_pair, sems.at[0, 0], sems.at[1, 0], pair)
    swap.start()
    swap.wait()
    work[mine, :] += got_pair[...]
    scatter = [
        remote(work.at[rows(core * half + c * piece, piece)], got_rest.at[o], sems.at[0, 1 + o], sems.at[1, 1 + o], 2 * c + core)
        for o, c in enumerate(others)
    ]
    for c in scatter:
        c.start()
    for c in scatter:
        c.wait()
    own = rows(core * half + chip * piece, piece)
    work[own, :] += jnp.sum(got_rest[...], axis=0)
    full[own, :] = work[own, :]
    gather = [
        remote(work.at[own], full.at[own], sems.at[0, chips + o], sems.at[1, chips + o], 2 * c + core) for o, c in enumerate(others)
    ]
    for c in gather:
        c.start()
    for c in gather:
        c.wait()
    last = remote(full.at[mine], full.at[mine], sems.at[0, 2 * chips - 1], sems.at[1, 2 * chips - 1], pair)
    last.start()
    last.wait()
    one_out[:, :LANES] = full[0:top, :]
    one_out[:, LANES:] = full[top : 2 * top, :]
    two_out[:, :LANES] = full[2 * top : 2 * top + classes, :]
    two_out[:, LANES:] = full[2 * top + lines : 2 * top + lines + classes, :]
    mean[...] = jnp.sum(full[tail : tail + 8, :], keepdims=True) / count[0:1, 0:1]


def prep_kernel(chunk, rows, src, dst, w, src_out, dst_out, w_out, counts, total):
    lines = src.shape[0]
    slots = src_out.shape[0]
    live = w[...] != 0.0
    halo = src[...] >= rows
    at = lambda shape, axis: lax.broadcasted_iota(jnp.int32, shape, axis)
    before = (at((LANES, LANES), 0) < at((LANES, LANES), 1)).astype(BF16)
    above = (at((lines, lines), 1) < at((lines, lines), 0)).astype(BF16)
    ones = jnp.ones((LANES, LANES), BF16)

    def rank(mask):
        m = mask.astype(F32).astype(BF16)
        return dot(m, before) + dot(above, dot(m, ones).astype(BF16))

    is_local, is_halo = jnp.logical_and(live, jnp.logical_not(halo)), jnp.logical_and(live, halo)
    n_local = jnp.sum(is_local.astype(F32)).astype(jnp.int32)
    n_halo = jnp.sum(is_halo.astype(F32)).astype(jnp.int32)
    local_chunks = (n_local + chunk - 1) // chunk
    counts[0] = local_chunks
    counts[1] = local_chunks + (n_halo + chunk - 1) // chunk
    pos = jnp.where(
        is_local, rank(is_local).astype(jnp.int32), jnp.where(is_halo, rank(is_halo).astype(jnp.int32) + local_chunks * chunk, -1)
    )
    line, lane = pos >> 7, pos & (LANES - 1)
    s = jnp.where(halo, src[...] - rows, src[...])
    d = dst[...]
    half_w = w[...] * 0.5
    w_a = half_w.astype(BF16).astype(F32)
    w_b = (half_w - w_a).astype(BF16).astype(F32)
    w_c = half_w - w_a - w_b
    high = ((s >> 8) * 8 + (d >> 8)).astype(F32)
    planes = [(s & 255).astype(F32), (d & 255).astype(F32), high, w_a, w_b, w_c]
    acc = jnp.zeros((len(planes) * slots, LANES), F32)
    for r in range(0, lines, 2):
        lhs, rhs = [], []
        for q in (r, r + 1):
            pick = at((slots, LANES), 0) == line[q : q + 1, :]
            lhs.append(jnp.concatenate([jnp.where(pick, p[q : q + 1, :], 0.0) for p in planes], axis=0))
            rhs.append((at((LANES, LANES), 0) == lane[q : q + 1, :]).astype(F32))
        acc += dot(jnp.concatenate(lhs, axis=1).astype(BF16), jnp.concatenate(rhs, axis=1).astype(BF16), COLS_A)
    total[...] = acc
    plane = lambda i: total[i * slots : (i + 1) * slots, :]
    high = plane(2).astype(jnp.int32)
    src_out[...] = ((high >> 3) * 256 + plane(0).astype(jnp.int32)) * 2
    dst_out[...] = ((high & 7) * 256 + plane(1).astype(jnp.int32)) * 2
    w_out[...] = (plane(3) + plane(4) + plane(5)) * 2.0


def local_kernel(chunk, n_acc, counts, from_idx, to_idx, w, table, out, *accs):
    for a in accs:
        fill_zero(a)
    walk_edges(0, counts[0] * (PREP_CHUNK // chunk), chunk, from_idx, to_idx, w, table, accs)

    @pl.loop(0, out.shape[0], step=STEP)
    def _(i):
        out[pl.ds(i, STEP), :] = functools.reduce(jnp.add, [a[pl.ds(i, STEP), :] for a in accs])


def halo_range(counts, chunk):
    return counts[0] * (PREP_CHUNK // chunk), counts[1] * (PREP_CHUNK // chunk)


def forward_halo(chunk, counts, src, dst, w, from_prev, from_next, part, htab, accs, unpack):
    unpack(from_prev, htab, 0)
    unpack(from_next, htab, htab.shape[0] // 4)
    copy_in(accs[0], part)
    for a in accs[1:]:
        fill_zero(a)
    first, last = halo_range(counts, chunk)
    walk_edges(first, last, chunk, src, dst, w, htab, accs)


def backward_halo(chunk, counts, src, dst, w, grad, back_prev, back_next, accs):
    for a in accs:
        fill_zero(a)
    first, last = halo_range(counts, chunk)
    walk_edges(first, last, chunk, dst, src, w, grad, accs)
    split = accs[0].shape[0] // 2
    if back_prev.shape[0] == split:

        @pl.loop(0, split, step=STEP)
        def _(i):
            back_prev[pl.ds(i, STEP), :] = functools.reduce(jnp.add, [a[pl.ds(i, STEP), :] for a in accs])
            back_next[pl.ds(i, STEP), :] = functools.reduce(jnp.add, [a[pl.ds(split + i, STEP), :] for a in accs])
        return
    halo = split // 2

    @pl.loop(0, halo // 2, step=256)
    def _(i):
        i = pl.multiple_of(i, 256)
        for start, out in ((0, back_prev), (halo, back_next)):
            a_even, a_odd = halves(accs, start + i, 256)
            b_even, b_odd = halves(accs, start + halo // 2 + i, 256)
            out[pl.ds(i, 256), :] = a_even
            out[pl.ds(halo // 2 + i, 256), :] = b_even
            out[pl.ds(halo + i, 256), :] = jnp.where(low_lanes(256), a_odd, swap_lanes(b_odd))


def hidden_kernel(chunk, counts, src, dst, w, send, from_prev, from_next, part, w2, hid, tab, to_prev, to_next, htab, tab_b, *accs):
    forward_halo(chunk, counts, src, dst, w, from_prev, from_next, part, htab, accs, unpack_plain)

    @pl.loop(0, hid.shape[0], step=256)
    def _(i):
        even, odd = halves(accs, i, 256)
        h = jnp.concatenate([jnp.maximum(even, 0.0), jnp.maximum(odd, 0.0)], axis=1).astype(BF16)
        hid[pl.ds(i, 256), :] = h
        t = dot(h, w2[...]).astype(BF16)
        tab_b[pl.ds(i, 256), :] = t
        t = t.astype(F32)
        put_halves(tab, i, 256, t[:, :LANES], t[:, LANES:])

    gather_packed(send, 0, tab_b, to_prev)
    gather_packed(send, send.shape[0] // 2, tab_b, to_next)


def loss_kernel(chunk, classes, counts, src, dst, w, count, from_prev, from_next, part, labels, mask, loss, grad, back_prev, back_next, htab, *accs):
    forward_halo(chunk, counts, src, dst, w, from_prev, from_next, part, htab, accs, unpack_rows)
    lane = lax.broadcasted_iota(jnp.int32, (LANES, LANES), 1)
    live = lane < classes - LANES
    scale = 1.0 / count[0:1, :]
    loss[...] = jnp.zeros_like(loss)

    @pl.loop(0, labels.shape[0])
    def _(b):
        even, odd = halves(accs, b * LANES, LANES)
        label = spread(labels[pl.ds(b, 1), :])
        keep = spread(mask[pl.ds(b, 1), :]).astype(F32)
        odd = jnp.where(live, odd, -jnp.inf)
        top = jnp.max(jnp.maximum(even, odd), axis=1, keepdims=True)
        total = jnp.sum(jnp.exp(even - top) + jnp.exp(odd - top), axis=1, keepdims=True)
        norm = top + jnp.log(total)
        hit_even, hit_odd = lane == label, lane + LANES == label
        picked = jnp.where(hit_even, even, 0.0) + jnp.where(hit_odd, odd, 0.0)
        per_row = jnp.where(lane == 0, norm, 0.0) - picked
        loss[...] += jnp.sum((keep * per_row).reshape(LANES // 8, 8, LANES), axis=0)
        d_even = (jnp.exp(even - norm) - hit_even.astype(F32)) * (keep * scale)
        d_odd = (jnp.exp(odd - norm) - hit_odd.astype(F32)) * (keep * scale)
        put_halves(grad, b * LANES, LANES, d_even, d_odd)

    backward_halo(chunk, counts, src, dst, w, grad, back_prev, back_next, accs)


def take_returns(send, part, got_prev, got_next, accs):
    copy_in(accs[0], part)
    for a in accs[1:]:
        fill_zero(a)
    return_rows(send, send.shape[0] // 2, got_prev, accs)
    return_rows(send, 0, got_next, accs)


def middle_kernel(chunk, counts, src, dst, w, send, got_prev, got_next, part, hid, w2, grad_two, grad, back_prev, back_next, returned, *accs):
    split = returned.shape[0] // 2
    unpack_rows(got_prev, returned, 0)
    unpack_rows(got_next, returned, split // 2)
    take_returns(send, part, returned.at[pl.ds(0, split)], returned.at[pl.ds(split, split)], accs)
    grad_two[...] = jnp.zeros_like(grad_two)

    @pl.loop(0, hid.shape[0], step=256)
    def _(i):
        even, odd = halves(accs, i, 256)
        d_tab = jnp.concatenate([even, odd], axis=1).astype(BF16)
        h = hid[pl.ds(i, 256), :]
        grad_two[...] += dot(d_tab, h, ROWS_A)
        d_hid = dot(d_tab, w2[...], COLS_A)
        d_pre = jnp.where(h > 0, d_hid, 0.0)
        put_halves(grad, i, 256, d_pre[:, :LANES], d_pre[:, LANES:])

    backward_halo(chunk, counts, src, dst, w, grad, back_prev, back_next, accs)


def last_kernel(send, got_prev, got_next, part, x, grad_one, *accs):
    take_returns(send, part, got_prev, got_next, accs)
    grad_one[...] = jnp.zeros_like(grad_one)

    @pl.loop(0, x.shape[0], step=256)
    def _(i):
        even, odd = halves(accs, i, 256)
        d_tab = jnp.concatenate([even, odd], axis=1).astype(BF16)
        grad_one[...] += dot(x[pl.ds(i, 256), :], d_tab, ROWS_A)


def call(body, name, outs, ins, scratch, flops=10**9, out_specs=None, collective=None, vmem=32):
    extra = {} if collective is None else dict(collective_id=collective, has_side_effects=True)
    return pl.pallas_call(
        body, name=name, out_shape=outs, in_specs=ins, out_specs=out_specs or jax.tree.map(lambda _: VMEM, outs),
        scratch_shapes=[pltpu.VMEM(s, F32) if isinstance(s, tuple) else s for s in scratch],
        compiler_params=pltpu.CompilerParams(vmem_limit_bytes=vmem * 2**20, **extra),
        cost_estimate=pl.CostEstimate(flops=flops, bytes_accessed=8 * 2**20, transcendentals=0),
    )


def solution(mesh):
    num_dev = mesh.shape[AXIS]
    to_next = [(d, (d + 1) % num_dev) for d in range(num_dev)]
    to_prev = [(d, (d - 1) % num_dev) for d in range(num_dev)]

    def step(x, w_one, w_two, send, edge_src, edge_dst, edge_w, labels, mask):
        rows, halo, edges, classes = x.shape[0], send.shape[1], edge_src.shape[0], w_two.shape[1]
        tab = (2 * rows, LANES)
        half = (2 * halo, LANES)
        sds = jax.ShapeDtypeStruct
        tab_f, half_f, half_b = sds(tab, F32), sds(half, F32), sds((halo, 2 * LANES), BF16)
        pack_f, pack_b = sds((3 * halo // 2, LANES), F32), sds((3 * halo // 2, LANES), BF16)
        tab_b = pltpu.VMEM((rows, 2 * LANES), BF16)
        one = sds((8, LANES), F32)
        dma = pltpu.SemaphoreType.DMA
        chunk_l, chunk_h = 64, 32
        lines = edges // LANES
        slots = lines + 8
        w2 = jnp.pad(w_two, ((0, 0), (0, 2 * LANES - classes))).astype(BF16)
        mask = mask.reshape(-1, LANES)
        send = send.reshape(-1) * 2

        tab_one, to_p, to_n, count = call(
            functools.partial(first_kernel, num_dev), "first", [tab_f, half_b, half_b, one], [VMEM] * 4,
            [tab_b, (8, LANES), (num_dev - 1, 8, LANES), dma((num_dev - 1,)), dma((num_dev - 1,))], collective=0,
        )(x, w_one, send.reshape(-1, LANES), mask)
        from_prev = lax.ppermute(to_n, AXIS, to_next)
        from_next = lax.ppermute(to_p, AXIS, to_prev)

        lined = lambda a: a.reshape(lines, LANES)
        ints = sds((slots, LANES), jnp.int32)
        src, dst, w, counts = call(
            functools.partial(prep_kernel, PREP_CHUNK, rows), "prep", [ints, ints, sds((slots, LANES), F32), sds((2,), jnp.int32)], [VMEM] * 3,
            [(6 * slots, LANES)], out_specs=[VMEM] * 3 + [SMEM],
        )(lined(edge_src), lined(edge_dst), lined(edge_w))
        src, dst, w = src.reshape(-1), dst.reshape(-1), w.reshape(-1)

        walk = [SMEM] * 4
        local = call(functools.partial(local_kernel, chunk_l, 4), "local_edges", tab_f, walk + [VMEM], [tab] * 4, 10**10)
        part = local(counts, src, dst, w, tab_one)
        hid, tab_two, to_p, to_n = call(
            functools.partial(hidden_kernel, chunk_h), "hidden", [sds((rows, 2 * LANES), BF16), tab_f, pack_b, pack_b],
            walk + [VMEM] * 5, [tab, tab_b] + [tab] * 4,
        )(counts, src, dst, w, send.reshape(-1, LANES), from_prev, from_next, part, w2)
        from_prev = lax.ppermute(to_n, AXIS, to_next)
        from_next = lax.ppermute(to_p, AXIS, to_prev)
        part = local(counts, src, dst, w, tab_two)
        loss, grad, to_p, to_n = call(
            functools.partial(loss_kernel, chunk_h, classes), "loss", [sds((8, LANES), F32), tab_f, pack_f, pack_f],
            walk + [VMEM] * 6, [tab] + [tab] * 4,
        )(counts, src, dst, w, count, from_prev, from_next, part, labels.reshape(-1, LANES), mask)
        got_prev = lax.ppermute(to_p, AXIS, to_prev)
        got_next = lax.ppermute(to_n, AXIS, to_next)
        part = local(counts, dst, src, w, grad)
        grad_two, grad, to_p, to_n = call(
            functools.partial(middle_kernel, chunk_h), "middle", [sds((2 * LANES, 2 * LANES), F32), tab_f, half_f, half_f],
            walk + [SMEM] + [VMEM] * 5, [tab] * 5,
        )(counts, src, dst, w, send, got_prev, got_next, part, hid, w2)
        got_prev = lax.ppermute(to_p, AXIS, to_prev)
        got_next = lax.ppermute(to_n, AXIS, to_next)
        part = local(counts, dst, src, w, grad)

        grad_one = call(last_kernel, "last", sds((x.shape[1], 2 * LANES), F32), [SMEM] + [VMEM] * 4, [tab] * 4)(send, got_prev, got_next, part, x)
        lines = 2 * x.shape[1] + 2 * (-(-classes // 8) * 8) + 8
        lines = -(-lines // (8 * num_dev)) * 8 * num_dev
        grad_one, grad_two, mean = call(
            functools.partial(reduce_kernel, num_dev), "reduce", [sds(grad_one.shape, F32), sds((classes, 2 * LANES), F32), sds((1, 1), F32)],
            [VMEM] * 4, [(lines, LANES), (lines, LANES), (lines // 2, LANES), (num_dev // 2 - 1, lines // num_dev, LANES), dma((2, num_dev))],
            collective=1, vmem=8,
        )(grad_one, grad_two, loss, count)
        return mean.reshape(()), grad_one, grad_two.T

    row = P(AXIS)
    return jax.shard_map(
        step, mesh=mesh, in_specs=(row, P(), P(), row, row, row, row, row, row), out_specs=(P(), P(), P()), check_vma=False
    )
```

```python
import functools

import jax
import jax.numpy as jnp
from jax import lax
from jax.experimental import pallas as pl
from jax.experimental.pallas import tpu as pltpu
from jax.sharding import PartitionSpec as P

AXIS = "graph"
LANES = 128
ROWS_A = (((0,), (0,)), ((), ()))
COLS_A = (((1,), (1,)), ((), ()))
F32, BF16 = jnp.float32, jnp.bfloat16
VMEM = pl.BlockSpec(memory_space=pltpu.VMEM)
SMEM = pl.BlockSpec(memory_space=pltpu.SMEM)
STEP = 512
PREP_CHUNK = 64
MESH = pl.DeviceIdType.MESH


def dot(a, b, dims=(((1,), (0,)), ((), ()))):
    return lax.dot_general(a, b, dims, preferred_element_type=F32)


def fill_zero(ref):
    zero = jnp.zeros((STEP, LANES), F32)

    @pl.loop(0, ref.shape[0], step=STEP)
    def _(i):
        ref[pl.ds(i, STEP), :] = zero


def copy_in(dst, src):
    @pl.loop(0, dst.shape[0], step=STEP)
    def _(i):
        dst[pl.ds(i, STEP), :] = src[pl.ds(i, STEP), :].astype(F32)


def walk_edges(first, last, chunk, from_idx, to_idx, w, table, accs):
    group = len(accs)

    def body(c, _):
        base = c * chunk
        w_chunk = w.at[pl.ds(pl.multiple_of(base, chunk), chunk)]
        for g in range(0, chunk, group):
            pend = []
            for u in range(group):
                k = base + g + u
                s = pl.multiple_of(from_idx[k], 2)
                d = pl.multiple_of(to_idx[k], 2)
                pend.append((d, accs[u][pl.ds(d, 2), :] + table[pl.ds(s, 2), :] * w_chunk[g + u : g + u + 1, :]))
            for u in range(group):
                accs[u][pl.ds(pend[u][0], 2), :] = pend[u][1]
        return 0

    lax.fori_loop(first, last, body, 0)


def one_hot_rows(idx, which, start, table):
    lane = lax.broadcasted_iota(jnp.int32, (LANES, LANES), 1)
    hot = []
    for q in range(2):
        want = spread(idx[which : which + 1, pl.ds(pl.multiple_of(start + q * LANES, LANES), LANES)])
        hot.append(
            jnp.concatenate([jnp.where(want == lane + LANES * j, 1.0, 0.0).astype(BF16) for j in range(table.shape[0] // LANES)], axis=1)
        )
    return dot(jnp.concatenate(hot, axis=0), table[...])


def low_lanes(rows):
    return lax.broadcasted_iota(jnp.int32, (rows, LANES), 1) < LANES // 2


def swap_lanes(v):
    return pltpu.roll(v, LANES // 2, 1)


def gather_rows(idx, which, table, out):
    @pl.loop(0, out.shape[0], step=256)
    def _(i):
        out[pl.ds(pl.multiple_of(i, 256), 256), :] = one_hot_rows(idx, which, i, table).astype(BF16)


def gather_packed(idx, which, table, out):
    halo = out.shape[0] * 2 // 3

    @pl.loop(0, halo // 2, step=256)
    def _(i):
        i = pl.multiple_of(i, 256)
        a = one_hot_rows(idx, which, i, table)
        b = one_hot_rows(idx, which, halo // 2 + i, table)
        out[pl.ds(i, 256), :] = a[:, :LANES].astype(BF16)
        out[pl.ds(halo // 2 + i, 256), :] = b[:, :LANES].astype(BF16)
        out[pl.ds(halo + i, 256), :] = jnp.where(low_lanes(256), a[:, LANES:], swap_lanes(b[:, LANES:])).astype(BF16)


def unpack_rows(got, table, start):
    halo = got.shape[0] * 2 // 3

    @pl.loop(0, halo // 2, step=256)
    def _(i):
        i = pl.multiple_of(i, 256)
        a, b, both = (got[pl.ds(k + i, 256), :].astype(F32) for k in (0, halo // 2, halo))
        put_halves(table, start + i, 256, a, jnp.where(low_lanes(256), both, 0.0))
        put_halves(table, start + halo // 2 + i, 256, b, jnp.where(low_lanes(256), swap_lanes(both), 0.0))


def unpack_plain(got, table, start):
    @pl.loop(0, got.shape[0], step=256)
    def _(i):
        t = got[pl.ds(i, 256), :].astype(F32)
        put_halves(table, start + i, 256, t[:, :LANES], t[:, LANES:])


def spread(row):
    return jnp.transpose(jnp.broadcast_to(row, (LANES, LANES)))


def return_rows(idx, start, vals, accs, chunk=32):
    group = len(accs)

    @pl.loop(0, vals.shape[0] // (2 * chunk))
    def _(c):
        block = vals.at[pl.ds(pl.multiple_of(c * 2 * chunk, 2 * chunk), 2 * chunk)]
        for g in range(0, chunk, group):
            pend = []
            for u in range(group):
                d = pl.multiple_of(idx[start + c * chunk + g + u], 2)
                pend.append((d, accs[u][pl.ds(d, 2), :] + block[2 * (g + u) : 2 * (g + u) + 2, :]))
            for u in range(group):
                accs[u][pl.ds(pend[u][0], 2), :] = pend[u][1]


def halves(accs, i, n):
    even = functools.reduce(jnp.add, [a[pl.ds(2 * i, n, stride=2), :] for a in accs])
    odd = functools.reduce(jnp.add, [a[pl.ds(2 * i + 1, n, stride=2), :] for a in accs])
    return even, odd


def put_halves(table, i, n, even, odd):
    table[pl.ds(2 * i, n, stride=2), :] = even
    table[pl.ds(2 * i + 1, n, stride=2), :] = odd


def greet(n):
    me = lax.axis_index(AXIS)
    barrier = pltpu.get_barrier_semaphore()
    for o in range(1, n):
        pl.semaphore_signal(barrier, inc=1, device_id=(lax.rem(me + o, n),), device_id_type=MESH)
    return me, lambda: pl.semaphore_wait(barrier, n - 1)


def remote(src, dst, send_sem, recv_sem, peer):
    return pltpu.make_async_remote_copy(
        src_ref=src, dst_ref=dst, send_sem=send_sem, recv_sem=recv_sem, device_id=(peer,), device_id_type=MESH
    )


def first_kernel(n, x, w1, send, mask, after, tab, to_prev, to_next, count, tab_b, mine, theirs, send_sem, recv_sem):
    me, met = greet(n)
    rows = x.shape[0]
    mask_f = mask[...].astype(F32)
    mine[...] = jnp.sum(mask_f.reshape(-1, 8, LANES), axis=0)
    w = w1[...].astype(BF16)

    @pl.loop(0, rows, step=256)
    def _(i):
        t = dot(x[pl.ds(i, 256), :], w).astype(BF16)
        tab_b[pl.ds(i, 256), :] = t
        t = t.astype(F32)
        put_halves(tab, i, 256, t[:, :LANES], t[:, LANES:])

    met()
    copies = [remote(mine, theirs.at[o - 1], send_sem.at[o - 1], recv_sem.at[o - 1], lax.rem(me + o, n)) for o in range(1, n)]
    for c in copies:
        c.start()
    gather_rows(send, 0, tab_b, to_prev)
    gather_rows(send, 1, tab_b, to_next)
    for c in copies:
        c.wait()
    total = mine[...] + jnp.sum(theirs[...], axis=0)
    count[...] = jnp.maximum(jnp.broadcast_to(jnp.sum(total, keepdims=True), count.shape), 1.0)


def reduce_kernel(n, one, two, loss, count, one_out, two_out, mean, work, full, got_pair, got_rest, sems):
    me = lax.axis_index(AXIS)
    chips, core = n // 2, lax.rem(me, 2)
    chip = lax.div(me, 2)
    pair = me + 1 - 2 * core
    others = [lax.rem(chip + o, chips) for o in range(1, chips)]
    barrier = pltpu.get_barrier_semaphore()
    for p in [pair] + [2 * c + core for c in others]:
        pl.semaphore_signal(barrier, inc=1, device_id=(p,), device_id_type=MESH)
    classes = two_out.shape[0]
    lines = -(-classes // 8) * 8
    top, wide = one.shape
    work[0:top, :] = one[:, :LANES]
    work[top : 2 * top, :] = one[:, LANES:]
    work[2 * top : 2 * top + lines, :] = two[:lines, :LANES]
    work[2 * top + lines : 2 * top + 2 * lines, :] = two[:lines, LANES:]
    tail = 2 * top + 2 * lines
    work[tail : tail + 8, :] = loss[...]
    work[tail + 8 :, :] = jnp.zeros((work.shape[0] - tail - 8, LANES), F32)
    pl.semaphore_wait(barrier, chips)

    half = work.shape[0] // 2
    piece = half // chips
    rows = lambda start, size: pl.ds(pl.multiple_of(start, 8), size)
    mine, other = rows(core * half, half), rows((1 - core) * half, half)
    swap = remote(work.at[other], got_pair, sems.at[0, 0], sems.at[1, 0], pair)
    swap.start()
    swap.wait()
    work[mine, :] += got_pair[...]
    scatter = [
        remote(work.at[rows(core * half + c * piece, piece)], got_rest.at[o], sems.at[0, 1 + o], sems.at[1, 1 + o], 2 * c + core)
        for o, c in enumerate(others)
    ]
    for c in scatter:
        c.start()
    for c in scatter:
        c.wait()
    own = rows(core * half + chip * piece, piece)
    work[own, :] += jnp.sum(got_rest[...], axis=0)
    full[own, :] = work[own, :]
    gather = [
        remote(work.at[own], full.at[own], sems.at[0, chips + o], sems.at[1, chips + o], 2 * c + core) for o, c in enumerate(others)
    ]
    for c in gather:
        c.start()
    for c in gather:
        c.wait()
    last = remote(full.at[mine], full.at[mine], sems.at[0, 2 * chips - 1], sems.at[1, 2 * chips - 1], pair)
    last.start()
    last.wait()
    one_out[:, :LANES] = full[0:top, :]
    one_out[:, LANES:] = full[top : 2 * top, :]
    two_out[:, :LANES] = full[2 * top : 2 * top + classes, :]
    two_out[:, LANES:] = full[2 * top + lines : 2 * top + lines + classes, :]
    mean[...] = jnp.sum(full[tail : tail + 8, :], keepdims=True) / count[0:1, 0:1]


def prep_kernel(chunk, rows, src, dst, w, send, src_out, dst_out, w_out, back, counts, total):
    lines = src.shape[0]
    slots = src_out.shape[0]
    per = send.shape[1] // LANES
    for i in range(2 * per):
        back[i : i + 1, :] = send[i // per : i // per + 1, (i % per) * LANES : (i % per + 1) * LANES] * 2
    live = w[...] != 0.0
    halo = src[...] >= rows
    at = lambda shape, axis: lax.broadcasted_iota(jnp.int32, shape, axis)
    before = (at((LANES, LANES), 0) < at((LANES, LANES), 1)).astype(BF16)
    above = (at((lines, lines), 1) < at((lines, lines), 0)).astype(BF16)
    ones = jnp.ones((LANES, LANES), BF16)

    def rank(mask):
        m = mask.astype(F32).astype(BF16)
        return dot(m, before) + dot(above, dot(m, ones).astype(BF16))

    is_local, is_halo = jnp.logical_and(live, jnp.logical_not(halo)), jnp.logical_and(live, halo)
    n_local = jnp.sum(is_local.astype(F32)).astype(jnp.int32)
    n_halo = jnp.sum(is_halo.astype(F32)).astype(jnp.int32)
    local_chunks = (n_local + chunk - 1) // chunk
    counts[0] = local_chunks
    counts[1] = local_chunks + (n_halo + chunk - 1) // chunk
    pos = jnp.where(
        is_local, rank(is_local).astype(jnp.int32), jnp.where(is_halo, rank(is_halo).astype(jnp.int32) + local_chunks * chunk, -1)
    )
    line, lane = pos >> 7, pos & (LANES - 1)
    s = jnp.where(halo, src[...] - rows, src[...])
    d = dst[...]
    half_w = w[...] * 0.5
    w_a = half_w.astype(BF16).astype(F32)
    w_b = (half_w - w_a).astype(BF16).astype(F32)
    w_c = half_w - w_a - w_b
    high = ((s >> 8) * 8 + (d >> 8)).astype(F32)
    planes = [(s & 255).astype(F32), (d & 255).astype(F32), high, w_a, w_b, w_c]
    acc = jnp.zeros((len(planes) * slots, LANES), F32)
    for r in range(0, lines, 2):
        lhs, rhs = [], []
        for q in (r, r + 1):
            pick = at((slots, LANES), 0) == line[q : q + 1, :]
            lhs.append(jnp.concatenate([jnp.where(pick, p[q : q + 1, :], 0.0) for p in planes], axis=0))
            rhs.append((at((LANES, LANES), 0) == lane[q : q + 1, :]).astype(F32))
        acc += dot(jnp.concatenate(lhs, axis=1).astype(BF16), jnp.concatenate(rhs, axis=1).astype(BF16), COLS_A)
    total[...] = acc
    plane = lambda i: total[i * slots : (i + 1) * slots, :]
    high = plane(2).astype(jnp.int32)
    src_out[...] = ((high >> 3) * 256 + plane(0).astype(jnp.int32)) * 2
    dst_out[...] = ((high & 7) * 256 + plane(1).astype(jnp.int32)) * 2
    total[0:slots, :] = (plane(3) + plane(4) + plane(5)) * 2.0

    @pl.loop(0, slots)
    def _(r):
        w_out[pl.ds(pl.multiple_of(r * LANES, LANES), LANES), :] = spread(total[pl.ds(r, 1), :])


def local_kernel(chunk, n_acc, counts, from_idx, to_idx, w, table, out, *accs):
    for a in accs:
        fill_zero(a)
    walk_edges(0, counts[0] * (PREP_CHUNK // chunk), chunk, from_idx, to_idx, w, table, accs)

    @pl.loop(0, out.shape[0], step=STEP)
    def _(i):
        out[pl.ds(i, STEP), :] = functools.reduce(jnp.add, [a[pl.ds(i, STEP), :] for a in accs])


def halo_range(counts, chunk):
    return counts[0] * (PREP_CHUNK // chunk), counts[1] * (PREP_CHUNK // chunk)


def forward_halo(chunk, counts, src, dst, w, from_prev, from_next, part, htab, accs, unpack):
    unpack(from_prev, htab, 0)
    unpack(from_next, htab, htab.shape[0] // 4)
    copy_in(accs[0], part)
    for a in accs[1:]:
        fill_zero(a)
    first, last = halo_range(counts, chunk)
    walk_edges(first, last, chunk, src, dst, w, htab, accs)


def backward_halo(chunk, counts, src, dst, w, grad, back_prev, back_next, accs):
    for a in accs:
        fill_zero(a)
    first, last = halo_range(counts, chunk)
    walk_edges(first, last, chunk, dst, src, w, grad, accs)
    split = accs[0].shape[0] // 2
    if back_prev.shape[0] == split:

        @pl.loop(0, split, step=STEP)
        def _(i):
            back_prev[pl.ds(i, STEP), :] = functools.reduce(jnp.add, [a[pl.ds(i, STEP), :] for a in accs])
            back_next[pl.ds(i, STEP), :] = functools.reduce(jnp.add, [a[pl.ds(split + i, STEP), :] for a in accs])
        return
    halo = split // 2

    @pl.loop(0, halo // 2, step=256)
    def _(i):
        i = pl.multiple_of(i, 256)
        for start, out in ((0, back_prev), (halo, back_next)):
            a_even, a_odd = halves(accs, start + i, 256)
            b_even, b_odd = halves(accs, start + halo // 2 + i, 256)
            out[pl.ds(i, 256), :] = a_even
            out[pl.ds(halo // 2 + i, 256), :] = b_even
            out[pl.ds(halo + i, 256), :] = jnp.where(low_lanes(256), a_odd, swap_lanes(b_odd))


def padded(w, buf):
    low = w.shape[0] // 8 * 8
    buf[low:, :] = jnp.zeros((buf.shape[0] - low, buf.shape[1]), F32)
    buf[0 : w.shape[0], :] = w[...]
    return buf[...].astype(BF16)


def hidden_kernel(chunk, counts, src, dst, w, send, from_prev, from_next, part, w2, hid, tab, to_prev, to_next, htab, tab_b, w2_pad, *accs):
    w2_b = padded(w2, w2_pad)
    forward_halo(chunk, counts, src, dst, w, from_prev, from_next, part, htab, accs, unpack_plain)

    @pl.loop(0, hid.shape[0], step=256)
    def _(i):
        even, odd = halves(accs, i, 256)
        h = jnp.concatenate([jnp.maximum(even, 0.0), jnp.maximum(odd, 0.0)], axis=1).astype(BF16)
        hid[pl.ds(i, 256), :] = h
        t = dot(h, w2_b, COLS_A).astype(BF16)
        tab_b[pl.ds(i, 256), :] = t
        t = t.astype(F32)
        put_halves(tab, i, 256, t[:, :LANES], t[:, LANES:])

    gather_packed(send, 0, tab_b, to_prev)
    gather_packed(send, 1, tab_b, to_next)


def loss_kernel(chunk, classes, counts, src, dst, w, count, from_prev, from_next, part, labels, mask, loss, grad, back_prev, back_next, htab, *accs):
    forward_halo(chunk, counts, src, dst, w, from_prev, from_next, part, htab, accs, unpack_rows)
    lane = lax.broadcasted_iota(jnp.int32, (LANES, LANES), 1)
    live = lane < classes - LANES
    scale = 1.0 / count[0:1, :]
    loss[...] = jnp.zeros_like(loss)

    @pl.loop(0, labels.shape[0] // 2)
    def _(pair):
        for b in (pair * 2, pair * 2 + 1):
            even, odd = halves(accs, b * LANES, LANES)
            label = spread(labels[pl.ds(b, 1), :])
            keep = spread(mask[pl.ds(b, 1), :]).astype(F32)
            odd = jnp.where(live, odd, -jnp.inf)
            top = jnp.max(jnp.maximum(even, odd), axis=1, keepdims=True)
            total = jnp.sum(jnp.exp(even - top) + jnp.exp(odd - top), axis=1, keepdims=True)
            norm = top + jnp.log(total)
            hit_even, hit_odd = lane == label, lane + LANES == label
            picked = jnp.where(hit_even, even, 0.0) + jnp.where(hit_odd, odd, 0.0)
            per_row = jnp.where(lane == 0, norm, 0.0) - picked
            loss[...] += jnp.sum((keep * per_row).reshape(LANES // 8, 8, LANES), axis=0)
            d_even = (jnp.exp(even - norm) - hit_even.astype(F32)) * (keep * scale)
            d_odd = (jnp.exp(odd - norm) - hit_odd.astype(F32)) * (keep * scale)
            put_halves(grad, b * LANES, LANES, d_even, d_odd)

    backward_halo(chunk, counts, src, dst, w, grad, back_prev, back_next, accs)


def take_returns(send, part, got_prev, got_next, accs):
    copy_in(accs[0], part)
    for a in accs[1:]:
        fill_zero(a)
    return_rows(send, send.shape[0] // 2, got_prev, accs)
    return_rows(send, 0, got_next, accs)


def middle_kernel(chunk, counts, src, dst, w, send, got_prev, got_next, part, hid, w2, grad_two, grad, back_prev, back_next, returned, w2_pad, *accs):
    w2_b = padded(w2, w2_pad)
    split = returned.shape[0] // 2
    unpack_rows(got_prev, returned, 0)
    unpack_rows(got_next, returned, split // 2)
    take_returns(send, part, returned.at[pl.ds(0, split)], returned.at[pl.ds(split, split)], accs)
    grad_two[...] = jnp.zeros_like(grad_two)

    @pl.loop(0, hid.shape[0], step=256)
    def _(i):
        even, odd = halves(accs, i, 256)
        d_tab = jnp.concatenate([even, odd], axis=1).astype(BF16)
        h = hid[pl.ds(i, 256), :]
        grad_two[...] += dot(d_tab, h, ROWS_A)
        d_hid = dot(d_tab, w2_b)
        d_pre = jnp.where(h > 0, d_hid, 0.0)
        put_halves(grad, i, 256, d_pre[:, :LANES], d_pre[:, LANES:])

    backward_halo(chunk, counts, src, dst, w, grad, back_prev, back_next, accs)


def last_kernel(send, got_prev, got_next, part, x, grad_one, *accs):
    take_returns(send, part, got_prev, got_next, accs)
    grad_one[...] = jnp.zeros_like(grad_one)

    @pl.loop(0, x.shape[0], step=256)
    def _(i):
        even, odd = halves(accs, i, 256)
        d_tab = jnp.concatenate([even, odd], axis=1).astype(BF16)
        grad_one[...] += dot(x[pl.ds(i, 256), :], d_tab, ROWS_A)


def call(body, name, outs, ins, scratch, flops=10**9, out_specs=None, collective=None, vmem=14):
    extra = {} if collective is None else dict(collective_id=collective, has_side_effects=True)
    return pl.pallas_call(
        body, name=name, out_shape=outs, in_specs=ins, out_specs=out_specs or jax.tree.map(lambda _: VMEM, outs),
        scratch_shapes=[pltpu.VMEM(s, F32) if isinstance(s, tuple) else s for s in scratch],
        compiler_params=pltpu.CompilerParams(vmem_limit_bytes=vmem * 2**20, **extra),
        cost_estimate=pl.CostEstimate(flops=flops, bytes_accessed=8 * 2**20, transcendentals=0),
    )


def solution(mesh):
    num_dev = mesh.shape[AXIS]
    to_next = [(d, (d + 1) % num_dev) for d in range(num_dev)]
    to_prev = [(d, (d - 1) % num_dev) for d in range(num_dev)]

    def step(x, w_one, w_two, send, edge_src, edge_dst, edge_w, labels, mask):
        rows, halo, edges, classes = x.shape[0], send.shape[1], edge_src.shape[0], w_two.shape[1]
        tab = (2 * rows, LANES)
        half = (2 * halo, LANES)
        sds = jax.ShapeDtypeStruct
        tab_f, half_f, half_b = sds(tab, F32), sds(half, F32), sds((halo, 2 * LANES), BF16)
        pack_f, pack_b = sds((3 * halo // 2, LANES), F32), sds((3 * halo // 2, LANES), BF16)
        tab_b = pltpu.VMEM((rows, 2 * LANES), BF16)
        one = sds((8, LANES), F32)
        dma = pltpu.SemaphoreType.DMA
        chunk_l, chunk_h = 64, 32
        lines = edges // LANES
        slots = lines + 8
        w2 = w_two.T
        w2_pad = (2 * LANES, 2 * LANES)
        mask = mask.reshape(-1, LANES)

        lined = lambda a: a.reshape(lines, LANES)
        ints = sds((slots, LANES), jnp.int32)
        src, dst, w, back, counts = call(
            functools.partial(prep_kernel, PREP_CHUNK, rows), "prep", [ints, ints, sds((slots * LANES, LANES), F32), sds((2 * halo // LANES, LANES), jnp.int32), sds((2,), jnp.int32)], [VMEM] * 4,
            [(6 * slots, LANES)], out_specs=[VMEM] * 4 + [SMEM], vmem=8,
        )(lined(edge_src), lined(edge_dst), lined(edge_w), send)
        src, dst, back = src.reshape(-1), dst.reshape(-1), back.reshape(-1)

        tab_one, to_p, to_n, count = call(
            functools.partial(first_kernel, num_dev), "first", [tab_f, half_b, half_b, one], [VMEM] * 4 + [SMEM],
            [tab_b, (8, LANES), (num_dev - 1, 8, LANES), dma((num_dev - 1,)), dma((num_dev - 1,))], collective=0, vmem=8,
        )(x, w_one, send, mask, counts)
        from_prev = lax.ppermute(to_n, AXIS, to_next)
        from_next = lax.ppermute(to_p, AXIS, to_prev)

        walk = [SMEM] * 3 + [VMEM]
        local = call(functools.partial(local_kernel, chunk_l, 4), "local_edges", tab_f, walk + [VMEM], [tab] * 4, 10**10)
        part = local(counts, src, dst, w, tab_one)
        hid, tab_two, to_p, to_n = call(
            functools.partial(hidden_kernel, chunk_h), "hidden", [sds((rows, 2 * LANES), BF16), tab_f, pack_b, pack_b],
            walk + [VMEM] * 5, [tab, tab_b, w2_pad] + [tab] * 4,
        )(counts, src, dst, w, send, from_prev, from_next, part, w2)
        from_prev = lax.ppermute(to_n, AXIS, to_next)
        from_next = lax.ppermute(to_p, AXIS, to_prev)
        part = local(counts, src, dst, w, tab_two)
        loss, grad, to_p, to_n = call(
            functools.partial(loss_kernel, chunk_h, classes), "loss", [sds((8, LANES), F32), tab_f, pack_f, pack_f],
            walk + [VMEM] * 6, [tab] + [tab] * 4,
        )(counts, src, dst, w, count, from_prev, from_next, part, labels.reshape(-1, LANES), mask)
        got_prev = lax.ppermute(to_p, AXIS, to_prev)
        got_next = lax.ppermute(to_n, AXIS, to_next)
        part = local(counts, dst, src, w, grad)
        grad_two, grad, to_p, to_n = call(
            functools.partial(middle_kernel, chunk_h), "middle", [sds((2 * LANES, 2 * LANES), F32), tab_f, half_f, half_f],
            walk + [SMEM] + [VMEM] * 5, [tab, w2_pad] + [tab] * 4,
        )(counts, src, dst, w, back, got_prev, got_next, part, hid, w2)
        got_prev = lax.ppermute(to_p, AXIS, to_prev)
        got_next = lax.ppermute(to_n, AXIS, to_next)
        part = local(counts, dst, src, w, grad)

        grad_one = call(last_kernel, "last", sds((x.shape[1], 2 * LANES), F32), [SMEM] + [VMEM] * 4, [tab] * 4)(back, got_prev, got_next, part, x)
        lines = 2 * x.shape[1] + 2 * (-(-classes // 8) * 8) + 8
        lines = -(-lines // (8 * num_dev)) * 8 * num_dev
        grad_one, grad_two, mean = call(
            functools.partial(reduce_kernel, num_dev), "reduce", [sds(grad_one.shape, F32), sds((classes, 2 * LANES), F32), sds((1, 1), F32)],
            [VMEM] * 4, [(lines, LANES), (lines, LANES), (lines // 2, LANES), (num_dev // 2 - 1, lines // num_dev, LANES), dma((2, num_dev))],
            collective=1, vmem=8,
        )(grad_one, grad_two, loss, count)
        return mean.reshape(()), grad_one, grad_two.T

    row = P(AXIS)
    return jax.shard_map(
        step, mesh=mesh, in_specs=(row, P(), P(), row, row, row, row, row, row), out_specs=(P(), P(), P()), check_vma=False
    )
```

```python
import functools

import jax
import jax.numpy as jnp
from jax import lax
from jax.experimental import pallas as pl
from jax.experimental.pallas import tpu as pltpu
from jax.sharding import PartitionSpec as P

AXIS = "graph"
LANES = 128
ROWS_A = (((0,), (0,)), ((), ()))
COLS_A = (((1,), (1,)), ((), ()))
F32, BF16 = jnp.float32, jnp.bfloat16
VMEM = pl.BlockSpec(memory_space=pltpu.VMEM)
SMEM = pl.BlockSpec(memory_space=pltpu.SMEM)
STEP = 512
PREP_CHUNK = 64
MESH = pl.DeviceIdType.MESH


def dot(a, b, dims=(((1,), (0,)), ((), ()))):
    return lax.dot_general(a, b, dims, preferred_element_type=F32)


def fill_zero(ref):
    zero = jnp.zeros((STEP, LANES), F32)

    @pl.loop(0, ref.shape[0], step=STEP)
    def _(i):
        ref[pl.ds(i, STEP), :] = zero


def copy_in(dst, src):
    @pl.loop(0, dst.shape[0], step=STEP)
    def _(i):
        dst[pl.ds(i, STEP), :] = src[pl.ds(i, STEP), :].astype(F32)


def walk_edges(first, last, chunk, from_idx, to_idx, w, table, accs):
    group = len(accs)

    def body(c, _):
        base = c * chunk
        w_chunk = w.at[pl.ds(pl.multiple_of(base, chunk), chunk)]
        for g in range(0, chunk, group):
            pend = []
            for u in range(group):
                k = base + g + u
                s = pl.multiple_of(from_idx[k], 2)
                d = pl.multiple_of(to_idx[k], 2)
                pend.append((d, accs[u][pl.ds(d, 2), :] + table[pl.ds(s, 2), :] * w_chunk[g + u : g + u + 1, :]))
            for u in range(group):
                accs[u][pl.ds(pend[u][0], 2), :] = pend[u][1]
        return 0

    lax.fori_loop(first, last, body, 0)


def one_hot_rows(idx, which, start, table):
    lane = lax.broadcasted_iota(jnp.int32, (LANES, LANES), 1)
    hot = []
    for q in range(2):
        want = spread(idx[which : which + 1, pl.ds(pl.multiple_of(start + q * LANES, LANES), LANES)])
        hot.append(
            jnp.concatenate([jnp.where(want == lane + LANES * j, 1.0, 0.0).astype(BF16) for j in range(table.shape[0] // LANES)], axis=1)
        )
    return dot(jnp.concatenate(hot, axis=0), table[...])


def low_lanes(rows):
    return lax.broadcasted_iota(jnp.int32, (rows, LANES), 1) < LANES // 2


def swap_lanes(v):
    return pltpu.roll(v, LANES // 2, 1)


def gather_rows(idx, which, table, out):
    @pl.loop(0, out.shape[0], step=256)
    def _(i):
        out[pl.ds(pl.multiple_of(i, 256), 256), :] = one_hot_rows(idx, which, i, table).astype(BF16)


def gather_packed(idx, which, table, out):
    halo = out.shape[0] * 2 // 3

    @pl.loop(0, halo // 2, step=256)
    def _(i):
        i = pl.multiple_of(i, 256)
        a = one_hot_rows(idx, which, i, table)
        b = one_hot_rows(idx, which, halo // 2 + i, table)
        out[pl.ds(i, 256), :] = a[:, :LANES].astype(BF16)
        out[pl.ds(halo // 2 + i, 256), :] = b[:, :LANES].astype(BF16)
        out[pl.ds(halo + i, 256), :] = jnp.where(low_lanes(256), a[:, LANES:], swap_lanes(b[:, LANES:])).astype(BF16)


def unpack_rows(got, table, start):
    halo = got.shape[0] * 2 // 3

    @pl.loop(0, halo // 2, step=256)
    def _(i):
        i = pl.multiple_of(i, 256)
        a, b, both = (got[pl.ds(k + i, 256), :].astype(F32) for k in (0, halo // 2, halo))
        put_halves(table, start + i, 256, a, jnp.where(low_lanes(256), both, 0.0))
        put_halves(table, start + halo // 2 + i, 256, b, jnp.where(low_lanes(256), swap_lanes(both), 0.0))


def unpack_plain(got, table, start):
    @pl.loop(0, got.shape[0], step=256)
    def _(i):
        t = got[pl.ds(i, 256), :].astype(F32)
        put_halves(table, start + i, 256, t[:, :LANES], t[:, LANES:])


def spread(row):
    return jnp.transpose(jnp.broadcast_to(row, (LANES, LANES)))


def return_rows(idx, start, vals, accs, chunk=32):
    group = len(accs)

    @pl.loop(0, vals.shape[0] // (2 * chunk))
    def _(c):
        block = vals.at[pl.ds(pl.multiple_of(c * 2 * chunk, 2 * chunk), 2 * chunk)]
        for g in range(0, chunk, group):
            pend = []
            for u in range(group):
                d = pl.multiple_of(idx[start + c * chunk + g + u], 2)
                pend.append((d, accs[u][pl.ds(d, 2), :] + block[2 * (g + u) : 2 * (g + u) + 2, :]))
            for u in range(group):
                accs[u][pl.ds(pend[u][0], 2), :] = pend[u][1]


def halves(accs, i, n):
    even = functools.reduce(jnp.add, [a[pl.ds(2 * i, n, stride=2), :] for a in accs])
    odd = functools.reduce(jnp.add, [a[pl.ds(2 * i + 1, n, stride=2), :] for a in accs])
    return even, odd


def put_halves(table, i, n, even, odd):
    table[pl.ds(2 * i, n, stride=2), :] = even
    table[pl.ds(2 * i + 1, n, stride=2), :] = odd


def greet(n):
    me = lax.axis_index(AXIS)
    barrier = pltpu.get_barrier_semaphore()
    for o in range(1, n):
        pl.semaphore_signal(barrier, inc=1, device_id=(lax.rem(me + o, n),), device_id_type=MESH)
    return me, lambda: pl.semaphore_wait(barrier, n - 1)


def remote(src, dst, send_sem, recv_sem, peer):
    return pltpu.make_async_remote_copy(
        src_ref=src, dst_ref=dst, send_sem=send_sem, recv_sem=recv_sem, device_id=(peer,), device_id_type=MESH
    )


def first_kernel(n, x, w1, send, mask, after, tab, to_prev, to_next, count, tab_b, mine, theirs, send_sem, recv_sem):
    me, met = greet(n)
    rows = x.shape[0]
    mask_f = mask[...].astype(F32)
    mine[...] = jnp.sum(mask_f.reshape(-1, 8, LANES), axis=0)
    w = w1[...].astype(BF16)

    @pl.loop(0, rows, step=256)
    def _(i):
        t = dot(x[pl.ds(i, 256), :], w).astype(BF16)
        tab_b[pl.ds(i, 256), :] = t
        t = t.astype(F32)
        put_halves(tab, i, 256, t[:, :LANES], t[:, LANES:])

    met()
    copies = [remote(mine, theirs.at[o - 1], send_sem.at[o - 1], recv_sem.at[o - 1], lax.rem(me + o, n)) for o in range(1, n)]
    for c in copies:
        c.start()
    gather_rows(send, 0, tab_b, to_prev)
    gather_rows(send, 1, tab_b, to_next)
    for c in copies:
        c.wait()
    total = mine[...] + jnp.sum(theirs[...], axis=0)
    count[...] = jnp.maximum(jnp.broadcast_to(jnp.sum(total, keepdims=True), count.shape), 1.0)


def reduce_kernel(n, one, two, loss, count, one_out, two_out, mean, work, full, got_pair, got_rest, sems):
    me = lax.axis_index(AXIS)
    chips, core = n // 2, lax.rem(me, 2)
    chip = lax.div(me, 2)
    pair = me + 1 - 2 * core
    others = [lax.rem(chip + o, chips) for o in range(1, chips)]
    barrier = pltpu.get_barrier_semaphore()
    for p in [pair] + [2 * c + core for c in others]:
        pl.semaphore_signal(barrier, inc=1, device_id=(p,), device_id_type=MESH)
    classes = two_out.shape[0]
    lines = -(-classes // 8) * 8
    top, wide = one.shape
    work[0:top, :] = one[:, :LANES]
    work[top : 2 * top, :] = one[:, LANES:]
    work[2 * top : 2 * top + lines, :] = two[:lines, :LANES]
    work[2 * top + lines : 2 * top + 2 * lines, :] = two[:lines, LANES:]
    tail = 2 * top + 2 * lines
    work[tail : tail + 8, :] = loss[...]
    work[tail + 8 :, :] = jnp.zeros((work.shape[0] - tail - 8, LANES), F32)
    pl.semaphore_wait(barrier, chips)

    half = work.shape[0] // 2
    piece = half // chips
    rows = lambda start, size: pl.ds(pl.multiple_of(start, 8), size)
    mine, other = rows(core * half, half), rows((1 - core) * half, half)
    swap = remote(work.at[other], got_pair, sems.at[0, 0], sems.at[1, 0], pair)
    swap.start()
    swap.wait()
    work[mine, :] += got_pair[...]
    scatter = [
        remote(work.at[rows(core * half + c * piece, piece)], got_rest.at[o], sems.at[0, 1 + o], sems.at[1, 1 + o], 2 * c + core)
        for o, c in enumerate(others)
    ]
    for c in scatter:
        c.start()
    for c in scatter:
        c.wait()
    own = rows(core * half + chip * piece, piece)
    work[own, :] += jnp.sum(got_rest[...], axis=0)
    full[own, :] = work[own, :]
    gather = [
        remote(work.at[own], full.at[own], sems.at[0, chips + o], sems.at[1, chips + o], 2 * c + core) for o, c in enumerate(others)
    ]
    for c in gather:
        c.start()
    for c in gather:
        c.wait()
    last = remote(full.at[mine], full.at[mine], sems.at[0, 2 * chips - 1], sems.at[1, 2 * chips - 1], pair)
    last.start()
    last.wait()
    one_out[:, :LANES] = full[0:top, :]
    one_out[:, LANES:] = full[top : 2 * top, :]
    two_out[:, :LANES] = full[2 * top : 2 * top + classes, :]
    two_out[:, LANES:] = full[2 * top + lines : 2 * top + lines + classes, :]
    mean[...] = jnp.sum(full[tail : tail + 8, :], keepdims=True) / count[0:1, 0:1]


def prep_kernel(chunk, rows, src, dst, w, src_out, dst_out, w_out, counts, total):
    lines = src.shape[0]
    slots = src_out.shape[0]
    live = w[...] != 0.0
    halo = src[...] >= rows
    at = lambda shape, axis: lax.broadcasted_iota(jnp.int32, shape, axis)
    before = (at((LANES, LANES), 0) < at((LANES, LANES), 1)).astype(BF16)
    above = (at((lines, lines), 1) < at((lines, lines), 0)).astype(BF16)
    ones = jnp.ones((LANES, LANES), BF16)

    def rank(mask):
        m = mask.astype(F32).astype(BF16)
        return dot(m, before) + dot(above, dot(m, ones).astype(BF16))

    is_local, is_halo = jnp.logical_and(live, jnp.logical_not(halo)), jnp.logical_and(live, halo)
    n_local = jnp.sum(is_local.astype(F32)).astype(jnp.int32)
    n_halo = jnp.sum(is_halo.astype(F32)).astype(jnp.int32)
    local_chunks = (n_local + chunk - 1) // chunk
    counts[0] = local_chunks
    counts[1] = local_chunks + (n_halo + chunk - 1) // chunk
    pos = jnp.where(
        is_local, rank(is_local).astype(jnp.int32), jnp.where(is_halo, rank(is_halo).astype(jnp.int32) + local_chunks * chunk, -1)
    )
    line, lane = pos >> 7, pos & (LANES - 1)
    s = jnp.where(halo, src[...] - rows, src[...])
    d = dst[...]
    half_w = w[...] * 0.5
    w_a = half_w.astype(BF16).astype(F32)
    w_b = (half_w - w_a).astype(BF16).astype(F32)
    w_c = half_w - w_a - w_b
    high = ((s >> 8) * 8 + (d >> 8)).astype(F32)
    planes = [(s & 255).astype(F32), (d & 255).astype(F32), high, w_a, w_b, w_c]
    acc = jnp.zeros((len(planes) * slots, LANES), F32)
    for r in range(0, lines, 2):
        lhs, rhs = [], []
        for q in (r, r + 1):
            pick = at((slots, LANES), 0) == line[q : q + 1, :]
            lhs.append(jnp.concatenate([jnp.where(pick, p[q : q + 1, :], 0.0) for p in planes], axis=0))
            rhs.append((at((LANES, LANES), 0) == lane[q : q + 1, :]).astype(F32))
        acc += dot(jnp.concatenate(lhs, axis=1).astype(BF16), jnp.concatenate(rhs, axis=1).astype(BF16), COLS_A)
    total[...] = acc
    plane = lambda i: total[i * slots : (i + 1) * slots, :]
    high = plane(2).astype(jnp.int32)
    src_out[...] = ((high >> 3) * 256 + plane(0).astype(jnp.int32)) * 2
    dst_out[...] = ((high & 7) * 256 + plane(1).astype(jnp.int32)) * 2
    total[0:slots, :] = (plane(3) + plane(4) + plane(5)) * 2.0

    @pl.loop(0, slots // 8)
    def _(r):
        for q in range(8):
            w_out[pl.ds(pl.multiple_of((r * 8 + q) * LANES, LANES), LANES), :] = spread(total[pl.ds(r * 8 + q, 1), :])


def local_kernel(chunk, n_acc, counts, from_idx, to_idx, w, table, out, *accs):
    for a in accs:
        fill_zero(a)
    walk_edges(0, counts[0] * (PREP_CHUNK // chunk), chunk, from_idx, to_idx, w, table, accs)

    @pl.loop(0, out.shape[0], step=STEP)
    def _(i):
        out[pl.ds(i, STEP), :] = functools.reduce(jnp.add, [a[pl.ds(i, STEP), :] for a in accs])


def halo_range(counts, chunk):
    return counts[0] * (PREP_CHUNK // chunk), counts[1] * (PREP_CHUNK // chunk)


def forward_halo(chunk, counts, src, dst, w, from_prev, from_next, part, htab, accs, unpack):
    unpack(from_prev, htab, 0)
    unpack(from_next, htab, htab.shape[0] // 4)
    copy_in(accs[0], part)
    for a in accs[1:]:
        fill_zero(a)
    first, last = halo_range(counts, chunk)
    walk_edges(first, last, chunk, src, dst, w, htab, accs)


def backward_halo(chunk, counts, src, dst, w, grad, back_prev, back_next, accs):
    for a in accs:
        fill_zero(a)
    first, last = halo_range(counts, chunk)
    walk_edges(first, last, chunk, dst, src, w, grad, accs)
    split = accs[0].shape[0] // 2
    if back_prev.shape[0] == split:

        @pl.loop(0, split, step=STEP)
        def _(i):
            back_prev[pl.ds(i, STEP), :] = functools.reduce(jnp.add, [a[pl.ds(i, STEP), :] for a in accs])
            back_next[pl.ds(i, STEP), :] = functools.reduce(jnp.add, [a[pl.ds(split + i, STEP), :] for a in accs])
        return
    halo = split // 2

    @pl.loop(0, halo // 2, step=256)
    def _(i):
        i = pl.multiple_of(i, 256)
        for start, out in ((0, back_prev), (halo, back_next)):
            a_even, a_odd = halves(accs, start + i, 256)
            b_even, b_odd = halves(accs, start + halo // 2 + i, 256)
            out[pl.ds(i, 256), :] = a_even
            out[pl.ds(halo // 2 + i, 256), :] = b_even
            out[pl.ds(halo + i, 256), :] = jnp.where(low_lanes(256), a_odd, swap_lanes(b_odd))


def padded(w, buf):
    low = w.shape[0] // 8 * 8
    buf[low:, :] = jnp.zeros((buf.shape[0] - low, buf.shape[1]), F32)
    buf[0 : w.shape[0], :] = w[...]
    return buf[...].astype(BF16)


def hidden_kernel(chunk, counts, src, dst, w, send, from_prev, from_next, part, w2, hid, tab, to_prev, to_next, back, htab, tab_b, w2_pad, *accs):
    w2_b = padded(w2, w2_pad)
    per = send.shape[1] // LANES
    for i in range(2 * per):
        back[i : i + 1, :] = send[i // per : i // per + 1, (i % per) * LANES : (i % per + 1) * LANES] * 2
    forward_halo(chunk, counts, src, dst, w, from_prev, from_next, part, htab, accs, unpack_plain)

    @pl.loop(0, hid.shape[0], step=256)
    def _(i):
        even, odd = halves(accs, i, 256)
        h = jnp.concatenate([jnp.maximum(even, 0.0), jnp.maximum(odd, 0.0)], axis=1).astype(BF16)
        hid[pl.ds(i, 256), :] = h
        t = dot(h, w2_b, COLS_A).astype(BF16)
        tab_b[pl.ds(i, 256), :] = t
        t = t.astype(F32)
        put_halves(tab, i, 256, t[:, :LANES], t[:, LANES:])

    gather_packed(send, 0, tab_b, to_prev)
    gather_packed(send, 1, tab_b, to_next)


def loss_kernel(chunk, classes, counts, src, dst, w, count, from_prev, from_next, part, labels, mask, loss, grad, back_prev, back_next, htab, *accs):
    forward_halo(chunk, counts, src, dst, w, from_prev, from_next, part, htab, accs, unpack_rows)
    lane = lax.broadcasted_iota(jnp.int32, (LANES, LANES), 1)
    live = lane < classes - LANES
    scale = 1.0 / count[0:1, :]
    loss[...] = jnp.zeros_like(loss)

    @pl.loop(0, labels.shape[0] // 2)
    def _(pair):
        for b in (pair * 2, pair * 2 + 1):
            even, odd = halves(accs, b * LANES, LANES)
            label = spread(labels[pl.ds(b, 1), :])
            keep = spread(mask[pl.ds(b, 1), :]).astype(F32)
            odd = jnp.where(live, odd, -jnp.inf)
            top = jnp.max(jnp.maximum(even, odd), axis=1, keepdims=True)
            total = jnp.sum(jnp.exp(even - top) + jnp.exp(odd - top), axis=1, keepdims=True)
            norm = top + jnp.log(total)
            hit_even, hit_odd = lane == label, lane + LANES == label
            picked = jnp.where(hit_even, even, 0.0) + jnp.where(hit_odd, odd, 0.0)
            per_row = jnp.where(lane == 0, norm, 0.0) - picked
            loss[...] += jnp.sum((keep * per_row).reshape(LANES // 8, 8, LANES), axis=0)
            d_even = (jnp.exp(even - norm) - hit_even.astype(F32)) * (keep * scale)
            d_odd = (jnp.exp(odd - norm) - hit_odd.astype(F32)) * (keep * scale)
            put_halves(grad, b * LANES, LANES, d_even, d_odd)

    backward_halo(chunk, counts, src, dst, w, grad, back_prev, back_next, accs)


def take_returns(send, part, got_prev, got_next, accs):
    copy_in(accs[0], part)
    for a in accs[1:]:
        fill_zero(a)
    return_rows(send, send.shape[0] // 2, got_prev, accs)
    return_rows(send, 0, got_next, accs)


def middle_kernel(chunk, counts, src, dst, w, send, got_prev, got_next, part, hid, w2, grad_two, grad, back_prev, back_next, returned, w2_pad, *accs):
    w2_b = padded(w2, w2_pad)
    split = returned.shape[0] // 2
    unpack_rows(got_prev, returned, 0)
    unpack_rows(got_next, returned, split // 2)
    take_returns(send, part, returned.at[pl.ds(0, split)], returned.at[pl.ds(split, split)], accs)
    grad_two[...] = jnp.zeros_like(grad_two)

    @pl.loop(0, hid.shape[0], step=256)
    def _(i):
        even, odd = halves(accs, i, 256)
        d_tab = jnp.concatenate([even, odd], axis=1).astype(BF16)
        h = hid[pl.ds(i, 256), :]
        grad_two[...] += dot(d_tab, h, ROWS_A)
        d_hid = dot(d_tab, w2_b)
        d_pre = jnp.where(h > 0, d_hid, 0.0)
        put_halves(grad, i, 256, d_pre[:, :LANES], d_pre[:, LANES:])

    backward_halo(chunk, counts, src, dst, w, grad, back_prev, back_next, accs)


def last_kernel(send, got_prev, got_next, part, x, grad_one, *accs):
    take_returns(send, part, got_prev, got_next, accs)
    grad_one[...] = jnp.zeros_like(grad_one)

    @pl.loop(0, x.shape[0], step=256)
    def _(i):
        even, odd = halves(accs, i, 256)
        d_tab = jnp.concatenate([even, odd], axis=1).astype(BF16)
        grad_one[...] += dot(x[pl.ds(i, 256), :], d_tab, ROWS_A)


def call(body, name, outs, ins, scratch, flops=10**9, out_specs=None, collective=None, vmem=14):
    extra = {} if collective is None else dict(collective_id=collective, has_side_effects=True)
    return pl.pallas_call(
        body, name=name, out_shape=outs, in_specs=ins, out_specs=out_specs or jax.tree.map(lambda _: VMEM, outs),
        scratch_shapes=[pltpu.VMEM(s, F32) if isinstance(s, tuple) else s for s in scratch],
        compiler_params=pltpu.CompilerParams(vmem_limit_bytes=vmem * 2**20, **extra),
        cost_estimate=pl.CostEstimate(flops=flops, bytes_accessed=8 * 2**20, transcendentals=0),
    )


def solution(mesh):
    num_dev = mesh.shape[AXIS]
    to_next = [(d, (d + 1) % num_dev) for d in range(num_dev)]
    to_prev = [(d, (d - 1) % num_dev) for d in range(num_dev)]

    def step(x, w_one, w_two, send, edge_src, edge_dst, edge_w, labels, mask):
        rows, halo, edges, classes = x.shape[0], send.shape[1], edge_src.shape[0], w_two.shape[1]
        tab = (2 * rows, LANES)
        half = (2 * halo, LANES)
        sds = jax.ShapeDtypeStruct
        tab_f, half_f, half_b = sds(tab, F32), sds(half, F32), sds((halo, 2 * LANES), BF16)
        pack_f, pack_b = sds((3 * halo // 2, LANES), F32), sds((3 * halo // 2, LANES), BF16)
        tab_b = pltpu.VMEM((rows, 2 * LANES), BF16)
        one = sds((8, LANES), F32)
        dma = pltpu.SemaphoreType.DMA
        chunk_l, chunk_h = 64, 32
        lines = edges // LANES
        slots = lines + 8
        w2 = w_two.T
        w2_pad = (2 * LANES, 2 * LANES)
        mask = mask.reshape(-1, LANES)

        lined = lambda a: a.reshape(lines, LANES)
        ints = sds((slots, LANES), jnp.int32)
        src, dst, w, counts = call(
            functools.partial(prep_kernel, PREP_CHUNK, rows), "prep", [ints, ints, sds((slots * LANES, LANES), F32), sds((2,), jnp.int32)], [VMEM] * 3,
            [(6 * slots, LANES)], out_specs=[VMEM] * 3 + [SMEM], vmem=8,
        )(lined(edge_src), lined(edge_dst), lined(edge_w))
        src, dst = src.reshape(-1), dst.reshape(-1)

        tab_one, to_p, to_n, count = call(
            functools.partial(first_kernel, num_dev), "first", [tab_f, half_b, half_b, one], [VMEM] * 4 + [SMEM],
            [tab_b, (8, LANES), (num_dev - 1, 8, LANES), dma((num_dev - 1,)), dma((num_dev - 1,))], collective=0, vmem=8,
        )(x, w_one, send, mask, counts)
        from_prev = lax.ppermute(to_n, AXIS, to_next)
        from_next = lax.ppermute(to_p, AXIS, to_prev)

        walk = [SMEM] * 3 + [VMEM]
        local = call(functools.partial(local_kernel, chunk_l, 4), "local_edges", tab_f, walk + [VMEM], [tab] * 4, 10**10)
        part = local(counts, src, dst, w, tab_one)
        hid, tab_two, to_p, to_n, back = call(
            functools.partial(hidden_kernel, chunk_h), "hidden", [sds((rows, 2 * LANES), BF16), tab_f, pack_b, pack_b, sds((2 * halo // LANES, LANES), jnp.int32)],
            walk + [VMEM] * 5, [tab, tab_b, w2_pad] + [tab] * 4,
        )(counts, src, dst, w, send, from_prev, from_next, part, w2)
        from_prev = lax.ppermute(to_n, AXIS, to_next)
        from_next = lax.ppermute(to_p, AXIS, to_prev)
        back = back.reshape(-1)
        part = local(counts, src, dst, w, tab_two)
        loss, grad, to_p, to_n = call(
            functools.partial(loss_kernel, chunk_h, classes), "loss", [sds((8, LANES), F32), tab_f, pack_f, pack_f],
            walk + [VMEM] * 6, [tab] + [tab] * 4,
        )(counts, src, dst, w, count, from_prev, from_next, part, labels.reshape(-1, LANES), mask)
        got_prev = lax.ppermute(to_p, AXIS, to_prev)
        got_next = lax.ppermute(to_n, AXIS, to_next)
        part = local(counts, dst, src, w, grad)
        grad_two, grad, to_p, to_n = call(
            functools.partial(middle_kernel, chunk_h), "middle", [sds((2 * LANES, 2 * LANES), F32), tab_f, half_f, half_f],
            walk + [SMEM] + [VMEM] * 5, [tab, w2_pad] + [tab] * 4,
        )(counts, src, dst, w, back, got_prev, got_next, part, hid, w2)
        got_prev = lax.ppermute(to_p, AXIS, to_prev)
        got_next = lax.ppermute(to_n, AXIS, to_next)
        part = local(counts, dst, src, w, grad)

        grad_one = call(last_kernel, "last", sds((x.shape[1], 2 * LANES), F32), [SMEM] + [VMEM] * 4, [tab] * 4)(back, got_prev, got_next, part, x)
        lines = 2 * x.shape[1] + 2 * (-(-classes // 8) * 8) + 8
        lines = -(-lines // (8 * num_dev)) * 8 * num_dev
        grad_one, grad_two, mean = call(
            functools.partial(reduce_kernel, num_dev), "reduce", [sds(grad_one.shape, F32), sds((classes, 2 * LANES), F32), sds((1, 1), F32)],
            [VMEM] * 4, [(lines, LANES), (lines, LANES), (lines // 2, LANES), (num_dev // 2 - 1, lines // num_dev, LANES), dma((2, num_dev))],
            collective=1, vmem=8,
        )(grad_one, grad_two, loss, count)
        return mean.reshape(()), grad_one, grad_two.T

    row = P(AXIS)
    return jax.shard_map(
        step, mesh=mesh, in_specs=(row, P(), P(), row, row, row, row, row, row), out_specs=(P(), P(), P()), check_vma=False
    )
```

```python
import functools

import jax
import jax.numpy as jnp
from jax import lax
from jax.experimental import pallas as pl
from jax.experimental.pallas import tpu as pltpu
from jax.sharding import PartitionSpec as P

AXIS = "graph"
LANES = 128
ROWS_A = (((0,), (0,)), ((), ()))
COLS_A = (((1,), (1,)), ((), ()))
F32, BF16 = jnp.float32, jnp.bfloat16
VMEM = pl.BlockSpec(memory_space=pltpu.VMEM)
SMEM = pl.BlockSpec(memory_space=pltpu.SMEM)
ANY = pl.BlockSpec(memory_space=pl.ANY)
STEP = 512
PREP_CHUNK = 64
SEGMENT = 1024
MESH = pl.DeviceIdType.MESH


def dot(a, b, dims=(((1,), (0,)), ((), ()))):
    return lax.dot_general(a, b, dims, preferred_element_type=F32)


def fill_zero(ref):
    zero = jnp.zeros((STEP, LANES), F32)

    @pl.loop(0, ref.shape[0], step=STEP)
    def _(i):
        ref[pl.ds(i, STEP), :] = zero


def copy_in(dst, src):
    @pl.loop(0, dst.shape[0], step=STEP)
    def _(i):
        dst[pl.ds(i, STEP), :] = src[pl.ds(i, STEP), :].astype(F32)


class Edges:
    def __init__(self, first, last, src, dst, w, src_s, dst_s, sems):
        self.first, self.last, self.w = first, last, w
        self.src, self.dst = src_s, dst_s
        self.pairs = ((src, src_s), (dst, dst_s))
        self.sems = sems

    def copies(self, seg):
        part = pl.ds(pl.multiple_of(seg * SEGMENT, SEGMENT), SEGMENT)
        return [pltpu.make_async_copy(a.at[part], b.at[part], self.sems.at[i, seg]) for i, (a, b) in enumerate(self.pairs)]

    def fetch(self):
        per = SEGMENT // PREP_CHUNK
        for seg in range(self.src.shape[0] // SEGMENT):

            @pl.when(jnp.logical_and(seg * per < self.last, (seg + 1) * per > self.first))
            def _():
                for c in self.copies(seg):
                    c.start()

    def walk(self, chunk, from_idx, to_idx, table, accs, wait):
        group, per, ratio = len(accs), SEGMENT // chunk, PREP_CHUNK // chunk
        first, last = self.first * ratio, self.last * ratio

        def body(c, _):
            base = c * chunk
            w_chunk = self.w.at[pl.ds(pl.multiple_of(base, chunk), chunk)]
            for g in range(0, chunk, group):
                pend = []
                for u in range(group):
                    k = base + g + u
                    s = pl.multiple_of(from_idx[k], 2)
                    d = pl.multiple_of(to_idx[k], 2)
                    pend.append((d, accs[u][pl.ds(d, 2), :] + table[pl.ds(s, 2), :] * w_chunk[g + u : g + u + 1, :]))
                for u in range(group):
                    accs[u][pl.ds(pend[u][0], 2), :] = pend[u][1]
            return 0

        if not wait:
            lax.fori_loop(first, last, body, 0)
            return

        def segment(seg, _):
            for c in self.copies(seg):
                c.wait()
            lax.fori_loop(jnp.maximum(first, seg * per), jnp.minimum(last, (seg + 1) * per), body, 0)
            return 0

        lax.fori_loop(first // per, (last + per - 1) // per, segment, 0)


def one_hot_rows(idx, which, start, table):
    lane = lax.broadcasted_iota(jnp.int32, (LANES, LANES), 1)
    hot = []
    for q in range(2):
        want = spread(idx[which : which + 1, pl.ds(pl.multiple_of(start + q * LANES, LANES), LANES)])
        hot.append(
            jnp.concatenate([jnp.where(want == lane + LANES * j, 1.0, 0.0).astype(BF16) for j in range(table.shape[0] // LANES)], axis=1)
        )
    return dot(jnp.concatenate(hot, axis=0), table[...])


def low_lanes(rows):
    return lax.broadcasted_iota(jnp.int32, (rows, LANES), 1) < LANES // 2


def swap_lanes(v):
    return pltpu.roll(v, LANES // 2, 1)


def gather_rows(idx, which, table, out):
    @pl.loop(0, out.shape[0], step=256)
    def _(i):
        out[pl.ds(pl.multiple_of(i, 256), 256), :] = one_hot_rows(idx, which, i, table).astype(BF16)


def gather_packed(idx, which, table, out):
    halo = out.shape[0] * 2 // 3

    @pl.loop(0, halo // 2, step=256)
    def _(i):
        i = pl.multiple_of(i, 256)
        a = one_hot_rows(idx, which, i, table)
        b = one_hot_rows(idx, which, halo // 2 + i, table)
        out[pl.ds(i, 256), :] = a[:, :LANES].astype(BF16)
        out[pl.ds(halo // 2 + i, 256), :] = b[:, :LANES].astype(BF16)
        out[pl.ds(halo + i, 256), :] = jnp.where(low_lanes(256), a[:, LANES:], swap_lanes(b[:, LANES:])).astype(BF16)


def unpack_rows(got, table, start):
    halo = got.shape[0] * 2 // 3

    @pl.loop(0, halo // 2, step=256)
    def _(i):
        i = pl.multiple_of(i, 256)
        a, b, both = (got[pl.ds(k + i, 256), :].astype(F32) for k in (0, halo // 2, halo))
        put_halves(table, start + i, 256, a, jnp.where(low_lanes(256), both, 0.0))
        put_halves(table, start + halo // 2 + i, 256, b, jnp.where(low_lanes(256), swap_lanes(both), 0.0))


def unpack_plain(got, table, start):
    @pl.loop(0, got.shape[0], step=256)
    def _(i):
        t = got[pl.ds(i, 256), :].astype(F32)
        put_halves(table, start + i, 256, t[:, :LANES], t[:, LANES:])


def spread(row):
    return jnp.transpose(jnp.broadcast_to(row, (LANES, LANES)))


def return_rows(idx, start, vals, accs, chunk=32):
    group = len(accs)

    @pl.loop(0, vals.shape[0] // (2 * chunk))
    def _(c):
        block = vals.at[pl.ds(pl.multiple_of(c * 2 * chunk, 2 * chunk), 2 * chunk)]
        for g in range(0, chunk, group):
            pend = []
            for u in range(group):
                d = pl.multiple_of(idx[start + c * chunk + g + u], 2)
                pend.append((d, accs[u][pl.ds(d, 2), :] + block[2 * (g + u) : 2 * (g + u) + 2, :]))
            for u in range(group):
                accs[u][pl.ds(pend[u][0], 2), :] = pend[u][1]


def halves(accs, i, n):
    even = functools.reduce(jnp.add, [a[pl.ds(2 * i, n, stride=2), :] for a in accs])
    odd = functools.reduce(jnp.add, [a[pl.ds(2 * i + 1, n, stride=2), :] for a in accs])
    return even, odd


def put_halves(table, i, n, even, odd):
    table[pl.ds(2 * i, n, stride=2), :] = even
    table[pl.ds(2 * i + 1, n, stride=2), :] = odd


def greet(n):
    me = lax.axis_index(AXIS)
    barrier = pltpu.get_barrier_semaphore()
    for o in range(1, n):
        pl.semaphore_signal(barrier, inc=1, device_id=(lax.rem(me + o, n),), device_id_type=MESH)
    return me, lambda: pl.semaphore_wait(barrier, n - 1)


def remote(src, dst, send_sem, recv_sem, peer):
    return pltpu.make_async_remote_copy(
        src_ref=src, dst_ref=dst, send_sem=send_sem, recv_sem=recv_sem, device_id=(peer,), device_id_type=MESH
    )


def first_kernel(x, w1, send, after, tab, to_prev, to_next, tab_b):
    rows = x.shape[0]
    w = w1[...].astype(BF16)

    @pl.loop(0, rows, step=256)
    def _(i):
        t = dot(x[pl.ds(i, 256), :], w).astype(BF16)
        tab_b[pl.ds(i, 256), :] = t
        t = t.astype(F32)
        put_halves(tab, i, 256, t[:, :LANES], t[:, LANES:])

    gather_rows(send, 0, tab_b, to_prev)
    gather_rows(send, 1, tab_b, to_next)


def reduce_kernel(n, one, two, loss, count, one_out, two_out, mean, work, full, got_pair, got_rest, sems):
    me = lax.axis_index(AXIS)
    chips, core = n // 2, lax.rem(me, 2)
    chip = lax.div(me, 2)
    pair = me + 1 - 2 * core
    others = [lax.rem(chip + o, chips) for o in range(1, chips)]
    barrier = pltpu.get_barrier_semaphore()
    for p in [pair] + [2 * c + core for c in others]:
        pl.semaphore_signal(barrier, inc=1, device_id=(p,), device_id_type=MESH)
    classes = two_out.shape[0]
    lines = -(-classes // 8) * 8
    top, wide = one.shape
    work[0:top, :] = one[:, :LANES]
    work[top : 2 * top, :] = one[:, LANES:]
    work[2 * top : 2 * top + lines, :] = two[:lines, :LANES]
    work[2 * top + lines : 2 * top + 2 * lines, :] = two[:lines, LANES:]
    tail = 2 * top + 2 * lines
    work[tail : tail + 8, :] = loss[...]
    work[tail + 8 :, :] = jnp.zeros((work.shape[0] - tail - 8, LANES), F32)
    pl.semaphore_wait(barrier, chips)

    half = work.shape[0] // 2
    piece = half // chips
    rows = lambda start, size: pl.ds(pl.multiple_of(start, 8), size)
    mine, other = rows(core * half, half), rows((1 - core) * half, half)
    swap = remote(work.at[other], got_pair, sems.at[0, 0], sems.at[1, 0], pair)
    swap.start()
    swap.wait()
    work[mine, :] += got_pair[...]
    scatter = [
        remote(work.at[rows(core * half + c * piece, piece)], got_rest.at[o], sems.at[0, 1 + o], sems.at[1, 1 + o], 2 * c + core)
        for o, c in enumerate(others)
    ]
    for c in scatter:
        c.start()
    for c in scatter:
        c.wait()
    own = rows(core * half + chip * piece, piece)
    work[own, :] += jnp.sum(got_rest[...], axis=0)
    full[own, :] = work[own, :]
    gather = [
        remote(work.at[own], full.at[own], sems.at[0, chips + o], sems.at[1, chips + o], 2 * c + core) for o, c in enumerate(others)
    ]
    for c in gather:
        c.start()
    for c in gather:
        c.wait()
    last = remote(full.at[mine], full.at[mine], sems.at[0, 2 * chips - 1], sems.at[1, 2 * chips - 1], pair)
    last.start()
    last.wait()
    one_out[:, :LANES] = full[0:top, :]
    one_out[:, LANES:] = full[top : 2 * top, :]
    two_out[:, :LANES] = full[2 * top : 2 * top + classes, :]
    two_out[:, LANES:] = full[2 * top + lines : 2 * top + lines + classes, :]
    mean[...] = jnp.sum(full[tail : tail + 8, :], keepdims=True) / count[0:1, 0:1]


def prep_kernel(n, chunk, rows, src, dst, w, mask, src_out, dst_out, w_out, counts, count, total, mine, theirs, send_sem, recv_sem):
    me, met = greet(n)
    mine[...] = jnp.sum(mask[...].astype(F32).reshape(-1, 8, LANES), axis=0)
    lines = src.shape[0]
    slots = src_out.shape[0]
    live = w[...] != 0.0
    halo = src[...] >= rows
    at = lambda shape, axis: lax.broadcasted_iota(jnp.int32, shape, axis)
    before = (at((LANES, LANES), 0) < at((LANES, LANES), 1)).astype(BF16)
    above = (at((lines, lines), 1) < at((lines, lines), 0)).astype(BF16)
    ones = jnp.ones((LANES, LANES), BF16)

    def rank(mask):
        m = mask.astype(F32).astype(BF16)
        return dot(m, before) + dot(above, dot(m, ones).astype(BF16))

    is_local, is_halo = jnp.logical_and(live, jnp.logical_not(halo)), jnp.logical_and(live, halo)
    n_local = jnp.sum(is_local.astype(F32)).astype(jnp.int32)
    n_halo = jnp.sum(is_halo.astype(F32)).astype(jnp.int32)
    local_chunks = (n_local + chunk - 1) // chunk
    counts[0] = local_chunks
    counts[1] = local_chunks + (n_halo + chunk - 1) // chunk
    pos = jnp.where(
        is_local, rank(is_local).astype(jnp.int32), jnp.where(is_halo, rank(is_halo).astype(jnp.int32) + local_chunks * chunk, -1)
    )
    line, lane = pos >> 7, pos & (LANES - 1)
    s = jnp.where(halo, src[...] - rows, src[...])
    d = dst[...]
    half_w = w[...] * 0.5
    w_a = half_w.astype(BF16).astype(F32)
    w_b = (half_w - w_a).astype(BF16).astype(F32)
    w_c = half_w - w_a - w_b
    high = ((s >> 8) * 8 + (d >> 8)).astype(F32)
    planes = [(s & 255).astype(F32), (d & 255).astype(F32), high, w_a, w_b, w_c]
    acc = jnp.zeros((len(planes) * slots, LANES), F32)
    for r in range(0, lines, 2):
        lhs, rhs = [], []
        for q in (r, r + 1):
            pick = at((slots, LANES), 0) == line[q : q + 1, :]
            lhs.append(jnp.concatenate([jnp.where(pick, p[q : q + 1, :], 0.0) for p in planes], axis=0))
            rhs.append((at((LANES, LANES), 0) == lane[q : q + 1, :]).astype(F32))
        acc += dot(jnp.concatenate(lhs, axis=1).astype(BF16), jnp.concatenate(rhs, axis=1).astype(BF16), COLS_A)
    met()
    copies = [remote(mine, theirs.at[o - 1], send_sem.at[o - 1], recv_sem.at[o - 1], lax.rem(me + o, n)) for o in range(1, n)]
    for c in copies:
        c.start()
    total[...] = acc
    plane = lambda i: total[i * slots : (i + 1) * slots, :]
    high = plane(2).astype(jnp.int32)
    src_out[...] = ((high >> 3) * 256 + plane(0).astype(jnp.int32)) * 2
    dst_out[...] = ((high & 7) * 256 + plane(1).astype(jnp.int32)) * 2
    total[0:slots, :] = (plane(3) + plane(4) + plane(5)) * 2.0

    @pl.loop(0, slots // 8)
    def _(r):
        for q in range(8):
            w_out[pl.ds(pl.multiple_of((r * 8 + q) * LANES, LANES), LANES), :] = spread(total[pl.ds(r * 8 + q, 1), :])

    for c in copies:
        c.wait()
    every = jnp.sum(mine[...] + jnp.sum(theirs[...], axis=0), keepdims=True)
    count[...] = jnp.maximum(jnp.broadcast_to(every, count.shape), 1.0)


def local_kernel(chunk, backward, counts, src, dst, w, table, out, src_s, dst_s, sems, *accs):
    edges = Edges(0, counts[0], src, dst, w, src_s, dst_s, sems)
    edges.fetch()
    for a in accs:
        fill_zero(a)
    edges.walk(chunk, *((dst_s, src_s) if backward else (src_s, dst_s)), table, accs, True)

    @pl.loop(0, out.shape[0], step=STEP)
    def _(i):
        out[pl.ds(i, STEP), :] = functools.reduce(jnp.add, [a[pl.ds(i, STEP), :] for a in accs])


def forward_halo(chunk, edges, from_prev, from_next, part, htab, accs, unpack):
    edges.fetch()
    unpack(from_prev, htab, 0)
    unpack(from_next, htab, htab.shape[0] // 4)
    copy_in(accs[0], part)
    for a in accs[1:]:
        fill_zero(a)
    edges.walk(chunk, edges.src, edges.dst, htab, accs, True)


def backward_halo(chunk, edges, grad, back_prev, back_next, accs, wait):
    for a in accs:
        fill_zero(a)
    edges.walk(chunk, edges.dst, edges.src, grad, accs, wait)
    split = accs[0].shape[0] // 2
    if back_prev.shape[0] == split:

        @pl.loop(0, split, step=STEP)
        def _(i):
            back_prev[pl.ds(i, STEP), :] = functools.reduce(jnp.add, [a[pl.ds(i, STEP), :] for a in accs])
            back_next[pl.ds(i, STEP), :] = functools.reduce(jnp.add, [a[pl.ds(split + i, STEP), :] for a in accs])
        return
    halo = split // 2

    @pl.loop(0, halo // 2, step=256)
    def _(i):
        i = pl.multiple_of(i, 256)
        for start, out in ((0, back_prev), (halo, back_next)):
            a_even, a_odd = halves(accs, start + i, 256)
            b_even, b_odd = halves(accs, start + halo // 2 + i, 256)
            out[pl.ds(i, 256), :] = a_even
            out[pl.ds(halo // 2 + i, 256), :] = b_even
            out[pl.ds(halo + i, 256), :] = jnp.where(low_lanes(256), a_odd, swap_lanes(b_odd))


def padded(w, buf):
    low = w.shape[0] // 8 * 8
    buf[low:, :] = jnp.zeros((buf.shape[0] - low, buf.shape[1]), F32)
    buf[0 : w.shape[0], :] = w[...]
    return buf[...].astype(BF16)


def hidden_kernel(chunk, counts, src, dst, w, send, from_prev, from_next, part, w2, hid, tab, to_prev, to_next, back, htab, tab_b, w2_pad, src_s, dst_s, sems, *accs):
    edges = Edges(counts[0], counts[1], src, dst, w, src_s, dst_s, sems)
    w2_b = padded(w2, w2_pad)
    per = send.shape[1] // LANES
    for i in range(2 * per):
        back[i : i + 1, :] = send[i // per : i // per + 1, (i % per) * LANES : (i % per + 1) * LANES] * 2
    forward_halo(chunk, edges, from_prev, from_next, part, htab, accs, unpack_plain)

    @pl.loop(0, hid.shape[0], step=256)
    def _(i):
        even, odd = halves(accs, i, 256)
        h = jnp.concatenate([jnp.maximum(even, 0.0), jnp.maximum(odd, 0.0)], axis=1).astype(BF16)
        hid[pl.ds(i, 256), :] = h
        t = dot(h, w2_b, COLS_A).astype(BF16)
        tab_b[pl.ds(i, 256), :] = t
        t = t.astype(F32)
        put_halves(tab, i, 256, t[:, :LANES], t[:, LANES:])

    gather_packed(send, 0, tab_b, to_prev)
    gather_packed(send, 1, tab_b, to_next)


def loss_kernel(chunk, classes, counts, src, dst, w, count, from_prev, from_next, part, labels, mask, loss, grad, back_prev, back_next, htab, src_s, dst_s, sems, *accs):
    edges = Edges(counts[0], counts[1], src, dst, w, src_s, dst_s, sems)
    forward_halo(chunk, edges, from_prev, from_next, part, htab, accs, unpack_rows)
    lane = lax.broadcasted_iota(jnp.int32, (LANES, LANES), 1)
    live = lane < classes - LANES
    scale = 1.0 / count[0:1, :]
    loss[...] = jnp.zeros_like(loss)

    @pl.loop(0, labels.shape[0] // 2)
    def _(pair):
        for b in (pair * 2, pair * 2 + 1):
            even, odd = halves(accs, b * LANES, LANES)
            label = spread(labels[pl.ds(b, 1), :])
            keep = spread(mask[pl.ds(b, 1), :]).astype(F32)
            odd = jnp.where(live, odd, -jnp.inf)
            top = jnp.max(jnp.maximum(even, odd), axis=1, keepdims=True)
            total = jnp.sum(jnp.exp(even - top) + jnp.exp(odd - top), axis=1, keepdims=True)
            norm = top + jnp.log(total)
            hit_even, hit_odd = lane == label, lane + LANES == label
            picked = jnp.where(hit_even, even, 0.0) + jnp.where(hit_odd, odd, 0.0)
            per_row = jnp.where(lane == 0, norm, 0.0) - picked
            loss[...] += jnp.sum((keep * per_row).reshape(LANES // 8, 8, LANES), axis=0)
            d_even = (jnp.exp(even - norm) - hit_even.astype(F32)) * (keep * scale)
            d_odd = (jnp.exp(odd - norm) - hit_odd.astype(F32)) * (keep * scale)
            put_halves(grad, b * LANES, LANES, d_even, d_odd)

    backward_halo(chunk, edges, grad, back_prev, back_next, accs, False)


def take_returns(send, part, got_prev, got_next, accs):
    copy_in(accs[0], part)
    for a in accs[1:]:
        fill_zero(a)
    return_rows(send, send.shape[0] // 2, got_prev, accs)
    return_rows(send, 0, got_next, accs)


def middle_kernel(chunk, counts, src, dst, w, send, got_prev, got_next, part, hid, w2, grad_two, grad, back_prev, back_next, returned, w2_pad, src_s, dst_s, sems, *accs):
    edges = Edges(counts[0], counts[1], src, dst, w, src_s, dst_s, sems)
    edges.fetch()
    w2_b = padded(w2, w2_pad)
    split = returned.shape[0] // 2
    unpack_rows(got_prev, returned, 0)
    unpack_rows(got_next, returned, split // 2)
    take_returns(send, part, returned.at[pl.ds(0, split)], returned.at[pl.ds(split, split)], accs)
    grad_two[...] = jnp.zeros_like(grad_two)

    @pl.loop(0, hid.shape[0], step=256)
    def _(i):
        even, odd = halves(accs, i, 256)
        d_tab = jnp.concatenate([even, odd], axis=1).astype(BF16)
        h = hid[pl.ds(i, 256), :]
        grad_two[...] += dot(d_tab, h, ROWS_A)
        d_hid = dot(d_tab, w2_b)
        d_pre = jnp.where(h > 0, d_hid, 0.0)
        put_halves(grad, i, 256, d_pre[:, :LANES], d_pre[:, LANES:])

    backward_halo(chunk, edges, grad, back_prev, back_next, accs, True)


def last_kernel(send, got_prev, got_next, part, x, grad_one, *accs):
    take_returns(send, part, got_prev, got_next, accs)
    grad_one[...] = jnp.zeros_like(grad_one)

    @pl.loop(0, x.shape[0], step=256)
    def _(i):
        even, odd = halves(accs, i, 256)
        d_tab = jnp.concatenate([even, odd], axis=1).astype(BF16)
        grad_one[...] += dot(x[pl.ds(i, 256), :], d_tab, ROWS_A)


def call(body, name, outs, ins, scratch, flops=10**9, out_specs=None, collective=None, vmem=14):
    extra = {} if collective is None else dict(collective_id=collective, has_side_effects=True)
    return pl.pallas_call(
        body, name=name, out_shape=outs, in_specs=ins, out_specs=out_specs or jax.tree.map(lambda _: VMEM, outs),
        scratch_shapes=[pltpu.VMEM(s, F32) if isinstance(s, tuple) else s for s in scratch],
        compiler_params=pltpu.CompilerParams(vmem_limit_bytes=vmem * 2**20, **extra),
        cost_estimate=pl.CostEstimate(flops=flops, bytes_accessed=8 * 2**20, transcendentals=0),
    )


def solution(mesh):
    num_dev = mesh.shape[AXIS]
    to_next = [(d, (d + 1) % num_dev) for d in range(num_dev)]
    to_prev = [(d, (d - 1) % num_dev) for d in range(num_dev)]

    def step(x, w_one, w_two, send, edge_src, edge_dst, edge_w, labels, mask):
        rows, halo, edges, classes = x.shape[0], send.shape[1], edge_src.shape[0], w_two.shape[1]
        tab = (2 * rows, LANES)
        half = (2 * halo, LANES)
        sds = jax.ShapeDtypeStruct
        tab_f, half_f, half_b = sds(tab, F32), sds(half, F32), sds((halo, 2 * LANES), BF16)
        pack_f, pack_b = sds((3 * halo // 2, LANES), F32), sds((3 * halo // 2, LANES), BF16)
        tab_b = pltpu.VMEM((rows, 2 * LANES), BF16)
        one = sds((8, LANES), F32)
        dma = pltpu.SemaphoreType.DMA
        chunk_l, chunk_h = 64, 32
        lines = edges // LANES
        slots = lines + 8
        w2 = w_two.T
        w2_pad = (2 * LANES, 2 * LANES)
        mask = mask.reshape(-1, LANES)

        lined = lambda a: a.reshape(lines, LANES)
        ints = sds((slots, LANES), jnp.int32)
        src, dst, w, counts, count = call(
            functools.partial(prep_kernel, num_dev, PREP_CHUNK, rows), "prep", [ints, ints, sds((slots * LANES, LANES), F32), sds((2,), jnp.int32), one], [VMEM] * 4,
            [(6 * slots, LANES), (8, LANES), (num_dev - 1, 8, LANES), dma((num_dev - 1,)), dma((num_dev - 1,))],
            out_specs=[VMEM] * 3 + [SMEM, VMEM], vmem=8, collective=0,
        )(lined(edge_src), lined(edge_dst), lined(edge_w), mask)
        src, dst = src.reshape(-1), dst.reshape(-1)

        tab_one, to_p, to_n = call(first_kernel, "first", [tab_f, half_b, half_b], [VMEM] * 3 + [SMEM], [tab_b], vmem=8)(x, w_one, send, counts)
        from_prev = lax.ppermute(to_n, AXIS, to_next)
        from_next = lax.ppermute(to_p, AXIS, to_prev)

        walk = [SMEM, ANY, ANY, VMEM]
        index = pltpu.SMEM((slots * LANES,), jnp.int32)
        walk_s = [index, index, dma((2, slots * LANES // SEGMENT))]
        local, local_back = (
            call(functools.partial(local_kernel, chunk_l, back), "local_edges", tab_f, walk + [VMEM], walk_s + [tab] * 4, 10**10)
            for back in (False, True)
        )
        part = local(counts, src, dst, w, tab_one)
        hid, tab_two, to_p, to_n, back = call(
            functools.partial(hidden_kernel, chunk_h), "hidden", [sds((rows, 2 * LANES), BF16), tab_f, pack_b, pack_b, sds((2 * halo // LANES, LANES), jnp.int32)],
            walk + [VMEM] * 5, [tab, tab_b, w2_pad] + walk_s + [tab] * 4,
        )(counts, src, dst, w, send, from_prev, from_next, part, w2)
        from_prev = lax.ppermute(to_n, AXIS, to_next)
        from_next = lax.ppermute(to_p, AXIS, to_prev)
        back = back.reshape(-1)
        part = local(counts, src, dst, w, tab_two)
        loss, grad, to_p, to_n = call(
            functools.partial(loss_kernel, chunk_h, classes), "loss", [sds((8, LANES), F32), tab_f, pack_f, pack_f],
            walk + [VMEM] * 6, [tab] + walk_s + [tab] * 4,
        )(counts, src, dst, w, count, from_prev, from_next, part, labels.reshape(-1, LANES), mask)
        got_prev = lax.ppermute(to_p, AXIS, to_prev)
        got_next = lax.ppermute(to_n, AXIS, to_next)
        part = local_back(counts, src, dst, w, grad)
        grad_two, grad, to_p, to_n = call(
            functools.partial(middle_kernel, chunk_h), "middle", [sds((2 * LANES, 2 * LANES), F32), tab_f, half_f, half_f],
            walk + [SMEM] + [VMEM] * 5, [tab, w2_pad] + walk_s + [tab] * 4,
        )(counts, src, dst, w, back, got_prev, got_next, part, hid, w2)
        got_prev = lax.ppermute(to_p, AXIS, to_prev)
        got_next = lax.ppermute(to_n, AXIS, to_next)
        part = local_back(counts, src, dst, w, grad)

        grad_one = call(last_kernel, "last", sds((x.shape[1], 2 * LANES), F32), [SMEM] + [VMEM] * 4, [tab] * 4)(back, got_prev, got_next, part, x)
        lines = 2 * x.shape[1] + 2 * (-(-classes // 8) * 8) + 8
        lines = -(-lines // (8 * num_dev)) * 8 * num_dev
        grad_one, grad_two, mean = call(
            functools.partial(reduce_kernel, num_dev), "reduce", [sds(grad_one.shape, F32), sds((classes, 2 * LANES), F32), sds((1, 1), F32)],
            [VMEM] * 4, [(lines, LANES), (lines, LANES), (lines // 2, LANES), (num_dev // 2 - 1, lines // num_dev, LANES), dma((2, num_dev))],
            collective=1, vmem=8,
        )(grad_one, grad_two, loss, count)
        return mean.reshape(()), grad_one, grad_two.T

    row = P(AXIS)
    return jax.shard_map(
        step, mesh=mesh, in_specs=(row, P(), P(), row, row, row, row, row, row), out_specs=(P(), P(), P()), check_vma=False
    )
```

```python
import functools

import jax
import jax.numpy as jnp
from jax import lax
from jax.experimental import pallas as pl
from jax.experimental.pallas import tpu as pltpu
from jax.sharding import PartitionSpec as P

AXIS = "graph"
LANES = 128
ROWS_A = (((0,), (0,)), ((), ()))
COLS_A = (((1,), (1,)), ((), ()))
F32, BF16 = jnp.float32, jnp.bfloat16
VMEM = pl.BlockSpec(memory_space=pltpu.VMEM)
SMEM = pl.BlockSpec(memory_space=pltpu.SMEM)
ANY = pl.BlockSpec(memory_space=pl.ANY)
STEP = 512
PREP_CHUNK = 64
SEGMENT = 1024
MESH = pl.DeviceIdType.MESH


def dot(a, b, dims=(((1,), (0,)), ((), ()))):
    return lax.dot_general(a, b, dims, preferred_element_type=F32)


def fill_zero(ref):
    zero = jnp.zeros((STEP, LANES), F32)

    @pl.loop(0, ref.shape[0], step=STEP)
    def _(i):
        ref[pl.ds(i, STEP), :] = zero


def copy_in(dst, src):
    @pl.loop(0, dst.shape[0], step=STEP)
    def _(i):
        dst[pl.ds(i, STEP), :] = src[pl.ds(i, STEP), :].astype(F32)


class Edges:
    def __init__(self, first, last, src, dst, w, src_s, dst_s, sems):
        self.first, self.last, self.w = first, last, w
        self.src, self.dst = src_s, dst_s
        self.pairs = ((src, src_s), (dst, dst_s))
        self.sems = sems

    def copies(self, seg):
        part = pl.ds(pl.multiple_of(seg * SEGMENT, SEGMENT), SEGMENT)
        return [pltpu.make_async_copy(a.at[part], b.at[part], self.sems.at[i, seg]) for i, (a, b) in enumerate(self.pairs)]

    def fetch(self):
        per = SEGMENT // PREP_CHUNK
        for seg in range(self.src.shape[0] // SEGMENT):

            @pl.when(jnp.logical_and(seg * per < self.last, (seg + 1) * per > self.first))
            def _():
                for c in self.copies(seg):
                    c.start()

    def walk(self, chunk, from_idx, to_idx, table, accs, wait):
        group, per, ratio = len(accs), SEGMENT // chunk, PREP_CHUNK // chunk
        first, last = self.first * ratio, self.last * ratio

        def body(c, _):
            base = c * chunk
            w_chunk = self.w.at[pl.ds(pl.multiple_of(base, chunk), chunk)]
            for g in range(0, chunk, group):
                pend = []
                for u in range(group):
                    k = base + g + u
                    s = pl.multiple_of(from_idx[k], 2)
                    d = pl.multiple_of(to_idx[k], 2)
                    pend.append((d, accs[u][pl.ds(d, 2), :] + table[pl.ds(s, 2), :] * w_chunk[g + u : g + u + 1, :]))
                for u in range(group):
                    accs[u][pl.ds(pend[u][0], 2), :] = pend[u][1]
            return 0

        if not wait:
            lax.fori_loop(first, last, body, 0)
            return

        def segment(seg, _):
            for c in self.copies(seg):
                c.wait()
            lax.fori_loop(jnp.maximum(first, seg * per), jnp.minimum(last, (seg + 1) * per), body, 0)
            return 0

        lax.fori_loop(first // per, (last + per - 1) // per, segment, 0)


def one_hot_rows(idx, which, start, table):
    lane = lax.broadcasted_iota(jnp.int32, (LANES, LANES), 1)
    hot = []
    for q in range(2):
        want = spread(idx[which : which + 1, pl.ds(pl.multiple_of(start + q * LANES, LANES), LANES)])
        hot.append(
            jnp.concatenate([jnp.where(want == lane + LANES * j, 1.0, 0.0).astype(BF16) for j in range(table.shape[0] // LANES)], axis=1)
        )
    return dot(jnp.concatenate(hot, axis=0), table[...])


def low_lanes(rows):
    return lax.broadcasted_iota(jnp.int32, (rows, LANES), 1) < LANES // 2


def swap_lanes(v):
    return pltpu.roll(v, LANES // 2, 1)


def fetch_index(send, idx, sems):
    parts = [pl.ds(i, LANES) for i in range(0, send.shape[1], LANES)]
    return [pltpu.make_async_copy(send.at[1, p], idx.at[p], sems.at[i]) for i, p in enumerate(parts)]


def gather_block(send, idx, i, table_b, table, buf):
    got = one_hot_rows(send, 0, i, table_b)
    out = buf.at[pl.ds(pl.multiple_of(2 * i, 512), 512)]
    for u in range(256):
        s = pl.multiple_of(idx[i + u] * 2, 2)
        out[2 * u : 2 * u + 2, :] = table[pl.ds(s, 2), :]
    return got


def gather_rows(send, idx, table_b, table, buf, to_prev, to_next):
    @pl.loop(0, to_prev.shape[0], step=256)
    def _(i):
        i = pl.multiple_of(i, 256)
        to_prev[pl.ds(i, 256), :] = gather_block(send, idx, i, table_b, table, buf).astype(BF16)

    @pl.loop(0, to_next.shape[0], step=256)
    def _(i):
        to_next[pl.ds(pl.multiple_of(i, 256), 256), :] = jnp.concatenate(halves([buf], i, 256), axis=1).astype(BF16)


def pack_rows(out, i, a_even, a_odd, b_even, b_odd):
    halo = out.shape[0] * 2 // 3
    out[pl.ds(i, 256), :] = a_even.astype(out.dtype)
    out[pl.ds(halo // 2 + i, 256), :] = b_even.astype(out.dtype)
    out[pl.ds(halo + i, 256), :] = jnp.where(low_lanes(256), a_odd, swap_lanes(b_odd)).astype(out.dtype)


def gather_packed(send, idx, table_b, table, buf, to_prev, to_next):
    half = to_prev.shape[0] // 3

    @pl.loop(0, half, step=256)
    def _(i):
        i = pl.multiple_of(i, 256)
        a = gather_block(send, idx, i, table_b, table, buf)
        b = gather_block(send, idx, half + i, table_b, table, buf)
        pack_rows(to_prev, i, a[:, :LANES], a[:, LANES:], b[:, :LANES], b[:, LANES:])

    @pl.loop(0, half, step=256)
    def _(i):
        i = pl.multiple_of(i, 256)
        pack_rows(to_next, i, *halves([buf], i, 256), *halves([buf], half + i, 256))


def unpack_rows(got, table, start):
    halo = got.shape[0] * 2 // 3

    @pl.loop(0, halo // 2, step=256)
    def _(i):
        i = pl.multiple_of(i, 256)
        a, b, both = (got[pl.ds(k + i, 256), :].astype(F32) for k in (0, halo // 2, halo))
        put_halves(table, start + i, 256, a, jnp.where(low_lanes(256), both, 0.0))
        put_halves(table, start + halo // 2 + i, 256, b, jnp.where(low_lanes(256), swap_lanes(both), 0.0))


def unpack_plain(got, table, start):
    @pl.loop(0, got.shape[0], step=256)
    def _(i):
        t = got[pl.ds(i, 256), :].astype(F32)
        put_halves(table, start + i, 256, t[:, :LANES], t[:, LANES:])


def spread(row):
    return jnp.transpose(jnp.broadcast_to(row, (LANES, LANES)))


def return_rows(idx, start, vals, accs, chunk=32):
    group = len(accs)

    @pl.loop(0, vals.shape[0] // (2 * chunk))
    def _(c):
        block = vals.at[pl.ds(pl.multiple_of(c * 2 * chunk, 2 * chunk), 2 * chunk)]
        for g in range(0, chunk, group):
            pend = []
            for u in range(group):
                d = pl.multiple_of(idx[start + c * chunk + g + u], 2)
                pend.append((d, accs[u][pl.ds(d, 2), :] + block[2 * (g + u) : 2 * (g + u) + 2, :]))
            for u in range(group):
                accs[u][pl.ds(pend[u][0], 2), :] = pend[u][1]


def halves(accs, i, n):
    even = functools.reduce(jnp.add, [a[pl.ds(2 * i, n, stride=2), :] for a in accs])
    odd = functools.reduce(jnp.add, [a[pl.ds(2 * i + 1, n, stride=2), :] for a in accs])
    return even, odd


def put_halves(table, i, n, even, odd):
    table[pl.ds(2 * i, n, stride=2), :] = even
    table[pl.ds(2 * i + 1, n, stride=2), :] = odd


def greet(n):
    me = lax.axis_index(AXIS)
    barrier = pltpu.get_barrier_semaphore()
    for o in range(1, n):
        pl.semaphore_signal(barrier, inc=1, device_id=(lax.rem(me + o, n),), device_id_type=MESH)
    return me, lambda: pl.semaphore_wait(barrier, n - 1)


def remote(src, dst, send_sem, recv_sem, peer):
    return pltpu.make_async_remote_copy(
        src_ref=src, dst_ref=dst, send_sem=send_sem, recv_sem=recv_sem, device_id=(peer,), device_id_type=MESH
    )


def first_kernel(x, w1, send, after, tab, to_prev, to_next, tab_b, buf, idx, sems):
    fetch = fetch_index(send, idx, sems)
    for c in fetch:
        c.start()
    rows = x.shape[0]
    w = w1[...].astype(BF16)

    @pl.loop(0, rows, step=256)
    def _(i):
        t = dot(x[pl.ds(i, 256), :], w).astype(BF16)
        tab_b[pl.ds(i, 256), :] = t
        t = t.astype(F32)
        put_halves(tab, i, 256, t[:, :LANES], t[:, LANES:])

    for c in fetch:
        c.wait()
    gather_rows(send, idx, tab_b, tab, buf, to_prev, to_next)


def count_kernel(n, mask, after, count, mine, theirs, send_sem, recv_sem):
    me, met = greet(n)
    mine[...] = jnp.sum(mask[...].astype(F32).reshape(-1, 8, LANES), axis=0)
    met()
    copies = [remote(mine, theirs.at[o - 1], send_sem.at[o - 1], recv_sem.at[o - 1], lax.rem(me + o, n)) for o in range(1, n)]
    for c in copies:
        c.start()
    for c in copies:
        c.wait()
    every = jnp.sum(mine[...] + jnp.sum(theirs[...], axis=0), keepdims=True)
    count[...] = jnp.maximum(jnp.broadcast_to(every, count.shape), 1.0)


def reduce_kernel(n, one, two, loss, count, one_out, two_out, mean, work, full, got_pair, got_rest, sems):
    me = lax.axis_index(AXIS)
    chips, core = n // 2, lax.rem(me, 2)
    chip = lax.div(me, 2)
    pair = me + 1 - 2 * core
    others = [lax.rem(chip + o, chips) for o in range(1, chips)]
    barrier = pltpu.get_barrier_semaphore()
    for p in [pair] + [2 * c + core for c in others]:
        pl.semaphore_signal(barrier, inc=1, device_id=(p,), device_id_type=MESH)
    classes = two_out.shape[0]
    lines = -(-classes // 8) * 8
    top, wide = one.shape
    work[0:top, :] = one[:, :LANES]
    work[top : 2 * top, :] = one[:, LANES:]
    work[2 * top : 2 * top + lines, :] = two[:lines, :LANES]
    work[2 * top + lines : 2 * top + 2 * lines, :] = two[:lines, LANES:]
    tail = 2 * top + 2 * lines
    work[tail : tail + 8, :] = loss[...]
    work[tail + 8 :, :] = jnp.zeros((work.shape[0] - tail - 8, LANES), F32)
    pl.semaphore_wait(barrier, chips)

    half = work.shape[0] // 2
    piece = half // chips
    rows = lambda start, size: pl.ds(pl.multiple_of(start, 8), size)
    mine, other = rows(core * half, half), rows((1 - core) * half, half)
    swap = remote(work.at[other], got_pair, sems.at[0, 0], sems.at[1, 0], pair)
    swap.start()
    swap.wait()
    work[mine, :] += got_pair[...]
    scatter = [
        remote(work.at[rows(core * half + c * piece, piece)], got_rest.at[o], sems.at[0, 1 + o], sems.at[1, 1 + o], 2 * c + core)
        for o, c in enumerate(others)
    ]
    for c in scatter:
        c.start()
    for c in scatter:
        c.wait()
    own = rows(core * half + chip * piece, piece)
    work[own, :] += jnp.sum(got_rest[...], axis=0)
    full[own, :] = work[own, :]
    gather = [
        remote(work.at[own], full.at[own], sems.at[0, chips + o], sems.at[1, chips + o], 2 * c + core) for o, c in enumerate(others)
    ]
    for c in gather:
        c.start()
    for c in gather:
        c.wait()
    last = remote(full.at[mine], full.at[mine], sems.at[0, 2 * chips - 1], sems.at[1, 2 * chips - 1], pair)
    last.start()
    last.wait()
    one_out[:, :LANES] = full[0:top, :]
    one_out[:, LANES:] = full[top : 2 * top, :]
    two_out[:, :LANES] = full[2 * top : 2 * top + classes, :]
    two_out[:, LANES:] = full[2 * top + lines : 2 * top + lines + classes, :]
    mean[...] = jnp.sum(full[tail : tail + 8, :], keepdims=True) / count[0:1, 0:1]


def prep_kernel(chunk, rows, src, dst, w, src_out, dst_out, w_out, counts, total):
    lines = src.shape[0]
    slots = src_out.shape[0]
    live = w[...] != 0.0
    halo = src[...] >= rows
    at = lambda shape, axis: lax.broadcasted_iota(jnp.int32, shape, axis)
    before = (at((LANES, LANES), 0) < at((LANES, LANES), 1)).astype(BF16)
    above = (at((lines, lines), 1) < at((lines, lines), 0)).astype(BF16)
    ones = jnp.ones((LANES, LANES), BF16)

    def rank(mask):
        m = mask.astype(F32).astype(BF16)
        return dot(m, before) + dot(above, dot(m, ones).astype(BF16))

    is_local, is_halo = jnp.logical_and(live, jnp.logical_not(halo)), jnp.logical_and(live, halo)
    n_local = jnp.sum(is_local.astype(F32)).astype(jnp.int32)
    n_halo = jnp.sum(is_halo.astype(F32)).astype(jnp.int32)
    local_chunks = (n_local + chunk - 1) // chunk
    counts[0] = local_chunks
    counts[1] = local_chunks + (n_halo + chunk - 1) // chunk
    pos = jnp.where(
        is_local, rank(is_local).astype(jnp.int32), jnp.where(is_halo, rank(is_halo).astype(jnp.int32) + local_chunks * chunk, -1)
    )
    line, lane = pos >> 7, pos & (LANES - 1)
    s = jnp.where(halo, src[...] - rows, src[...])
    d = dst[...]
    half_w = w[...] * 0.5
    w_a = half_w.astype(BF16).astype(F32)
    w_b = (half_w - w_a).astype(BF16).astype(F32)
    w_c = half_w - w_a - w_b
    high = ((s >> 8) * 8 + (d >> 8)).astype(F32)
    planes = [(s & 255).astype(F32), (d & 255).astype(F32), high, w_a, w_b, w_c]
    acc = jnp.zeros((len(planes) * slots, LANES), F32)
    for r in range(0, lines, 2):
        lhs, rhs = [], []
        for q in (r, r + 1):
            pick = at((slots, LANES), 0) == line[q : q + 1, :]
            lhs.append(jnp.concatenate([jnp.where(pick, p[q : q + 1, :], 0.0) for p in planes], axis=0))
            rhs.append((at((LANES, LANES), 0) == lane[q : q + 1, :]).astype(F32))
        acc += dot(jnp.concatenate(lhs, axis=1).astype(BF16), jnp.concatenate(rhs, axis=1).astype(BF16), COLS_A)
    total[...] = acc
    plane = lambda i: total[i * slots : (i + 1) * slots, :]
    high = plane(2).astype(jnp.int32)
    src_out[...] = ((high >> 3) * 256 + plane(0).astype(jnp.int32)) * 2
    dst_out[...] = ((high & 7) * 256 + plane(1).astype(jnp.int32)) * 2
    total[0:slots, :] = (plane(3) + plane(4) + plane(5)) * 2.0

    @pl.loop(0, slots // 8)
    def _(r):
        for q in range(8):
            w_out[pl.ds(pl.multiple_of((r * 8 + q) * LANES, LANES), LANES), :] = spread(total[pl.ds(r * 8 + q, 1), :])


def local_kernel(chunk, backward, counts, src, dst, w, table, out, src_s, dst_s, sems, *accs):
    edges = Edges(0, counts[0], src, dst, w, src_s, dst_s, sems)
    edges.fetch()
    for a in accs:
        fill_zero(a)
    edges.walk(chunk, *((dst_s, src_s) if backward else (src_s, dst_s)), table, accs, True)

    @pl.loop(0, out.shape[0], step=STEP)
    def _(i):
        out[pl.ds(i, STEP), :] = functools.reduce(jnp.add, [a[pl.ds(i, STEP), :] for a in accs])


def forward_halo(chunk, edges, from_prev, from_next, part, htab, accs, unpack):
    edges.fetch()
    unpack(from_prev, htab, 0)
    unpack(from_next, htab, htab.shape[0] // 4)
    copy_in(accs[0], part)
    for a in accs[1:]:
        fill_zero(a)
    edges.walk(chunk, edges.src, edges.dst, htab, accs, True)


def backward_halo(chunk, edges, grad, back_prev, back_next, accs, wait):
    for a in accs:
        fill_zero(a)
    edges.walk(chunk, edges.dst, edges.src, grad, accs, wait)
    split = accs[0].shape[0] // 2
    if back_prev.shape[0] == split:

        @pl.loop(0, split, step=STEP)
        def _(i):
            back_prev[pl.ds(i, STEP), :] = functools.reduce(jnp.add, [a[pl.ds(i, STEP), :] for a in accs])
            back_next[pl.ds(i, STEP), :] = functools.reduce(jnp.add, [a[pl.ds(split + i, STEP), :] for a in accs])
        return
    halo = split // 2

    @pl.loop(0, halo // 2, step=256)
    def _(i):
        i = pl.multiple_of(i, 256)
        for start, out in ((0, back_prev), (halo, back_next)):
            pack_rows(out, i, *halves(accs, start + i, 256), *halves(accs, start + halo // 2 + i, 256))


def padded(w, buf):
    low = w.shape[0] // 8 * 8
    buf[low:, :] = jnp.zeros((buf.shape[0] - low, buf.shape[1]), F32)
    buf[0 : w.shape[0], :] = w[...]
    return buf[...].astype(BF16)


def hidden_kernel(chunk, counts, src, dst, w, send, from_prev, from_next, part, w2, hid, tab, to_prev, to_next, back, htab, tab_b, w2_pad, buf, idx, idx_sems, src_s, dst_s, sems, *accs):
    fetch = fetch_index(send, idx, idx_sems)
    for c in fetch:
        c.start()
    edges = Edges(counts[0], counts[1], src, dst, w, src_s, dst_s, sems)
    w2_b = padded(w2, w2_pad)
    per = send.shape[1] // LANES
    for i in range(2 * per):
        back[i : i + 1, :] = send[i // per : i // per + 1, (i % per) * LANES : (i % per + 1) * LANES] * 2
    forward_halo(chunk, edges, from_prev, from_next, part, htab, accs, unpack_plain)

    @pl.loop(0, hid.shape[0], step=256)
    def _(i):
        even, odd = halves(accs, i, 256)
        h = jnp.concatenate([jnp.maximum(even, 0.0), jnp.maximum(odd, 0.0)], axis=1).astype(BF16)
        hid[pl.ds(i, 256), :] = h
        t = dot(h, w2_b, COLS_A).astype(BF16)
        tab_b[pl.ds(i, 256), :] = t
        t = t.astype(F32)
        put_halves(tab, i, 256, t[:, :LANES], t[:, LANES:])

    for c in fetch:
        c.wait()
    gather_packed(send, idx, tab_b, tab, buf, to_prev, to_next)


def loss_kernel(chunk, classes, counts, src, dst, w, count, from_prev, from_next, part, labels, mask, loss, grad, back_prev, back_next, htab, src_s, dst_s, sems, *accs):
    edges = Edges(counts[0], counts[1], src, dst, w, src_s, dst_s, sems)
    forward_halo(chunk, edges, from_prev, from_next, part, htab, accs, unpack_rows)
    lane = lax.broadcasted_iota(jnp.int32, (LANES, LANES), 1)
    live = lane < classes - LANES
    scale = 1.0 / count[0:1, :]
    loss[...] = jnp.zeros_like(loss)

    @pl.loop(0, labels.shape[0] // 2)
    def _(pair):
        for b in (pair * 2, pair * 2 + 1):
            even, odd = halves(accs, b * LANES, LANES)
            label = spread(labels[pl.ds(b, 1), :])
            keep = spread(mask[pl.ds(b, 1), :]).astype(F32)
            odd = jnp.where(live, odd, -jnp.inf)
            top = jnp.max(jnp.maximum(even, odd), axis=1, keepdims=True)
            total = jnp.sum(jnp.exp(even - top) + jnp.exp(odd - top), axis=1, keepdims=True)
            norm = top + jnp.log(total)
            hit_even, hit_odd = lane == label, lane + LANES == label
            picked = jnp.where(hit_even, even, 0.0) + jnp.where(hit_odd, odd, 0.0)
            per_row = jnp.where(lane == 0, norm, 0.0) - picked
            loss[...] += jnp.sum((keep * per_row).reshape(LANES // 8, 8, LANES), axis=0)
            d_even = (jnp.exp(even - norm) - hit_even.astype(F32)) * (keep * scale)
            d_odd = (jnp.exp(odd - norm) - hit_odd.astype(F32)) * (keep * scale)
            put_halves(grad, b * LANES, LANES, d_even, d_odd)

    backward_halo(chunk, edges, grad, back_prev, back_next, accs, False)


def take_returns(send, part, got_prev, got_next, accs):
    copy_in(accs[0], part)
    for a in accs[1:]:
        fill_zero(a)
    return_rows(send, send.shape[0] // 2, got_prev, accs)
    return_rows(send, 0, got_next, accs)


def middle_kernel(chunk, counts, src, dst, w, send, got_prev, got_next, part, hid, w2, grad_two, grad, back_prev, back_next, returned, w2_pad, src_s, dst_s, sems, *accs):
    edges = Edges(counts[0], counts[1], src, dst, w, src_s, dst_s, sems)
    edges.fetch()
    w2_b = padded(w2, w2_pad)
    split = returned.shape[0] // 2
    unpack_rows(got_prev, returned, 0)
    unpack_rows(got_next, returned, split // 2)
    take_returns(send, part, returned.at[pl.ds(0, split)], returned.at[pl.ds(split, split)], accs)
    grad_two[...] = jnp.zeros_like(grad_two)

    @pl.loop(0, hid.shape[0], step=256)
    def _(i):
        even, odd = halves(accs, i, 256)
        d_tab = jnp.concatenate([even, odd], axis=1).astype(BF16)
        h = hid[pl.ds(i, 256), :]
        grad_two[...] += dot(d_tab, h, ROWS_A)
        d_hid = dot(d_tab, w2_b)
        d_pre = jnp.where(h > 0, d_hid, 0.0)
        put_halves(grad, i, 256, d_pre[:, :LANES], d_pre[:, LANES:])

    backward_halo(chunk, edges, grad, back_prev, back_next, accs, True)


def last_kernel(send, got_prev, got_next, part, x, grad_one, *accs):
    take_returns(send, part, got_prev, got_next, accs)
    grad_one[...] = jnp.zeros_like(grad_one)

    @pl.loop(0, x.shape[0], step=256)
    def _(i):
        even, odd = halves(accs, i, 256)
        d_tab = jnp.concatenate([even, odd], axis=1).astype(BF16)
        grad_one[...] += dot(x[pl.ds(i, 256), :], d_tab, ROWS_A)


def call(body, name, outs, ins, scratch, flops=10**9, out_specs=None, collective=None, vmem=14):
    extra = {} if collective is None else dict(collective_id=collective, has_side_effects=True)
    return pl.pallas_call(
        body, name=name, out_shape=outs, in_specs=ins, out_specs=out_specs or jax.tree.map(lambda _: VMEM, outs),
        scratch_shapes=[pltpu.VMEM(s, F32) if isinstance(s, tuple) else s for s in scratch],
        compiler_params=pltpu.CompilerParams(vmem_limit_bytes=vmem * 2**20, **extra),
        cost_estimate=pl.CostEstimate(flops=flops, bytes_accessed=8 * 2**20, transcendentals=0),
    )


def solution(mesh):
    num_dev = mesh.shape[AXIS]
    to_next = [(d, (d + 1) % num_dev) for d in range(num_dev)]
    to_prev = [(d, (d - 1) % num_dev) for d in range(num_dev)]

    def step(x, w_one, w_two, send, edge_src, edge_dst, edge_w, labels, mask):
        rows, halo, edges, classes = x.shape[0], send.shape[1], edge_src.shape[0], w_two.shape[1]
        tab = (2 * rows, LANES)
        half = (2 * halo, LANES)
        sds = jax.ShapeDtypeStruct
        tab_f, half_f, half_b = sds(tab, F32), sds(half, F32), sds((halo, 2 * LANES), BF16)
        pack_f, pack_b = sds((3 * halo // 2, LANES), F32), sds((3 * halo // 2, LANES), BF16)
        tab_b = pltpu.VMEM((rows, 2 * LANES), BF16)
        one = sds((8, LANES), F32)
        dma = pltpu.SemaphoreType.DMA
        chunk_l, chunk_h = 64, 32
        lines = edges // LANES
        slots = lines + 8
        w2 = w_two.T
        w2_pad = (2 * LANES, 2 * LANES)
        mask = mask.reshape(-1, LANES)

        lined = lambda a: a.reshape(lines, LANES)
        ints = sds((slots, LANES), jnp.int32)
        src, dst, w, counts = call(
            functools.partial(prep_kernel, PREP_CHUNK, rows), "prep", [ints, ints, sds((slots * LANES, LANES), F32), sds((2,), jnp.int32)], [VMEM] * 3,
            [(6 * slots, LANES)], out_specs=[VMEM] * 3 + [SMEM], vmem=8,
        )(lined(edge_src), lined(edge_dst), lined(edge_w))
        src, dst = src.reshape(-1), dst.reshape(-1)

        list_s = [pltpu.SMEM((halo,), jnp.int32), dma((halo // LANES,))]
        tab_one, to_p, to_n = call(first_kernel, "first", [tab_f, half_b, half_b], [VMEM] * 3 + [SMEM], [tab_b, half] + list_s, vmem=8)(x, w_one, send, counts)
        from_prev = lax.ppermute(to_n, AXIS, to_next)
        from_next = lax.ppermute(to_p, AXIS, to_prev)

        walk = [SMEM, ANY, ANY, VMEM]
        index = pltpu.SMEM((slots * LANES,), jnp.int32)
        walk_s = [index, index, dma((2, slots * LANES // SEGMENT))]
        local, local_back = (
            call(functools.partial(local_kernel, chunk_l, back), "local_edges", tab_f, walk + [VMEM], walk_s + [tab] * 4, 10**10)
            for back in (False, True)
        )
        part = local(counts, src, dst, w, tab_one)
        count = call(
            functools.partial(count_kernel, num_dev), "count", one, [VMEM, ANY],
            [(8, LANES), (num_dev - 1, 8, LANES), dma((num_dev - 1,)), dma((num_dev - 1,))], vmem=2, collective=0, flops=10**9,
        )(mask, part)
        hid, tab_two, to_p, to_n, back = call(
            functools.partial(hidden_kernel, chunk_h), "hidden", [sds((rows, 2 * LANES), BF16), tab_f, pack_b, pack_b, sds((2 * halo // LANES, LANES), jnp.int32)],
            walk + [VMEM] * 5, [tab, tab_b, w2_pad, half] + list_s + walk_s + [tab] * 4,
        )(counts, src, dst, w, send, from_prev, from_next, part, w2)
        from_prev = lax.ppermute(to_n, AXIS, to_next)
        from_next = lax.ppermute(to_p, AXIS, to_prev)
        back = back.reshape(-1)
        part = local(counts, src, dst, w, tab_two)
        loss, grad, to_p, to_n = call(
            functools.partial(loss_kernel, chunk_h, classes), "loss", [sds((8, LANES), F32), tab_f, pack_f, pack_f],
            walk + [VMEM] * 6, [tab] + walk_s + [tab] * 4,
        )(counts, src, dst, w, count, from_prev, from_next, part, labels.reshape(-1, LANES), mask)
        got_prev = lax.ppermute(to_p, AXIS, to_prev)
        got_next = lax.ppermute(to_n, AXIS, to_next)
        part = local_back(counts, src, dst, w, grad)
        grad_two, grad, to_p, to_n = call(
            functools.partial(middle_kernel, chunk_h), "middle", [sds((2 * LANES, 2 * LANES), F32), tab_f, half_f, half_f],
            walk + [SMEM] + [VMEM] * 5, [tab, w2_pad] + walk_s + [tab] * 4,
        )(counts, src, dst, w, back, got_prev, got_next, part, hid, w2)
        got_prev = lax.ppermute(to_p, AXIS, to_prev)
        got_next = lax.ppermute(to_n, AXIS, to_next)
        part = local_back(counts, src, dst, w, grad)

        grad_one = call(last_kernel, "last", sds((x.shape[1], 2 * LANES), F32), [SMEM] + [VMEM] * 4, [tab] * 4)(back, got_prev, got_next, part, x)
        lines = 2 * x.shape[1] + 2 * (-(-classes // 8) * 8) + 8
        lines = -(-lines // (8 * num_dev)) * 8 * num_dev
        grad_one, grad_two, mean = call(
            functools.partial(reduce_kernel, num_dev), "reduce", [sds(grad_one.shape, F32), sds((classes, 2 * LANES), F32), sds((1, 1), F32)],
            [VMEM] * 4, [(lines, LANES), (lines, LANES), (lines // 2, LANES), (num_dev // 2 - 1, lines // num_dev, LANES), dma((2, num_dev))],
            collective=1, vmem=8,
        )(grad_one, grad_two, loss, count)
        return mean.reshape(()), grad_one, grad_two.T

    row = P(AXIS)
    return jax.shard_map(
        step, mesh=mesh, in_specs=(row, P(), P(), row, row, row, row, row, row), out_specs=(P(), P(), P()), check_vma=False
    )
```

```python
import functools

import jax
import jax.numpy as jnp
from jax import lax
from jax.experimental import pallas as pl
from jax.experimental.pallas import tpu as pltpu
from jax.sharding import PartitionSpec as P

AXIS = "graph"
LANES = 128
ROWS_A = (((0,), (0,)), ((), ()))
COLS_A = (((1,), (1,)), ((), ()))
F32, BF16 = jnp.float32, jnp.bfloat16
VMEM = pl.BlockSpec(memory_space=pltpu.VMEM)
SMEM = pl.BlockSpec(memory_space=pltpu.SMEM)
ANY = pl.BlockSpec(memory_space=pl.ANY)
STEP = 512
PREP_CHUNK = 64
SEGMENT = 1024
MESH = pl.DeviceIdType.MESH


def dot(a, b, dims=(((1,), (0,)), ((), ()))):
    return lax.dot_general(a, b, dims, preferred_element_type=F32)


def fill_zero(ref):
    zero = jnp.zeros((STEP, LANES), F32)

    @pl.loop(0, ref.shape[0], step=STEP)
    def _(i):
        ref[pl.ds(i, STEP), :] = zero


def copy_in(dst, src):
    @pl.loop(0, dst.shape[0], step=STEP)
    def _(i):
        dst[pl.ds(i, STEP), :] = src[pl.ds(i, STEP), :].astype(F32)


class Edges:
    def __init__(self, first, last, src, dst, w, src_s, dst_s, sems):
        self.first, self.last, self.w = first, last, w
        self.src, self.dst = src_s, dst_s
        self.pairs = ((src, src_s), (dst, dst_s))
        self.sems = sems

    def copies(self, seg):
        part = pl.ds(pl.multiple_of(seg * SEGMENT, SEGMENT), SEGMENT)
        return [pltpu.make_async_copy(a.at[part], b.at[part], self.sems.at[i, seg]) for i, (a, b) in enumerate(self.pairs)]

    def fetch(self):
        per = SEGMENT // PREP_CHUNK
        for seg in range(self.src.shape[0] // SEGMENT):

            @pl.when(jnp.logical_and(seg * per < self.last, (seg + 1) * per > self.first))
            def _():
                for c in self.copies(seg):
                    c.start()

    def walk(self, chunk, from_idx, to_idx, table, accs, wait):
        group, per, ratio = len(accs), SEGMENT // chunk, PREP_CHUNK // chunk
        first, last = self.first * ratio, self.last * ratio

        def body(c, _):
            base = c * chunk
            w_chunk = self.w.at[pl.ds(pl.multiple_of(base, chunk), chunk)]
            for g in range(0, chunk, group):
                pend = []
                for u in range(group):
                    k = base + g + u
                    s = pl.multiple_of(from_idx[k], 2)
                    d = pl.multiple_of(to_idx[k], 2)
                    pend.append((d, accs[u][pl.ds(d, 2), :] + table[pl.ds(s, 2), :] * w_chunk[g + u : g + u + 1, :]))
                for u in range(group):
                    accs[u][pl.ds(pend[u][0], 2), :] = pend[u][1]
            return 0

        if not wait:
            lax.fori_loop(first, last, body, 0)
            return

        def segment(seg, _):
            for c in self.copies(seg):
                c.wait()
            lax.fori_loop(jnp.maximum(first, seg * per), jnp.minimum(last, (seg + 1) * per), body, 0)
            return 0

        lax.fori_loop(first // per, (last + per - 1) // per, segment, 0)


def one_hot_rows(idx, which, start, table):
    lane = lax.broadcasted_iota(jnp.int32, (LANES, LANES), 1)
    hot = []
    for q in range(2):
        want = spread(idx[which : which + 1, pl.ds(pl.multiple_of(start + q * LANES, LANES), LANES)])
        hot.append(
            jnp.concatenate([jnp.where(want == lane + LANES * j, 1.0, 0.0).astype(BF16) for j in range(table.shape[0] // LANES)], axis=1)
        )
    return dot(jnp.concatenate(hot, axis=0), table[...])


def low_lanes(rows):
    return lax.broadcasted_iota(jnp.int32, (rows, LANES), 1) < LANES // 2


def swap_lanes(v):
    return pltpu.roll(v, LANES // 2, 1)


def fetch_index(send, idx, sems):
    parts = [pl.ds(i, LANES) for i in range(0, send.shape[1], LANES)]
    return [pltpu.make_async_copy(send.at[1, p], idx.at[p], sems.at[i]) for i, p in enumerate(parts)]


def gather_block(send, idx, i, table_b, table, buf):
    got = one_hot_rows(send, 0, i, table_b)
    out = buf.at[pl.ds(pl.multiple_of(2 * i, 512), 512)]
    for u in range(256):
        s = pl.multiple_of(idx[i + u] * 2, 2)
        out[2 * u : 2 * u + 2, :] = table[pl.ds(s, 2), :]
    return got


def gather_rows(send, idx, table_b, table, buf, to_prev, to_next):
    @pl.loop(0, to_prev.shape[0], step=256)
    def _(i):
        i = pl.multiple_of(i, 256)
        to_prev[pl.ds(i, 256), :] = gather_block(send, idx, i, table_b, table, buf).astype(BF16)

    @pl.loop(0, to_next.shape[0], step=256)
    def _(i):
        to_next[pl.ds(pl.multiple_of(i, 256), 256), :] = jnp.concatenate(halves([buf], i, 256), axis=1).astype(BF16)


def pack_rows(out, i, a_even, a_odd, b_even, b_odd):
    halo = out.shape[0] * 2 // 3
    out[pl.ds(i, 256), :] = a_even.astype(out.dtype)
    out[pl.ds(halo // 2 + i, 256), :] = b_even.astype(out.dtype)
    out[pl.ds(halo + i, 256), :] = jnp.where(low_lanes(256), a_odd, swap_lanes(b_odd)).astype(out.dtype)


def gather_packed(send, idx, table_b, table, buf, to_prev, to_next):
    half = to_prev.shape[0] // 3

    @pl.loop(0, half, step=256)
    def _(i):
        i = pl.multiple_of(i, 256)
        a = gather_block(send, idx, i, table_b, table, buf)
        b = gather_block(send, idx, half + i, table_b, table, buf)
        pack_rows(to_prev, i, a[:, :LANES], a[:, LANES:], b[:, :LANES], b[:, LANES:])

    @pl.loop(0, half, step=256)
    def _(i):
        i = pl.multiple_of(i, 256)
        pack_rows(to_next, i, *halves([buf], i, 256), *halves([buf], half + i, 256))


def unpack_rows(got, table, start):
    halo = got.shape[0] * 2 // 3

    @pl.loop(0, halo // 2, step=256)
    def _(i):
        i = pl.multiple_of(i, 256)
        a, b, both = (got[pl.ds(k + i, 256), :].astype(F32) for k in (0, halo // 2, halo))
        put_halves(table, start + i, 256, a, jnp.where(low_lanes(256), both, 0.0))
        put_halves(table, start + halo // 2 + i, 256, b, jnp.where(low_lanes(256), swap_lanes(both), 0.0))


def unpack_plain(got, table, start):
    @pl.loop(0, got.shape[0], step=256)
    def _(i):
        t = got[pl.ds(i, 256), :].astype(F32)
        put_halves(table, start + i, 256, t[:, :LANES], t[:, LANES:])


def spread(row):
    return jnp.transpose(jnp.broadcast_to(row, (LANES, LANES)))


def return_rows(idx, start, vals, accs, chunk=32):
    group = len(accs)

    @pl.loop(0, vals.shape[0] // (2 * chunk))
    def _(c):
        block = vals.at[pl.ds(pl.multiple_of(c * 2 * chunk, 2 * chunk), 2 * chunk)]
        for g in range(0, chunk, group):
            pend = []
            for u in range(group):
                d = pl.multiple_of(idx[start + c * chunk + g + u], 2)
                pend.append((d, accs[u][pl.ds(d, 2), :] + block[2 * (g + u) : 2 * (g + u) + 2, :]))
            for u in range(group):
                accs[u][pl.ds(pend[u][0], 2), :] = pend[u][1]


def halves(accs, i, n):
    even = functools.reduce(jnp.add, [a[pl.ds(2 * i, n, stride=2), :] for a in accs])
    odd = functools.reduce(jnp.add, [a[pl.ds(2 * i + 1, n, stride=2), :] for a in accs])
    return even, odd


def put_halves(table, i, n, even, odd):
    table[pl.ds(2 * i, n, stride=2), :] = even
    table[pl.ds(2 * i + 1, n, stride=2), :] = odd


def greet(n):
    me = lax.axis_index(AXIS)
    barrier = pltpu.get_barrier_semaphore()
    for o in range(1, n):
        pl.semaphore_signal(barrier, inc=1, device_id=(lax.rem(me + o, n),), device_id_type=MESH)
    return me, lambda: pl.semaphore_wait(barrier, n - 1)


def remote(src, dst, send_sem, recv_sem, peer):
    return pltpu.make_async_remote_copy(
        src_ref=src, dst_ref=dst, send_sem=send_sem, recv_sem=recv_sem, device_id=(peer,), device_id_type=MESH
    )


def first_kernel(x, w1, send, after, tab, to_prev, to_next, tab_b, buf, idx, sems):
    fetch = fetch_index(send, idx, sems)
    for c in fetch:
        c.start()
    rows = x.shape[0]
    w = w1[...].astype(BF16)

    @pl.loop(0, rows, step=256)
    def _(i):
        t = dot(x[pl.ds(i, 256), :], w).astype(BF16)
        tab_b[pl.ds(i, 256), :] = t
        t = t.astype(F32)
        put_halves(tab, i, 256, t[:, :LANES], t[:, LANES:])

    for c in fetch:
        c.wait()
    gather_rows(send, idx, tab_b, tab, buf, to_prev, to_next)


def reduce_kernel(n, one, two, loss, count, one_out, two_out, mean, work, full, got_pair, got_rest, sems):
    me = lax.axis_index(AXIS)
    chips, core = n // 2, lax.rem(me, 2)
    chip = lax.div(me, 2)
    pair = me + 1 - 2 * core
    others = [lax.rem(chip + o, chips) for o in range(1, chips)]
    barrier = pltpu.get_barrier_semaphore()
    for p in [pair] + [2 * c + core for c in others]:
        pl.semaphore_signal(barrier, inc=1, device_id=(p,), device_id_type=MESH)
    classes = two_out.shape[0]
    lines = -(-classes // 8) * 8
    top, wide = one.shape
    work[0:top, :] = one[:, :LANES]
    work[top : 2 * top, :] = one[:, LANES:]
    work[2 * top : 2 * top + lines, :] = two[:lines, :LANES]
    work[2 * top + lines : 2 * top + 2 * lines, :] = two[:lines, LANES:]
    tail = 2 * top + 2 * lines
    work[tail : tail + 8, :] = loss[...]
    work[tail + 8 :, :] = jnp.zeros((work.shape[0] - tail - 8, LANES), F32)
    pl.semaphore_wait(barrier, chips)

    half = work.shape[0] // 2
    piece = half // chips
    rows = lambda start, size: pl.ds(pl.multiple_of(start, 8), size)
    mine, other = rows(core * half, half), rows((1 - core) * half, half)
    swap = remote(work.at[other], got_pair, sems.at[0, 0], sems.at[1, 0], pair)
    swap.start()
    swap.wait()
    work[mine, :] += got_pair[...]
    scatter = [
        remote(work.at[rows(core * half + c * piece, piece)], got_rest.at[o], sems.at[0, 1 + o], sems.at[1, 1 + o], 2 * c + core)
        for o, c in enumerate(others)
    ]
    for c in scatter:
        c.start()
    for c in scatter:
        c.wait()
    own = rows(core * half + chip * piece, piece)
    work[own, :] += jnp.sum(got_rest[...], axis=0)
    full[own, :] = work[own, :]
    gather = [
        remote(work.at[own], full.at[own], sems.at[0, chips + o], sems.at[1, chips + o], 2 * c + core) for o, c in enumerate(others)
    ]
    for c in gather:
        c.start()
    for c in gather:
        c.wait()
    last = remote(full.at[mine], full.at[mine], sems.at[0, 2 * chips - 1], sems.at[1, 2 * chips - 1], pair)
    last.start()
    last.wait()
    one_out[:, :LANES] = full[0:top, :]
    one_out[:, LANES:] = full[top : 2 * top, :]
    two_out[:, :LANES] = full[2 * top : 2 * top + classes, :]
    two_out[:, LANES:] = full[2 * top + lines : 2 * top + lines + classes, :]
    mean[...] = jnp.sum(full[tail : tail + 8, :], keepdims=True) / count[0:1, 0:1]


def prep_kernel(n, chunk, rows, packed, mask, src_out, dst_out, w_out, counts, count, total, mine, theirs, send_sem, recv_sem):
    me, met = greet(n)
    mine[...] = jnp.sum(mask[...].astype(F32).reshape(-1, 8, LANES), axis=0)
    lines = packed.shape[0] // 2
    slots = src_out.shape[0]
    both = packed[:lines, :].astype(jnp.int32)
    src, d, w = both >> 11, both & 2047, packed[lines:, :]
    live = w != 0.0
    halo = src >= rows
    at = lambda shape, axis: lax.broadcasted_iota(jnp.int32, shape, axis)
    before = (at((LANES, LANES), 0) < at((LANES, LANES), 1)).astype(BF16)
    above = (at((lines, lines), 1) < at((lines, lines), 0)).astype(BF16)
    ones = jnp.ones((LANES, LANES), BF16)

    def rank(mask):
        m = mask.astype(F32).astype(BF16)
        return dot(m, before) + dot(above, dot(m, ones).astype(BF16))

    is_local, is_halo = jnp.logical_and(live, jnp.logical_not(halo)), jnp.logical_and(live, halo)
    n_local = jnp.sum(is_local.astype(F32)).astype(jnp.int32)
    n_halo = jnp.sum(is_halo.astype(F32)).astype(jnp.int32)
    local_chunks = (n_local + chunk - 1) // chunk
    counts[0] = local_chunks
    counts[1] = local_chunks + (n_halo + chunk - 1) // chunk
    pos = jnp.where(
        is_local, rank(is_local).astype(jnp.int32), jnp.where(is_halo, rank(is_halo).astype(jnp.int32) + local_chunks * chunk, -1)
    )
    line, lane = pos >> 7, pos & (LANES - 1)
    s = jnp.where(halo, src - rows, src)
    half_w = w * 0.5
    w_a = half_w.astype(BF16).astype(F32)
    w_b = (half_w - w_a).astype(BF16).astype(F32)
    w_c = half_w - w_a - w_b
    high = ((s >> 8) * 8 + (d >> 8)).astype(F32)
    planes = [(s & 255).astype(F32), (d & 255).astype(F32), high, w_a, w_b, w_c]
    met()
    copies = [remote(mine, theirs.at[o - 1], send_sem.at[o - 1], recv_sem.at[o - 1], lax.rem(me + o, n)) for o in range(1, n)]
    for c in copies:
        c.start()
    acc = jnp.zeros((len(planes) * slots, LANES), F32)
    for r in range(0, lines, 2):
        lhs, rhs = [], []
        for q in (r, r + 1):
            pick = at((slots, LANES), 0) == line[q : q + 1, :]
            lhs.append(jnp.concatenate([jnp.where(pick, p[q : q + 1, :], 0.0) for p in planes], axis=0))
            rhs.append((at((LANES, LANES), 0) == lane[q : q + 1, :]).astype(F32))
        acc += dot(jnp.concatenate(lhs, axis=1).astype(BF16), jnp.concatenate(rhs, axis=1).astype(BF16), COLS_A)
    total[...] = acc
    plane = lambda i: total[i * slots : (i + 1) * slots, :]
    high = plane(2).astype(jnp.int32)
    src_out[...] = ((high >> 3) * 256 + plane(0).astype(jnp.int32)) * 2
    dst_out[...] = ((high & 7) * 256 + plane(1).astype(jnp.int32)) * 2
    total[0:slots, :] = (plane(3) + plane(4) + plane(5)) * 2.0

    @pl.loop(0, slots // 8)
    def _(r):
        for q in range(8):
            w_out[pl.ds(pl.multiple_of((r * 8 + q) * LANES, LANES), LANES), :] = spread(total[pl.ds(r * 8 + q, 1), :])

    for c in copies:
        c.wait()
    every = jnp.sum(mine[...] + jnp.sum(theirs[...], axis=0), keepdims=True)
    count[...] = jnp.maximum(jnp.broadcast_to(every, count.shape), 1.0)


def local_kernel(chunk, backward, counts, src, dst, w, table, out, src_s, dst_s, sems, *accs):
    edges = Edges(0, counts[0], src, dst, w, src_s, dst_s, sems)
    edges.fetch()
    for a in accs:
        fill_zero(a)
    edges.walk(chunk, *((dst_s, src_s) if backward else (src_s, dst_s)), table, accs, True)

    @pl.loop(0, out.shape[0], step=STEP)
    def _(i):
        out[pl.ds(i, STEP), :] = functools.reduce(jnp.add, [a[pl.ds(i, STEP), :] for a in accs])


def forward_halo(chunk, edges, from_prev, from_next, part, htab, accs, unpack):
    edges.fetch()
    unpack(from_prev, htab, 0)
    unpack(from_next, htab, htab.shape[0] // 4)
    copy_in(accs[0], part)
    for a in accs[1:]:
        fill_zero(a)
    edges.walk(chunk, edges.src, edges.dst, htab, accs, True)


def backward_halo(chunk, edges, grad, back_prev, back_next, accs, wait):
    for a in accs:
        fill_zero(a)
    edges.walk(chunk, edges.dst, edges.src, grad, accs, wait)
    split = accs[0].shape[0] // 2
    if back_prev.shape[0] == split:

        @pl.loop(0, split, step=STEP)
        def _(i):
            back_prev[pl.ds(i, STEP), :] = functools.reduce(jnp.add, [a[pl.ds(i, STEP), :] for a in accs])
            back_next[pl.ds(i, STEP), :] = functools.reduce(jnp.add, [a[pl.ds(split + i, STEP), :] for a in accs])
        return
    halo = split // 2

    @pl.loop(0, halo // 2, step=256)
    def _(i):
        i = pl.multiple_of(i, 256)
        for start, out in ((0, back_prev), (halo, back_next)):
            pack_rows(out, i, *halves(accs, start + i, 256), *halves(accs, start + halo // 2 + i, 256))


def padded(w, buf):
    low = w.shape[0] // 8 * 8
    buf[low:, :] = jnp.zeros((buf.shape[0] - low, buf.shape[1]), F32)
    buf[0 : w.shape[0], :] = w[...]
    return buf[...].astype(BF16)


def hidden_kernel(chunk, counts, src, dst, w, send, from_prev, from_next, part, w2, hid, tab, to_prev, to_next, back, htab, tab_b, w2_pad, buf, idx, idx_sems, src_s, dst_s, sems, *accs):
    fetch = fetch_index(send, idx, idx_sems)
    for c in fetch:
        c.start()
    edges = Edges(counts[0], counts[1], src, dst, w, src_s, dst_s, sems)
    w2_b = padded(w2, w2_pad)
    per = send.shape[1] // LANES
    for i in range(2 * per):
        back[i : i + 1, :] = send[i // per : i // per + 1, (i % per) * LANES : (i % per + 1) * LANES] * 2
    forward_halo(chunk, edges, from_prev, from_next, part, htab, accs, unpack_plain)

    @pl.loop(0, hid.shape[0], step=256)
    def _(i):
        even, odd = halves(accs, i, 256)
        h = jnp.concatenate([jnp.maximum(even, 0.0), jnp.maximum(odd, 0.0)], axis=1).astype(BF16)
        hid[pl.ds(i, 256), :] = h
        t = dot(h, w2_b, COLS_A).astype(BF16)
        tab_b[pl.ds(i, 256), :] = t
        t = t.astype(F32)
        put_halves(tab, i, 256, t[:, :LANES], t[:, LANES:])

    for c in fetch:
        c.wait()
    gather_packed(send, idx, tab_b, tab, buf, to_prev, to_next)


def loss_kernel(chunk, classes, counts, src, dst, w, count, from_prev, from_next, part, labels, mask, loss, grad, back_prev, back_next, htab, src_s, dst_s, sems, *accs):
    edges = Edges(counts[0], counts[1], src, dst, w, src_s, dst_s, sems)
    forward_halo(chunk, edges, from_prev, from_next, part, htab, accs, unpack_rows)
    lane = lax.broadcasted_iota(jnp.int32, (LANES, LANES), 1)
    live = lane < classes - LANES
    scale = 1.0 / count[0:1, :]
    loss[...] = jnp.zeros_like(loss)

    @pl.loop(0, labels.shape[0] // 2)
    def _(pair):
        for b in (pair * 2, pair * 2 + 1):
            even, odd = halves(accs, b * LANES, LANES)
            label = spread(labels[pl.ds(b, 1), :])
            keep = spread(mask[pl.ds(b, 1), :]).astype(F32)
            odd = jnp.where(live, odd, -jnp.inf)
            top = jnp.max(jnp.maximum(even, odd), axis=1, keepdims=True)
            total = jnp.sum(jnp.exp(even - top) + jnp.exp(odd - top), axis=1, keepdims=True)
            norm = top + jnp.log(total)
            hit_even, hit_odd = lane == label, lane + LANES == label
            picked = jnp.where(hit_even, even, 0.0) + jnp.where(hit_odd, odd, 0.0)
            per_row = jnp.where(lane == 0, norm, 0.0) - picked
            loss[...] += jnp.sum((keep * per_row).reshape(LANES // 8, 8, LANES), axis=0)
            d_even = (jnp.exp(even - norm) - hit_even.astype(F32)) * (keep * scale)
            d_odd = (jnp.exp(odd - norm) - hit_odd.astype(F32)) * (keep * scale)
            put_halves(grad, b * LANES, LANES, d_even, d_odd)

    backward_halo(chunk, edges, grad, back_prev, back_next, accs, False)


def take_returns(send, part, got_prev, got_next, accs):
    copy_in(accs[0], part)
    for a in accs[1:]:
        fill_zero(a)
    return_rows(send, send.shape[0] // 2, got_prev, accs)
    return_rows(send, 0, got_next, accs)


def middle_kernel(chunk, counts, src, dst, w, send, got_prev, got_next, part, hid, w2, grad_two, grad, back_prev, back_next, returned, w2_pad, src_s, dst_s, sems, *accs):
    edges = Edges(counts[0], counts[1], src, dst, w, src_s, dst_s, sems)
    edges.fetch()
    w2_b = padded(w2, w2_pad)
    split = returned.shape[0] // 2
    unpack_rows(got_prev, returned, 0)
    unpack_rows(got_next, returned, split // 2)
    take_returns(send, part, returned.at[pl.ds(0, split)], returned.at[pl.ds(split, split)], accs)
    grad_two[...] = jnp.zeros_like(grad_two)

    @pl.loop(0, hid.shape[0], step=256)
    def _(i):
        even, odd = halves(accs, i, 256)
        d_tab = jnp.concatenate([even, odd], axis=1).astype(BF16)
        h = hid[pl.ds(i, 256), :]
        grad_two[...] += dot(d_tab, h, ROWS_A)
        d_hid = dot(d_tab, w2_b)
        d_pre = jnp.where(h > 0, d_hid, 0.0)
        put_halves(grad, i, 256, d_pre[:, :LANES], d_pre[:, LANES:])

    backward_halo(chunk, edges, grad, back_prev, back_next, accs, True)


def last_kernel(send, got_prev, got_next, part, x, grad_one, *accs):
    take_returns(send, part, got_prev, got_next, accs)
    grad_one[...] = jnp.zeros_like(grad_one)

    @pl.loop(0, x.shape[0], step=256)
    def _(i):
        even, odd = halves(accs, i, 256)
        d_tab = jnp.concatenate([even, odd], axis=1).astype(BF16)
        grad_one[...] += dot(x[pl.ds(i, 256), :], d_tab, ROWS_A)


def call(body, name, outs, ins, scratch, flops=10**9, out_specs=None, collective=None, vmem=14):
    extra = {} if collective is None else dict(collective_id=collective, has_side_effects=True)
    return pl.pallas_call(
        body, name=name, out_shape=outs, in_specs=ins, out_specs=out_specs or jax.tree.map(lambda _: VMEM, outs),
        scratch_shapes=[pltpu.VMEM(s, F32) if isinstance(s, tuple) else s for s in scratch],
        compiler_params=pltpu.CompilerParams(vmem_limit_bytes=vmem * 2**20, **extra),
        cost_estimate=pl.CostEstimate(flops=flops, bytes_accessed=8 * 2**20, transcendentals=0),
    )


def solution(mesh):
    num_dev = mesh.shape[AXIS]
    to_next = [(d, (d + 1) % num_dev) for d in range(num_dev)]
    to_prev = [(d, (d - 1) % num_dev) for d in range(num_dev)]

    def step(x, w_one, w_two, send, edge_src, edge_dst, edge_w, labels, mask):
        rows, halo, edges, classes = x.shape[0], send.shape[1], edge_src.shape[0], w_two.shape[1]
        tab = (2 * rows, LANES)
        half = (2 * halo, LANES)
        sds = jax.ShapeDtypeStruct
        tab_f, half_f, half_b = sds(tab, F32), sds(half, F32), sds((halo, 2 * LANES), BF16)
        pack_f, pack_b = sds((3 * halo // 2, LANES), F32), sds((3 * halo // 2, LANES), BF16)
        tab_b = pltpu.VMEM((rows, 2 * LANES), BF16)
        one = sds((8, LANES), F32)
        dma = pltpu.SemaphoreType.DMA
        chunk_l, chunk_h = 64, 32
        lines = edges // LANES
        slots = lines + 8
        w2 = w_two.T
        w2_pad = (2 * LANES, 2 * LANES)
        mask = mask.reshape(-1, LANES)

        packed = jnp.concatenate([(edge_src * 2048 + edge_dst).astype(F32), edge_w]).reshape(2 * lines, LANES)
        ints = sds((slots, LANES), jnp.int32)
        src, dst, w, counts, count = call(
            functools.partial(prep_kernel, num_dev, PREP_CHUNK, rows), "prep", [ints, ints, sds((slots * LANES, LANES), F32), sds((2,), jnp.int32), one], [VMEM] * 2,
            [(6 * slots, LANES), (8, LANES), (num_dev - 1, 8, LANES), dma((num_dev - 1,)), dma((num_dev - 1,))],
            out_specs=[VMEM] * 3 + [SMEM, VMEM], vmem=8, collective=0,
        )(packed, mask)
        src, dst = src.reshape(-1), dst.reshape(-1)

        list_s = [pltpu.SMEM((halo,), jnp.int32), dma((halo // LANES,))]
        tab_one, to_p, to_n = call(first_kernel, "first", [tab_f, half_b, half_b], [VMEM] * 3 + [SMEM], [tab_b, half] + list_s, vmem=8)(x, w_one, send, counts)
        from_prev = lax.ppermute(to_n, AXIS, to_next)
        from_next = lax.ppermute(to_p, AXIS, to_prev)

        walk = [SMEM, ANY, ANY, VMEM]
        index = pltpu.SMEM((slots * LANES,), jnp.int32)
        walk_s = [index, index, dma((2, slots * LANES // SEGMENT))]
        local, local_back = (
            call(functools.partial(local_kernel, chunk_l, back), "local_edges", tab_f, walk + [VMEM], walk_s + [tab] * 4, 10**10)
            for back in (False, True)
        )
        part = local(counts, src, dst, w, tab_one)
        hid, tab_two, to_p, to_n, back = call(
            functools.partial(hidden_kernel, chunk_h), "hidden", [sds((rows, 2 * LANES), BF16), tab_f, pack_b, pack_b, sds((2 * halo // LANES, LANES), jnp.int32)],
            walk + [VMEM] * 5, [tab, tab_b, w2_pad, half] + list_s + walk_s + [tab] * 4,
        )(counts, src, dst, w, send, from_prev, from_next, part, w2)
        from_prev = lax.ppermute(to_n, AXIS, to_next)
        from_next = lax.ppermute(to_p, AXIS, to_prev)
        back = back.reshape(-1)
        part = local(counts, src, dst, w, tab_two)
        loss, grad, to_p, to_n = call(
            functools.partial(loss_kernel, chunk_h, classes), "loss", [sds((8, LANES), F32), tab_f, pack_f, pack_f],
            walk + [VMEM] * 6, [tab] + walk_s + [tab] * 4,
        )(counts, src, dst, w, count, from_prev, from_next, part, labels.reshape(-1, LANES), mask)
        got_prev = lax.ppermute(to_p, AXIS, to_prev)
        got_next = lax.ppermute(to_n, AXIS, to_next)
        part = local_back(counts, src, dst, w, grad)
        grad_two, grad, to_p, to_n = call(
            functools.partial(middle_kernel, chunk_h), "middle", [sds((2 * LANES, 2 * LANES), F32), tab_f, half_f, half_f],
            walk + [SMEM] + [VMEM] * 5, [tab, w2_pad] + walk_s + [tab] * 4,
        )(counts, src, dst, w, back, got_prev, got_next, part, hid, w2)
        got_prev = lax.ppermute(to_p, AXIS, to_prev)
        got_next = lax.ppermute(to_n, AXIS, to_next)
        part = local_back(counts, src, dst, w, grad)

        grad_one = call(last_kernel, "last", sds((x.shape[1], 2 * LANES), F32), [SMEM] + [VMEM] * 4, [tab] * 4)(back, got_prev, got_next, part, x)
        lines = 2 * x.shape[1] + 2 * (-(-classes // 8) * 8) + 8
        lines = -(-lines // (8 * num_dev)) * 8 * num_dev
        grad_one, grad_two, mean = call(
            functools.partial(reduce_kernel, num_dev), "reduce", [sds(grad_one.shape, F32), sds((classes, 2 * LANES), F32), sds((1, 1), F32)],
            [VMEM] * 4, [(lines, LANES), (lines, LANES), (lines // 2, LANES), (num_dev // 2 - 1, lines // num_dev, LANES), dma((2, num_dev))],
            collective=1, vmem=8,
        )(grad_one, grad_two, loss, count)
        return mean.reshape(()), grad_one, grad_two.T

    row = P(AXIS)
    return jax.shard_map(
        step, mesh=mesh, in_specs=(row, P(), P(), row, row, row, row, row, row), out_specs=(P(), P(), P()), check_vma=False
    )
```

```python
import functools

import jax
import jax.numpy as jnp
from jax import lax
from jax.experimental import pallas as pl
from jax.experimental.pallas import tpu as pltpu
from jax.sharding import PartitionSpec as P

AXIS = "graph"
LANES = 128
ROWS_A = (((0,), (0,)), ((), ()))
COLS_A = (((1,), (1,)), ((), ()))
F32, BF16 = jnp.float32, jnp.bfloat16
VMEM = pl.BlockSpec(memory_space=pltpu.VMEM)
SMEM = pl.BlockSpec(memory_space=pltpu.SMEM)
ANY = pl.BlockSpec(memory_space=pl.ANY)
STEP = 512
PREP_CHUNK = 64
SEGMENT = 1024
MESH = pl.DeviceIdType.MESH


def dot(a, b, dims=(((1,), (0,)), ((), ()))):
    return lax.dot_general(a, b, dims, preferred_element_type=F32)


def fill_zero(ref):
    zero = jnp.zeros((STEP, LANES), F32)

    @pl.loop(0, ref.shape[0], step=STEP)
    def _(i):
        ref[pl.ds(i, STEP), :] = zero


def copy_in(dst, src):
    @pl.loop(0, dst.shape[0], step=STEP)
    def _(i):
        dst[pl.ds(i, STEP), :] = src[pl.ds(i, STEP), :].astype(F32)


class Edges:
    def __init__(self, first, last, src, dst, w, src_s, dst_s, sems):
        self.first, self.last, self.w = first, last, w
        self.src, self.dst = src_s, dst_s
        self.pairs = ((src, src_s), (dst, dst_s))
        self.sems = sems

    def copies(self, seg):
        part = pl.ds(pl.multiple_of(seg * SEGMENT, SEGMENT), SEGMENT)
        return [pltpu.make_async_copy(a.at[part], b.at[part], self.sems.at[i, seg]) for i, (a, b) in enumerate(self.pairs)]

    def fetch(self):
        per = SEGMENT // PREP_CHUNK
        for seg in range(self.src.shape[0] // SEGMENT):

            @pl.when(jnp.logical_and(seg * per < self.last, (seg + 1) * per > self.first))
            def _():
                for c in self.copies(seg):
                    c.start()

    def walk(self, chunk, from_idx, to_idx, table, accs, wait):
        group, per, ratio = len(accs), SEGMENT // chunk, PREP_CHUNK // chunk
        first, last = self.first * ratio, self.last * ratio

        def body(c, _):
            base = c * chunk
            w_chunk = self.w.at[pl.ds(pl.multiple_of(base, chunk), chunk)]
            for g in range(0, chunk, group):
                pend = []
                for u in range(group):
                    k = base + g + u
                    s = pl.multiple_of(from_idx[k], 2)
                    d = pl.multiple_of(to_idx[k], 2)
                    pend.append((d, accs[u][pl.ds(d, 2), :] + table[pl.ds(s, 2), :] * w_chunk[g + u : g + u + 1, :]))
                for u in range(group):
                    accs[u][pl.ds(pend[u][0], 2), :] = pend[u][1]
            return 0

        if not wait:
            lax.fori_loop(first, last, body, 0)
            return

        def segment(seg, _):
            for c in self.copies(seg):
                c.wait()
            lax.fori_loop(jnp.maximum(first, seg * per), jnp.minimum(last, (seg + 1) * per), body, 0)
            return 0

        lax.fori_loop(first // per, (last + per - 1) // per, segment, 0)


def one_hot_rows(idx, which, start, table):
    lane = lax.broadcasted_iota(jnp.int32, (LANES, LANES), 1)
    hot = []
    for q in range(2):
        want = spread(idx[which : which + 1, pl.ds(pl.multiple_of(start + q * LANES, LANES), LANES)])
        hot.append(
            jnp.concatenate([jnp.where(want == lane + LANES * j, 1.0, 0.0).astype(BF16) for j in range(table.shape[0] // LANES)], axis=1)
        )
    return dot(jnp.concatenate(hot, axis=0), table[...])


def low_lanes(rows):
    return lax.broadcasted_iota(jnp.int32, (rows, LANES), 1) < LANES // 2


def swap_lanes(v):
    return pltpu.roll(v, LANES // 2, 1)


def fetch_index(send, idx, sems):
    parts = [pl.ds(i, LANES) for i in range(0, send.shape[1], LANES)]
    return [pltpu.make_async_copy(send.at[1, p], idx.at[p], sems.at[i]) for i, p in enumerate(parts)]


def gather_block(send, idx, i, table_b, table, buf):
    got = one_hot_rows(send, 0, i, table_b)
    out = buf.at[pl.ds(pl.multiple_of(2 * i, 512), 512)]
    for u in range(256):
        s = pl.multiple_of(idx[i + u] * 2, 2)
        out[2 * u : 2 * u + 2, :] = table[pl.ds(s, 2), :]
    return got


def gather_rows(send, idx, table_b, table, buf, to_prev, to_next):
    @pl.loop(0, to_prev.shape[0], step=256)
    def _(i):
        i = pl.multiple_of(i, 256)
        to_prev[pl.ds(i, 256), :] = gather_block(send, idx, i, table_b, table, buf).astype(BF16)

    @pl.loop(0, to_next.shape[0], step=256)
    def _(i):
        to_next[pl.ds(pl.multiple_of(i, 256), 256), :] = jnp.concatenate(halves([buf], i, 256), axis=1).astype(BF16)


def pack_rows(out, i, a_even, a_odd, b_even, b_odd):
    halo = out.shape[0] * 2 // 3
    out[pl.ds(i, 256), :] = a_even.astype(out.dtype)
    out[pl.ds(halo // 2 + i, 256), :] = b_even.astype(out.dtype)
    out[pl.ds(halo + i, 256), :] = jnp.where(low_lanes(256), a_odd, swap_lanes(b_odd)).astype(out.dtype)


def gather_packed(send, idx, table_b, table, buf, to_prev, to_next):
    half = to_prev.shape[0] // 3

    @pl.loop(0, half, step=256)
    def _(i):
        i = pl.multiple_of(i, 256)
        a = gather_block(send, idx, i, table_b, table, buf)
        b = gather_block(send, idx, half + i, table_b, table, buf)
        pack_rows(to_prev, i, a[:, :LANES], a[:, LANES:], b[:, :LANES], b[:, LANES:])

    @pl.loop(0, half, step=256)
    def _(i):
        i = pl.multiple_of(i, 256)
        pack_rows(to_next, i, *halves([buf], i, 256), *halves([buf], half + i, 256))


def unpack_rows(got, table, start):
    halo = got.shape[0] * 2 // 3

    @pl.loop(0, halo // 2, step=256)
    def _(i):
        i = pl.multiple_of(i, 256)
        a, b, both = (got[pl.ds(k + i, 256), :].astype(F32) for k in (0, halo // 2, halo))
        put_halves(table, start + i, 256, a, jnp.where(low_lanes(256), both, 0.0))
        put_halves(table, start + halo // 2 + i, 256, b, jnp.where(low_lanes(256), swap_lanes(both), 0.0))


def unpack_plain(got, table, start):
    @pl.loop(0, got.shape[0], step=256)
    def _(i):
        t = got[pl.ds(i, 256), :].astype(F32)
        put_halves(table, start + i, 256, t[:, :LANES], t[:, LANES:])


def spread(row):
    return jnp.transpose(jnp.broadcast_to(row, (LANES, LANES)))


def return_rows(idx, start, vals, accs, chunk=32):
    group = len(accs)

    @pl.loop(0, vals.shape[0] // (2 * chunk))
    def _(c):
        block = vals.at[pl.ds(pl.multiple_of(c * 2 * chunk, 2 * chunk), 2 * chunk)]
        for g in range(0, chunk, group):
            pend = []
            for u in range(group):
                d = pl.multiple_of(idx[start + c * chunk + g + u], 2)
                pend.append((d, accs[u][pl.ds(d, 2), :] + block[2 * (g + u) : 2 * (g + u) + 2, :]))
            for u in range(group):
                accs[u][pl.ds(pend[u][0], 2), :] = pend[u][1]


def halves(accs, i, n):
    even = functools.reduce(jnp.add, [a[pl.ds(2 * i, n, stride=2), :] for a in accs])
    odd = functools.reduce(jnp.add, [a[pl.ds(2 * i + 1, n, stride=2), :] for a in accs])
    return even, odd


def put_halves(table, i, n, even, odd):
    table[pl.ds(2 * i, n, stride=2), :] = even
    table[pl.ds(2 * i + 1, n, stride=2), :] = odd


def greet(n):
    me = lax.axis_index(AXIS)
    barrier = pltpu.get_barrier_semaphore()
    for o in range(1, n):
        pl.semaphore_signal(barrier, inc=1, device_id=(lax.rem(me + o, n),), device_id_type=MESH)
    return me, lambda: pl.semaphore_wait(barrier, n - 1)


def remote(src, dst, send_sem, recv_sem, peer):
    return pltpu.make_async_remote_copy(
        src_ref=src, dst_ref=dst, send_sem=send_sem, recv_sem=recv_sem, device_id=(peer,), device_id_type=MESH
    )


def first_kernel(x, w1, send, after, tab, to_prev, to_next, tab_b, buf, idx, sems):
    fetch = fetch_index(send, idx, sems)
    for c in fetch:
        c.start()
    rows = x.shape[0]
    w = w1[...].astype(BF16)

    @pl.loop(0, rows, step=256)
    def _(i):
        t = dot(x[pl.ds(i, 256), :], w).astype(BF16)
        tab_b[pl.ds(i, 256), :] = t
        t = t.astype(F32)
        put_halves(tab, i, 256, t[:, :LANES], t[:, LANES:])

    for c in fetch:
        c.wait()
    gather_rows(send, idx, tab_b, tab, buf, to_prev, to_next)


def reduce_kernel(n, one, two, loss, count, one_out, two_out, mean, work, full, got_pair, got_rest, sems):
    me = lax.axis_index(AXIS)
    chips, core = n // 2, lax.rem(me, 2)
    chip = lax.div(me, 2)
    pair = me + 1 - 2 * core
    others = [lax.rem(chip + o, chips) for o in range(1, chips)]
    barrier = pltpu.get_barrier_semaphore()
    for p in [pair] + [2 * c + core for c in others]:
        pl.semaphore_signal(barrier, inc=1, device_id=(p,), device_id_type=MESH)
    classes = two_out.shape[0]
    lines = -(-classes // 8) * 8
    top, wide = one.shape
    work[0:top, :] = one[:, :LANES]
    work[top : 2 * top, :] = one[:, LANES:]
    work[2 * top : 2 * top + lines, :] = two[:lines, :LANES]
    work[2 * top + lines : 2 * top + 2 * lines, :] = two[:lines, LANES:]
    tail = 2 * top + 2 * lines
    work[tail : tail + 8, :] = loss[...]
    work[tail + 8 :, :] = jnp.zeros((work.shape[0] - tail - 8, LANES), F32)
    pl.semaphore_wait(barrier, chips)

    half = work.shape[0] // 2
    piece = half // chips
    rows = lambda start, size: pl.ds(pl.multiple_of(start, 8), size)
    mine, other = rows(core * half, half), rows((1 - core) * half, half)
    swap = remote(work.at[other], got_pair, sems.at[0, 0], sems.at[1, 0], pair)
    swap.start()
    swap.wait()
    work[mine, :] += got_pair[...]
    scatter = [
        remote(work.at[rows(core * half + c * piece, piece)], got_rest.at[o], sems.at[0, 1 + o], sems.at[1, 1 + o], 2 * c + core)
        for o, c in enumerate(others)
    ]
    for c in scatter:
        c.start()
    for c in scatter:
        c.wait()
    own = rows(core * half + chip * piece, piece)
    work[own, :] += jnp.sum(got_rest[...], axis=0)
    full[own, :] = work[own, :]
    gather = [
        remote(work.at[own], full.at[own], sems.at[0, chips + o], sems.at[1, chips + o], 2 * c + core) for o, c in enumerate(others)
    ]
    for c in gather:
        c.start()
    for c in gather:
        c.wait()
    last = remote(full.at[mine], full.at[mine], sems.at[0, 2 * chips - 1], sems.at[1, 2 * chips - 1], pair)
    last.start()
    last.wait()
    one_out[:, :LANES] = full[0:top, :]
    one_out[:, LANES:] = full[top : 2 * top, :]
    two_out[:, :LANES] = full[2 * top : 2 * top + classes, :]
    two_out[:, LANES:] = full[2 * top + lines : 2 * top + lines + classes, :]
    mean[...] = jnp.sum(full[tail : tail + 8, :], keepdims=True) / count[0:1, 0:1]


def prep_kernel(n, chunk, rows, packed, mask, src_out, dst_out, w_out, counts, count, total, values, places, mine, theirs, send_sem, recv_sem):
    me, met = greet(n)
    mine[...] = jnp.sum(mask[...].astype(F32).reshape(-1, 8, LANES), axis=0)
    lines = packed.shape[0] // 2
    slots = src_out.shape[0]
    both = packed[:lines, :].astype(jnp.int32)
    src, d, w = both >> 11, both & 2047, packed[lines:, :]
    live = w != 0.0
    halo = src >= rows
    at = lambda shape, axis: lax.broadcasted_iota(jnp.int32, shape, axis)
    before = (at((LANES, LANES), 0) < at((LANES, LANES), 1)).astype(BF16)
    above = (at((lines, lines), 1) < at((lines, lines), 0)).astype(BF16)
    ones = jnp.ones((LANES, LANES), BF16)

    def rank(mask):
        m = mask.astype(F32).astype(BF16)
        return dot(m, before) + dot(above, dot(m, ones).astype(BF16))

    is_local, is_halo = jnp.logical_and(live, jnp.logical_not(halo)), jnp.logical_and(live, halo)
    n_local = jnp.sum(is_local.astype(F32)).astype(jnp.int32)
    n_halo = jnp.sum(is_halo.astype(F32)).astype(jnp.int32)
    local_chunks = (n_local + chunk - 1) // chunk
    counts[0] = local_chunks
    counts[1] = local_chunks + (n_halo + chunk - 1) // chunk
    pos = jnp.where(
        is_local, rank(is_local).astype(jnp.int32), jnp.where(is_halo, rank(is_halo).astype(jnp.int32) + local_chunks * chunk, -1)
    )
    line, lane = pos >> 7, pos & (LANES - 1)
    s = jnp.where(halo, src - rows, src)
    half_w = w * 0.5
    w_a = half_w.astype(BF16).astype(F32)
    w_b = (half_w - w_a).astype(BF16).astype(F32)
    w_c = half_w - w_a - w_b
    high = ((s >> 8) * 8 + (d >> 8)).astype(F32)
    planes = [(s & 255).astype(F32), (d & 255).astype(F32), high, w_a, w_b, w_c]
    for i, p in enumerate(planes):
        values[i * lines : (i + 1) * lines, :] = p
    places[:lines, :] = line
    places[lines:, :] = lane
    met()
    copies = [remote(mine, theirs.at[o - 1], send_sem.at[o - 1], recv_sem.at[o - 1], lax.rem(me + o, n)) for o in range(1, n)]
    for c in copies:
        c.start()
    total[...] = jnp.zeros_like(total)

    @pl.loop(0, lines, step=8)
    def _(base):
        acc = None
        for r in range(0, 8, 2):
            lhs, rhs = [], []
            for q in (r, r + 1):
                row = lambda i: pl.ds(i * lines + base + q, 1)
                pick = at((slots, LANES), 0) == places[row(0), :]
                lhs.append(jnp.concatenate([jnp.where(pick, values[row(i), :], 0.0) for i in range(len(planes))], axis=0))
                rhs.append((at((LANES, LANES), 0) == places[row(1), :]).astype(F32))
            part = dot(jnp.concatenate(lhs, axis=1).astype(BF16), jnp.concatenate(rhs, axis=1).astype(BF16), COLS_A)
            acc = part if acc is None else acc + part
        total[...] += acc

    plane = lambda i: total[i * slots : (i + 1) * slots, :]
    high = plane(2).astype(jnp.int32)
    src_out[...] = ((high >> 3) * 256 + plane(0).astype(jnp.int32)) * 2
    dst_out[...] = ((high & 7) * 256 + plane(1).astype(jnp.int32)) * 2
    total[0:slots, :] = (plane(3) + plane(4) + plane(5)) * 2.0

    @pl.loop(0, slots // 8)
    def _(r):
        for q in range(8):
            w_out[pl.ds(pl.multiple_of((r * 8 + q) * LANES, LANES), LANES), :] = spread(total[pl.ds(r * 8 + q, 1), :])

    for c in copies:
        c.wait()
    every = jnp.sum(mine[...] + jnp.sum(theirs[...], axis=0), keepdims=True)
    count[...] = jnp.maximum(jnp.broadcast_to(every, count.shape), 1.0)


def local_kernel(chunk, backward, counts, src, dst, w, table, out, src_s, dst_s, sems, *accs):
    edges = Edges(0, counts[0], src, dst, w, src_s, dst_s, sems)
    edges.fetch()
    for a in accs:
        fill_zero(a)
    edges.walk(chunk, *((dst_s, src_s) if backward else (src_s, dst_s)), table, accs, True)

    @pl.loop(0, out.shape[0], step=STEP)
    def _(i):
        out[pl.ds(i, STEP), :] = functools.reduce(jnp.add, [a[pl.ds(i, STEP), :] for a in accs])


def forward_halo(chunk, edges, from_prev, from_next, part, htab, accs, unpack):
    edges.fetch()
    unpack(from_prev, htab, 0)
    unpack(from_next, htab, htab.shape[0] // 4)
    copy_in(accs[0], part)
    for a in accs[1:]:
        fill_zero(a)
    edges.walk(chunk, edges.src, edges.dst, htab, accs, True)


def backward_halo(chunk, edges, grad, back_prev, back_next, accs, wait):
    for a in accs:
        fill_zero(a)
    edges.walk(chunk, edges.dst, edges.src, grad, accs, wait)
    split = accs[0].shape[0] // 2
    if back_prev.shape[0] == split:

        @pl.loop(0, split, step=STEP)
        def _(i):
            back_prev[pl.ds(i, STEP), :] = functools.reduce(jnp.add, [a[pl.ds(i, STEP), :] for a in accs])
            back_next[pl.ds(i, STEP), :] = functools.reduce(jnp.add, [a[pl.ds(split + i, STEP), :] for a in accs])
        return
    halo = split // 2

    @pl.loop(0, halo // 2, step=256)
    def _(i):
        i = pl.multiple_of(i, 256)
        for start, out in ((0, back_prev), (halo, back_next)):
            pack_rows(out, i, *halves(accs, start + i, 256), *halves(accs, start + halo // 2 + i, 256))


def padded(w, buf):
    low = w.shape[0] // 8 * 8
    buf[low:, :] = jnp.zeros((buf.shape[0] - low, buf.shape[1]), F32)
    buf[0 : w.shape[0], :] = w[...]
    return buf[...].astype(BF16)


def hidden_kernel(chunk, counts, src, dst, w, send, from_prev, from_next, part, w2, hid, tab, to_prev, to_next, back, htab, tab_b, w2_pad, buf, idx, idx_sems, src_s, dst_s, sems, *accs):
    fetch = fetch_index(send, idx, idx_sems)
    for c in fetch:
        c.start()
    edges = Edges(counts[0], counts[1], src, dst, w, src_s, dst_s, sems)
    w2_b = padded(w2, w2_pad)
    per = send.shape[1] // LANES
    for i in range(2 * per):
        back[i : i + 1, :] = send[i // per : i // per + 1, (i % per) * LANES : (i % per + 1) * LANES] * 2
    forward_halo(chunk, edges, from_prev, from_next, part, htab, accs, unpack_plain)

    @pl.loop(0, hid.shape[0], step=256)
    def _(i):
        even, odd = halves(accs, i, 256)
        h = jnp.concatenate([jnp.maximum(even, 0.0), jnp.maximum(odd, 0.0)], axis=1).astype(BF16)
        hid[pl.ds(i, 256), :] = h
        t = dot(h, w2_b, COLS_A).astype(BF16)
        tab_b[pl.ds(i, 256), :] = t
        t = t.astype(F32)
        put_halves(tab, i, 256, t[:, :LANES], t[:, LANES:])

    for c in fetch:
        c.wait()
    gather_packed(send, idx, tab_b, tab, buf, to_prev, to_next)


def loss_kernel(chunk, classes, counts, src, dst, w, count, from_prev, from_next, part, labels, mask, loss, grad, back_prev, back_next, htab, src_s, dst_s, sems, *accs):
    edges = Edges(counts[0], counts[1], src, dst, w, src_s, dst_s, sems)
    forward_halo(chunk, edges, from_prev, from_next, part, htab, accs, unpack_rows)
    lane = lax.broadcasted_iota(jnp.int32, (LANES, LANES), 1)
    live = lane < classes - LANES
    scale = 1.0 / count[0:1, :]
    loss[...] = jnp.zeros_like(loss)

    @pl.loop(0, labels.shape[0] // 2)
    def _(pair):
        for b in (pair * 2, pair * 2 + 1):
            even, odd = halves(accs, b * LANES, LANES)
            label = spread(labels[pl.ds(b, 1), :])
            keep = spread(mask[pl.ds(b, 1), :]).astype(F32)
            odd = jnp.where(live, odd, -jnp.inf)
            top = jnp.max(jnp.maximum(even, odd), axis=1, keepdims=True)
            total = jnp.sum(jnp.exp(even - top) + jnp.exp(odd - top), axis=1, keepdims=True)
            norm = top + jnp.log(total)
            hit_even, hit_odd = lane == label, lane + LANES == label
            picked = jnp.where(hit_even, even, 0.0) + jnp.where(hit_odd, odd, 0.0)
            per_row = jnp.where(lane == 0, norm, 0.0) - picked
            loss[...] += jnp.sum((keep * per_row).reshape(LANES // 8, 8, LANES), axis=0)
            d_even = (jnp.exp(even - norm) - hit_even.astype(F32)) * (keep * scale)
            d_odd = (jnp.exp(odd - norm) - hit_odd.astype(F32)) * (keep * scale)
            put_halves(grad, b * LANES, LANES, d_even, d_odd)

    backward_halo(chunk, edges, grad, back_prev, back_next, accs, False)


def take_returns(send, part, got_prev, got_next, accs):
    copy_in(accs[0], part)
    for a in accs[1:]:
        fill_zero(a)
    return_rows(send, send.shape[0] // 2, got_prev, accs)
    return_rows(send, 0, got_next, accs)


def middle_kernel(chunk, counts, src, dst, w, send, got_prev, got_next, part, hid, w2, grad_two, grad, back_prev, back_next, returned, w2_pad, src_s, dst_s, sems, *accs):
    edges = Edges(counts[0], counts[1], src, dst, w, src_s, dst_s, sems)
    edges.fetch()
    w2_b = padded(w2, w2_pad)
    split = returned.shape[0] // 2
    unpack_rows(got_prev, returned, 0)
    unpack_rows(got_next, returned, split // 2)
    take_returns(send, part, returned.at[pl.ds(0, split)], returned.at[pl.ds(split, split)], accs)
    grad_two[...] = jnp.zeros_like(grad_two)

    @pl.loop(0, hid.shape[0], step=256)
    def _(i):
        even, odd = halves(accs, i, 256)
        d_tab = jnp.concatenate([even, odd], axis=1).astype(BF16)
        h = hid[pl.ds(i, 256), :]
        grad_two[...] += dot(d_tab, h, ROWS_A)
        d_hid = dot(d_tab, w2_b)
        d_pre = jnp.where(h > 0, d_hid, 0.0)
        put_halves(grad, i, 256, d_pre[:, :LANES], d_pre[:, LANES:])

    backward_halo(chunk, edges, grad, back_prev, back_next, accs, True)


def last_kernel(send, got_prev, got_next, part, x, grad_one, *accs):
    take_returns(send, part, got_prev, got_next, accs)
    grad_one[...] = jnp.zeros_like(grad_one)

    @pl.loop(0, x.shape[0], step=256)
    def _(i):
        even, odd = halves(accs, i, 256)
        d_tab = jnp.concatenate([even, odd], axis=1).astype(BF16)
        grad_one[...] += dot(x[pl.ds(i, 256), :], d_tab, ROWS_A)


def call(body, name, outs, ins, scratch, flops=10**9, out_specs=None, collective=None, vmem=14):
    extra = {} if collective is None else dict(collective_id=collective, has_side_effects=True)
    return pl.pallas_call(
        body, name=name, out_shape=outs, in_specs=ins, out_specs=out_specs or jax.tree.map(lambda _: VMEM, outs),
        scratch_shapes=[pltpu.VMEM(s, F32) if isinstance(s, tuple) else s for s in scratch],
        compiler_params=pltpu.CompilerParams(vmem_limit_bytes=vmem * 2**20, **extra),
        cost_estimate=pl.CostEstimate(flops=flops, bytes_accessed=8 * 2**20, transcendentals=0),
    )


def solution(mesh):
    num_dev = mesh.shape[AXIS]
    to_next = [(d, (d + 1) % num_dev) for d in range(num_dev)]
    to_prev = [(d, (d - 1) % num_dev) for d in range(num_dev)]

    def step(x, w_one, w_two, send, edge_src, edge_dst, edge_w, labels, mask):
        rows, halo, edges, classes = x.shape[0], send.shape[1], edge_src.shape[0], w_two.shape[1]
        tab = (2 * rows, LANES)
        half = (2 * halo, LANES)
        sds = jax.ShapeDtypeStruct
        tab_f, half_f, half_b = sds(tab, F32), sds(half, F32), sds((halo, 2 * LANES), BF16)
        pack_f, pack_b = sds((3 * halo // 2, LANES), F32), sds((3 * halo // 2, LANES), BF16)
        tab_b = pltpu.VMEM((rows, 2 * LANES), BF16)
        one = sds((8, LANES), F32)
        dma = pltpu.SemaphoreType.DMA
        chunk_l, chunk_h = 64, 32
        lines = edges // LANES
        slots = lines + 8
        w2 = w_two.T
        w2_pad = (2 * LANES, 2 * LANES)
        mask = mask.reshape(-1, LANES)

        packed = jnp.concatenate([(edge_src * 2048 + edge_dst).astype(F32), edge_w]).reshape(2 * lines, LANES)
        ints = sds((slots, LANES), jnp.int32)
        src, dst, w, counts, count = call(
            functools.partial(prep_kernel, num_dev, PREP_CHUNK, rows), "prep", [ints, ints, sds((slots * LANES, LANES), F32), sds((2,), jnp.int32), one], [VMEM] * 2,
            [(6 * slots, LANES), (6 * lines, LANES), pltpu.VMEM((2 * lines, LANES), jnp.int32), (8, LANES), (num_dev - 1, 8, LANES)]
            + [dma((num_dev - 1,))] * 2,
            out_specs=[VMEM] * 3 + [SMEM, VMEM], vmem=8, collective=0,
        )(packed, mask)
        src, dst = src.reshape(-1), dst.reshape(-1)

        list_s = [pltpu.SMEM((halo,), jnp.int32), dma((halo // LANES,))]
        tab_one, to_p, to_n = call(first_kernel, "first", [tab_f, half_b, half_b], [VMEM] * 3 + [SMEM], [tab_b, half] + list_s, vmem=8)(x, w_one, send, counts)
        from_prev = lax.ppermute(to_n, AXIS, to_next)
        from_next = lax.ppermute(to_p, AXIS, to_prev)

        walk = [SMEM, ANY, ANY, VMEM]
        index = pltpu.SMEM((slots * LANES,), jnp.int32)
        walk_s = [index, index, dma((2, slots * LANES // SEGMENT))]
        local, local_back = (
            call(functools.partial(local_kernel, chunk_l, back), "local_edges", tab_f, walk + [VMEM], walk_s + [tab] * 4, 10**10)
            for back in (False, True)
        )
        part = local(counts, src, dst, w, tab_one)
        hid, tab_two, to_p, to_n, back = call(
            functools.partial(hidden_kernel, chunk_h), "hidden", [sds((rows, 2 * LANES), BF16), tab_f, pack_b, pack_b, sds((2 * halo // LANES, LANES), jnp.int32)],
            walk + [VMEM] * 5, [tab, tab_b, w2_pad, half] + list_s + walk_s + [tab] * 4,
        )(counts, src, dst, w, send, from_prev, from_next, part, w2)
        from_prev = lax.ppermute(to_n, AXIS, to_next)
        from_next = lax.ppermute(to_p, AXIS, to_prev)
        back = back.reshape(-1)
        part = local(counts, src, dst, w, tab_two)
        loss, grad, to_p, to_n = call(
            functools.partial(loss_kernel, chunk_h, classes), "loss", [sds((8, LANES), F32), tab_f, pack_f, pack_f],
            walk + [VMEM] * 6, [tab] + walk_s + [tab] * 4,
        )(counts, src, dst, w, count, from_prev, from_next, part, labels.reshape(-1, LANES), mask)
        got_prev = lax.ppermute(to_p, AXIS, to_prev)
        got_next = lax.ppermute(to_n, AXIS, to_next)
        part = local_back(counts, src, dst, w, grad)
        grad_two, grad, to_p, to_n = call(
            functools.partial(middle_kernel, chunk_h), "middle", [sds((2 * LANES, 2 * LANES), F32), tab_f, half_f, half_f],
            walk + [SMEM] + [VMEM] * 5, [tab, w2_pad] + walk_s + [tab] * 4,
        )(counts, src, dst, w, back, got_prev, got_next, part, hid, w2)
        got_prev = lax.ppermute(to_p, AXIS, to_prev)
        got_next = lax.ppermute(to_n, AXIS, to_next)
        part = local_back(counts, src, dst, w, grad)

        grad_one = call(last_kernel, "last", sds((x.shape[1], 2 * LANES), F32), [SMEM] + [VMEM] * 4, [tab] * 4)(back, got_prev, got_next, part, x)
        lines = 2 * x.shape[1] + 2 * (-(-classes // 8) * 8) + 8
        lines = -(-lines // (8 * num_dev)) * 8 * num_dev
        grad_one, grad_two, mean = call(
            functools.partial(reduce_kernel, num_dev), "reduce", [sds(grad_one.shape, F32), sds((classes, 2 * LANES), F32), sds((1, 1), F32)],
            [VMEM] * 4, [(lines, LANES), (lines, LANES), (lines // 2, LANES), (num_dev // 2 - 1, lines // num_dev, LANES), dma((2, num_dev))],
            collective=1, vmem=8,
        )(grad_one, grad_two, loss, count)
        return mean.reshape(()), grad_one, grad_two.T

    row = P(AXIS)
    return jax.shard_map(
        step, mesh=mesh, in_specs=(row, P(), P(), row, row, row, row, row, row), out_specs=(P(), P(), P()), check_vma=False
    )
```

```python
import functools

import jax
import jax.numpy as jnp
from jax import lax
from jax.experimental import pallas as pl
from jax.experimental.pallas import tpu as pltpu
from jax.sharding import PartitionSpec as P

AXIS = "graph"
LANES = 128
ROWS_A = (((0,), (0,)), ((), ()))
COLS_A = (((1,), (1,)), ((), ()))
F32, BF16 = jnp.float32, jnp.bfloat16
VMEM = pl.BlockSpec(memory_space=pltpu.VMEM)
SMEM = pl.BlockSpec(memory_space=pltpu.SMEM)
ANY = pl.BlockSpec(memory_space=pl.ANY)
STEP = 512
BLOCK = 256
BYTE = 256
SUB = 8
TILE = (SUB, LANES)
SQUARE = (LANES, LANES)
PREP_CHUNK = 64
SEGMENT = 1024
MESH = pl.DeviceIdType.MESH


def dot(a, b, dims=(((1,), (0,)), ((), ()))):
    return lax.dot_general(a, b, dims, preferred_element_type=F32)


def fill_zero(ref):
    zero = jnp.zeros((STEP, LANES), F32)

    @pl.loop(0, ref.shape[0], step=STEP)
    def _(i):
        ref[pl.ds(i, STEP), :] = zero


def copy_in(dst, src):
    @pl.loop(0, dst.shape[0], step=STEP)
    def _(i):
        dst[pl.ds(i, STEP), :] = src[pl.ds(i, STEP), :].astype(F32)


class Edges:
    def __init__(self, first, last, w, arrays, smem, sems):
        self.first, self.last, self.w = first, last, w
        self.pairs = tuple(zip(arrays, smem))
        self.sems = sems

    def copies(self, seg):
        part = pl.ds(pl.multiple_of(seg * SEGMENT, SEGMENT), SEGMENT)
        return [pltpu.make_async_copy(a.at[part], b.at[part], self.sems.at[i, seg]) for i, (a, b) in enumerate(self.pairs)]

    def fetch(self):
        per = SEGMENT // PREP_CHUNK
        for seg in range(self.pairs[0][1].shape[0] // SEGMENT):

            @pl.when(jnp.logical_and(seg * per < self.last, (seg + 1) * per > self.first))
            def _():
                for c in self.copies(seg):
                    c.start()

    def walk(self, chunk, from_idx, to_idx, table, accs, wait):
        group, per, ratio = len(accs), SEGMENT // chunk, PREP_CHUNK // chunk
        first, last = self.first * ratio, self.last * ratio

        def body(c, _):
            base = c * chunk
            w_chunk = self.w.at[pl.ds(pl.multiple_of(base, chunk), chunk)]
            for g in range(0, chunk, group):
                pend = []
                for u in range(group):
                    k = base + g + u
                    s = pl.multiple_of(from_idx[k], 2)
                    d = pl.multiple_of(to_idx[k], 2)
                    pend.append((d, accs[u][pl.ds(d, 2), :] + table[pl.ds(s, 2), :] * w_chunk[g + u : g + u + 1, :]))
                for u in range(group):
                    accs[u][pl.ds(pend[u][0], 2), :] = pend[u][1]
            return 0

        if not wait:
            lax.fori_loop(first, last, body, 0)
            return

        def segment(seg, _):
            for c in self.copies(seg):
                c.wait()
            lax.fori_loop(jnp.maximum(first, seg * per), jnp.minimum(last, (seg + 1) * per), body, 0)
            return 0

        lax.fori_loop(first // per, (last + per - 1) // per, segment, 0)


def one_hot_rows(idx, which, start, table):
    lane = across(SQUARE)
    hot = []
    for q in range(2):
        want = spread(idx[which : which + 1, pl.ds(pl.multiple_of(start + q * LANES, LANES), LANES)])
        hot.append(
            stack_lanes([jnp.where(want == lane + LANES * j, 1.0, 0.0).astype(BF16) for j in range(table.shape[0] // LANES)])
        )
    return dot(stack_rows(hot), table[...])


def low_lanes(rows):
    return across((rows, LANES)) < LANES // 2


def swap_lanes(v):
    return pltpu.roll(v, LANES // 2, 1)


def fetch_index(send, idx, sems):
    parts = [pl.ds(i, LANES) for i in range(0, send.shape[1], LANES)]
    return [pltpu.make_async_copy(send.at[1, p], idx.at[p], sems.at[i]) for i, p in enumerate(parts)]


def gather_block(send, idx, i, table_b, table, buf):
    got = one_hot_rows(send, 0, i, table_b)
    out = buf.at[pl.ds(pl.multiple_of(2 * i, 512), 512)]
    for u in range(BLOCK):
        s = pl.multiple_of(idx[i + u] * 2, 2)
        out[2 * u : 2 * u + 2, :] = table[pl.ds(s, 2), :]
    return got


def gather_rows(send, idx, table_b, table, buf, to_prev, to_next):
    @pl.loop(0, to_prev.shape[0], step=BLOCK)
    def _(i):
        i = pl.multiple_of(i, BLOCK)
        to_prev[pl.ds(i, BLOCK), :] = gather_block(send, idx, i, table_b, table, buf).astype(BF16)

    @pl.loop(0, to_next.shape[0], step=BLOCK)
    def _(i):
        to_next[pl.ds(pl.multiple_of(i, BLOCK), BLOCK), :] = stack_lanes(halves([buf], i, BLOCK)).astype(BF16)


def pack_rows(out, i, half, a_even, a_odd, b_even, b_odd):
    n = a_even.shape[0]
    out[pl.ds(i, n), :] = a_even.astype(out.dtype)
    out[pl.ds(half + i, n), :] = b_even.astype(out.dtype)
    out[pl.ds(2 * half + i, n), :] = jnp.where(low_lanes(n), a_odd, swap_lanes(b_odd)).astype(out.dtype)


def gather_packed(send, idx, table_b, table, buf, to_prev, to_next):
    half = to_prev.shape[0] // 3

    @pl.loop(0, half, step=BLOCK)
    def _(i):
        i = pl.multiple_of(i, BLOCK)
        a = gather_block(send, idx, i, table_b, table, buf)
        b = gather_block(send, idx, half + i, table_b, table, buf)
        pack_rows(to_prev, i, half, a[:, :LANES], a[:, LANES:], b[:, :LANES], b[:, LANES:])

    @pl.loop(0, half, step=BLOCK)
    def _(i):
        i = pl.multiple_of(i, BLOCK)
        pack_rows(to_next, i, half, *halves([buf], i, BLOCK), *halves([buf], half + i, BLOCK))


def unpack_rows(got, table, start, half=None):
    half = got.shape[0] // 3 if half is None else half
    n = half // 2

    @pl.loop(0, half, step=n)
    def _(i):
        i = pl.multiple_of(i, n)
        a, b, both = (got[pl.ds(k + i, n), :].astype(F32) for k in (0, half, 2 * half))
        put_halves(table, start + i, n, a, jnp.where(low_lanes(n), both, 0.0))
        put_halves(table, start + half + i, n, b, jnp.where(low_lanes(n), swap_lanes(both), 0.0))


def unpack_plain(got, table, start):
    @pl.loop(0, got.shape[0], step=BLOCK)
    def _(i):
        t = got[pl.ds(i, BLOCK), :].astype(F32)
        put_halves(table, start + i, BLOCK, t[:, :LANES], t[:, LANES:])


def spread(row):
    return jnp.transpose(jnp.broadcast_to(row, SQUARE))


def return_rows(back, slots, start, count, vals, accs, chunk=32):
    group = len(accs)

    def body(c, _):
        block = vals.at[pl.ds(pl.multiple_of(c * 2 * chunk, 2 * chunk), 2 * chunk)]
        for g in range(0, chunk, group):
            pend = []
            for u in range(group):
                d = pl.multiple_of(back[slots[start + c * chunk + g + u]], 2)
                pend.append((d, accs[u][pl.ds(d, 2), :] + block[2 * (g + u) : 2 * (g + u) + 2, :]))
            for u in range(group):
                accs[u][pl.ds(pend[u][0], 2), :] = pend[u][1]
        return 0

    lax.fori_loop(0, (count + chunk - 1) // chunk, body, 0)


def group(i, n, which):
    return pl.ds(2 * i + which, n, stride=2), slice(None)


def halves(accs, i, n):
    return [functools.reduce(jnp.add, [a[group(i, n, k)] for a in accs]) for k in range(2)]


def put_halves(table, i, n, *parts):
    for k, part in enumerate(parts):
        table[group(i, n, k)] = part


def stack_rows(parts):
    return jnp.concatenate(parts, axis=0)


def stack_lanes(parts):
    return jnp.concatenate(parts, axis=1)


def down(shape):
    return lax.broadcasted_iota(jnp.int32, shape, 0)


def across(shape):
    return lax.broadcasted_iota(jnp.int32, shape, 1)


def prefix(mask, above):
    m = mask.astype(BF16)
    before = (down(SQUARE) < across(SQUARE)).astype(BF16)
    return dot(m, before) + dot(above, dot(m, jnp.ones(SQUARE, BF16)).astype(BF16))


def rank_halo(halo, counts, src, used, src_back, lists):
    lines = used.shape[0]
    side = lines // 2
    i, j = down((lines, lines)), across((lines, lines))
    above = jnp.logical_and(j < i, (j >= side) == (i >= side)).astype(F32).astype(BF16)
    rank = prefix(used[...], above).astype(jnp.int32)
    low, high = rank & (LANES - 1), rank >> 7
    table = stack_rows([low.astype(F32), high.astype(F32)]).astype(BF16)

    def line(r, _):
        slot = src[pl.ds(r, 1), :] >> 1
        h, l = slot >> 7, slot & (LANES - 1)
        got = dot(table, (down(SQUARE) == l).astype(F32).astype(BF16))
        got = jnp.where(down((lines, LANES)) == h, got[:lines] + LANES * got[lines:], 0.0)
        got = jnp.sum(got, axis=0, keepdims=True).astype(jnp.int32)
        src_back[pl.ds(r, 1), :] = (got + jnp.where(h >= side, halo, 0)) * 2
        return 0

    ratio = LANES // PREP_CHUNK
    lax.fori_loop(counts[0] // ratio, (counts[1] + ratio - 1) // ratio, line, 0)
    for k in range(2):
        acc = jnp.zeros((24, LANES), F32)
        for hh in range(side):
            q = k * side + hh
            pick = jnp.where(down(TILE) == high[q : q + 1, :], used[q : q + 1, :], 0.0)
            lhs = stack_rows([pick * across(TILE).astype(F32), pick * hh, pick]).astype(BF16)
            acc += dot(lhs, (down(SQUARE) == low[q : q + 1, :]).astype(F32).astype(BF16), COLS_A)
        slots = acc[0:8] + LANES * acc[8:16]
        lists[k * side : (k + 1) * side, :] = jnp.where(acc[16:24] > 0.0, slots[:side], -1.0)


def first_kernel(compact, halo, x, w1, send, counts, src, w, used, tab, to_prev, to_next, w_out, src_back, lists, tab_b, buf, idx, sems):
    fetch = fetch_index(send, idx, sems)
    for c in fetch:
        c.start()
    rows = x.shape[0]
    w1_b = w1[...].astype(BF16)

    @pl.loop(0, rows, step=BLOCK)
    def _(i):
        t = dot(x[pl.ds(i, BLOCK), :], w1_b).astype(BF16)
        tab_b[pl.ds(i, BLOCK), :] = t
        t = t.astype(F32)
        put_halves(tab, i, BLOCK, t[:, :LANES], t[:, LANES:])

    @pl.loop(0, w.shape[0] // SUB)
    def _(r):
        for q in range(SUB):
            w_out[pl.ds(pl.multiple_of((r * SUB + q) * LANES, LANES), LANES), :] = spread(w[pl.ds(r * SUB + q, 1), :])

    src_back[...] = src[...]
    if compact:
        rank_halo(halo, counts, src, used, src_back, lists)
    else:
        line = down(lists.shape)
        line = jnp.where(line >= lists.shape[0] // 2, line - lists.shape[0] // 2, line)
        lists[...] = (line * LANES + across(lists.shape)).astype(F32)
    for c in fetch:
        c.wait()
    gather_rows(send, idx, tab_b, tab, buf, to_prev, to_next)


def greet(n):
    me = lax.axis_index(AXIS)
    barrier = pltpu.get_barrier_semaphore()
    for o in range(1, n):
        pl.semaphore_signal(barrier, inc=1, device_id=(lax.rem(me + o, n),), device_id_type=MESH)
    return me, lambda: pl.semaphore_wait(barrier, n - 1)


def remote(src, dst, send_sem, recv_sem, peer):
    return pltpu.make_async_remote_copy(
        src_ref=src, dst_ref=dst, send_sem=send_sem, recv_sem=recv_sem, device_id=(peer,), device_id_type=MESH
    )


def reduce_kernel(n, one, two, loss, count, one_out, two_out, mean, work, full, got_pair, got_rest, sems):
    me = lax.axis_index(AXIS)
    chips, core = n // 2, lax.rem(me, 2)
    chip = lax.div(me, 2)
    pair = me + 1 - 2 * core
    others = [lax.rem(chip + o, chips) for o in range(1, chips)]
    barrier = pltpu.get_barrier_semaphore()
    for p in [pair] + [2 * c + core for c in others]:
        pl.semaphore_signal(barrier, inc=1, device_id=(p,), device_id_type=MESH)
    classes = two_out.shape[0]
    lines = -(-classes // SUB) * SUB
    top, wide = one.shape
    work[0:top, :] = one[:, :LANES]
    work[top : 2 * top, :] = one[:, LANES:]
    work[2 * top : 2 * top + lines, :] = two[:lines, :LANES]
    work[2 * top + lines : 2 * top + 2 * lines, :] = two[:lines, LANES:]
    tail = 2 * top + 2 * lines
    work[tail : tail + SUB, :] = loss[...]
    work[tail + SUB :, :] = jnp.zeros((work.shape[0] - tail - SUB, LANES), F32)
    pl.semaphore_wait(barrier, chips)

    half = work.shape[0] // 2
    piece = half // chips
    rows = lambda start, size: pl.ds(pl.multiple_of(start, SUB), size)
    mine, other = rows(core * half, half), rows((1 - core) * half, half)
    swap = remote(work.at[other], got_pair, sems.at[0, 0], sems.at[1, 0], pair)
    swap.start()
    swap.wait()
    work[mine, :] += got_pair[...]
    scatter = [
        remote(work.at[rows(core * half + c * piece, piece)], got_rest.at[o], sems.at[0, 1 + o], sems.at[1, 1 + o], 2 * c + core)
        for o, c in enumerate(others)
    ]
    for c in scatter:
        c.start()
    for c in scatter:
        c.wait()
    own = rows(core * half + chip * piece, piece)
    work[own, :] += jnp.sum(got_rest[...], axis=0)
    full[own, :] = work[own, :]
    gather = [
        remote(work.at[own], full.at[own], sems.at[0, chips + o], sems.at[1, chips + o], 2 * c + core) for o, c in enumerate(others)
    ]
    for c in gather:
        c.start()
    for c in gather:
        c.wait()
    last = remote(full.at[mine], full.at[mine], sems.at[0, 2 * chips - 1], sems.at[1, 2 * chips - 1], pair)
    last.start()
    last.wait()
    one_out[:, :LANES] = full[0:top, :]
    one_out[:, LANES:] = full[top : 2 * top, :]
    two_out[:, :LANES] = full[2 * top : 2 * top + classes, :]
    two_out[:, LANES:] = full[2 * top + lines : 2 * top + lines + classes, :]
    mean[...] = jnp.sum(full[tail : tail + SUB, :], keepdims=True) / count[0:1, 0:1]


def prep_kernel(n, chunk, rows, packed, mask, src_out, dst_out, w_out, used, counts, count, need, total, values, places, hits, mine, theirs, send_sem, recv_sem):
    me, met = greet(n)
    lines = packed.shape[0] // 2
    slots = src_out.shape[0]
    both = packed[:lines, :].astype(jnp.int32)
    src, d, w = both >> 11, both & 2047, packed[lines:, :]
    live = w != 0.0
    halo = src >= rows
    above = (across((lines, lines)) < down((lines, lines))).astype(F32).astype(BF16)
    is_local, is_halo = jnp.logical_and(live, jnp.logical_not(halo)), jnp.logical_and(live, halo)
    rank = lambda m: prefix(m.astype(F32), above).astype(jnp.int32)
    n_local = jnp.sum(is_local.astype(F32)).astype(jnp.int32)
    n_halo = jnp.sum(is_halo.astype(F32)).astype(jnp.int32)
    local_chunks = (n_local + chunk - 1) // chunk
    counts[0] = local_chunks
    counts[1] = local_chunks + (n_halo + chunk - 1) // chunk
    pos = jnp.where(is_local, rank(is_local), jnp.where(is_halo, rank(is_halo) + local_chunks * chunk, -1))
    s = jnp.where(halo, src - rows, src)
    half_w = w * 0.5
    w_a = half_w.astype(BF16).astype(F32)
    w_b = (half_w - w_a).astype(BF16).astype(F32)
    w_c = half_w - w_a - w_b
    high = ((s >> 8) * 8 + (d >> 8)).astype(F32)
    planes = [(s % BYTE).astype(F32), (d % BYTE).astype(F32), high, w_a, w_b, w_c]
    for i, p in enumerate(planes):
        values[i * lines : (i + 1) * lines, :] = p
    for i, p in enumerate((pos >> 7, pos & (LANES - 1), jnp.where(is_halo, s >> 7, -1), s & (LANES - 1))):
        places[i * lines : (i + 1) * lines, :] = p
    row = lambda i, q: pl.ds(i * lines + q, 1)
    spot = lambda size, i, q: (down((size, LANES)) == places[row(i, q), :]).astype(F32)
    hits[...] = jnp.zeros_like(hits)

    @pl.loop(0, lines, step=SUB)
    def _(base):
        acc = None
        for r in range(0, SUB, 2):
            lhs = stack_lanes([spot(hits.shape[0], 2, base + q) for q in (r, r + 1)]).astype(BF16)
            rhs = stack_lanes([spot(LANES, 3, base + q) for q in (r, r + 1)]).astype(BF16)
            part = dot(lhs, rhs, COLS_A)
            acc = part if acc is None else acc + part
        hits[...] += acc

    flags = (hits[...] > 0.0).astype(F32)
    used[...] = flags
    side = hits.shape[0] // 2
    most = jnp.maximum(jnp.sum(flags[:side], keepdims=True), jnp.sum(flags[side:], keepdims=True))
    mine[:SUB, :] = jnp.sum(mask[...].astype(F32).reshape(-1, *TILE), axis=0)
    mine[SUB:, :] = jnp.broadcast_to(most, TILE)
    met()
    copies = [remote(mine, theirs.at[o - 1], send_sem.at[o - 1], recv_sem.at[o - 1], lax.rem(me + o, n)) for o in range(1, n)]
    for c in copies:
        c.start()
    total[...] = jnp.zeros_like(total)

    @pl.loop(0, lines, step=SUB)
    def _(base):
        acc = None
        for r in range(0, SUB, 2):
            lhs, rhs = [], []
            for q in (base + r, base + r + 1):
                pick = down((slots, LANES)) == places[row(0, q), :]
                lhs.append(stack_rows([jnp.where(pick, values[row(i, q), :], 0.0) for i in range(len(planes))]))
                rhs.append(spot(LANES, 1, q))
            part = dot(stack_lanes(lhs).astype(BF16), stack_lanes(rhs).astype(BF16), COLS_A)
            acc = part if acc is None else acc + part
        total[...] += acc

    plane = lambda i: total[i * slots : (i + 1) * slots, :]
    high = plane(2).astype(jnp.int32)
    src_out[...] = ((high >> 3) * BYTE + plane(0).astype(jnp.int32)) * 2
    dst_out[...] = ((high & 7) * BYTE + plane(1).astype(jnp.int32)) * 2
    w_out[...] = (plane(3) + plane(4) + plane(5)) * 2.0
    for c in copies:
        c.wait()
    every = jnp.sum(mine[:SUB, :] + jnp.sum(theirs[:, :SUB, :], axis=0), keepdims=True)
    count[...] = jnp.maximum(jnp.broadcast_to(every, count.shape), 1.0)
    need[...] = jnp.maximum(mine[SUB:, :], jnp.max(theirs[:, SUB:, :], axis=0))


def local_kernel(chunk, backward, counts, src, dst, w, table, out, src_s, dst_s, sems, *accs):
    edges = Edges(0, counts[0], w, (src, dst), (src_s, dst_s), sems)
    edges.fetch()
    for a in accs:
        fill_zero(a)
    edges.walk(chunk, *((dst_s, src_s) if backward else (src_s, dst_s)), table, accs, True)

    @pl.loop(0, out.shape[0], step=STEP)
    def _(i):
        out[pl.ds(i, STEP), :] = functools.reduce(jnp.add, [a[pl.ds(i, STEP), :] for a in accs])


def forward_halo(chunk, edges, src_s, dst_s, from_prev, from_next, part, htab, accs, unpack):
    edges.fetch()
    unpack(from_prev, htab, 0)
    unpack(from_next, htab, htab.shape[0] // 4)
    copy_in(accs[0], part)
    for a in accs[1:]:
        fill_zero(a)
    edges.walk(chunk, src_s, dst_s, htab, accs, True)


def backward_halo(chunk, edges, src_s, dst_s, grad, back_prev, back_next, accs, wait, lists=None):
    for a in accs:
        fill_zero(a)
    edges.walk(chunk, dst_s, src_s, grad, accs, wait)
    split = accs[0].shape[0] // 2
    if lists is None:

        @pl.loop(0, back_prev.shape[0], step=BLOCK)
        def _(i):
            back_prev[pl.ds(i, BLOCK), :] = functools.reduce(jnp.add, [a[pl.ds(i, BLOCK), :] for a in accs])
            back_next[pl.ds(i, BLOCK), :] = functools.reduce(jnp.add, [a[pl.ds(split + i, BLOCK), :] for a in accs])
        return
    side = lists.shape[0] // 2
    half = (back_prev.shape[0] - side) // 3
    n = half // 2
    for k, out in enumerate((back_prev, back_next)):
        start = k * (split // 2)

        @pl.loop(0, half, step=n)
        def _(i):
            i = pl.multiple_of(i, n)
            pack_rows(out, i, half, *halves(accs, start + i, n), *halves(accs, start + half + i, n))

        out[3 * half : 3 * half + side, :] = lists[k * side : (k + 1) * side, :]


def padded(w, buf):
    low = w.shape[0] // SUB * SUB
    buf[low:, :] = jnp.zeros((buf.shape[0] - low, buf.shape[1]), F32)
    buf[0 : w.shape[0], :] = w[...]
    return buf[...].astype(BF16)


def hidden_kernel(chunk, counts, src, dst, w, send, from_prev, from_next, part, w2, hid, tab, to_prev, to_next, back, htab, tab_b, w2_pad, buf, idx, idx_sems, src_s, dst_s, sems, *accs):
    fetch = fetch_index(send, idx, idx_sems)
    for c in fetch:
        c.start()
    edges = Edges(counts[0], counts[1], w, (src, dst), (src_s, dst_s), sems)
    w2_b = padded(w2, w2_pad)
    per = send.shape[1] // LANES
    for i in range(2 * per):
        back[i : i + 1, :] = send[i // per : i // per + 1, (i % per) * LANES : (i % per + 1) * LANES] * 2
    forward_halo(chunk, edges, src_s, dst_s, from_prev, from_next, part, htab, accs, unpack_plain)

    @pl.loop(0, hid.shape[0], step=BLOCK)
    def _(i):
        even, odd = halves(accs, i, BLOCK)
        h = stack_lanes([jnp.maximum(even, 0.0), jnp.maximum(odd, 0.0)]).astype(BF16)
        hid[pl.ds(i, BLOCK), :] = h
        t = dot(h, w2_b, COLS_A).astype(BF16)
        tab_b[pl.ds(i, BLOCK), :] = t
        t = t.astype(F32)
        put_halves(tab, i, BLOCK, t[:, :LANES], t[:, LANES:])

    for c in fetch:
        c.wait()
    gather_packed(send, idx, tab_b, tab, buf, to_prev, to_next)


def loss_kernel(chunk, classes, counts, src, dst, w, src_back, lists, count, from_prev, from_next, part, labels, mask, loss, grad, back_prev, back_next, htab, src_s, dst_s, back_s, sems, *accs):
    edges = Edges(counts[0], counts[1], w, (src, dst, src_back), (src_s, dst_s, back_s), sems)
    forward_halo(chunk, edges, src_s, dst_s, from_prev, from_next, part, htab, accs, unpack_rows)
    lane = across(SQUARE)
    live = lane < classes - LANES
    scale = 1.0 / count[0:1, :]
    loss[...] = jnp.zeros_like(loss)

    @pl.loop(0, labels.shape[0] // 2)
    def _(pair):
        for b in (pair * 2, pair * 2 + 1):
            even, odd = halves(accs, b * LANES, LANES)
            label = spread(labels[pl.ds(b, 1), :])
            keep = spread(mask[pl.ds(b, 1), :]).astype(F32)
            odd = jnp.where(live, odd, -jnp.inf)
            top = jnp.max(jnp.maximum(even, odd), axis=1, keepdims=True)
            total = jnp.sum(jnp.exp(even - top) + jnp.exp(odd - top), axis=1, keepdims=True)
            norm = top + jnp.log(total)
            hit_even, hit_odd = lane == label, lane + LANES == label
            picked = jnp.where(hit_even, even, 0.0) + jnp.where(hit_odd, odd, 0.0)
            per_row = jnp.where(lane == 0, norm, 0.0) - picked
            loss[...] += jnp.sum((keep * per_row).reshape(LANES // SUB, *TILE), axis=0)
            d_even = (jnp.exp(even - norm) - hit_even.astype(F32)) * (keep * scale)
            d_odd = (jnp.exp(odd - norm) - hit_odd.astype(F32)) * (keep * scale)
            put_halves(grad, b * LANES, LANES, d_even, d_odd)

    backward_halo(chunk, edges, back_s, dst_s, grad, back_prev, back_next, accs, False, lists)


def take_returns(back, slots, counts, part, got_prev, got_next, accs):
    return_rows(back, slots, 0, counts[0], got_prev, accs)
    return_rows(back, slots, slots.shape[0] // 2, counts[1], got_next, accs)


def fetch_lines(lines, smem, sems):
    return [pltpu.make_async_copy(lines.at[i], smem.at[pl.ds(i * LANES, LANES)], sems.at[i]) for i in range(lines.shape[0])]


def middle_kernel(chunk, counts, src, dst, w, back, got_prev, got_next, part, hid, w2, grad_two, grad, back_prev, back_next, slots, n_back, returned, w2_pad, slot_s, slot_sems, src_s, dst_s, sems, *accs):
    edges = Edges(counts[0], counts[1], w, (src, dst), (src_s, dst_s), sems)
    edges.fetch()
    side = slots.shape[0] // 2
    half = (got_prev.shape[0] - side) // 3
    for k, got in enumerate((got_prev, got_next)):
        slot = got[3 * half :, :].astype(jnp.int32)
        slots[k * side : (k + 1) * side, :] = jnp.maximum(slot, 0) + (1 - k) * side * LANES
        n_back[k] = jnp.sum((slot >= 0).astype(F32)).astype(jnp.int32)
    w2_b = padded(w2, w2_pad)
    unpack_rows(got_prev, returned, 0, half)
    unpack_rows(got_next, returned, 2 * half, half)
    fetch = fetch_lines(slots, slot_s, slot_sems)
    for c in fetch:
        c.start()
    copy_in(accs[0], part)
    for a in accs[1:]:
        fill_zero(a)
    for c in fetch:
        c.wait()
    take_returns(back, slot_s, n_back, part, returned.at[pl.ds(0, 4 * half)], returned.at[pl.ds(4 * half, 4 * half)], accs)
    grad_two[...] = jnp.zeros_like(grad_two)

    @pl.loop(0, hid.shape[0], step=BLOCK)
    def _(i):
        even, odd = halves(accs, i, BLOCK)
        d_tab = stack_lanes([even, odd]).astype(BF16)
        h = hid[pl.ds(i, BLOCK), :]
        grad_two[...] += dot(d_tab, h, ROWS_A)
        d_hid = dot(d_tab, w2_b)
        d_pre = jnp.where(h > 0, d_hid, 0.0)
        put_halves(grad, i, BLOCK, d_pre[:, :LANES], d_pre[:, LANES:])

    backward_halo(chunk, edges, src_s, dst_s, grad, back_prev, back_next, accs, True)


def last_kernel(back, n_back, slots, got_prev, got_next, part, x, grad_one, slot_s, slot_sems, *accs):
    fetch = fetch_lines(slots, slot_s, slot_sems)
    for c in fetch:
        c.start()
    copy_in(accs[0], part)
    for a in accs[1:]:
        fill_zero(a)
    for c in fetch:
        c.wait()
    take_returns(back, slot_s, n_back, part, got_prev, got_next, accs)
    grad_one[...] = jnp.zeros_like(grad_one)

    @pl.loop(0, x.shape[0], step=BLOCK)
    def _(i):
        even, odd = halves(accs, i, BLOCK)
        d_tab = stack_lanes([even, odd]).astype(BF16)
        grad_one[...] += dot(x[pl.ds(i, BLOCK), :], d_tab, ROWS_A)


def call(body, name, outs, ins, scratch, out_specs=None, collective=None, vmem=14):
    extra = {} if collective is None else dict(collective_id=collective, has_side_effects=True)
    return pl.pallas_call(
        body, name=name, out_shape=outs, in_specs=ins, out_specs=out_specs or jax.tree.map(lambda _: VMEM, outs),
        scratch_shapes=[pltpu.VMEM(s, F32) if isinstance(s, tuple) else s for s in scratch],
        compiler_params=pltpu.CompilerParams(vmem_limit_bytes=vmem * 2**20, **extra),
        cost_estimate=pl.CostEstimate(flops=10**10, bytes_accessed=10**7, transcendentals=0),
    )


def solution(mesh):
    num_dev = mesh.shape[AXIS]
    to_next = [(d, (d + 1) % num_dev) for d in range(num_dev)]
    to_prev = [(d, (d - 1) % num_dev) for d in range(num_dev)]

    def step(x, w_one, w_two, send, edge_src, edge_dst, edge_w, labels, mask):
        rows, halo, edges, classes = x.shape[0], send.shape[1], edge_src.shape[0], w_two.shape[1]
        tab, half, w2_pad = (2 * rows, LANES), (2 * halo, LANES), (2 * LANES, 2 * LANES)
        sds = jax.ShapeDtypeStruct
        tab_f = sds(tab, F32)
        half_b, pack_b = sds((halo, 2 * LANES), BF16), sds((3 * halo // 2, LANES), BF16)
        tab_b = pltpu.VMEM((rows, 2 * LANES), BF16)
        one = sds(TILE, F32)
        dma = pltpu.SemaphoreType.DMA
        chunk_l, chunk_h = 64, 32
        lines = edges // LANES
        slots = lines + 8
        side = halo // LANES
        w2 = w_two.T
        mask = mask.reshape(-1, LANES)
        labels = labels.reshape(-1, LANES)
        packed = jnp.concatenate([(edge_src * 2048 + edge_dst).astype(F32), edge_w]).reshape(2 * lines, LANES)
        ints = sds((slots, LANES), jnp.int32)
        sided = sds((2 * side, LANES), F32)
        src, dst, w_lines, used, counts, count, need = call(
            functools.partial(prep_kernel, num_dev, PREP_CHUNK, rows), "prep",
            [ints, ints, sds((slots, LANES), F32), sided, sds((2,), jnp.int32), one, one], [VMEM] * 2,
            [(6 * slots, LANES), (6 * lines, LANES), pltpu.VMEM((4 * lines, LANES), jnp.int32), sided.shape, (16, LANES), (num_dev - 1, 16, LANES)]
            + [dma((num_dev - 1,))] * 2,
            out_specs=[VMEM] * 4 + [SMEM, VMEM, VMEM], vmem=8, collective=0,
        )(packed, mask)

        def run(limit):
            compact = limit < halo
            pack_f, half_f = sds((3 * limit // 2 + side, LANES), F32), sds((2 * limit, LANES), F32)
            list_s = [pltpu.SMEM((halo,), jnp.int32), dma((side,))]
            tab_one, to_p, to_n, w, src_back, lists = call(
                functools.partial(first_kernel, compact, halo), "first", [tab_f, half_b, half_b, sds((slots * LANES, LANES), F32), ints, sided],
                [VMEM] * 3 + [SMEM] + [VMEM] * 3, [tab_b, half] + list_s, vmem=8,
            )(x, w_one, send, counts, src, w_lines, used)
            from_prev = lax.ppermute(to_n, AXIS, to_next)
            from_next = lax.ppermute(to_p, AXIS, to_prev)
            flat, flat_dst, flat_back = src.reshape(-1), dst.reshape(-1), src_back.reshape(-1)

            walk = [SMEM, ANY, ANY, VMEM]
            index = pltpu.SMEM((slots * LANES,), jnp.int32)
            walk_s = lambda n: [index] * n + [dma((n, slots * LANES // SEGMENT))]
            slot_s = [pltpu.SMEM((2 * halo,), jnp.int32), dma((2 * side,))]
            local, local_back = (
                call(functools.partial(local_kernel, chunk_l, back), "local_edges", tab_f, walk + [VMEM], walk_s(2) + [tab] * 4)
                for back in (False, True)
            )
            part = local(counts, flat, flat_dst, w, tab_one)
            hid, tab_two, to_p, to_n, back = call(
                functools.partial(hidden_kernel, chunk_h), "hidden",
                [sds((rows, 2 * LANES), BF16), tab_f, pack_b, pack_b, sds((2 * side, LANES), jnp.int32)],
                walk + [VMEM] * 5, [tab, tab_b, w2_pad, half] + list_s + walk_s(2) + [tab] * 4,
            )(counts, flat, flat_dst, w, send, from_prev, from_next, part, w2)
            from_prev = lax.ppermute(to_n, AXIS, to_next)
            from_next = lax.ppermute(to_p, AXIS, to_prev)
            back = back.reshape(-1)
            part = local(counts, flat, flat_dst, w, tab_two)
            loss, grad, to_p, to_n = call(
                functools.partial(loss_kernel, chunk_h, classes), "loss", [one, tab_f, pack_f, pack_f],
                walk + [ANY] + [VMEM] * 7, [tab] + walk_s(3) + [tab] * 4,
            )(counts, flat, flat_dst, w, flat_back, lists, count, from_prev, from_next, part, labels, mask)
            got_prev = lax.ppermute(to_p, AXIS, to_prev)
            got_next = lax.ppermute(to_n, AXIS, to_next)
            part = local_back(counts, flat, flat_dst, w, grad)
            grad_two, grad, to_p, to_n, slot, n_back = call(
                functools.partial(middle_kernel, chunk_h), "middle",
                [sds(w2_pad, F32), tab_f, half_f, half_f, sds((2 * side, LANES), jnp.int32), sds((2,), jnp.int32)],
                walk + [SMEM] + [VMEM] * 5, [(4 * limit, LANES), w2_pad] + slot_s + walk_s(2) + [tab] * 4, out_specs=[VMEM] * 5 + [SMEM],
            )(counts, flat_back, flat_dst, w, back, got_prev, got_next, part, hid, w2)
            got_prev = lax.ppermute(to_p, AXIS, to_prev)
            got_next = lax.ppermute(to_n, AXIS, to_next)
            part = local_back(counts, flat, flat_dst, w, grad)
            grad_one = call(
                last_kernel, "last", sds((x.shape[1], 2 * LANES), F32), [SMEM, SMEM, ANY] + [VMEM] * 4, slot_s + [tab] * 4
            )(back, n_back, slot, got_prev, got_next, part, x)
            return grad_one, grad_two, loss

        few = halo * 5 // 8
        grad_one, grad_two, loss = lax.cond(need[0, 0] > few, lambda: run(halo), lambda: run(few))
        unit = SUB * num_dev
        lines = 2 * (x.shape[1] + -(-classes // SUB) * SUB) + SUB
        lines = -(-lines // unit) * unit
        grad_one, grad_two, mean = call(
            functools.partial(reduce_kernel, num_dev), "reduce", [sds(grad_one.shape, F32), sds((classes, 2 * LANES), F32), sds((1, 1), F32)],
            [VMEM] * 4, [(lines, LANES), (lines, LANES), (lines // 2, LANES), (num_dev // 2 - 1, lines // num_dev, LANES), dma((2, num_dev))],
            collective=1, vmem=8,
        )(grad_one, grad_two, loss, count)
        return mean.reshape(()), grad_one, grad_two.T

    row = P(AXIS)
    return jax.shard_map(
        step, mesh=mesh, in_specs=(row, P(), P(), row, row, row, row, row, row), out_specs=(P(), P(), P()), check_vma=False
    )
```

```python
import functools

import jax
import jax.numpy as jnp
from jax import lax
from jax.experimental import pallas as pl
from jax.experimental.pallas import tpu as pltpu
from jax.sharding import PartitionSpec as P

AXIS = "graph"
LANES = 128
ROWS_A = (((0,), (0,)), ((), ()))
COLS_A = (((1,), (1,)), ((), ()))
F32, BF16 = jnp.float32, jnp.bfloat16
VMEM = pl.BlockSpec(memory_space=pltpu.VMEM)
SMEM = pl.BlockSpec(memory_space=pltpu.SMEM)
ANY = pl.BlockSpec(memory_space=pl.ANY)
STEP = 512
BLOCK = 256
BYTE = 256
SUB = 8
TILE = (SUB, LANES)
SQUARE = (LANES, LANES)
PREP_CHUNK = 64
SEGMENT = 1024
MESH = pl.DeviceIdType.MESH


def dot(a, b, dims=(((1,), (0,)), ((), ()))):
    return lax.dot_general(a, b, dims, preferred_element_type=F32)


def fill_zero(ref):
    zero = jnp.zeros((BLOCK, LANES), F32)

    @pl.loop(0, ref.shape[0], step=BLOCK)
    def _(i):
        ref[pl.ds(i, BLOCK), :] = zero


def copy_in(dst, src):
    @pl.loop(0, dst.shape[0], step=STEP)
    def _(i):
        dst[pl.ds(i, STEP), :] = src[pl.ds(i, STEP), :].astype(F32)


class Edges:
    def __init__(self, first, last, w, arrays, smem, sems):
        self.first, self.last, self.w = first, last, w
        self.pairs = tuple(zip(arrays, smem))
        self.sems = sems

    def copies(self, seg):
        part = pl.ds(pl.multiple_of(seg * SEGMENT, SEGMENT), SEGMENT)
        return [pltpu.make_async_copy(a.at[part], b.at[part], self.sems.at[i, seg]) for i, (a, b) in enumerate(self.pairs)]

    def fetch(self):
        per = SEGMENT // PREP_CHUNK
        for seg in range(self.pairs[0][1].shape[0] // SEGMENT):

            @pl.when(jnp.logical_and(seg * per < self.last, (seg + 1) * per > self.first))
            def _():
                for c in self.copies(seg):
                    c.start()

    def walk(self, chunk, from_idx, to_idx, table, accs, wait):
        group, per, ratio = len(accs), SEGMENT // chunk, PREP_CHUNK // chunk
        first, last = self.first * ratio, self.last * ratio

        def body(c, _):
            base = c * chunk
            w_chunk = self.w.at[pl.ds(pl.multiple_of(base, chunk), chunk)]
            for g in range(0, chunk, group):
                pend = []
                for u in range(group):
                    k = base + g + u
                    s = pl.multiple_of(from_idx[k], 2)
                    d = pl.multiple_of(to_idx[k], 2)
                    pend.append((d, accs[u][pl.ds(d, 2), :] + table[pl.ds(s, 2), :] * w_chunk[g + u : g + u + 1, :]))
                for u in range(group):
                    accs[u][pl.ds(pend[u][0], 2), :] = pend[u][1]
            return 0

        if not wait:
            lax.fori_loop(first, last, body, 0)
            return

        def segment(seg, _):
            for c in self.copies(seg):
                c.wait()
            lax.fori_loop(jnp.maximum(first, seg * per), jnp.minimum(last, (seg + 1) * per), body, 0)
            return 0

        lax.fori_loop(first // per, (last + per - 1) // per, segment, 0)


def one_hot_rows(idx, which, start, table):
    lane = across(SQUARE)
    hot = []
    for q in range(2):
        want = spread(idx[which : which + 1, pl.ds(pl.multiple_of(start + q * LANES, LANES), LANES)])
        hot.append(
            stack_lanes([jnp.where(want == lane + LANES * j, 1.0, 0.0).astype(BF16) for j in range(table.shape[0] // LANES)])
        )
    return dot(stack_rows(hot), table[...])


def low_lanes(rows):
    return across((rows, LANES)) < LANES // 2


def swap_lanes(v):
    return pltpu.roll(v, LANES // 2, 1)


def fetch_index(send, idx, sems):
    parts = [pl.ds(i, LANES) for i in range(0, send.shape[1], LANES)]
    return [pltpu.make_async_copy(send.at[1, p], idx.at[p], sems.at[i]) for i, p in enumerate(parts)]


def gather_block(send, idx, i, table_b, table, buf):
    got = one_hot_rows(send, 0, i, table_b)
    out = buf.at[pl.ds(pl.multiple_of(2 * i, 512), 512)]
    for u in range(BLOCK):
        s = pl.multiple_of(idx[i + u] * 2, 2)
        out[2 * u : 2 * u + 2, :] = table[pl.ds(s, 2), :]
    return got


def gather_rows(send, idx, table_b, table, buf, to_prev, to_next):
    @pl.loop(0, to_prev.shape[0], step=BLOCK)
    def _(i):
        i = pl.multiple_of(i, BLOCK)
        to_prev[pl.ds(i, BLOCK), :] = gather_block(send, idx, i, table_b, table, buf).astype(BF16)

    @pl.loop(0, to_next.shape[0], step=BLOCK)
    def _(i):
        to_next[pl.ds(pl.multiple_of(i, BLOCK), BLOCK), :] = stack_lanes(halves([buf], i, BLOCK)).astype(BF16)


def pack_rows(out, i, half, a_even, a_odd, b_even, b_odd):
    n = a_even.shape[0]
    out[pl.ds(i, n), :] = a_even.astype(out.dtype)
    out[pl.ds(half + i, n), :] = b_even.astype(out.dtype)
    out[pl.ds(2 * half + i, n), :] = jnp.where(low_lanes(n), a_odd, swap_lanes(b_odd)).astype(out.dtype)


def gather_packed(send, idx, table_b, table, buf, to_prev, to_next):
    half = to_prev.shape[0] // 3

    @pl.loop(0, half, step=BLOCK)
    def _(i):
        i = pl.multiple_of(i, BLOCK)
        a = gather_block(send, idx, i, table_b, table, buf)
        b = gather_block(send, idx, half + i, table_b, table, buf)
        pack_rows(to_prev, i, half, a[:, :LANES], a[:, LANES:], b[:, :LANES], b[:, LANES:])

    @pl.loop(0, half, step=BLOCK)
    def _(i):
        i = pl.multiple_of(i, BLOCK)
        pack_rows(to_next, i, half, *halves([buf], i, BLOCK), *halves([buf], half + i, BLOCK))


def unpack_rows(got, table, start, half=None):
    half = got.shape[0] // 3 if half is None else half
    n = half // 2

    @pl.loop(0, half, step=n)
    def _(i):
        i = pl.multiple_of(i, n)
        a, b, both = (got[pl.ds(k + i, n), :].astype(F32) for k in (0, half, 2 * half))
        put_halves(table, start + i, n, a, jnp.where(low_lanes(n), both, 0.0))
        put_halves(table, start + half + i, n, b, jnp.where(low_lanes(n), swap_lanes(both), 0.0))


def unpack_plain(got, table, start):
    @pl.loop(0, got.shape[0], step=BLOCK)
    def _(i):
        t = got[pl.ds(i, BLOCK), :].astype(F32)
        put_halves(table, start + i, BLOCK, t[:, :LANES], t[:, LANES:])


def spread(row):
    return jnp.transpose(jnp.broadcast_to(row, SQUARE))


def return_rows(back, slots, start, count, vals, accs, chunk=32):
    group = len(accs)

    def body(c, _):
        block = vals.at[pl.ds(pl.multiple_of(c * 2 * chunk, 2 * chunk), 2 * chunk)]
        for g in range(0, chunk, group):
            pend = []
            for u in range(group):
                d = pl.multiple_of(back[slots[start + c * chunk + g + u]], 2)
                pend.append((d, accs[u][pl.ds(d, 2), :] + block[2 * (g + u) : 2 * (g + u) + 2, :]))
            for u in range(group):
                accs[u][pl.ds(pend[u][0], 2), :] = pend[u][1]
        return 0

    lax.fori_loop(0, (count + chunk - 1) // chunk, body, 0)


def group(i, n, which):
    return pl.ds(2 * i + which, n, stride=2), slice(None)


def halves(accs, i, n):
    return [functools.reduce(jnp.add, [a[group(i, n, k)] for a in accs]) for k in range(2)]


def put_halves(table, i, n, *parts):
    for k, part in enumerate(parts):
        table[group(i, n, k)] = part


def stack_rows(parts):
    return jnp.concatenate(parts, axis=0)


def stack_lanes(parts):
    return jnp.concatenate(parts, axis=1)


def down(shape):
    return lax.broadcasted_iota(jnp.int32, shape, 0)


def across(shape):
    return lax.broadcasted_iota(jnp.int32, shape, 1)


def prefix(mask, above):
    m = mask.astype(BF16)
    before = (down(SQUARE) < across(SQUARE)).astype(BF16)
    return dot(m, before) + dot(above, dot(m, jnp.ones(SQUARE, BF16)).astype(BF16))


def rank_halo(halo, counts, src, used, src_back, lists):
    lines = used.shape[0]
    side = lines // 2
    i, j = down((lines, lines)), across((lines, lines))
    above = jnp.logical_and(j < i, (j >= side) == (i >= side)).astype(F32).astype(BF16)
    rank = prefix(used[...], above).astype(jnp.int32)
    low, high = rank & (LANES - 1), rank >> 7
    table = stack_rows([low.astype(F32), high.astype(F32)]).astype(BF16)

    quad = 4

    def four(c, _):
        slot = [src[pl.ds(c * quad + q, 1), :] >> 1 for q in range(quad)]
        spots = stack_lanes([(down(SQUARE) == (t & (LANES - 1))).astype(F32) for t in slot]).astype(BF16)
        got = dot(table, spots)
        h = stack_lanes(slot) >> 7
        got = jnp.where(down(got[:lines].shape) == h, got[:lines] + LANES * got[lines:], 0.0)
        got = (jnp.sum(got, axis=0, keepdims=True).astype(jnp.int32) + jnp.where(h >= side, halo, 0)) * 2
        for q in range(quad):
            src_back[pl.ds(c * quad + q, 1), :] = got[:, q * LANES : (q + 1) * LANES]
        return 0

    ratio = quad * LANES // PREP_CHUNK
    lax.fori_loop(counts[0] // ratio, (counts[1] + ratio - 1) // ratio, four, 0)
    for k in range(2):
        acc = jnp.zeros((24, LANES), F32)
        for hh in range(side):
            q = k * side + hh
            pick = jnp.where(down(TILE) == high[q : q + 1, :], used[q : q + 1, :], 0.0)
            lhs = stack_rows([pick * across(TILE).astype(F32), pick * hh, pick]).astype(BF16)
            acc += dot(lhs, (down(SQUARE) == low[q : q + 1, :]).astype(F32).astype(BF16), COLS_A)
        slots = acc[0:8] + LANES * acc[8:16]
        lists[k * side : (k + 1) * side, :] = jnp.where(acc[16:24] > 0.0, slots[:side], -1.0)


def first_kernel(compact, halo, x, w1, send, counts, src, w, used, tab, to_prev, to_next, w_out, src_back, lists, tab_b, buf, idx, sems):
    fetch = fetch_index(send, idx, sems)
    for c in fetch:
        c.start()
    rows = x.shape[0]
    w1_b = w1[...].astype(BF16)

    @pl.loop(0, rows, step=BLOCK)
    def _(i):
        t = dot(x[pl.ds(i, BLOCK), :], w1_b).astype(BF16)
        tab_b[pl.ds(i, BLOCK), :] = t
        t = t.astype(F32)
        put_halves(tab, i, BLOCK, t[:, :LANES], t[:, LANES:])

    @pl.loop(0, w.shape[0] // SUB)
    def _(r):
        for q in range(SUB):
            w_out[pl.ds(pl.multiple_of((r * SUB + q) * LANES, LANES), LANES), :] = spread(w[pl.ds(r * SUB + q, 1), :])

    src_back[...] = src[...]
    if compact:
        rank_halo(halo, counts, src, used, src_back, lists)
    else:
        line = down(lists.shape)
        line = jnp.where(line >= lists.shape[0] // 2, line - lists.shape[0] // 2, line)
        lists[...] = (line * LANES + across(lists.shape)).astype(F32)
    for c in fetch:
        c.wait()
    gather_rows(send, idx, tab_b, tab, buf, to_prev, to_next)


def greet(n):
    me = lax.axis_index(AXIS)
    barrier = pltpu.get_barrier_semaphore()
    for o in range(1, n):
        pl.semaphore_signal(barrier, inc=1, device_id=(lax.rem(me + o, n),), device_id_type=MESH)
    return me, lambda: pl.semaphore_wait(barrier, n - 1)


def remote(src, dst, send_sem, recv_sem, peer):
    return pltpu.make_async_remote_copy(
        src_ref=src, dst_ref=dst, send_sem=send_sem, recv_sem=recv_sem, device_id=(peer,), device_id_type=MESH
    )


def reduce_kernel(n, one, two, loss, count, one_out, two_out, mean, work, full, got_pair, got_rest, sems):
    me = lax.axis_index(AXIS)
    chips, core = n // 2, lax.rem(me, 2)
    chip = lax.div(me, 2)
    pair = me + 1 - 2 * core
    others = [lax.rem(chip + o, chips) for o in range(1, chips)]
    barrier = pltpu.get_barrier_semaphore()
    for p in [pair] + [2 * c + core for c in others]:
        pl.semaphore_signal(barrier, inc=1, device_id=(p,), device_id_type=MESH)
    classes = two_out.shape[0]
    lines = -(-classes // SUB) * SUB
    top, wide = one.shape
    work[0:top, :] = one[:, :LANES]
    work[top : 2 * top, :] = one[:, LANES:]
    work[2 * top : 2 * top + lines, :] = two[:lines, :LANES]
    work[2 * top + lines : 2 * top + 2 * lines, :] = two[:lines, LANES:]
    tail = 2 * top + 2 * lines
    work[tail : tail + SUB, :] = loss[...]
    work[tail + SUB :, :] = jnp.zeros((work.shape[0] - tail - SUB, LANES), F32)
    pl.semaphore_wait(barrier, chips)

    half = work.shape[0] // 2
    piece = half // chips
    spot = lambda c, k: pl.ds(pl.multiple_of(k * half + c * piece, SUB), piece)
    link = lambda kind, o, src, dst, peer: remote(src, dst, sems.at[0, kind * chips + o], sems.at[1, kind * chips + o], peer)
    order = list(enumerate(others + [chip]))
    swap = [link(0, o, work.at[spot(c, 1 - core)], got_pair.at[pl.ds(o * piece, piece)], pair) for o, c in order]
    for c in swap:
        c.start()
    scatter = [link(1, o, work.at[spot(c, core)], got_rest.at[o], 2 * c + core) for o, c in order[:-1]]
    for o, c in order:
        swap[o].wait_recv()
        work[spot(c, core), :] += got_pair[o * piece : (o + 1) * piece, :]
        if o:
            scatter[o - 1].start()
    for c in scatter:
        c.wait_recv()
    own = spot(chip, core)
    work[own, :] += jnp.sum(got_rest[...], axis=0)
    full[own, :] = work[own, :]
    for c in swap + scatter:
        c.wait_send()
    gather = [link(2, o, work.at[own], full.at[own], 2 * c + core) for o, c in order[:-1]]
    for c in gather:
        c.start()
    forward = [link(3, chips - 1, work.at[own], full.at[own], pair)]
    forward[0].start()
    for o, _ in order[:-1]:
        gather[o].wait_recv()
        came = spot(lax.rem(chip + chips - 1 - o, chips), core)
        forward.append(link(3, o, full.at[came], full.at[came], pair))
        forward[-1].start()
    for c in gather:
        c.wait_send()
    for c in forward:
        c.wait()
    one_out[:, :LANES] = full[0:top, :]
    one_out[:, LANES:] = full[top : 2 * top, :]
    two_out[:, :LANES] = full[2 * top : 2 * top + classes, :]
    two_out[:, LANES:] = full[2 * top + lines : 2 * top + lines + classes, :]
    mean[...] = jnp.sum(full[tail : tail + SUB, :], keepdims=True) / count[0:1, 0:1]


def prep_kernel(n, chunk, rows, packed, weight, mask, src_out, dst_out, w_out, used, counts, count, need, total, values, places, hits, mine, theirs, send_sem, recv_sem):
    me, met = greet(n)
    lines, slots = packed.shape[0], src_out.shape[0]
    src, d, w = packed[...] >> 11, packed[...] & 2047, weight[...]
    live = w != 0.0
    halo = src >= rows
    above = (across((lines, lines)) < down((lines, lines))).astype(F32).astype(BF16)
    is_local, is_halo = jnp.logical_and(live, jnp.logical_not(halo)), jnp.logical_and(live, halo)
    rank = lambda m: prefix(m.astype(F32), above).astype(jnp.int32)
    n_local = jnp.sum(is_local.astype(F32)).astype(jnp.int32)
    n_halo = jnp.sum(is_halo.astype(F32)).astype(jnp.int32)
    local_chunks = (n_local + chunk - 1) // chunk
    counts[0] = local_chunks
    counts[1] = local_chunks + (n_halo + chunk - 1) // chunk
    pos = jnp.where(is_local, rank(is_local), jnp.where(is_halo, rank(is_halo) + local_chunks * chunk, -1))
    s = jnp.where(halo, src - rows, src)
    half_w = w * 0.5
    w_a = half_w.astype(BF16).astype(F32)
    w_b = (half_w - w_a).astype(BF16).astype(F32)
    w_c = half_w - w_a - w_b
    high = ((s >> 8) * 8 + (d >> 8)).astype(F32)
    planes = [(s % BYTE).astype(F32), (d % BYTE).astype(F32), high, w_a, w_b, w_c]
    for i, p in enumerate(planes):
        values[i * lines : (i + 1) * lines, :] = p
    for i, p in enumerate((pos >> 7, pos & (LANES - 1), jnp.where(is_halo, s >> 7, -1), s & (LANES - 1))):
        places[i * lines : (i + 1) * lines, :] = p
    row = lambda i, q: pl.ds(i * lines + q, 1)
    spot = lambda size, i, q: (down((size, LANES)) == places[row(i, q), :]).astype(F32)
    hits[...] = jnp.zeros_like(hits)

    @pl.loop(0, lines, step=SUB)
    def _(base):
        acc = None
        for r in range(0, SUB, 2):
            lhs = stack_lanes([spot(hits.shape[0], 2, base + q) for q in (r, r + 1)]).astype(BF16)
            rhs = stack_lanes([spot(LANES, 3, base + q) for q in (r, r + 1)]).astype(BF16)
            part = dot(lhs, rhs, COLS_A)
            acc = part if acc is None else acc + part
        hits[...] += acc

    flags = (hits[...] > 0.0).astype(F32)
    used[...] = flags
    side = hits.shape[0] // 2
    most = jnp.maximum(jnp.sum(flags[:side], keepdims=True), jnp.sum(flags[side:], keepdims=True))
    mine[:1, :] = jnp.sum(mask[...].astype(F32), axis=0, keepdims=True)
    mine[1:, :] = jnp.broadcast_to(most, (1, LANES))
    met()
    copies = [remote(mine, theirs.at[o - 1], send_sem.at[o - 1], recv_sem.at[o - 1], lax.rem(me + o, n)) for o in range(1, n)]
    for c in copies:
        c.start()
    total[...] = jnp.zeros_like(total)

    @pl.loop(0, lines, step=SUB)
    def _(base):
        acc = None
        for r in range(0, SUB, 2):
            lhs, rhs = [], []
            for q in (base + r, base + r + 1):
                pick = down((slots, LANES)) == places[row(0, q), :]
                lhs.append(stack_rows([jnp.where(pick, values[row(i, q), :], 0.0) for i in range(len(planes))]))
                rhs.append(spot(LANES, 1, q))
            part = dot(stack_lanes(lhs).astype(BF16), stack_lanes(rhs).astype(BF16), COLS_A)
            acc = part if acc is None else acc + part
        total[...] += acc

    plane = lambda i: total[i * slots : (i + 1) * slots, :]
    high = plane(2).astype(jnp.int32)
    src_out[...] = ((high >> 3) * BYTE + plane(0).astype(jnp.int32)) * 2
    dst_out[...] = ((high & 7) * BYTE + plane(1).astype(jnp.int32)) * 2
    w_out[...] = (plane(3) + plane(4) + plane(5)) * 2.0
    for c in copies:
        c.wait()
    every = jnp.sum(mine[:1, :] + jnp.sum(theirs[:, :1, :], axis=0), keepdims=True)
    count[...] = jnp.maximum(jnp.broadcast_to(every, count.shape), 1.0)
    need[...] = jnp.broadcast_to(jnp.maximum(mine[1:, :], jnp.max(theirs[:, 1:, :], axis=0)), need.shape)


def local_kernel(chunk, backward, counts, src, dst, w, table, out, src_s, dst_s, sems, *accs):
    edges = Edges(0, counts[0], w, (src, dst), (src_s, dst_s), sems)
    edges.fetch()
    for a in accs:
        fill_zero(a)
    edges.walk(chunk, *((dst_s, src_s) if backward else (src_s, dst_s)), table, accs, True)

    @pl.loop(0, out.shape[0], step=STEP)
    def _(i):
        out[pl.ds(i, STEP), :] = functools.reduce(jnp.add, [a[pl.ds(i, STEP), :] for a in accs])


def forward_halo(chunk, edges, src_s, dst_s, from_prev, from_next, part, htab, accs, unpack):
    edges.fetch()
    unpack(from_prev, htab, 0)
    unpack(from_next, htab, htab.shape[0] // 4)
    copy_in(accs[0], part)
    for a in accs[1:]:
        fill_zero(a)
    edges.walk(chunk, src_s, dst_s, htab, accs, True)


def backward_halo(limit, chunk, edges, src_s, dst_s, grad, back_prev, back_next, accs, wait, lists=None):
    split = accs[0].shape[0] // 2
    for a in accs:
        for start in (0, split):
            fill_zero(a.at[pl.ds(start, limit * 2)])
    edges.walk(chunk, dst_s, src_s, grad, accs, wait)
    if lists is None:

        @pl.loop(0, back_prev.shape[0], step=BLOCK)
        def _(i):
            back_prev[pl.ds(i, BLOCK), :] = functools.reduce(jnp.add, [a[pl.ds(i, BLOCK), :] for a in accs])
            back_next[pl.ds(i, BLOCK), :] = functools.reduce(jnp.add, [a[pl.ds(split + i, BLOCK), :] for a in accs])
        return
    side = lists.shape[0] // 2
    half = (back_prev.shape[0] - side) // 3
    n = half // 2
    for k, out in enumerate((back_prev, back_next)):
        start = k * (split // 2)

        @pl.loop(0, half, step=n)
        def _(i):
            i = pl.multiple_of(i, n)
            pack_rows(out, i, half, *halves(accs, start + i, n), *halves(accs, start + half + i, n))

        out[3 * half : 3 * half + side, :] = lists[k * side : (k + 1) * side, :]


def padded(w, buf):
    low = w.shape[0] // SUB * SUB
    buf[low:, :] = jnp.zeros((buf.shape[0] - low, buf.shape[1]), F32)
    buf[0 : w.shape[0], :] = w[...]
    return buf[...].astype(BF16)


def hidden_kernel(chunk, counts, src, dst, w, send, from_prev, from_next, part, w2, hid, tab, to_prev, to_next, back, htab, tab_b, w2_pad, buf, idx, idx_sems, src_s, dst_s, sems, *accs):
    fetch = fetch_index(send, idx, idx_sems)
    for c in fetch:
        c.start()
    edges = Edges(counts[0], counts[1], w, (src, dst), (src_s, dst_s), sems)
    w2_b = padded(w2, w2_pad)
    per = send.shape[1] // LANES
    for i in range(2 * per):
        back[i : i + 1, :] = send[i // per : i // per + 1, (i % per) * LANES : (i % per + 1) * LANES] * 2
    forward_halo(chunk, edges, src_s, dst_s, from_prev, from_next, part, htab, accs, unpack_plain)

    @pl.loop(0, hid.shape[0], step=STEP)
    def _(i):
        even, odd = halves(accs, i, STEP)
        h = stack_lanes([jnp.maximum(even, 0.0), jnp.maximum(odd, 0.0)]).astype(BF16)
        hid[pl.ds(i, STEP), :] = h
        t = dot(h, w2_b, COLS_A).astype(BF16)
        tab_b[pl.ds(i, STEP), :] = t
        t = t.astype(F32)
        put_halves(tab, i, STEP, t[:, :LANES], t[:, LANES:])

    for c in fetch:
        c.wait()
    gather_packed(send, idx, tab_b, tab, buf, to_prev, to_next)


def loss_kernel(limit, quad, chunk, classes, counts, src, dst, w, src_back, lists, count, from_prev, from_next, part, labels, mask, loss, grad, back_prev, back_next, htab, src_s, dst_s, back_s, sems, *accs):
    edges = Edges(counts[0], counts[1], w, (src, dst, src_back), (src_s, dst_s, back_s), sems)
    forward_halo(chunk, edges, src_s, dst_s, from_prev, from_next, part, htab, accs, unpack_rows)
    lane = across(SQUARE)
    live = lane < classes - LANES
    scale = 1.0 / count[0:1, :]
    loss[...] = jnp.zeros_like(loss)

    @pl.loop(0, labels.shape[0], step=quad)
    def _(first):
        for b in [first + q for q in range(quad)]:
            even, odd = halves(accs, b * LANES, LANES)
            odd = jnp.where(live, odd, -jnp.inf)
            keep = spread(mask[pl.ds(b, 1), :])
            label = jnp.where(keep > 0, spread(labels[pl.ds(b, 1), :]), -1)
            hit_even, hit_odd = lane == label, lane + LANES == label
            top = jnp.max(jnp.maximum(even, odd), axis=1, keepdims=True)
            exp_even, exp_odd = jnp.exp(even - top), jnp.exp(odd - top)
            total = jnp.sum(exp_even + exp_odd, axis=1, keepdims=True)
            norm = jnp.where(jnp.logical_and(lane == 0, keep > 0), top + jnp.log(total), 0.0)
            per_row = norm - jnp.where(hit_even, even, jnp.where(hit_odd, odd, 0.0))
            loss[...] += jnp.sum(per_row.reshape(LANES // SUB, *TILE), axis=0)
            share = keep.astype(F32) * scale * (1.0 / total)
            put_halves(
                grad, b * LANES, LANES, *(e * share - jnp.where(hit, scale, 0.0) for e, hit in ((exp_even, hit_even), (exp_odd, hit_odd)))
            )

    backward_halo(limit, chunk, edges, back_s, dst_s, grad, back_prev, back_next, accs, False, lists)


def take_returns(back, slots, counts, part, got_prev, got_next, accs):
    return_rows(back, slots, 0, counts[0], got_prev, accs)
    return_rows(back, slots, slots.shape[0] // 2, counts[1], got_next, accs)


def fetch_lines(lines, smem, sems):
    return [pltpu.make_async_copy(lines.at[i], smem.at[pl.ds(i * LANES, LANES)], sems.at[i]) for i in range(lines.shape[0])]


def middle_kernel(limit, chunk, counts, src, dst, w, back, got_prev, got_next, part, hid, w2, grad_two, grad, back_prev, back_next, slots, n_back, returned, w2_pad, slot_s, slot_sems, src_s, dst_s, sems, *accs):
    edges = Edges(counts[0], counts[1], w, (src, dst), (src_s, dst_s), sems)
    edges.fetch()
    side = slots.shape[0] // 2
    half = (got_prev.shape[0] - side) // 3
    for k, got in enumerate((got_prev, got_next)):
        slot = got[3 * half :, :].astype(jnp.int32)
        slots[k * side : (k + 1) * side, :] = jnp.maximum(slot, 0) + (1 - k) * side * LANES
        n_back[k] = jnp.sum((slot >= 0).astype(F32)).astype(jnp.int32)
    w2_b = padded(w2, w2_pad)
    unpack_rows(got_prev, returned, 0, half)
    unpack_rows(got_next, returned, 2 * half, half)
    fetch = fetch_lines(slots, slot_s, slot_sems)
    for c in fetch:
        c.start()
    copy_in(accs[0], part)
    for a in accs[1:]:
        fill_zero(a)
    for c in fetch:
        c.wait()
    take_returns(back, slot_s, n_back, part, returned.at[pl.ds(0, 4 * half)], returned.at[pl.ds(4 * half, 4 * half)], accs)
    grad_two[...] = jnp.zeros_like(grad_two)

    @pl.loop(0, hid.shape[0], step=STEP)
    def _(i):
        even, odd = halves(accs, i, STEP)
        d_tab = stack_lanes([even, odd]).astype(BF16)
        h = hid[pl.ds(i, STEP), :]
        grad_two[...] += dot(d_tab, h, ROWS_A)
        d_hid = dot(d_tab, w2_b)
        d_pre = jnp.where(h > 0, d_hid, 0.0)
        put_halves(grad, i, STEP, d_pre[:, :LANES], d_pre[:, LANES:])

    backward_halo(limit, chunk, edges, src_s, dst_s, grad, back_prev, back_next, accs, True)


def last_kernel(back, n_back, slots, got_prev, got_next, part, x, grad_one, slot_s, slot_sems, *accs):
    fetch = fetch_lines(slots, slot_s, slot_sems)
    for c in fetch:
        c.start()
    copy_in(accs[0], part)
    for a in accs[1:]:
        fill_zero(a)
    for c in fetch:
        c.wait()
    take_returns(back, slot_s, n_back, part, got_prev, got_next, accs)
    grad_one[...] = jnp.zeros_like(grad_one)

    @pl.loop(0, x.shape[0], step=STEP)
    def _(i):
        even, odd = halves(accs, i, STEP)
        d_tab = stack_lanes([even, odd]).astype(BF16)
        grad_one[...] += dot(x[pl.ds(i, STEP), :], d_tab, ROWS_A)


def call(body, name, outs, ins, scratch, out_specs=None, collective=None, vmem=14):
    extra = {} if collective is None else dict(collective_id=collective, has_side_effects=True)
    return pl.pallas_call(
        body, name=name, out_shape=outs, in_specs=ins, out_specs=out_specs or jax.tree.map(lambda _: VMEM, outs),
        scratch_shapes=[pltpu.VMEM(s, F32) if isinstance(s, tuple) else s for s in scratch],
        compiler_params=pltpu.CompilerParams(vmem_limit_bytes=vmem * 2**20, **extra),
        cost_estimate=pl.CostEstimate(flops=10**10, bytes_accessed=10**7, transcendentals=0),
    )


def solution(mesh):
    num_dev = mesh.shape[AXIS]
    to_next = [(d, (d + 1) % num_dev) for d in range(num_dev)]
    to_prev = [(d, (d - 1) % num_dev) for d in range(num_dev)]

    def step(x, w_one, w_two, send, edge_src, edge_dst, edge_w, labels, mask):
        rows, halo, edges, classes = x.shape[0], send.shape[1], edge_src.shape[0], w_two.shape[1]
        tab, half, w2_pad = (2 * rows, LANES), (2 * halo, LANES), (2 * LANES, 2 * LANES)
        sds = jax.ShapeDtypeStruct
        tab_f = sds(tab, F32)
        half_b, pack_b = sds((halo, 2 * LANES), BF16), sds((3 * halo // 2, LANES), BF16)
        tab_b = pltpu.VMEM((rows, 2 * LANES), BF16)
        one = sds(TILE, F32)
        dma = pltpu.SemaphoreType.DMA
        chunk_l, chunk_h = 64, 32
        lines = edges // LANES
        slots = lines + 8
        side = halo // LANES
        w2 = w_two.T
        mask = mask.reshape(-1, LANES)
        labels = labels.reshape(-1, LANES)
        packed = (edge_src * 2048 + edge_dst).reshape(lines, LANES)
        ints = sds((slots, LANES), jnp.int32)
        sided = sds((2 * side, LANES), F32)
        src, dst, w_lines, used, counts, count, need = call(
            functools.partial(prep_kernel, num_dev, PREP_CHUNK, rows), "prep",
            [ints, ints, sds((slots, LANES), F32), sided, sds((2,), jnp.int32), one, one], [VMEM] * 3,
            [(6 * slots, LANES), (6 * lines, LANES), pltpu.VMEM((4 * lines, LANES), jnp.int32), sided.shape, (2, LANES), (num_dev - 1, 2, LANES)]
            + [dma((num_dev - 1,))] * 2,
            out_specs=[VMEM] * 4 + [SMEM, VMEM, VMEM], vmem=8, collective=0,
        )(packed, edge_w.reshape(lines, LANES), mask)

        def run(limit):
            compact = limit < halo
            pack_f, half_f = sds((3 * limit // 2 + side, LANES), F32), sds((2 * limit, LANES), F32)
            list_s = [pltpu.SMEM((halo,), jnp.int32), dma((side,))]
            tab_one, to_p, to_n, w, src_back, lists = call(
                functools.partial(first_kernel, compact, halo), "first", [tab_f, half_b, half_b, sds((slots * LANES, LANES), F32), ints, sided],
                [VMEM] * 3 + [SMEM] + [VMEM] * 3, [tab_b, half] + list_s, vmem=8,
            )(x, w_one, send, counts, src, w_lines, used)
            from_prev = lax.ppermute(to_n, AXIS, to_next)
            from_next = lax.ppermute(to_p, AXIS, to_prev)
            flat, flat_dst, flat_back = src.reshape(-1), dst.reshape(-1), src_back.reshape(-1)

            four = [tab] * 4
            walk = [SMEM, ANY, ANY, VMEM]
            index = pltpu.SMEM((slots * LANES,), jnp.int32)
            walk_s = lambda n: [index] * n + [dma((n, slots * LANES // SEGMENT))]
            slot_s = [pltpu.SMEM((2 * halo,), jnp.int32), dma((2 * side,))]
            local, local_back = (
                call(functools.partial(local_kernel, chunk_l, back), "local_edges", tab_f, walk + [VMEM], walk_s(2) + four)
                for back in (False, True)
            )
            part = local(counts, flat, flat_dst, w, tab_one)
            hid, tab_two, to_p, to_n, back = call(
                functools.partial(hidden_kernel, chunk_h), "hidden",
                [sds((rows, 2 * LANES), BF16), tab_f, pack_b, pack_b, sds((2 * side, LANES), jnp.int32)],
                walk + [VMEM] * 5, [tab, tab_b, w2_pad, half] + list_s + walk_s(2) + four,
            )(counts, flat, flat_dst, w, send, from_prev, from_next, part, w2)
            from_prev = lax.ppermute(to_n, AXIS, to_next)
            from_next = lax.ppermute(to_p, AXIS, to_prev)
            back = back.reshape(-1)
            part = local(counts, flat, flat_dst, w, tab_two)
            loss, grad, to_p, to_n = call(
                functools.partial(loss_kernel, limit, 4, chunk_h, classes), "loss", [one, tab_f, pack_f, pack_f],
                walk + [ANY] + [VMEM] * 7, [tab] + walk_s(3) + four,
            )(counts, flat, flat_dst, w, flat_back, lists, count, from_prev, from_next, part, labels, mask)
            got_prev = lax.ppermute(to_p, AXIS, to_prev)
            got_next = lax.ppermute(to_n, AXIS, to_next)
            part = local_back(counts, flat, flat_dst, w, grad)
            grad_two, grad, to_p, to_n, slot, n_back = call(
                functools.partial(middle_kernel, limit, chunk_h), "middle",
                [sds(w2_pad, F32), tab_f, half_f, half_f, sds((2 * side, LANES), jnp.int32), sds((2,), jnp.int32)],
                walk + [SMEM] + [VMEM] * 5, [(4 * limit, LANES), w2_pad] + slot_s + walk_s(2) + four, out_specs=[VMEM] * 5 + [SMEM],
            )(counts, flat_back, flat_dst, w, back, got_prev, got_next, part, hid, w2)
            got_prev = lax.ppermute(to_p, AXIS, to_prev)
            got_next = lax.ppermute(to_n, AXIS, to_next)
            part = local_back(counts, flat, flat_dst, w, grad)
            grad_one = call(
                last_kernel, "last", sds((x.shape[1], 2 * LANES), F32), [SMEM, SMEM, ANY] + [VMEM] * 4, slot_s + four
            )(back, n_back, slot, got_prev, got_next, part, x)
            return grad_one, grad_two, loss

        few = halo * 5 // 8
        grad_one, grad_two, loss = lax.cond(need[0, 0] > few, lambda: run(halo), lambda: run(few))
        unit = SUB * num_dev
        lines = 2 * (x.shape[1] + -(-classes // SUB) * SUB) + SUB
        lines = -(-lines // unit) * unit
        grad_one, grad_two, mean = call(
            functools.partial(reduce_kernel, num_dev), "reduce", [sds(grad_one.shape, F32), sds((classes, 2 * LANES), F32), sds((1, 1), F32)],
            [VMEM] * 4, [(lines, LANES), (lines, LANES), (lines // 2, LANES), (num_dev // 2 - 1, lines // num_dev, LANES), dma((2, 2 * num_dev))],
            collective=1, vmem=8,
        )(grad_one, grad_two, loss, count)
        return mean.reshape(()), grad_one, grad_two.T

    row = P(AXIS)
    return jax.shard_map(
        step, mesh=mesh, in_specs=(row, P(), P(), row, row, row, row, row, row), out_specs=(P(), P(), P()), check_vma=False
    )
```

```python
import functools

import jax
import jax.numpy as jnp
from jax import lax
from jax.experimental import pallas as pl
from jax.experimental.pallas import tpu as pltpu
from jax.sharding import PartitionSpec as P

AXIS = "graph"
LANES = 128
ROWS_A = (((0,), (0,)), ((), ()))
COLS_A = (((1,), (1,)), ((), ()))
F32, BF16 = jnp.float32, jnp.bfloat16
VMEM = pl.BlockSpec(memory_space=pltpu.VMEM)
SMEM = pl.BlockSpec(memory_space=pltpu.SMEM)
ANY = pl.BlockSpec(memory_space=pl.ANY)
STEP = 512
BLOCK = 256
BYTE = BLOCK
SUB = 8
TILE = (SUB, LANES)
SQUARE = (LANES, LANES)
PREP_CHUNK = 64
SMALL = PREP_CHUNK
SEGMENT = 1024
MESH = pl.DeviceIdType.MESH


def dot(a, b, dims=(((1,), (0,)), ((), ()))):
    return lax.dot_general(a, b, dims, preferred_element_type=F32)


def fill_zero(ref):
    step = BLOCK if ref.shape[0] % BLOCK == 0 else SMALL
    zero = jnp.zeros((step, LANES), F32)

    @pl.loop(0, ref.shape[0], step=step)
    def _(i):
        ref[pl.ds(i, step), :] = zero


def copy_in(dst, src):
    @pl.loop(0, dst.shape[0], step=STEP)
    def _(i):
        dst[pl.ds(i, STEP), :] = src[pl.ds(i, STEP), :].astype(F32)


class Edges:
    def __init__(self, first, last, w, arrays, smem, sems):
        self.first, self.last, self.w = first, last, w
        self.pairs = tuple(zip(arrays, smem))
        self.sems = sems

    def copies(self, seg):
        part = pl.ds(pl.multiple_of(seg * SEGMENT, SEGMENT), SEGMENT)
        return [pltpu.make_async_copy(a.at[part], b.at[part], self.sems.at[i, seg]) for i, (a, b) in enumerate(self.pairs)]

    def fetch(self):
        per = SEGMENT // PREP_CHUNK
        for seg in range(self.pairs[0][1].shape[0] // SEGMENT):

            @pl.when(jnp.logical_and(seg * per < self.last, (seg + 1) * per > self.first))
            def _():
                for c in self.copies(seg):
                    c.start()

    def walk(self, chunk, from_idx, to_idx, table, accs, wait):
        group, per, ratio = len(accs), SEGMENT // chunk, PREP_CHUNK // chunk
        first, last = self.first * ratio, self.last * ratio

        def body(c, _):
            base = c * chunk
            w_chunk = self.w.at[pl.ds(pl.multiple_of(base, chunk), chunk)]
            for g in range(0, chunk, group):
                pend = []
                for u in range(group):
                    k = base + g + u
                    s = pl.multiple_of(from_idx[k], 2)
                    d = pl.multiple_of(to_idx[k], 2)
                    pend.append((d, accs[u][pl.ds(d, 2), :] + table[pl.ds(s, 2), :] * w_chunk[g + u : g + u + 1, :]))
                for u in range(group):
                    accs[u][pl.ds(pend[u][0], 2), :] = pend[u][1]
            return 0

        if not wait:
            lax.fori_loop(first, last, body, 0)
            return

        def segment(seg, _):
            for c in self.copies(seg):
                c.wait()
            lax.fori_loop(jnp.maximum(first, seg * per), jnp.minimum(last, (seg + 1) * per), body, 0)
            return 0

        lax.fori_loop(first // per, (last + per - 1) // per, segment, 0)


def one_hot_rows(idx, which, start, table):
    lane = across(SQUARE)
    hot = []
    for q in range(2):
        want = spread(idx[which : which + 1, pl.ds(pl.multiple_of(start + q * LANES, LANES), LANES)])
        hot.append(
            stack_lanes([jnp.where(want == lane + LANES * j, 1.0, 0.0).astype(BF16) for j in range(table.shape[0] // LANES)])
        )
    return dot(stack_rows(hot), table[...])


def low_lanes(rows):
    return across((rows, LANES)) < LANES // 2


def swap_lanes(v):
    return pltpu.roll(v, LANES // 2, 1)


def fetch_index(send, idx, sems):
    parts = [pl.ds(i, LANES) for i in range(0, send.shape[1], LANES)]
    return [pltpu.make_async_copy(send.at[1, p], idx.at[p], sems.at[i]) for i, p in enumerate(parts)]


def gather_block(send, idx, i, table_b, table, buf):
    got = one_hot_rows(send, 0, i, table_b)
    out = buf.at[pl.ds(pl.multiple_of(2 * i, 512), 512)]
    for u in range(BLOCK):
        s = pl.multiple_of(idx[i + u] * 2, 2)
        out[2 * u : 2 * u + 2, :] = table[pl.ds(s, 2), :]
    return got


def gather_rows(send, idx, table_b, table, buf, to_prev, to_next):
    @pl.loop(0, to_prev.shape[0], step=BLOCK)
    def _(i):
        i = pl.multiple_of(i, BLOCK)
        to_prev[pl.ds(i, BLOCK), :] = gather_block(send, idx, i, table_b, table, buf).astype(BF16)

    @pl.loop(0, to_next.shape[0], step=BLOCK)
    def _(i):
        to_next[pl.ds(pl.multiple_of(i, BLOCK), BLOCK), :] = stack_lanes(halves([buf], i, BLOCK)).astype(BF16)


def pack_rows(out, i, half, a_even, a_odd, b_even, b_odd):
    n = a_even.shape[0]
    out[pl.ds(i, n), :] = a_even.astype(out.dtype)
    out[pl.ds(half + i, n), :] = b_even.astype(out.dtype)
    out[pl.ds(2 * half + i, n), :] = jnp.where(low_lanes(n), a_odd, swap_lanes(b_odd)).astype(out.dtype)


def gather_packed(send, idx, table_b, table, buf, to_prev, to_next):
    half = to_prev.shape[0] // 3

    @pl.loop(0, half, step=BLOCK)
    def _(i):
        i = pl.multiple_of(i, BLOCK)
        a = gather_block(send, idx, i, table_b, table, buf)
        b = gather_block(send, idx, half + i, table_b, table, buf)
        pack_rows(to_prev, i, half, a[:, :LANES], a[:, LANES:], b[:, :LANES], b[:, LANES:])

    @pl.loop(0, half, step=BLOCK)
    def _(i):
        i = pl.multiple_of(i, BLOCK)
        pack_rows(to_next, i, half, *halves([buf], i, BLOCK), *halves([buf], half + i, BLOCK))


def unpack_rows(got, table, start, half=None):
    half = got.shape[0] // 3 if half is None else half
    n = half // 2

    @pl.loop(0, half, step=n)
    def _(i):
        i = pl.multiple_of(i, n)
        a, b, both = (got[pl.ds(k + i, n), :].astype(F32) for k in (0, half, 2 * half))
        put_halves(table, start + i, n, a, jnp.where(low_lanes(n), both, 0.0))
        put_halves(table, start + half + i, n, b, jnp.where(low_lanes(n), swap_lanes(both), 0.0))


def unpack_plain(got, table, start):
    @pl.loop(0, got.shape[0], step=BLOCK)
    def _(i):
        t = got[pl.ds(i, BLOCK), :].astype(F32)
        put_halves(table, start + i, BLOCK, t[:, :LANES], t[:, LANES:])


def spread(row):
    return jnp.transpose(jnp.broadcast_to(row, SQUARE))


def return_rows(back, slots, start, count, vals, accs, chunk=32):
    group = len(accs)

    def body(c, _):
        block = vals.at[pl.ds(pl.multiple_of(c * 2 * chunk, 2 * chunk), 2 * chunk)]
        for g in range(0, chunk, group):
            pend = []
            for u in range(group):
                d = pl.multiple_of(back[slots[start + c * chunk + g + u]], 2)
                pend.append((d, accs[u][pl.ds(d, 2), :] + block[2 * (g + u) : 2 * (g + u) + 2, :]))
            for u in range(group):
                accs[u][pl.ds(pend[u][0], 2), :] = pend[u][1]
        return 0

    lax.fori_loop(0, (count + chunk - 1) // chunk, body, 0)


def group(i, n, which):
    return pl.ds(2 * i + which, n, stride=2), slice(None)


def halves(accs, i, n):
    return [functools.reduce(jnp.add, [a[group(i, n, k)] for a in accs]) for k in range(2)]


def put_halves(table, i, n, *parts):
    for k, part in enumerate(parts):
        table[group(i, n, k)] = part


def stack_rows(parts):
    return jnp.concatenate(parts, axis=0)


def stack_lanes(parts):
    return jnp.concatenate(parts, axis=1)


def down(shape):
    return lax.broadcasted_iota(jnp.int32, shape, 0)


def across(shape):
    return lax.broadcasted_iota(jnp.int32, shape, 1)


def prefix(mask, above):
    m = mask.astype(BF16)
    before = (down(SQUARE) < across(SQUARE)).astype(BF16)
    return dot(m, before) + dot(above, dot(m, jnp.ones(SQUARE, BF16)).astype(BF16))


def rank_halo(halo, counts, src, used, src_back, lists):
    lines = used.shape[0]
    side = lines // 2
    i, j = down((lines, lines)), across((lines, lines))
    above = jnp.logical_and(j < i, (j >= side) == (i >= side)).astype(F32).astype(BF16)
    rank = prefix(used[...], above).astype(jnp.int32)
    low, high = rank & (LANES - 1), rank >> 7
    table = stack_rows([low.astype(F32), high.astype(F32)]).astype(BF16)

    quad = 4

    def four(c, _):
        slot = [src[pl.ds(c * quad + q, 1), :] >> 1 for q in range(quad)]
        spots = stack_lanes([(down(SQUARE) == (t & (LANES - 1))).astype(F32) for t in slot]).astype(BF16)
        got = dot(table, spots)
        h = stack_lanes(slot) >> 7
        got = jnp.where(down(got[:lines].shape) == h, got[:lines] + LANES * got[lines:], 0.0)
        got = (jnp.sum(got, axis=0, keepdims=True).astype(jnp.int32) + jnp.where(h >= side, halo, 0)) * 2
        for q in range(quad):
            src_back[pl.ds(c * quad + q, 1), :] = got[:, q * LANES : (q + 1) * LANES]
        return 0

    ratio = quad * LANES // PREP_CHUNK
    lax.fori_loop(counts[0] // ratio, (counts[1] + ratio - 1) // ratio, four, 0)
    for k in range(2):
        acc = jnp.zeros((24, LANES), F32)
        for hh in range(side):
            q = k * side + hh
            pick = jnp.where(down(TILE) == high[q : q + 1, :], used[q : q + 1, :], 0.0)
            lhs = stack_rows([pick * across(TILE).astype(F32), pick * hh, pick]).astype(BF16)
            acc += dot(lhs, (down(SQUARE) == low[q : q + 1, :]).astype(F32).astype(BF16), COLS_A)
        slots = acc[0:8] + LANES * acc[8:16]
        lists[k * side : (k + 1) * side, :] = jnp.where(acc[16:24] > 0.0, slots[:side], -1.0)


def first_kernel(compact, halo, x, w1, send, counts, src, w, used, tab, to_prev, to_next, w_out, src_back, lists, tab_b, buf, idx, sems):
    fetch = fetch_index(send, idx, sems)
    for c in fetch:
        c.start()
    rows = x.shape[0]
    w1_b = w1[...].astype(BF16)

    @pl.loop(0, rows, step=BLOCK)
    def _(i):
        t = dot(x[pl.ds(i, BLOCK), :], w1_b).astype(BF16)
        tab_b[pl.ds(i, BLOCK), :] = t
        t = t.astype(F32)
        put_halves(tab, i, BLOCK, t[:, :LANES], t[:, LANES:])

    @pl.loop(0, w.shape[0] // SUB)
    def _(r):
        for q in range(SUB):
            w_out[pl.ds(pl.multiple_of((r * SUB + q) * LANES, LANES), LANES), :] = spread(w[pl.ds(r * SUB + q, 1), :])

    src_back[...] = src[...]
    if compact:
        rank_halo(halo, counts, src, used, src_back, lists)
    else:
        line = down(lists.shape)
        line = jnp.where(line >= lists.shape[0] // 2, line - lists.shape[0] // 2, line)
        lists[...] = (line * LANES + across(lists.shape)).astype(F32)
    for c in fetch:
        c.wait()
    gather_rows(send, idx, tab_b, tab, buf, to_prev, to_next)


def greet(n):
    me = lax.axis_index(AXIS)
    barrier = pltpu.get_barrier_semaphore()
    for o in range(1, n):
        pl.semaphore_signal(barrier, inc=1, device_id=(lax.rem(me + o, n),), device_id_type=MESH)
    return me, lambda: pl.semaphore_wait(barrier, n - 1)


def remote(src, dst, send_sem, recv_sem, peer):
    return pltpu.make_async_remote_copy(
        src_ref=src, dst_ref=dst, send_sem=send_sem, recv_sem=recv_sem, device_id=(peer,), device_id_type=MESH
    )


def reduce_kernel(n, one, two, loss, count, one_out, two_out, mean, work, full, got_pair, got_rest, sems):
    me = lax.axis_index(AXIS)
    chips, core = n // 2, lax.rem(me, 2)
    chip = lax.div(me, 2)
    pair = me + 1 - 2 * core
    others = [lax.rem(chip + o, chips) for o in range(1, chips)]
    barrier = pltpu.get_barrier_semaphore()
    for p in [pair] + [2 * c + core for c in others]:
        pl.semaphore_signal(barrier, inc=1, device_id=(p,), device_id_type=MESH)
    classes = two_out.shape[0]
    lines = -(-classes // SUB) * SUB
    top, wide = one.shape
    work[0:top, :] = one[:, :LANES]
    work[top : 2 * top, :] = one[:, LANES:]
    work[2 * top : 2 * top + lines, :] = two[:lines, :LANES]
    work[2 * top + lines : 2 * top + 2 * lines, :] = two[:lines, LANES:]
    tail = 2 * top + 2 * lines
    work[tail : tail + SUB, :] = loss[...]
    work[tail + SUB :, :] = jnp.zeros((work.shape[0] - tail - SUB, LANES), F32)
    pl.semaphore_wait(barrier, chips)

    half = work.shape[0] // 2
    piece = half // chips
    spot = lambda c, k: pl.ds(pl.multiple_of(k * half + c * piece, SUB), piece)
    link = lambda kind, o, src, dst, peer: remote(src, dst, sems.at[0, kind * chips + o], sems.at[1, kind * chips + o], peer)
    order = list(enumerate(others + [chip]))
    swap = [link(0, o, work.at[spot(c, 1 - core)], got_pair.at[pl.ds(o * piece, piece)], pair) for o, c in order]
    for c in swap:
        c.start()
    scatter = [link(1, o, work.at[spot(c, core)], got_rest.at[o], 2 * c + core) for o, c in order[:-1]]
    for o, c in order:
        swap[o].wait_recv()
        work[spot(c, core), :] += got_pair[o * piece : (o + 1) * piece, :]
        if o:
            scatter[o - 1].start()
    for c in scatter:
        c.wait_recv()
    own = spot(chip, core)
    work[own, :] += jnp.sum(got_rest[...], axis=0)
    full[own, :] = work[own, :]
    for c in swap + scatter:
        c.wait_send()
    gather = [link(2, o, work.at[own], full.at[own], 2 * c + core) for o, c in order[:-1]]
    for c in gather:
        c.start()
    forward = [link(3, chips - 1, work.at[own], full.at[own], pair)]
    forward[0].start()
    for o, _ in order[:-1]:
        gather[o].wait_recv()
        came = spot(lax.rem(chip + chips - 1 - o, chips), core)
        forward.append(link(3, o, full.at[came], full.at[came], pair))
        forward[-1].start()
    for c in gather:
        c.wait_send()
    for c in forward:
        c.wait()
    one_out[:, :LANES] = full[0:top, :]
    one_out[:, LANES:] = full[top : 2 * top, :]
    two_out[:, :LANES] = full[2 * top : 2 * top + classes, :]
    two_out[:, LANES:] = full[2 * top + lines : 2 * top + lines + classes, :]
    mean[...] = jnp.sum(full[tail : tail + SUB, :], keepdims=True) / count[0:1, 0:1]


def prep_kernel(n, chunk, rows, src_in, dst_in, w_in, mask, src_out, dst_out, w_out, used, counts, count, need, total, values, places, hits, mine, theirs, send_sem, recv_sem):
    me, met = greet(n)
    lines, slots = src_in.shape[0], src_out.shape[0]
    src, d, half_w = src_in[...], dst_in[...], w_in[...] * 0.5
    live = w_in[...] != 0.0
    halo = src >= rows
    above = (across((lines, lines)) < down((lines, lines))).astype(F32).astype(BF16)
    is_local, is_halo = jnp.logical_and(live, jnp.logical_not(halo)), jnp.logical_and(live, halo)
    rank = lambda m: prefix(m.astype(F32), above).astype(jnp.int32)
    n_local = jnp.sum(is_local.astype(F32)).astype(jnp.int32)
    n_halo = jnp.sum(is_halo.astype(F32)).astype(jnp.int32)
    local_chunks = (n_local + chunk - 1) // chunk
    counts[0] = local_chunks
    counts[1] = local_chunks + (n_halo + chunk - 1) // chunk
    pos = jnp.where(is_local, rank(is_local), jnp.where(is_halo, rank(is_halo) + local_chunks * chunk, -1))
    s = jnp.where(halo, src - rows, src)
    w_a = half_w.astype(BF16).astype(F32)
    w_b = (half_w - w_a).astype(BF16).astype(F32)
    w_c = half_w - w_a - w_b
    high = ((s >> 8) * 8 + (d >> 8)).astype(F32)
    planes = [(s % BYTE).astype(F32), (d % BYTE).astype(F32), high, w_a, w_b, w_c]
    for i, p in enumerate(planes):
        values[i * lines : (i + 1) * lines, :] = p
    for i, p in enumerate((pos >> 7, pos & (LANES - 1), jnp.where(is_halo, s >> 7, -1), s & (LANES - 1))):
        places[i * lines : (i + 1) * lines, :] = p
    row = lambda i, q: pl.ds(i * lines + q, 1)
    spot = lambda size, i, q: (down((size, LANES)) == places[row(i, q), :]).astype(F32)
    hits[...] = jnp.zeros_like(hits)

    @pl.loop(0, lines, step=SUB)
    def _(base):
        acc = None
        for r in range(0, SUB, 2):
            lhs = stack_lanes([spot(hits.shape[0], 2, base + q) for q in (r, r + 1)]).astype(BF16)
            rhs = stack_lanes([spot(LANES, 3, base + q) for q in (r, r + 1)]).astype(BF16)
            part = dot(lhs, rhs, COLS_A)
            acc = part if acc is None else acc + part
        hits[...] += acc

    flags = (hits[...] > 0.0).astype(F32)
    used[...] = flags
    side = hits.shape[0] // 2
    most = jnp.maximum(jnp.sum(flags[:side], keepdims=True), jnp.sum(flags[side:], keepdims=True))
    mine[:1, :] = jnp.sum(mask[...].astype(F32), axis=0, keepdims=True)
    mine[1:, :] = jnp.broadcast_to(most, (1, LANES))
    met()
    copies = [remote(mine, theirs.at[o - 1], send_sem.at[o - 1], recv_sem.at[o - 1], lax.rem(me + o, n)) for o in range(1, n)]
    for c in copies:
        c.start()
    total[...] = jnp.zeros_like(total)

    @pl.loop(0, lines, step=SUB)
    def _(base):
        acc = None
        for r in range(0, SUB, 2):
            lhs, rhs = [], []
            for q in (base + r, base + r + 1):
                pick = down((slots, LANES)) == places[row(0, q), :]
                lhs.append(stack_rows([jnp.where(pick, values[row(i, q), :], 0.0) for i in range(len(planes))]))
                rhs.append(spot(LANES, 1, q))
            part = dot(stack_lanes(lhs).astype(BF16), stack_lanes(rhs).astype(BF16), COLS_A)
            acc = part if acc is None else acc + part
        total[...] += acc

    plane = lambda i: total[i * slots : (i + 1) * slots, :]
    high = plane(2).astype(jnp.int32)
    src_out[...] = ((high >> 3) * BYTE + plane(0).astype(jnp.int32)) * 2
    dst_out[...] = ((high & 7) * BYTE + plane(1).astype(jnp.int32)) * 2
    w_out[...] = (plane(3) + plane(4) + plane(5)) * 2.0
    for c in copies:
        c.wait()
    every = jnp.sum(mine[:1, :] + jnp.sum(theirs[:, :1, :], axis=0), keepdims=True)
    count[...] = jnp.maximum(jnp.broadcast_to(every, count.shape), 1.0)
    need[0] = jnp.max(jnp.maximum(mine[1:, :], jnp.max(theirs[:, 1:, :], axis=0))).astype(jnp.int32)


def local_kernel(chunk, backward, counts, src, dst, w, table, out, src_s, dst_s, sems, *accs):
    edges = Edges(0, counts[0], w, (src, dst), (src_s, dst_s), sems)
    edges.fetch()
    for a in accs:
        fill_zero(a)
    edges.walk(chunk, *((dst_s, src_s) if backward else (src_s, dst_s)), table, accs, True)

    @pl.loop(0, out.shape[0], step=STEP)
    def _(i):
        out[pl.ds(i, STEP), :] = functools.reduce(jnp.add, [a[pl.ds(i, STEP), :] for a in accs])


def forward_halo(chunk, edges, src_s, dst_s, from_prev, from_next, part, htab, accs, unpack):
    edges.fetch()
    unpack(from_prev, htab, 0)
    unpack(from_next, htab, htab.shape[0] // 4)
    copy_in(accs[0], part)
    for a in accs[1:]:
        fill_zero(a)
    edges.walk(chunk, src_s, dst_s, htab, accs, True)


def backward_halo(limit, chunk, edges, src_s, dst_s, grad, back_prev, back_next, accs, wait, lists=None):
    split = accs[0].shape[0] // 2
    for a in accs:
        for start in (0, split):
            fill_zero(a.at[pl.ds(start, limit * 2)])
    edges.walk(chunk, dst_s, src_s, grad, accs, wait)
    if lists is None:

        @pl.loop(0, back_prev.shape[0], step=SMALL)
        def _(i):
            back_prev[pl.ds(i, SMALL), :] = functools.reduce(jnp.add, [a[pl.ds(i, SMALL), :] for a in accs])
            back_next[pl.ds(i, SMALL), :] = functools.reduce(jnp.add, [a[pl.ds(split + i, SMALL), :] for a in accs])
        return
    side = lists.shape[0] // 2
    half = (back_prev.shape[0] - side) // 3
    n = half // 2
    for k, out in enumerate((back_prev, back_next)):
        start = k * (split // 2)

        @pl.loop(0, half, step=n)
        def _(i):
            i = pl.multiple_of(i, n)
            pack_rows(out, i, half, *halves(accs, start + i, n), *halves(accs, start + half + i, n))

        out[3 * half : 3 * half + side, :] = lists[k * side : (k + 1) * side, :]


def padded(w, buf):
    low = w.shape[0] // SUB * SUB
    buf[low:, :] = jnp.zeros((buf.shape[0] - low, buf.shape[1]), F32)
    buf[0 : w.shape[0], :] = w[...]
    return buf[...].astype(BF16)


def hidden_kernel(chunk, counts, src, dst, w, send, from_prev, from_next, part, w2, hid, tab, to_prev, to_next, back, htab, tab_b, w2_pad, buf, idx, idx_sems, src_s, dst_s, sems, *accs):
    fetch = fetch_index(send, idx, idx_sems)
    for c in fetch:
        c.start()
    edges = Edges(counts[0], counts[1], w, (src, dst), (src_s, dst_s), sems)
    w2_b = padded(w2, w2_pad)
    per = send.shape[1] // LANES
    for i in range(2 * per):
        back[i : i + 1, :] = send[i // per : i // per + 1, (i % per) * LANES : (i % per + 1) * LANES] * 2
    forward_halo(chunk, edges, src_s, dst_s, from_prev, from_next, part, htab, accs, unpack_plain)

    @pl.loop(0, hid.shape[0], step=STEP)
    def _(i):
        even, odd = halves(accs, i, STEP)
        h = stack_lanes([jnp.maximum(even, 0.0), jnp.maximum(odd, 0.0)]).astype(BF16)
        hid[pl.ds(i, STEP), :] = h
        t = dot(h, w2_b, COLS_A).astype(BF16)
        tab_b[pl.ds(i, STEP), :] = t
        t = t.astype(F32)
        put_halves(tab, i, STEP, t[:, :LANES], t[:, LANES:])

    for c in fetch:
        c.wait()
    gather_packed(send, idx, tab_b, tab, buf, to_prev, to_next)


def loss_kernel(limit, quad, chunk, classes, counts, src, dst, w, src_back, lists, count, from_prev, from_next, part, labels, mask, loss, grad, back_prev, back_next, htab, src_s, dst_s, back_s, sems, *accs):
    edges = Edges(counts[0], counts[1], w, (src, dst, src_back), (src_s, dst_s, back_s), sems)
    forward_halo(chunk, edges, src_s, dst_s, from_prev, from_next, part, htab, accs, unpack_rows)
    lane = across(SQUARE)
    live = lane < classes - LANES
    scale = 1.0 / count[0:1, :]
    loss[...] = jnp.zeros_like(loss)

    @pl.loop(0, labels.shape[0], step=quad)
    def _(first):
        for b in [first + q for q in range(quad)]:
            even, odd = halves(accs, b * LANES, LANES)
            odd = jnp.where(live, odd, -jnp.inf)
            keep = spread(mask[pl.ds(b, 1), :])
            label = jnp.where(keep > 0, spread(labels[pl.ds(b, 1), :]), -1)
            hit_even, hit_odd = lane == label, lane + LANES == label
            top = jnp.max(jnp.maximum(even, odd), axis=1, keepdims=True)
            exp_even, exp_odd = jnp.exp(even - top), jnp.exp(odd - top)
            total = jnp.sum(exp_even + exp_odd, axis=1, keepdims=True)
            norm = jnp.where(jnp.logical_and(lane == 0, keep > 0), top + jnp.log(total), 0.0)
            per_row = norm - jnp.where(hit_even, even, jnp.where(hit_odd, odd, 0.0))
            loss[...] += jnp.sum(per_row.reshape(LANES // SUB, *TILE), axis=0)
            share = keep.astype(F32) * scale * (1.0 / total)
            put_halves(
                grad, b * LANES, LANES, *(e * share - jnp.where(hit, scale, 0.0) for e, hit in ((exp_even, hit_even), (exp_odd, hit_odd)))
            )

    backward_halo(limit, chunk, edges, back_s, dst_s, grad, back_prev, back_next, accs, False, lists)


def take_returns(back, slots, counts, part, got_prev, got_next, accs):
    return_rows(back, slots, 0, counts[0], got_prev, accs)
    return_rows(back, slots, slots.shape[0] // 2, counts[1], got_next, accs)


def fetch_lines(lines, smem, sems):
    return [pltpu.make_async_copy(lines.at[i], smem.at[pl.ds(i * LANES, LANES)], sems.at[i]) for i in range(lines.shape[0])]


def middle_kernel(limit, chunk, counts, src, dst, w, back, got_prev, got_next, part, hid, w2, grad_two, grad, back_prev, back_next, slots, n_back, returned, w2_pad, slot_s, slot_sems, src_s, dst_s, sems, *accs):
    edges = Edges(counts[0], counts[1], w, (src, dst), (src_s, dst_s), sems)
    edges.fetch()
    side = slots.shape[0] // 2
    half = (got_prev.shape[0] - side) // 3
    for k, got in enumerate((got_prev, got_next)):
        slot = got[3 * half :, :].astype(jnp.int32)
        slots[k * side : (k + 1) * side, :] = jnp.maximum(slot, 0) + (1 - k) * side * LANES
        n_back[k] = jnp.sum((slot >= 0).astype(F32)).astype(jnp.int32)
    w2_b = padded(w2, w2_pad)
    unpack_rows(got_prev, returned, 0, half)
    unpack_rows(got_next, returned, 2 * half, half)
    fetch = fetch_lines(slots, slot_s, slot_sems)
    for c in fetch:
        c.start()
    copy_in(accs[0], part)
    for a in accs[1:]:
        fill_zero(a)
    for c in fetch:
        c.wait()
    take_returns(back, slot_s, n_back, part, returned.at[pl.ds(0, 4 * half)], returned.at[pl.ds(4 * half, 4 * half)], accs)
    grad_two[...] = jnp.zeros_like(grad_two)

    @pl.loop(0, hid.shape[0], step=STEP)
    def _(i):
        even, odd = halves(accs, i, STEP)
        d_tab = stack_lanes([even, odd]).astype(BF16)
        h = hid[pl.ds(i, STEP), :]
        grad_two[...] += dot(d_tab, h, ROWS_A)
        d_hid = dot(d_tab, w2_b)
        d_pre = jnp.where(h > 0, d_hid, 0.0)
        put_halves(grad, i, STEP, d_pre[:, :LANES], d_pre[:, LANES:])

    backward_halo(limit, chunk, edges, src_s, dst_s, grad, back_prev, back_next, accs, True)


def last_kernel(back, n_back, slots, got_prev, got_next, part, x, grad_one, slot_s, slot_sems, *accs):
    fetch = fetch_lines(slots, slot_s, slot_sems)
    for c in fetch:
        c.start()
    copy_in(accs[0], part)
    for a in accs[1:]:
        fill_zero(a)
    for c in fetch:
        c.wait()
    take_returns(back, slot_s, n_back, part, got_prev, got_next, accs)
    grad_one[...] = jnp.zeros_like(grad_one)

    @pl.loop(0, x.shape[0], step=STEP)
    def _(i):
        even, odd = halves(accs, i, STEP)
        d_tab = stack_lanes([even, odd]).astype(BF16)
        grad_one[...] += dot(x[pl.ds(i, STEP), :], d_tab, ROWS_A)


def call(body, name, outs, ins, scratch, out_specs=None, collective=None, vmem=14):
    extra = {} if collective is None else dict(collective_id=collective, has_side_effects=True)
    return pl.pallas_call(
        body, name=name, out_shape=outs, in_specs=ins, out_specs=out_specs or jax.tree.map(lambda _: VMEM, outs),
        scratch_shapes=[pltpu.VMEM(s, F32) if isinstance(s, tuple) else s for s in scratch],
        compiler_params=pltpu.CompilerParams(vmem_limit_bytes=vmem * 2**20, **extra),
        cost_estimate=pl.CostEstimate(flops=10**10, bytes_accessed=10**7, transcendentals=0),
    )


def solution(mesh):
    num_dev = mesh.shape[AXIS]
    to_next = [(d, (d + 1) % num_dev) for d in range(num_dev)]
    to_prev = [(d, (d - 1) % num_dev) for d in range(num_dev)]

    def step(x, w_one, w_two, send, edge_src, edge_dst, edge_w, labels, mask):
        rows, halo, edges, classes = x.shape[0], send.shape[1], edge_src.shape[0], w_two.shape[1]
        tab, half, w2_pad = (2 * rows, LANES), (2 * halo, LANES), (2 * LANES, 2 * LANES)
        sds = jax.ShapeDtypeStruct
        tab_f = sds(tab, F32)
        half_b, pack_b = sds((halo, 2 * LANES), BF16), sds((3 * halo // 2, LANES), BF16)
        tab_b = pltpu.VMEM((rows, 2 * LANES), BF16)
        one = sds(TILE, F32)
        dma = pltpu.SemaphoreType.DMA
        chunk_l, chunk_h = 64, 32
        lines = edges // LANES
        slots = lines + 8
        side = halo // LANES
        w2 = w_two.T
        mask = mask.reshape(-1, LANES)
        labels = labels.reshape(-1, LANES)
        lined = [a.reshape(lines, LANES) for a in (edge_src, edge_dst, edge_w)]
        ints = sds((slots, LANES), jnp.int32)
        sided = sds((2 * side, LANES), F32)
        src, dst, w_lines, used, counts, count, need = call(
            functools.partial(prep_kernel, num_dev, PREP_CHUNK, rows), "prep",
            [ints, ints, sds((slots, LANES), F32), sided, sds((2,), jnp.int32), one, sds((1,), jnp.int32)], [VMEM] * 4,
            [(6 * slots, LANES), (6 * lines, LANES), pltpu.VMEM((4 * lines, LANES), jnp.int32), sided.shape, (2, LANES), (num_dev - 1, 2, LANES)]
            + [dma((num_dev - 1,))] * 2,
            out_specs=[VMEM] * 4 + [SMEM, VMEM, SMEM], vmem=60, collective=0,
        )(*lined, mask)

        def run(limit):
            compact = limit < halo
            pack_f, half_f = sds((3 * limit // 2 + side, LANES), F32), sds((2 * limit, LANES), F32)
            list_s = [pltpu.SMEM((halo,), jnp.int32), dma((side,))]
            tab_one, to_p, to_n, w, src_back, lists = call(
                functools.partial(first_kernel, compact, halo), "first", [tab_f, half_b, half_b, sds((slots * LANES, LANES), F32), ints, sided],
                [VMEM] * 3 + [SMEM] + [VMEM] * 3, [tab_b, half] + list_s, vmem=8,
            )(x, w_one, send, counts, src, w_lines, used)
            from_prev = lax.ppermute(to_n, AXIS, to_next)
            from_next = lax.ppermute(to_p, AXIS, to_prev)
            flat, flat_dst, flat_back = src.reshape(-1), dst.reshape(-1), src_back.reshape(-1)

            four = [tab] * 4
            walk = [SMEM, ANY, ANY, VMEM]
            index = pltpu.SMEM((slots * LANES,), jnp.int32)
            walk_s = lambda n: [index] * n + [dma((n, slots * LANES // SEGMENT))]
            slot_s = [pltpu.SMEM((2 * halo,), jnp.int32), dma((2 * side,))]
            local, local_back = (
                call(functools.partial(local_kernel, chunk_l, back), "local_edges", tab_f, walk + [VMEM], walk_s(2) + four)
                for back in (False, True)
            )
            part = local(counts, flat, flat_dst, w, tab_one)
            hid, tab_two, to_p, to_n, back = call(
                functools.partial(hidden_kernel, chunk_h), "hidden",
                [sds((rows, 2 * LANES), BF16), tab_f, pack_b, pack_b, sds((2 * side, LANES), jnp.int32)],
                walk + [VMEM] * 5, [tab, tab_b, w2_pad, half] + list_s + walk_s(2) + four,
            )(counts, flat, flat_dst, w, send, from_prev, from_next, part, w2)
            from_prev = lax.ppermute(to_n, AXIS, to_next)
            from_next = lax.ppermute(to_p, AXIS, to_prev)
            back = back.reshape(-1)
            part = local(counts, flat, flat_dst, w, tab_two)
            loss, grad, to_p, to_n = call(
                functools.partial(loss_kernel, limit, 4, chunk_h, classes), "loss", [one, tab_f, pack_f, pack_f],
                walk + [ANY] + [VMEM] * 7, [tab] + walk_s(3) + four,
            )(counts, flat, flat_dst, w, flat_back, lists, count, from_prev, from_next, part, labels, mask)
            got_prev = lax.ppermute(to_p, AXIS, to_prev)
            got_next = lax.ppermute(to_n, AXIS, to_next)
            part = local_back(counts, flat, flat_dst, w, grad)
            grad_two, grad, to_p, to_n, slot, n_back = call(
                functools.partial(middle_kernel, limit, chunk_h), "middle",
                [sds(w2_pad, F32), tab_f, half_f, half_f, sds((2 * side, LANES), jnp.int32), sds((2,), jnp.int32)],
                walk + [SMEM] + [VMEM] * 5, [(4 * limit, LANES), w2_pad] + slot_s + walk_s(2) + four, out_specs=[VMEM] * 5 + [SMEM],
            )(counts, flat_back, flat_dst, w, back, got_prev, got_next, part, hid, w2)
            got_prev = lax.ppermute(to_p, AXIS, to_prev)
            got_next = lax.ppermute(to_n, AXIS, to_next)
            part = local_back(counts, flat, flat_dst, w, grad)
            grad_one = call(
                last_kernel, "last", sds((x.shape[1], 2 * LANES), F32), [SMEM, SMEM, ANY] + [VMEM] * 4, slot_s + four
            )(back, n_back, slot, got_prev, got_next, part, x)
            return grad_one, grad_two, loss

        few = halo // 32 * 19
        grad_one, grad_two, loss = lax.cond(need.reshape(()) > few, lambda: run(halo), lambda: run(few))
        unit = SUB * num_dev
        lines = 2 * (x.shape[1] + -(-classes // SUB) * SUB) + SUB
        lines = -(-lines // unit) * unit
        grad_one, grad_two, mean = call(
            functools.partial(reduce_kernel, num_dev), "reduce", [sds(grad_one.shape, F32), sds((classes, 2 * LANES), F32), sds((1, 1), F32)],
            [VMEM] * 4, [(lines, LANES), (lines, LANES), (lines // 2, LANES), (num_dev // 2 - 1, lines // num_dev, LANES), dma((2, 2 * num_dev))],
            collective=1, vmem=8,
        )(grad_one, grad_two, loss, count)
        return mean.reshape(()), grad_one, grad_two.T

    row = P(AXIS)
    return jax.shard_map(
        step, mesh=mesh, in_specs=(row, P(), P(), row, row, row, row, row, row), out_specs=(P(), P(), P()), check_vma=False
    )
```

```python
import functools

import jax
import jax.numpy as jnp
from jax import lax
from jax.experimental import pallas as pl
from jax.experimental.pallas import tpu as pltpu
from jax.sharding import PartitionSpec as P

AXIS = "graph"
LANES = 128
ROWS_A = (((0,), (0,)), ((), ()))
COLS_A = (((1,), (1,)), ((), ()))
F32, BF16 = jnp.float32, jnp.bfloat16
VMEM = pl.BlockSpec(memory_space=pltpu.VMEM)
SMEM = pl.BlockSpec(memory_space=pltpu.SMEM)
ANY = pl.BlockSpec(memory_space=pl.ANY)
STEP = 512
BLOCK = 256
BYTE = BLOCK
SUB = 8
TILE = (SUB, LANES)
SQUARE = (LANES, LANES)
PREP_CHUNK = 64
SMALL = PREP_CHUNK
SEGMENT = 384
MESH = pl.DeviceIdType.MESH


def dot(a, b, dims=(((1,), (0,)), ((), ()))):
    return lax.dot_general(a, b, dims, preferred_element_type=F32)


def fill_zero(ref):
    step = BLOCK if ref.shape[0] % BLOCK == 0 else SMALL
    zero = jnp.zeros((step, LANES), F32)

    @pl.loop(0, ref.shape[0], step=step)
    def _(i):
        ref[pl.ds(i, step), :] = zero


def copy_in(dst, src):
    @pl.loop(0, dst.shape[0], step=STEP)
    def _(i):
        dst[pl.ds(i, STEP), :] = src[pl.ds(i, STEP), :].astype(F32)


class Edges:
    def __init__(self, first, last, w, arrays, smem, sems):
        self.first, self.last, self.w, self.sems = first, last, w, sems
        self.size = smem[0].shape[0]
        self.smem = [smem[k * SUB : (k + 1) * SUB] for k in range(len(arrays))]
        self.arrays = arrays

    def copies(self, seg):
        done = []
        for a, parts in zip(self.arrays, self.smem):
            for t, part in enumerate(parts):
                start = pl.multiple_of(seg * SEGMENT, LANES)
                src = a.at[pl.ds(pl.multiple_of(t * self.size + start, LANES), SEGMENT)]
                done.append(pltpu.make_async_copy(src, part.at[pl.ds(start, SEGMENT)], self.sems.at[len(done), seg]))
        return done

    def fetch(self):
        per = SEGMENT * SUB // PREP_CHUNK
        for seg in range(self.size // SEGMENT):

            @pl.when(jnp.logical_and(seg * per < self.last, (seg + 1) * per > self.first))
            def _():
                for c in self.copies(seg):
                    c.start()

    def walk(self, source, target, table, accs, wait):
        group, per, rows = len(accs), SEGMENT * SUB // PREP_CHUNK, PREP_CHUNK // SUB
        from_idx, to_idx = self.smem[source], self.smem[target]

        def body(c, _):
            weights = [self.w.at[pl.ds(pl.multiple_of(c * rows + t * self.size, SUB), rows)] for t in range(SUB)]
            for v in range(rows):
                i = c * rows + v
                for g in range(0, SUB, group):
                    pend = []
                    for u in range(group):
                        s = pl.multiple_of(from_idx[g + u][i], 2)
                        d = pl.multiple_of(to_idx[g + u][i], 2)
                        pend.append((d, accs[u][pl.ds(d, 2), :] + table[pl.ds(s, 2), :] * weights[g + u][v : v + 1, :]))
                    for u in range(group):
                        accs[u][pl.ds(pend[u][0], 2), :] = pend[u][1]
            return 0

        if not wait:
            lax.fori_loop(self.first, self.last, body, 0)
            return

        def segment(seg, _):
            for c in self.copies(seg):
                c.wait()
            lax.fori_loop(jnp.maximum(self.first, seg * per), jnp.minimum(self.last, (seg + 1) * per), body, 0)
            return 0

        lax.fori_loop(self.first // per, (self.last + per - 1) // per, segment, 0)


def one_hot_rows(idx, which, start, table):
    lane = across(SQUARE)
    hot = []
    for q in range(2):
        want = spread(idx[which : which + 1, pl.ds(pl.multiple_of(start + q * LANES, LANES), LANES)])
        hot.append(
            stack_lanes([jnp.where(want == lane + LANES * j, 1.0, 0.0).astype(BF16) for j in range(table.shape[0] // LANES)])
        )
    return dot(stack_rows(hot), table[...])


def low_lanes(rows):
    return across((rows, LANES)) < LANES // 2


def swap_lanes(v):
    return pltpu.roll(v, LANES // 2, 1)


def fetch_index(send, idx, sems):
    parts = [pl.ds(i, LANES) for i in range(0, send.shape[1], LANES)]
    return [pltpu.make_async_copy(send.at[1, p], idx.at[p], sems.at[i]) for i, p in enumerate(parts)]


def gather_block(send, idx, i, table_b, table, buf):
    got = one_hot_rows(send, 0, i, table_b)
    out = buf.at[pl.ds(pl.multiple_of(2 * i, 512), 512)]
    for u in range(BLOCK):
        s = pl.multiple_of(idx[i + u] * 2, 2)
        out[2 * u : 2 * u + 2, :] = table[pl.ds(s, 2), :]
    return got


def gather_rows(send, idx, table_b, table, buf, to_prev, to_next, also):
    @pl.loop(0, to_prev.shape[0], step=BLOCK)
    def _(i):
        i = pl.multiple_of(i, BLOCK)
        to_prev[pl.ds(i, BLOCK), :] = gather_block(send, idx, i, table_b, table, buf).astype(BF16)
        also(i)

    @pl.loop(0, to_next.shape[0], step=BLOCK)
    def _(i):
        to_next[pl.ds(pl.multiple_of(i, BLOCK), BLOCK), :] = stack_lanes(halves([buf], i, BLOCK)).astype(BF16)


def pack_rows(out, i, half, a_even, a_odd, b_even, b_odd):
    n = a_even.shape[0]
    out[pl.ds(i, n), :] = a_even.astype(out.dtype)
    out[pl.ds(half + i, n), :] = b_even.astype(out.dtype)
    out[pl.ds(2 * half + i, n), :] = jnp.where(low_lanes(n), a_odd, swap_lanes(b_odd)).astype(out.dtype)


def gather_packed(send, idx, table_b, table, buf, to_prev, to_next):
    half = to_prev.shape[0] // 3

    @pl.loop(0, half, step=BLOCK)
    def _(i):
        i = pl.multiple_of(i, BLOCK)
        a = gather_block(send, idx, i, table_b, table, buf)
        b = gather_block(send, idx, half + i, table_b, table, buf)
        pack_rows(to_prev, i, half, a[:, :LANES], a[:, LANES:], b[:, :LANES], b[:, LANES:])

    @pl.loop(0, half, step=BLOCK)
    def _(i):
        i = pl.multiple_of(i, BLOCK)
        pack_rows(to_next, i, half, *halves([buf], i, BLOCK), *halves([buf], half + i, BLOCK))


def unpack_rows(got, table, start, half=None):
    half = got.shape[0] // 3 if half is None else half
    n = half // 2

    @pl.loop(0, half, step=n)
    def _(i):
        i = pl.multiple_of(i, n)
        a, b, both = (got[pl.ds(k + i, n), :].astype(F32) for k in (0, half, 2 * half))
        put_halves(table, start + i, n, a, jnp.where(low_lanes(n), both, 0.0))
        put_halves(table, start + half + i, n, b, jnp.where(low_lanes(n), swap_lanes(both), 0.0))


def unpack_plain(got, table, start):
    @pl.loop(0, got.shape[0], step=BLOCK)
    def _(i):
        t = got[pl.ds(i, BLOCK), :].astype(F32)
        put_halves(table, start + i, BLOCK, t[:, :LANES], t[:, LANES:])


def spread(row):
    return jnp.transpose(jnp.broadcast_to(row, SQUARE))


def return_rows(back, slots, start, count, vals, accs, chunk=32):
    group = len(accs)

    def body(c, _):
        block = vals.at[pl.ds(pl.multiple_of(c * 2 * chunk, 2 * chunk), 2 * chunk)]
        for g in range(0, chunk, group):
            pend = []
            for u in range(group):
                d = pl.multiple_of(back[slots[start + c * chunk + g + u]], 2)
                pend.append((d, accs[u][pl.ds(d, 2), :] + block[2 * (g + u) : 2 * (g + u) + 2, :]))
            for u in range(group):
                accs[u][pl.ds(pend[u][0], 2), :] = pend[u][1]
        return 0

    lax.fori_loop(0, (count + chunk - 1) // chunk, body, 0)


def group(i, n, which):
    return pl.ds(2 * i + which, n, stride=2), slice(None)


def halves(accs, i, n):
    return [functools.reduce(jnp.add, [a[group(i, n, k)] for a in accs]) for k in range(2)]


def put_halves(table, i, n, *parts):
    for k, part in enumerate(parts):
        table[group(i, n, k)] = part


def stack_rows(parts):
    return jnp.concatenate(parts, axis=0)


def stack_lanes(parts):
    return jnp.concatenate(parts, axis=1)


def down(shape):
    return lax.broadcasted_iota(jnp.int32, shape, 0)


def across(shape):
    return lax.broadcasted_iota(jnp.int32, shape, 1)


def prefix(mask, above):
    m = mask.astype(BF16)
    before = (down(SQUARE) < across(SQUARE)).astype(BF16)
    return dot(m, before) + dot(above, dot(m, jnp.ones(SQUARE, BF16)).astype(BF16))


def rank_halo(halo, counts, src, used, src_back, lists):
    lines = used.shape[0]
    side = lines // 2
    i, j = down((lines, lines)), across((lines, lines))
    above = jnp.logical_and(j < i, (j >= side) == (i >= side)).astype(F32).astype(BF16)
    rank = prefix(used[...], above).astype(jnp.int32)
    low, high = rank & (LANES - 1), rank >> 7
    table = stack_rows([low.astype(F32), high.astype(F32)]).astype(BF16)

    per = src.shape[0] // SUB

    def eight(c, _):
        rows = [pl.ds(t * per + c, 1) for t in range(SUB)]
        slot = [src[r, :] >> 1 for r in rows]
        spots = stack_lanes([(down(SQUARE) == (t & (LANES - 1))).astype(F32) for t in slot]).astype(BF16)
        got = dot(table, spots)
        h = stack_lanes(slot) >> 7
        got = jnp.where(down(got[:lines].shape) == h, got[:lines] + LANES * got[lines:], 0.0)
        got = (jnp.sum(got, axis=0, keepdims=True).astype(jnp.int32) + jnp.where(h >= side, halo, 0)) * 2
        for q, r in enumerate(rows):
            src_back[r, :] = got[:, q * LANES : (q + 1) * LANES]
        return 0

    ratio = SUB * LANES // PREP_CHUNK
    lax.fori_loop(counts[0] // ratio, (counts[1] + ratio - 1) // ratio, eight, 0)
    for k in range(2):
        acc = jnp.zeros((24, LANES), F32)
        for hh in range(side):
            q = k * side + hh
            pick = jnp.where(down(TILE) == high[q : q + 1, :], used[q : q + 1, :], 0.0)
            lhs = stack_rows([pick * across(TILE).astype(F32), pick * hh, pick]).astype(BF16)
            acc += dot(lhs, (down(SQUARE) == low[q : q + 1, :]).astype(F32).astype(BF16), COLS_A)
        slots = acc[:SUB] + LANES * acc[SUB:16]
        lists[k * side : (k + 1) * side, :] = jnp.where(acc[16:24] > 0.0, slots[:side], -1.0)


def first_kernel(compact, halo, x, w1, send, counts, src, w, used, tab, to_prev, to_next, w_out, src_back, lists, tab_b, buf, idx, sems):
    fetch = fetch_index(send, idx, sems)
    for c in fetch:
        c.start()
    rows = x.shape[0]
    w1_b = w1[...].astype(BF16)

    @pl.loop(0, rows, step=BLOCK)
    def _(i):
        t = dot(x[pl.ds(i, BLOCK), :], w1_b).astype(BF16)
        tab_b[pl.ds(i, BLOCK), :] = t
        t = t.astype(F32)
        put_halves(tab, i, BLOCK, t[:, :LANES], t[:, LANES:])

    src_back[...] = src[...]
    if compact:
        rank_halo(halo, counts, src, used, src_back, lists)
    else:
        line = down(lists.shape)
        line = jnp.where(line >= lists.shape[0] // 2, line - lists.shape[0] // 2, line)
        lists[...] = (line * LANES + across(lists.shape)).astype(F32)
    for c in fetch:
        c.wait()
    share = w.shape[0] * BLOCK // halo

    def widen(i):
        for q in range(share):
            r = i // BLOCK * share + q
            w_out[pl.ds(pl.multiple_of(r * LANES, LANES), LANES), :] = spread(w[pl.ds(r, 1), :])

    gather_rows(send, idx, tab_b, tab, buf, to_prev, to_next, widen)


def greet(n):
    me = lax.axis_index(AXIS)
    barrier = pltpu.get_barrier_semaphore()
    for o in range(1, n):
        pl.semaphore_signal(barrier, inc=1, device_id=(lax.rem(me + o, n),), device_id_type=MESH)
    return me, lambda: pl.semaphore_wait(barrier, n - 1)


def remote(src, dst, send_sem, recv_sem, peer):
    return pltpu.make_async_remote_copy(
        src_ref=src, dst_ref=dst, send_sem=send_sem, recv_sem=recv_sem, device_id=(peer,), device_id_type=MESH
    )


def reduce_kernel(n, one, two, loss, count, one_out, two_out, mean, work, full, got_pair, got_rest, sems):
    me = lax.axis_index(AXIS)
    chips, core = n // 2, lax.rem(me, 2)
    chip = lax.div(me, 2)
    pair = me + 1 - 2 * core
    others = [lax.rem(chip + o, chips) for o in range(1, chips)]
    barrier = pltpu.get_barrier_semaphore()
    for p in [pair] + [2 * c + core for c in others]:
        pl.semaphore_signal(barrier, inc=1, device_id=(p,), device_id_type=MESH)
    classes = two_out.shape[0]
    lines = -(-classes // SUB) * SUB
    top, wide = one.shape
    work[:top, :] = one[:, :LANES]
    work[top : 2 * top, :] = one[:, LANES:]
    work[2 * top : 2 * top + lines, :] = two[:lines, :LANES]
    work[2 * top + lines : 2 * top + 2 * lines, :] = two[:lines, LANES:]
    tail = 2 * top + 2 * lines
    work[tail : tail + SUB, :] = loss[...]
    work[tail + SUB :, :] = jnp.zeros((work.shape[0] - tail - SUB, LANES), F32)
    pl.semaphore_wait(barrier, chips)

    half = work.shape[0] // 2
    piece = half // chips
    spot = lambda c, k: pl.ds(pl.multiple_of(k * half + c * piece, SUB), piece)
    link = lambda kind, o, src, dst, peer: remote(src, dst, sems.at[0, kind * chips + o], sems.at[1, kind * chips + o], peer)
    order = list(enumerate(others + [chip]))
    swap = [link(0, o, work.at[spot(c, 1 - core)], got_pair.at[pl.ds(o * piece, piece)], pair) for o, c in order]
    for c in swap:
        c.start()
    scatter = [link(1, o, work.at[spot(c, core)], got_rest.at[o], 2 * c + core) for o, c in order[:-1]]
    for o, c in order:
        swap[o].wait_recv()
        work[spot(c, core), :] += got_pair[o * piece : (o + 1) * piece, :]
        if o:
            scatter[o - 1].start()
    for c in scatter:
        c.wait_recv()
    own = spot(chip, core)
    work[own, :] += jnp.sum(got_rest[...], axis=0)
    full[own, :] = work[own, :]
    for c in swap + scatter:
        c.wait_send()
    gather = [link(2, o, work.at[own], full.at[own], 2 * c + core) for o, c in order[:-1]]
    for c in gather:
        c.start()
    forward = [link(3, chips - 1, work.at[own], full.at[own], pair)]
    forward[0].start()
    for o, _ in order[:-1]:
        gather[o].wait_recv()
        came = spot(lax.rem(chip + chips - 1 - o, chips), core)
        forward.append(link(3, o, full.at[came], full.at[came], pair))
        forward[-1].start()
    for c in gather:
        c.wait_send()
    for c in forward:
        c.wait()
    one_out[:, :LANES] = full[:top, :]
    one_out[:, LANES:] = full[top : 2 * top, :]
    two_out[:, :LANES] = full[2 * top : 2 * top + classes, :]
    two_out[:, LANES:] = full[2 * top + lines : 2 * top + lines + classes, :]
    mean[...] = jnp.sum(full[tail : tail + SUB, :], keepdims=True) / count[:1, :1]


def prep_kernel(n, chunk, rows, src_in, dst_in, w_in, mask, src_out, dst_out, w_out, used, counts, count, need, total, values, places, hits, mine, theirs, send_sem, recv_sem):
    me, met = greet(n)
    lines, slots = src_in.shape[0], src_out.shape[0]
    src, d, half_w = src_in[...], dst_in[...], w_in[...] * 0.5
    live = w_in[...] != 0.0
    halo = src >= rows
    above = (across((lines, lines)) < down((lines, lines))).astype(F32).astype(BF16)
    is_local, is_halo = jnp.logical_and(live, jnp.logical_not(halo)), jnp.logical_and(live, halo)
    rank = lambda m: prefix(m.astype(F32), above).astype(jnp.int32)
    n_local = jnp.sum(is_local.astype(F32)).astype(jnp.int32)
    n_halo = jnp.sum(is_halo.astype(F32)).astype(jnp.int32)
    local_chunks = (n_local + chunk - 1) // chunk
    counts[0] = local_chunks
    counts[1] = local_chunks + (n_halo + chunk - 1) // chunk
    pos = jnp.where(is_local, rank(is_local), jnp.where(is_halo, rank(is_halo) + local_chunks * chunk, -1))
    pos = jnp.where(pos < 0, pos, (pos & (SUB - 1)) * (slots * LANES // SUB) + (pos >> 3))
    s = jnp.where(halo, src - rows, src)
    w_a = half_w.astype(BF16).astype(F32)
    w_b = (half_w - w_a).astype(BF16).astype(F32)
    w_c = half_w - w_a - w_b
    high = ((s >> 8) * 8 + (d >> 8)).astype(F32)
    planes = [(s % BYTE).astype(F32), (d % BYTE).astype(F32), high, w_a, w_b, w_c]
    for i, p in enumerate(planes):
        values[i * lines : (i + 1) * lines, :] = p
    for i, p in enumerate((pos >> 7, pos & (LANES - 1), jnp.where(is_halo, s >> 7, -1), s & (LANES - 1))):
        places[i * lines : (i + 1) * lines, :] = p
    row = lambda i, q: pl.ds(i * lines + q, 1)
    spot = lambda size, i, q: (down((size, LANES)) == places[row(i, q), :]).astype(F32)
    hits[...] = jnp.zeros_like(hits)

    @pl.loop(0, lines, step=SUB)
    def _(base):
        acc = None
        for r in range(0, SUB, 2):
            lhs = stack_lanes([spot(hits.shape[0], 2, base + q) for q in (r, r + 1)]).astype(BF16)
            rhs = stack_lanes([spot(LANES, 3, base + q) for q in (r, r + 1)]).astype(BF16)
            part = dot(lhs, rhs, COLS_A)
            acc = part if acc is None else acc + part
        hits[...] += acc

    flags = (hits[...] > 0.0).astype(F32)
    used[...] = flags
    side = hits.shape[0] // 2
    most = jnp.maximum(jnp.sum(flags[:side], keepdims=True), jnp.sum(flags[side:], keepdims=True))
    mine[:1, :] = jnp.sum(mask[...].astype(F32), axis=0, keepdims=True)
    mine[1:, :] = jnp.broadcast_to(most, (1, LANES))
    met()
    copies = [remote(mine, theirs.at[o - 1], send_sem.at[o - 1], recv_sem.at[o - 1], lax.rem(me + o, n)) for o in range(1, n)]
    for c in copies:
        c.start()
    total[...] = jnp.zeros_like(total)

    @pl.loop(0, lines, step=SUB)
    def _(base):
        acc = None
        for r in range(0, SUB, 2):
            lhs, rhs = [], []
            for q in (base + r, base + r + 1):
                pick = down((slots, LANES)) == places[row(0, q), :]
                lhs.append(stack_rows([jnp.where(pick, values[row(i, q), :], 0.0) for i in range(len(planes))]))
                rhs.append(spot(LANES, 1, q))
            part = dot(stack_lanes(lhs).astype(BF16), stack_lanes(rhs).astype(BF16), COLS_A)
            acc = part if acc is None else acc + part
        total[...] += acc

    plane = lambda i: total[i * slots : (i + 1) * slots, :]
    high = plane(2).astype(jnp.int32)
    src_out[...] = ((high >> 3) * BYTE + plane(0).astype(jnp.int32)) * 2
    dst_out[...] = ((high & 7) * BYTE + plane(1).astype(jnp.int32)) * 2
    w_out[...] = (plane(3) + plane(4) + plane(5)) * 2.0
    for c in copies:
        c.wait()
    every = jnp.sum(mine[:1, :] + jnp.sum(theirs[:, :1, :], axis=0), keepdims=True)
    count[...] = jnp.maximum(jnp.broadcast_to(every, count.shape), 1.0)
    need[0] = jnp.max(jnp.maximum(mine[1:, :], jnp.max(theirs[:, 1:, :], axis=0))).astype(jnp.int32)


def split_scratch(scratch, arrays):
    n = arrays * SUB
    return scratch[:n], scratch[n], scratch[n + 1 :]


def local_kernel(backward, counts, src, dst, w, table, out, *scratch):
    smem, sems, accs = split_scratch(scratch, 2)
    edges = Edges(0, counts[0], w, (src, dst), smem, sems)
    edges.fetch()
    for a in accs:
        fill_zero(a)
    edges.walk(int(backward), int(not backward), table, accs, True)

    @pl.loop(0, out.shape[0], step=STEP)
    def _(i):
        out[pl.ds(i, STEP), :] = functools.reduce(jnp.add, [a[pl.ds(i, STEP), :] for a in accs])


def forward_halo(edges, from_prev, from_next, part, htab, accs, unpack):
    edges.fetch()
    unpack(from_prev, htab, 0)
    unpack(from_next, htab, htab.shape[0] // 4)
    copy_in(accs[0], part)
    for a in accs[1:]:
        fill_zero(a)
    edges.walk(0, 1, htab, accs, True)


def backward_halo(limit, edges, target, grad, back_prev, back_next, accs, wait, lists=None):
    split = accs[0].shape[0] // 2
    for a in accs:
        for start in (0, split):
            fill_zero(a.at[pl.ds(start, limit * 2)])
    edges.walk(1, target, grad, accs, wait)
    if lists is None:

        @pl.loop(0, back_prev.shape[0], step=SMALL)
        def _(i):
            back_prev[pl.ds(i, SMALL), :] = functools.reduce(jnp.add, [a[pl.ds(i, SMALL), :] for a in accs])
            back_next[pl.ds(i, SMALL), :] = functools.reduce(jnp.add, [a[pl.ds(split + i, SMALL), :] for a in accs])
        return
    side = lists.shape[0] // 2
    half = (back_prev.shape[0] - side) // 3
    n = half // 2
    for k, out in enumerate((back_prev, back_next)):
        start = k * (split // 2)

        @pl.loop(0, half, step=n)
        def _(i):
            i = pl.multiple_of(i, n)
            pack_rows(out, i, half, *halves(accs, start + i, n), *halves(accs, start + half + i, n))

        out[3 * half : 3 * half + side, :] = lists[k * side : (k + 1) * side, :]


def padded(w, buf):
    low = w.shape[0] // SUB * SUB
    buf[low:, :] = jnp.zeros((buf.shape[0] - low, buf.shape[1]), F32)
    buf[:w.shape[0], :] = w[...]
    return buf[...].astype(BF16)


def hidden_kernel(counts, src, dst, w, send, from_prev, from_next, part, w2, hid, tab, to_prev, to_next, back, htab, tab_b, w2_pad, buf, idx, idx_sems, *scratch):
    smem, sems, accs = split_scratch(scratch, 2)
    fetch = fetch_index(send, idx, idx_sems)
    for c in fetch:
        c.start()
    edges = Edges(counts[0], counts[1], w, (src, dst), smem, sems)
    w2_b = padded(w2, w2_pad)
    per = send.shape[1] // LANES
    for i in range(2 * per):
        back[i : i + 1, :] = send[i // per : i // per + 1, (i % per) * LANES : (i % per + 1) * LANES] * 2
    forward_halo(edges, from_prev, from_next, part, htab, accs, unpack_plain)

    @pl.loop(0, hid.shape[0], step=STEP)
    def _(i):
        even, odd = halves(accs, i, STEP)
        h = stack_lanes([jnp.maximum(even, 0.0), jnp.maximum(odd, 0.0)]).astype(BF16)
        hid[pl.ds(i, STEP), :] = h
        t = dot(h, w2_b, COLS_A).astype(BF16)
        tab_b[pl.ds(i, STEP), :] = t
        t = t.astype(F32)
        put_halves(tab, i, STEP, t[:, :LANES], t[:, LANES:])

    for c in fetch:
        c.wait()
    gather_packed(send, idx, tab_b, tab, buf, to_prev, to_next)


def loss_kernel(limit, quad, classes, counts, src, dst, w, src_back, lists, count, from_prev, from_next, part, labels, mask, loss, grad, back_prev, back_next, htab, *scratch):
    smem, sems, accs = split_scratch(scratch, 3)
    edges = Edges(counts[0], counts[1], w, (src, dst, src_back), smem, sems)
    forward_halo(edges, from_prev, from_next, part, htab, accs, unpack_rows)
    lane = across(SQUARE)
    live = lane < classes - LANES
    scale = 1.0 / count[:1, :]
    loss[...] = jnp.zeros_like(loss)

    @pl.loop(0, labels.shape[0], step=quad)
    def _(first):
        for b in [first + q for q in range(quad)]:
            even, odd = halves(accs, b * LANES, LANES)
            odd = jnp.where(live, odd, -jnp.inf)
            keep = spread(mask[pl.ds(b, 1), :])
            label = jnp.where(keep > 0, spread(labels[pl.ds(b, 1), :]), -1)
            hit_even, hit_odd = lane == label, lane + LANES == label
            top = jnp.max(jnp.maximum(even, odd), axis=1, keepdims=True)
            exp_even, exp_odd = jnp.exp(even - top), jnp.exp(odd - top)
            total = jnp.sum(exp_even + exp_odd, axis=1, keepdims=True)
            norm = jnp.where(jnp.logical_and(lane == 0, keep > 0), top + jnp.log(total), 0.0)
            per_row = norm - jnp.where(hit_even, even, jnp.where(hit_odd, odd, 0.0))
            loss[...] += jnp.sum(per_row.reshape(LANES // SUB, *TILE), axis=0)
            share = keep.astype(F32) * scale * (1.0 / total)
            put_halves(
                grad, b * LANES, LANES, *(e * share - jnp.where(hit, scale, 0.0) for e, hit in ((exp_even, hit_even), (exp_odd, hit_odd)))
            )

    backward_halo(limit, edges, 2, grad, back_prev, back_next, accs, False, lists)


def take_returns(back, slots, counts, part, got_prev, got_next, accs):
    return_rows(back, slots, 0, counts[0], got_prev, accs)
    return_rows(back, slots, slots.shape[0] // 2, counts[1], got_next, accs)


def fetch_lines(lines, smem, sems):
    return [pltpu.make_async_copy(lines.at[i], smem.at[pl.ds(i * LANES, LANES)], sems.at[i]) for i in range(lines.shape[0])]


def middle_kernel(limit, counts, src, dst, w, back, got_prev, got_next, part, hid, w2, grad_two, grad, back_prev, back_next, slots, n_back, returned, w2_pad, slot_s, slot_sems, *scratch):
    smem, sems, accs = split_scratch(scratch, 2)
    edges = Edges(counts[0], counts[1], w, (src, dst), smem, sems)
    edges.fetch()
    side = slots.shape[0] // 2
    half = (got_prev.shape[0] - side) // 3
    for k, got in enumerate((got_prev, got_next)):
        slot = got[3 * half :, :].astype(jnp.int32)
        slots[k * side : (k + 1) * side, :] = jnp.maximum(slot, 0) + (1 - k) * side * LANES
        n_back[k] = jnp.sum((slot >= 0).astype(F32)).astype(jnp.int32)
    w2_b = padded(w2, w2_pad)
    unpack_rows(got_prev, returned, 0, half)
    unpack_rows(got_next, returned, 2 * half, half)
    fetch = fetch_lines(slots, slot_s, slot_sems)
    for c in fetch:
        c.start()
    copy_in(accs[0], part)
    for a in accs[1:]:
        fill_zero(a)
    for c in fetch:
        c.wait()
    take_returns(back, slot_s, n_back, part, returned.at[pl.ds(0, 4 * half)], returned.at[pl.ds(4 * half, 4 * half)], accs)
    grad_two[...] = jnp.zeros_like(grad_two)

    @pl.loop(0, hid.shape[0], step=STEP)
    def _(i):
        even, odd = halves(accs, i, STEP)
        d_tab = stack_lanes([even, odd]).astype(BF16)
        h = hid[pl.ds(i, STEP), :]
        grad_two[...] += dot(d_tab, h, ROWS_A)
        d_hid = dot(d_tab, w2_b)
        d_pre = jnp.where(h > 0, d_hid, 0.0)
        put_halves(grad, i, STEP, d_pre[:, :LANES], d_pre[:, LANES:])

    backward_halo(limit, edges, 0, grad, back_prev, back_next, accs, True)


def last_kernel(back, n_back, slots, got_prev, got_next, part, x, grad_one, slot_s, slot_sems, *accs):
    fetch = fetch_lines(slots, slot_s, slot_sems)
    for c in fetch:
        c.start()
    copy_in(accs[0], part)
    for a in accs[1:]:
        fill_zero(a)
    for c in fetch:
        c.wait()
    take_returns(back, slot_s, n_back, part, got_prev, got_next, accs)
    grad_one[...] = jnp.zeros_like(grad_one)

    @pl.loop(0, x.shape[0], step=STEP)
    def _(i):
        even, odd = halves(accs, i, STEP)
        d_tab = stack_lanes([even, odd]).astype(BF16)
        grad_one[...] += dot(x[pl.ds(i, STEP), :], d_tab, ROWS_A)


def call(body, name, outs, ins, scratch, out_specs=None, collective=None, vmem=14):
    extra = {} if collective is None else dict(collective_id=collective, has_side_effects=True)
    return pl.pallas_call(
        body, name=name, out_shape=outs, in_specs=ins, out_specs=out_specs or jax.tree.map(lambda _: VMEM, outs),
        scratch_shapes=[pltpu.VMEM(s, F32) if isinstance(s, tuple) else s for s in scratch],
        compiler_params=pltpu.CompilerParams(vmem_limit_bytes=vmem * 2**20, **extra),
        cost_estimate=pl.CostEstimate(flops=10**10, bytes_accessed=10**7, transcendentals=0),
    )


def solution(mesh):
    num_dev = mesh.shape[AXIS]
    to_next = [(d, (d + 1) % num_dev) for d in range(num_dev)]
    to_prev = [(d, (d - 1) % num_dev) for d in range(num_dev)]

    def step(x, w_one, w_two, send, edge_src, edge_dst, edge_w, labels, mask):
        rows, halo, edges, classes = x.shape[0], send.shape[1], edge_src.shape[0], w_two.shape[1]
        tab, half, w2_pad = (2 * rows, LANES), (2 * halo, LANES), (2 * LANES, 2 * LANES)
        sds = jax.ShapeDtypeStruct
        tab_f = sds(tab, F32)
        half_b, pack_b = sds((halo, 2 * LANES), BF16), sds((3 * halo // 2, LANES), BF16)
        tab_b = pltpu.VMEM((rows, 2 * LANES), BF16)
        one = sds(TILE, F32)
        dma = pltpu.SemaphoreType.DMA
        lines = edges // LANES
        slots = lines + 8
        side = halo // LANES
        w2 = w_two.T
        mask = mask.reshape(-1, LANES)
        labels = labels.reshape(-1, LANES)
        lined = [a.reshape(lines, LANES) for a in (edge_src, edge_dst, edge_w)]
        ints = sds((slots, LANES), jnp.int32)
        sided = sds((2 * side, LANES), F32)
        src, dst, w_lines, used, counts, count, need = call(
            functools.partial(prep_kernel, num_dev, PREP_CHUNK, rows), "prep",
            [ints, ints, sds((slots, LANES), F32), sided, sds((2,), jnp.int32), one, sds((1,), jnp.int32)], [VMEM] * 4,
            [(6 * slots, LANES), (6 * lines, LANES), pltpu.VMEM((4 * lines, LANES), jnp.int32), sided.shape, (2, LANES), (num_dev - 1, 2, LANES)]
            + [dma((num_dev - 1,))] * 2,
            out_specs=[VMEM] * 4 + [SMEM, VMEM, SMEM], vmem=60, collective=0,
        )(*lined, mask)

        def run(limit):
            compact = limit < halo
            pack_f, half_f = sds((3 * limit // 2 + side, LANES), F32), sds((2 * limit, LANES), F32)
            list_s = [pltpu.SMEM((halo,), jnp.int32), dma((side,))]
            tab_one, to_p, to_n, w, src_back, lists = call(
                functools.partial(first_kernel, compact, halo), "first", [tab_f, half_b, half_b, sds((slots * LANES, LANES), F32), ints, sided],
                [VMEM] * 3 + [SMEM] + [VMEM] * 3, [tab_b, half] + list_s, vmem=8,
            )(x, w_one, send, counts, src, w_lines, used)
            from_prev = lax.ppermute(to_n, AXIS, to_next)
            from_next = lax.ppermute(to_p, AXIS, to_prev)
            flat, flat_dst, flat_back = src.reshape(-1), dst.reshape(-1), src_back.reshape(-1)

            four = [tab] * 4
            walk = [SMEM, ANY, ANY, VMEM]
            size = slots * LANES // SUB
            walk_s = lambda n: [pltpu.SMEM((size,), jnp.int32)] * (n * SUB) + [dma((n * SUB, size // SEGMENT))]
            slot_s = [pltpu.SMEM((2 * halo,), jnp.int32), dma((2 * side,))]
            local, local_back = (
                call(functools.partial(local_kernel, back), "local_edges", tab_f, walk + [VMEM], walk_s(2) + four + four, vmem=22)
                for back in (False, True)
            )
            part = local(counts, flat, flat_dst, w, tab_one)
            hid, tab_two, to_p, to_n, back = call(
                hidden_kernel, "hidden",
                [sds((rows, 2 * LANES), BF16), tab_f, pack_b, pack_b, sds((2 * side, LANES), jnp.int32)],
                walk + [VMEM] * 5, [tab, tab_b, w2_pad, half] + list_s + walk_s(2) + four,
            )(counts, flat, flat_dst, w, send, from_prev, from_next, part, w2)
            from_prev = lax.ppermute(to_n, AXIS, to_next)
            from_next = lax.ppermute(to_p, AXIS, to_prev)
            back = back.reshape(-1)
            part = local(counts, flat, flat_dst, w, tab_two)
            loss, grad, to_p, to_n = call(
                functools.partial(loss_kernel, limit, 4, classes), "loss", [one, tab_f, pack_f, pack_f],
                walk + [ANY] + [VMEM] * 7, [tab] + walk_s(3) + four,
            )(counts, flat, flat_dst, w, flat_back, lists, count, from_prev, from_next, part, labels, mask)
            got_prev = lax.ppermute(to_p, AXIS, to_prev)
            got_next = lax.ppermute(to_n, AXIS, to_next)
            part = local_back(counts, flat, flat_dst, w, grad)
            grad_two, grad, to_p, to_n, slot, n_back = call(
                functools.partial(middle_kernel, limit), "middle",
                [sds(w2_pad, F32), tab_f, half_f, half_f, sds((2 * side, LANES), jnp.int32), sds((2,), jnp.int32)],
                walk + [SMEM] + [VMEM] * 5, [(4 * limit, LANES), w2_pad] + slot_s + walk_s(2) + four, out_specs=[VMEM] * 5 + [SMEM],
            )(counts, flat_back, flat_dst, w, back, got_prev, got_next, part, hid, w2)
            got_prev = lax.ppermute(to_p, AXIS, to_prev)
            got_next = lax.ppermute(to_n, AXIS, to_next)
            part = local_back(counts, flat, flat_dst, w, grad)
            grad_one = call(
                last_kernel, "last", sds((x.shape[1], 2 * LANES), F32), [SMEM, SMEM, ANY] + [VMEM] * 4, slot_s + four
            )(back, n_back, slot, got_prev, got_next, part, x)
            return grad_one, grad_two, loss

        few = halo // 32 * 19
        grad_one, grad_two, loss = lax.cond(need.reshape(()) > few, lambda: run(halo), lambda: run(few))
        unit = SUB * num_dev
        lines = 2 * (x.shape[1] + -(-classes // SUB) * SUB) + SUB
        lines = -(-lines // unit) * unit
        grad_one, grad_two, mean = call(
            functools.partial(reduce_kernel, num_dev), "reduce", [sds(grad_one.shape, F32), sds((classes, 2 * LANES), F32), sds((1, 1), F32)],
            [VMEM] * 4, [(lines, LANES), (lines, LANES), (lines // 2, LANES), (num_dev // 2 - 1, lines // num_dev, LANES), dma((2, 2 * num_dev))],
            collective=1, vmem=8,
        )(grad_one, grad_two, loss, count)
        return mean.reshape(()), grad_one, grad_two.T

    row = P(AXIS)
    return jax.shard_map(
        step, mesh=mesh, in_specs=(row, P(), P(), row, row, row, row, row, row), out_specs=(P(), P(), P()), check_vma=False
    )
```

```python
import functools

import jax
import jax.numpy as jnp
from jax import lax
from jax.experimental import pallas as pl
from jax.experimental.pallas import tpu as pltpu
from jax.sharding import PartitionSpec as P

AXIS = "graph"
LANES = 128
ROWS_A = (((0,), (0,)), ((), ()))
COLS_A = (((1,), (1,)), ((), ()))
F32, BF16 = jnp.float32, jnp.bfloat16
VMEM = pl.BlockSpec(memory_space=pltpu.VMEM)
SMEM = pl.BlockSpec(memory_space=pltpu.SMEM)
ANY = pl.BlockSpec(memory_space=pl.ANY)
STEP = 512
BLOCK = 256
BYTE = BLOCK
SUB = 8
TILE = (SUB, LANES)
SQUARE = (LANES, LANES)
PREP_CHUNK = 64
SMALL = PREP_CHUNK
SEGMENT = 1024
MESH = pl.DeviceIdType.MESH


def dot(a, b, dims=(((1,), (0,)), ((), ()))):
    return lax.dot_general(a, b, dims, preferred_element_type=F32)


def fill_zero(ref):
    step = BLOCK if ref.shape[0] % BLOCK == 0 else SMALL
    zero = jnp.zeros((step, LANES), F32)

    @pl.loop(0, ref.shape[0], step=step)
    def _(i):
        ref[pl.ds(i, step), :] = zero


def copy_in(dst, src):
    @pl.loop(0, dst.shape[0], step=STEP)
    def _(i):
        dst[pl.ds(i, STEP), :] = src[pl.ds(i, STEP), :].astype(F32)


class Edges:
    def __init__(self, first, last, w, arrays, smem, sems):
        self.first, self.last, self.w = first, last, w
        self.pairs = tuple(zip(arrays, smem))
        self.sems = sems

    def copies(self, seg):
        part = pl.ds(pl.multiple_of(seg * SEGMENT, SEGMENT), SEGMENT)
        return [pltpu.make_async_copy(a.at[part], b.at[part], self.sems.at[i, seg]) for i, (a, b) in enumerate(self.pairs)]

    def fetch(self):
        per = SEGMENT // PREP_CHUNK
        for seg in range(self.pairs[0][1].shape[0] // SEGMENT):

            @pl.when(jnp.logical_and(seg * per < self.last, (seg + 1) * per > self.first))
            def _():
                for c in self.copies(seg):
                    c.start()

    def walk(self, chunk, from_idx, to_idx, table, accs, wait):
        group, per, ratio = len(accs), SEGMENT // chunk, PREP_CHUNK // chunk
        first, last = self.first * ratio, self.last * ratio

        def body(c, _):
            base = c * chunk
            w_chunk = self.w.at[pl.ds(pl.multiple_of(base, chunk), chunk)]
            for g in range(0, chunk, group):
                pend = []
                for u in range(group):
                    k = base + g + u
                    s = pl.multiple_of(from_idx[k], 2)
                    d = pl.multiple_of(to_idx[k], 2)
                    pend.append((d, accs[u][pl.ds(d, 2), :] + table[pl.ds(s, 2), :] * w_chunk[g + u : g + u + 1, :]))
                for u in range(group):
                    accs[u][pl.ds(pend[u][0], 2), :] = pend[u][1]
            return 0

        if not wait:
            lax.fori_loop(first, last, body, 0)
            return

        def segment(seg, _):
            for c in self.copies(seg):
                c.wait()
            lax.fori_loop(jnp.maximum(first, seg * per), jnp.minimum(last, (seg + 1) * per), body, 0)
            return 0

        lax.fori_loop(first // per, (last + per - 1) // per, segment, 0)


def one_hot_rows(idx, which, start, table):
    lane = across(SQUARE)
    hot = []
    for q in range(2):
        want = spread(idx[which : which + 1, pl.ds(pl.multiple_of(start + q * LANES, LANES), LANES)])
        hot.append(
            stack_lanes([jnp.where(want == lane + LANES * j, 1.0, 0.0).astype(BF16) for j in range(table.shape[0] // LANES)])
        )
    return dot(stack_rows(hot), table[...])


def low_lanes(rows):
    return across((rows, LANES)) < LANES // 2


def swap_lanes(v):
    return pltpu.roll(v, LANES // 2, 1)


def fetch_index(send, idx, sems):
    parts = [pl.ds(i, LANES) for i in range(0, send.shape[1], LANES)]
    return [pltpu.make_async_copy(send.at[1, p], idx.at[p], sems.at[i]) for i, p in enumerate(parts)]


def gather_block(send, idx, i, table_b, table, buf):
    got = one_hot_rows(send, 0, i, table_b)
    out = buf.at[pl.ds(pl.multiple_of(2 * i, 512), 512)]
    for u in range(BLOCK):
        s = pl.multiple_of(idx[i + u] * 2, 2)
        out[2 * u : 2 * u + 2, :] = table[pl.ds(s, 2), :]
    return got


def gather_rows(send, idx, table_b, table, buf, to_prev, to_next, also):
    @pl.loop(0, to_prev.shape[0], step=BLOCK)
    def _(i):
        i = pl.multiple_of(i, BLOCK)
        to_prev[pl.ds(i, BLOCK), :] = gather_block(send, idx, i, table_b, table, buf).astype(BF16)
        also(i)

    @pl.loop(0, to_next.shape[0], step=BLOCK)
    def _(i):
        to_next[pl.ds(pl.multiple_of(i, BLOCK), BLOCK), :] = stack_lanes(halves([buf], i, BLOCK)).astype(BF16)


def pack_rows(out, i, half, a_even, a_odd, b_even, b_odd):
    n = a_even.shape[0]
    out[pl.ds(i, n), :] = a_even.astype(out.dtype)
    out[pl.ds(half + i, n), :] = b_even.astype(out.dtype)
    out[pl.ds(2 * half + i, n), :] = jnp.where(low_lanes(n), a_odd, swap_lanes(b_odd)).astype(out.dtype)


def gather_packed(send, idx, table_b, table, buf, to_prev, to_next):
    half = to_prev.shape[0] // 3

    @pl.loop(0, half, step=BLOCK)
    def _(i):
        i = pl.multiple_of(i, BLOCK)
        a = gather_block(send, idx, i, table_b, table, buf)
        b = gather_block(send, idx, half + i, table_b, table, buf)
        pack_rows(to_prev, i, half, a[:, :LANES], a[:, LANES:], b[:, :LANES], b[:, LANES:])

    @pl.loop(0, half, step=BLOCK)
    def _(i):
        i = pl.multiple_of(i, BLOCK)
        pack_rows(to_next, i, half, *halves([buf], i, BLOCK), *halves([buf], half + i, BLOCK))


def unpack_rows(got, table, start, half=None):
    half = got.shape[0] // 3 if half is None else half
    n = half // 2

    @pl.loop(0, half, step=n)
    def _(i):
        i = pl.multiple_of(i, n)
        a, b, both = (got[pl.ds(k + i, n), :].astype(F32) for k in (0, half, 2 * half))
        put_halves(table, start + i, n, a, jnp.where(low_lanes(n), both, 0.0))
        put_halves(table, start + half + i, n, b, jnp.where(low_lanes(n), swap_lanes(both), 0.0))


def unpack_plain(got, table, start):
    @pl.loop(0, got.shape[0], step=BLOCK)
    def _(i):
        t = got[pl.ds(i, BLOCK), :].astype(F32)
        put_halves(table, start + i, BLOCK, t[:, :LANES], t[:, LANES:])


def spread(row):
    return jnp.transpose(jnp.broadcast_to(row, SQUARE))


def return_rows(back, slots, start, count, vals, accs, chunk=32):
    group = len(accs)

    def body(c, _):
        block = vals.at[pl.ds(pl.multiple_of(c * 2 * chunk, 2 * chunk), 2 * chunk)]
        for g in range(0, chunk, group):
            pend = []
            for u in range(group):
                d = pl.multiple_of(back[slots[start + c * chunk + g + u]], 2)
                pend.append((d, accs[u][pl.ds(d, 2), :] + block[2 * (g + u) : 2 * (g + u) + 2, :]))
            for u in range(group):
                accs[u][pl.ds(pend[u][0], 2), :] = pend[u][1]
        return 0

    lax.fori_loop(0, (count + chunk - 1) // chunk, body, 0)


def group(i, n, which):
    return pl.ds(2 * i + which, n, stride=2), slice(None)


def halves(accs, i, n):
    return [functools.reduce(jnp.add, [a[group(i, n, k)] for a in accs]) for k in range(2)]


def put_halves(table, i, n, *parts):
    for k, part in enumerate(parts):
        table[group(i, n, k)] = part


def stack_rows(parts):
    return jnp.concatenate(parts, axis=0)


def stack_lanes(parts):
    return jnp.concatenate(parts, axis=1)


def down(shape):
    return lax.broadcasted_iota(jnp.int32, shape, 0)


def across(shape):
    return lax.broadcasted_iota(jnp.int32, shape, 1)


def prefix(mask, above):
    m = mask.astype(BF16)
    before = (down(SQUARE) < across(SQUARE)).astype(BF16)
    return dot(m, before) + dot(above, dot(m, jnp.ones(SQUARE, BF16)).astype(BF16))


def rank_halo(halo, counts, src, used, src_back, lists):
    lines = used.shape[0]
    side = lines // 2
    i, j = down((lines, lines)), across((lines, lines))
    above = jnp.logical_and(j < i, (j >= side) == (i >= side)).astype(F32).astype(BF16)
    rank = prefix(used[...], above).astype(jnp.int32)
    low, high = rank & (LANES - 1), rank >> 7
    table = stack_rows([low.astype(F32), high.astype(F32)]).astype(BF16)

    quad = 4

    def four(c, _):
        slot = [src[pl.ds(c * quad + q, 1), :] >> 1 for q in range(quad)]
        spots = stack_lanes([(down(SQUARE) == (t & (LANES - 1))).astype(F32) for t in slot]).astype(BF16)
        got = dot(table, spots)
        h = stack_lanes(slot) >> 7
        got = jnp.where(down(got[:lines].shape) == h, got[:lines] + LANES * got[lines:], 0.0)
        got = (jnp.sum(got, axis=0, keepdims=True).astype(jnp.int32) + jnp.where(h >= side, halo, 0)) * 2
        for q in range(quad):
            src_back[pl.ds(c * quad + q, 1), :] = got[:, q * LANES : (q + 1) * LANES]
        return 0

    ratio = quad * LANES // PREP_CHUNK
    lax.fori_loop(counts[0] // ratio, (counts[1] + ratio - 1) // ratio, four, 0)
    for k in range(2):
        acc = jnp.zeros((24, LANES), F32)
        for hh in range(side):
            q = k * side + hh
            pick = jnp.where(down(TILE) == high[q : q + 1, :], used[q : q + 1, :], 0.0)
            lhs = stack_rows([pick * across(TILE).astype(F32), pick * hh, pick]).astype(BF16)
            acc += dot(lhs, (down(SQUARE) == low[q : q + 1, :]).astype(F32).astype(BF16), COLS_A)
        slots = acc[:8] + LANES * acc[8:16]
        lists[k * side : (k + 1) * side, :] = jnp.where(acc[16:24] > 0.0, slots[:side], -1.0)


def first_kernel(compact, halo, tab, tab_b, send, counts, src, w, used, to_prev, to_next, w_out, src_back, lists, buf, idx, sems):
    fetch = fetch_index(send, idx, sems)
    for c in fetch:
        c.start()
    src_back[...] = src[...]
    if compact:
        rank_halo(halo, counts, src, used, src_back, lists)
    else:
        line = down(lists.shape)
        line = jnp.where(line >= lists.shape[0] // 2, line - lists.shape[0] // 2, line)
        lists[...] = (line * LANES + across(lists.shape)).astype(F32)
    for c in fetch:
        c.wait()
    share = w.shape[0] * BLOCK // halo

    def widen(i):
        for q in range(share):
            r = i // BLOCK * share + q
            w_out[pl.ds(pl.multiple_of(r * LANES, LANES), LANES), :] = spread(w[pl.ds(r, 1), :])

    gather_rows(send, idx, tab_b, tab, buf, to_prev, to_next, widen)


def greet(n):
    me = lax.axis_index(AXIS)
    barrier = pltpu.get_barrier_semaphore()
    for o in range(1, n):
        pl.semaphore_signal(barrier, inc=1, device_id=(lax.rem(me + o, n),), device_id_type=MESH)
    return me, lambda: pl.semaphore_wait(barrier, n - 1)


def remote(src, dst, send_sem, recv_sem, peer):
    return pltpu.make_async_remote_copy(
        src_ref=src, dst_ref=dst, send_sem=send_sem, recv_sem=recv_sem, device_id=(peer,), device_id_type=MESH
    )


def reduce_kernel(n, one, two, loss, count, one_out, two_out, mean, work, full, got_pair, got_rest, sems):
    me = lax.axis_index(AXIS)
    chips, core = n // 2, lax.rem(me, 2)
    chip = lax.div(me, 2)
    pair = me + 1 - 2 * core
    others = [lax.rem(chip + o, chips) for o in range(1, chips)]
    barrier = pltpu.get_barrier_semaphore()
    for p in [pair] + [2 * c + core for c in others]:
        pl.semaphore_signal(barrier, inc=1, device_id=(p,), device_id_type=MESH)
    classes = two_out.shape[0]
    lines = -(-classes // SUB) * SUB
    top, wide = one.shape
    work[:top, :] = one[:, :LANES]
    work[top : 2 * top, :] = one[:, LANES:]
    work[2 * top : 2 * top + lines, :] = two[:lines, :LANES]
    work[2 * top + lines : 2 * top + 2 * lines, :] = two[:lines, LANES:]
    tail = 2 * top + 2 * lines
    work[tail : tail + SUB, :] = loss[...]
    work[tail + SUB :, :] = jnp.zeros((work.shape[0] - tail - SUB, LANES), F32)
    pl.semaphore_wait(barrier, chips)

    half = work.shape[0] // 2
    piece = half // chips
    spot = lambda c, k: pl.ds(pl.multiple_of(k * half + c * piece, SUB), piece)
    link = lambda kind, o, src, dst, peer: remote(src, dst, sems.at[0, kind * chips + o], sems.at[1, kind * chips + o], peer)
    order = list(enumerate(others + [chip]))
    swap = [link(0, o, work.at[spot(c, 1 - core)], got_pair.at[pl.ds(o * piece, piece)], pair) for o, c in order]
    for c in swap:
        c.start()
    scatter = [link(1, o, work.at[spot(c, core)], got_rest.at[o], 2 * c + core) for o, c in order[:-1]]
    for o, c in order:
        swap[o].wait_recv()
        work[spot(c, core), :] += got_pair[o * piece : (o + 1) * piece, :]
        if o:
            scatter[o - 1].start()
    for c in scatter:
        c.wait_recv()
    own = spot(chip, core)
    work[own, :] += jnp.sum(got_rest[...], axis=0)
    full[own, :] = work[own, :]
    for c in swap + scatter:
        c.wait_send()
    gather = [link(2, o, work.at[own], full.at[own], 2 * c + core) for o, c in order[:-1]]
    for c in gather:
        c.start()
    forward = [link(3, chips - 1, work.at[own], full.at[own], pair)]
    forward[0].start()
    for o, _ in order[:-1]:
        gather[o].wait_recv()
        came = spot(lax.rem(chip + chips - 1 - o, chips), core)
        forward.append(link(3, o, full.at[came], full.at[came], pair))
        forward[-1].start()
    for c in gather:
        c.wait_send()
    for c in forward:
        c.wait()
    one_out[:, :LANES] = full[:top, :]
    one_out[:, LANES:] = full[top : 2 * top, :]
    two_out[:, :LANES] = full[2 * top : 2 * top + classes, :]
    two_out[:, LANES:] = full[2 * top + lines : 2 * top + lines + classes, :]
    mean[...] = jnp.sum(full[tail : tail + SUB, :], keepdims=True) / count[:1, :1]


def prep_kernel(n, chunk, rows, src_in, dst_in, w_in, mask, x, w1, tab, tab_b, src_out, dst_out, w_out, used, counts, count, need, total, values, places, hits, mine, theirs, send_sem, recv_sem):
    me, met = greet(n)
    lines, slots = src_in.shape[0], src_out.shape[0]
    src, d, half_w = src_in[...], dst_in[...], w_in[...] * 0.5
    live = w_in[...] != 0.0
    halo = src >= rows
    above = (across((lines, lines)) < down((lines, lines))).astype(F32).astype(BF16)
    is_local, is_halo = jnp.logical_and(live, jnp.logical_not(halo)), jnp.logical_and(live, halo)
    rank = lambda m: prefix(m.astype(F32), above).astype(jnp.int32)
    n_local = jnp.sum(is_local.astype(F32)).astype(jnp.int32)
    n_halo = jnp.sum(is_halo.astype(F32)).astype(jnp.int32)
    local_chunks = (n_local + chunk - 1) // chunk
    counts[0] = local_chunks
    counts[1] = local_chunks + (n_halo + chunk - 1) // chunk
    pos = jnp.where(is_local, rank(is_local), jnp.where(is_halo, rank(is_halo) + local_chunks * chunk, -1))
    s = jnp.where(halo, src - rows, src)
    w_a = half_w.astype(BF16).astype(F32)
    w_b = (half_w - w_a).astype(BF16).astype(F32)
    w_c = half_w - w_a - w_b
    high = ((s >> 8) * 8 + (d >> 8)).astype(F32)
    planes = [(s % BYTE).astype(F32), (d % BYTE).astype(F32), high, w_a, w_b, w_c]
    for i, p in enumerate(planes):
        values[i * lines : (i + 1) * lines, :] = p
    for i, p in enumerate((pos >> 7, pos & (LANES - 1), jnp.where(is_halo, s >> 7, -1), s & (LANES - 1))):
        places[i * lines : (i + 1) * lines, :] = p
    row = lambda i, q: pl.ds(i * lines + q, 1)
    spot = lambda size, i, q: (down((size, LANES)) == places[row(i, q), :]).astype(F32)
    hits[...] = jnp.zeros_like(hits)

    @pl.loop(0, lines, step=SUB)
    def _(base):
        acc = None
        for r in range(0, SUB, 2):
            lhs = stack_lanes([spot(hits.shape[0], 2, base + q) for q in (r, r + 1)]).astype(BF16)
            rhs = stack_lanes([spot(LANES, 3, base + q) for q in (r, r + 1)]).astype(BF16)
            part = dot(lhs, rhs, COLS_A)
            acc = part if acc is None else acc + part
        hits[...] += acc

    flags = (hits[...] > 0.0).astype(F32)
    used[...] = flags
    side = hits.shape[0] // 2
    most = jnp.maximum(jnp.sum(flags[:side], keepdims=True), jnp.sum(flags[side:], keepdims=True))
    mine[:1, :] = jnp.sum(mask[...].astype(F32), axis=0, keepdims=True)
    mine[1:, :] = jnp.broadcast_to(most, (1, LANES))
    met()
    copies = [remote(mine, theirs.at[o - 1], send_sem.at[o - 1], recv_sem.at[o - 1], lax.rem(me + o, n)) for o in range(1, n)]
    for c in copies:
        c.start()
    total[...] = jnp.zeros_like(total)

    @pl.loop(0, lines, step=SUB)
    def _(base):
        acc = None
        for r in range(0, SUB, 2):
            lhs, rhs = [], []
            for q in (base + r, base + r + 1):
                pick = down((slots, LANES)) == places[row(0, q), :]
                lhs.append(stack_rows([jnp.where(pick, values[row(i, q), :], 0.0) for i in range(len(planes))]))
                rhs.append(spot(LANES, 1, q))
            part = dot(stack_lanes(lhs).astype(BF16), stack_lanes(rhs).astype(BF16), COLS_A)
            acc = part if acc is None else acc + part
        total[...] += acc

    plane = lambda i: total[i * slots : (i + 1) * slots, :]
    high = plane(2).astype(jnp.int32)
    w1_b = w1[...].astype(BF16)

    @pl.loop(0, rows, step=STEP)
    def _(i):
        t = dot(x[pl.ds(i, STEP), :], w1_b).astype(BF16)
        tab_b[pl.ds(i, STEP), :] = t
        t = t.astype(F32)
        put_halves(tab, i, STEP, t[:, :LANES], t[:, LANES:])

    src_out[...] = ((high >> 3) * BYTE + plane(0).astype(jnp.int32)) * 2
    dst_out[...] = ((high & 7) * BYTE + plane(1).astype(jnp.int32)) * 2
    w_out[...] = (plane(3) + plane(4) + plane(5)) * 2.0
    for c in copies:
        c.wait()
    every = jnp.sum(mine[:1, :] + jnp.sum(theirs[:, :1, :], axis=0), keepdims=True)
    count[...] = jnp.maximum(jnp.broadcast_to(every, count.shape), 1.0)
    need[0] = jnp.max(jnp.maximum(mine[1:, :], jnp.max(theirs[:, 1:, :], axis=0))).astype(jnp.int32)


def local_kernel(chunk, backward, counts, src, dst, w, table, out, src_s, dst_s, sems, *accs):
    edges = Edges(0, counts[0], w, (src, dst), (src_s, dst_s), sems)
    edges.fetch()
    for a in accs:
        fill_zero(a)
    edges.walk(chunk, *((dst_s, src_s) if backward else (src_s, dst_s)), table, accs, True)

    @pl.loop(0, out.shape[0], step=STEP)
    def _(i):
        out[pl.ds(i, STEP), :] = functools.reduce(jnp.add, [a[pl.ds(i, STEP), :] for a in accs])


def forward_halo(chunk, edges, src_s, dst_s, from_prev, from_next, part, htab, accs, unpack):
    edges.fetch()
    unpack(from_prev, htab, 0)
    unpack(from_next, htab, htab.shape[0] // 4)
    copy_in(accs[0], part)
    for a in accs[1:]:
        fill_zero(a)
    edges.walk(chunk, src_s, dst_s, htab, accs, True)


def backward_halo(limit, chunk, edges, src_s, dst_s, grad, back_prev, back_next, accs, wait, lists=None):
    split = accs[0].shape[0] // 2
    for a in accs:
        for start in (0, split):
            fill_zero(a.at[pl.ds(start, limit * 2)])
    edges.walk(chunk, dst_s, src_s, grad, accs, wait)
    if lists is None:

        @pl.loop(0, back_prev.shape[0], step=SMALL)
        def _(i):
            back_prev[pl.ds(i, SMALL), :] = functools.reduce(jnp.add, [a[pl.ds(i, SMALL), :] for a in accs])
            back_next[pl.ds(i, SMALL), :] = functools.reduce(jnp.add, [a[pl.ds(split + i, SMALL), :] for a in accs])
        return
    side = lists.shape[0] // 2
    half = (back_prev.shape[0] - side) // 3
    n = half // 2
    for k, out in enumerate((back_prev, back_next)):
        start = k * (split // 2)

        @pl.loop(0, half, step=n)
        def _(i):
            i = pl.multiple_of(i, n)
            pack_rows(out, i, half, *halves(accs, start + i, n), *halves(accs, start + half + i, n))

        out[3 * half : 3 * half + side, :] = lists[k * side : (k + 1) * side, :]


def padded(w, buf):
    low = w.shape[0] // SUB * SUB
    buf[low:, :] = jnp.zeros((buf.shape[0] - low, buf.shape[1]), F32)
    buf[:w.shape[0], :] = w[...]
    return buf[...].astype(BF16)


def hidden_kernel(chunk, counts, src, dst, w, send, from_prev, from_next, part, w2, hid, tab, to_prev, to_next, back, htab, tab_b, w2_pad, buf, idx, idx_sems, src_s, dst_s, sems, *accs):
    fetch = fetch_index(send, idx, idx_sems)
    for c in fetch:
        c.start()
    edges = Edges(counts[0], counts[1], w, (src, dst), (src_s, dst_s), sems)
    w2_b = padded(w2, w2_pad)
    per = send.shape[1] // LANES
    for i in range(2 * per):
        back[i : i + 1, :] = send[i // per : i // per + 1, (i % per) * LANES : (i % per + 1) * LANES] * 2
    forward_halo(chunk, edges, src_s, dst_s, from_prev, from_next, part, htab, accs, unpack_plain)

    @pl.loop(0, hid.shape[0], step=STEP)
    def _(i):
        even, odd = halves(accs, i, STEP)
        h = stack_lanes([jnp.maximum(even, 0.0), jnp.maximum(odd, 0.0)]).astype(BF16)
        hid[pl.ds(i, STEP), :] = h
        t = dot(h, w2_b, COLS_A).astype(BF16)
        tab_b[pl.ds(i, STEP), :] = t
        t = t.astype(F32)
        put_halves(tab, i, STEP, t[:, :LANES], t[:, LANES:])

    for c in fetch:
        c.wait()
    gather_packed(send, idx, tab_b, tab, buf, to_prev, to_next)


def loss_kernel(limit, quad, chunk, classes, counts, src, dst, w, src_back, lists, count, from_prev, from_next, part, labels, mask, loss, grad, back_prev, back_next, htab, src_s, dst_s, back_s, sems, *accs):
    edges = Edges(counts[0], counts[1], w, (src, dst, src_back), (src_s, dst_s, back_s), sems)
    forward_halo(chunk, edges, src_s, dst_s, from_prev, from_next, part, htab, accs, unpack_rows)
    lane = across(SQUARE)
    live = lane < classes - LANES
    scale = 1.0 / count[:1, :]
    loss[...] = jnp.zeros_like(loss)

    @pl.loop(0, labels.shape[0], step=quad)
    def _(first):
        for b in [first + q for q in range(quad)]:
            even, odd = halves(accs, b * LANES, LANES)
            odd = jnp.where(live, odd, -jnp.inf)
            keep = spread(mask[pl.ds(b, 1), :])
            label = jnp.where(keep > 0, spread(labels[pl.ds(b, 1), :]), -1)
            hit_even, hit_odd = lane == label, lane + LANES == label
            top = jnp.max(jnp.maximum(even, odd), axis=1, keepdims=True)
            exp_even, exp_odd = jnp.exp(even - top), jnp.exp(odd - top)
            total = jnp.sum(exp_even + exp_odd, axis=1, keepdims=True)
            norm = jnp.where(jnp.logical_and(lane == 0, keep > 0), top + jnp.log(total), 0.0)
            per_row = norm - jnp.where(hit_even, even, jnp.where(hit_odd, odd, 0.0))
            loss[...] += jnp.sum(per_row.reshape(LANES // SUB, *TILE), axis=0)
            share = keep.astype(F32) * scale * (1.0 / total)
            put_halves(
                grad, b * LANES, LANES, *(e * share - jnp.where(hit, scale, 0.0) for e, hit in ((exp_even, hit_even), (exp_odd, hit_odd)))
            )

    backward_halo(limit, chunk, edges, back_s, dst_s, grad, back_prev, back_next, accs, False, lists)


def take_returns(back, slots, counts, part, got_prev, got_next, accs):
    return_rows(back, slots, 0, counts[0], got_prev, accs)
    return_rows(back, slots, slots.shape[0] // 2, counts[1], got_next, accs)


def fetch_lines(lines, smem, sems):
    return [pltpu.make_async_copy(lines.at[i], smem.at[pl.ds(i * LANES, LANES)], sems.at[i]) for i in range(lines.shape[0])]


def middle_kernel(limit, chunk, counts, src, dst, w, back, got_prev, got_next, part, hid, w2, grad_two, grad, back_prev, back_next, slots, n_back, returned, w2_pad, slot_s, slot_sems, src_s, dst_s, sems, *accs):
    edges = Edges(counts[0], counts[1], w, (src, dst), (src_s, dst_s), sems)
    edges.fetch()
    side = slots.shape[0] // 2
    half = (got_prev.shape[0] - side) // 3
    for k, got in enumerate((got_prev, got_next)):
        slot = got[3 * half :, :].astype(jnp.int32)
        slots[k * side : (k + 1) * side, :] = jnp.maximum(slot, 0) + (1 - k) * side * LANES
        n_back[k] = jnp.sum((slot >= 0).astype(F32)).astype(jnp.int32)
    w2_b = padded(w2, w2_pad)
    unpack_rows(got_prev, returned, 0, half)
    unpack_rows(got_next, returned, 2 * half, half)
    fetch = fetch_lines(slots, slot_s, slot_sems)
    for c in fetch:
        c.start()
    copy_in(accs[0], part)
    for a in accs[1:]:
        fill_zero(a)
    for c in fetch:
        c.wait()
    take_returns(back, slot_s, n_back, part, returned.at[pl.ds(0, 4 * half)], returned.at[pl.ds(4 * half, 4 * half)], accs)
    grad_two[...] = jnp.zeros_like(grad_two)

    @pl.loop(0, hid.shape[0], step=STEP)
    def _(i):
        even, odd = halves(accs, i, STEP)
        d_tab = stack_lanes([even, odd]).astype(BF16)
        h = hid[pl.ds(i, STEP), :]
        grad_two[...] += dot(d_tab, h, ROWS_A)
        d_hid = dot(d_tab, w2_b)
        d_pre = jnp.where(h > 0, d_hid, 0.0)
        put_halves(grad, i, STEP, d_pre[:, :LANES], d_pre[:, LANES:])

    backward_halo(limit, chunk, edges, src_s, dst_s, grad, back_prev, back_next, accs, True)


def last_kernel(back, n_back, slots, got_prev, got_next, part, x, grad_one, slot_s, slot_sems, *accs):
    fetch = fetch_lines(slots, slot_s, slot_sems)
    for c in fetch:
        c.start()
    copy_in(accs[0], part)
    for a in accs[1:]:
        fill_zero(a)
    for c in fetch:
        c.wait()
    take_returns(back, slot_s, n_back, part, got_prev, got_next, accs)
    grad_one[...] = jnp.zeros_like(grad_one)

    @pl.loop(0, x.shape[0], step=STEP)
    def _(i):
        even, odd = halves(accs, i, STEP)
        d_tab = stack_lanes([even, odd]).astype(BF16)
        grad_one[...] += dot(x[pl.ds(i, STEP), :], d_tab, ROWS_A)


def call(body, name, outs, ins, scratch, out_specs=None, collective=None, vmem=14):
    extra = {} if collective is None else dict(collective_id=collective, has_side_effects=True)
    return pl.pallas_call(
        body, name=name, out_shape=outs, in_specs=ins, out_specs=out_specs or jax.tree.map(lambda _: VMEM, outs),
        scratch_shapes=[pltpu.VMEM(s, F32) if isinstance(s, tuple) else s for s in scratch],
        compiler_params=pltpu.CompilerParams(vmem_limit_bytes=vmem * 2**20, **extra),
        cost_estimate=pl.CostEstimate(flops=10**10, bytes_accessed=10**7, transcendentals=0),
    )


def solution(mesh):
    num_dev = mesh.shape[AXIS]
    to_next = [(d, (d + 1) % num_dev) for d in range(num_dev)]
    to_prev = [(d, (d - 1) % num_dev) for d in range(num_dev)]

    def step(x, w_one, w_two, send, edge_src, edge_dst, edge_w, labels, mask):
        rows, halo, edges, classes = x.shape[0], send.shape[1], edge_src.shape[0], w_two.shape[1]
        tab, half, w2_pad = (2 * rows, LANES), (2 * halo, LANES), (2 * LANES, 2 * LANES)
        sds = jax.ShapeDtypeStruct
        tab_f = sds(tab, F32)
        half_b, pack_b = sds((halo, 2 * LANES), BF16), sds((3 * halo // 2, LANES), BF16)
        wide_b = pltpu.VMEM((rows, 2 * LANES), BF16)
        one = sds(TILE, F32)
        dma = pltpu.SemaphoreType.DMA
        chunk_l, chunk_h = 64, 32
        lines = edges // LANES
        slots = lines + 8
        side = halo // LANES
        w2 = w_two.T
        mask = mask.reshape(-1, LANES)
        labels = labels.reshape(-1, LANES)
        lined = [a.reshape(lines, LANES) for a in (edge_src, edge_dst, edge_w)]
        ints = sds((slots, LANES), jnp.int32)
        sided = sds((2 * side, LANES), F32)
        tab_one, tab_b, src, dst, w_lines, used, counts, count, need = call(
            functools.partial(prep_kernel, num_dev, PREP_CHUNK, rows), "prep",
            [tab_f, sds((rows, 2 * LANES), BF16), ints, ints, sds((slots, LANES), F32), sided, sds((2,), jnp.int32), one, sds((1,), jnp.int32)],
            [VMEM] * 6,
            [(6 * slots, LANES), (6 * lines, LANES), pltpu.VMEM((4 * lines, LANES), jnp.int32), sided.shape, (2, LANES), (num_dev - 1, 2, LANES)]
            + [dma((num_dev - 1,))] * 2,
            out_specs=[VMEM] * 6 + [SMEM, VMEM, SMEM], vmem=60, collective=0,
        )(*lined, mask, x, w_one)

        def run(limit):
            compact = limit < halo
            pack_f, half_f = sds((3 * limit // 2 + side, LANES), F32), sds((2 * limit, LANES), F32)
            list_s = [pltpu.SMEM((halo,), jnp.int32), dma((side,))]
            to_p, to_n, w, src_back, lists = call(
                functools.partial(first_kernel, compact, halo), "first", [half_b, half_b, sds((slots * LANES, LANES), F32), ints, sided],
                [VMEM] * 3 + [SMEM] + [VMEM] * 3, [half] + list_s, vmem=8,
            )(tab_one, tab_b, send, counts, src, w_lines, used)
            from_prev = lax.ppermute(to_n, AXIS, to_next)
            from_next = lax.ppermute(to_p, AXIS, to_prev)
            flat, flat_dst, flat_back = src.reshape(-1), dst.reshape(-1), src_back.reshape(-1)

            four = [tab] * 4
            walk = [SMEM, ANY, ANY, VMEM]
            index = pltpu.SMEM((slots * LANES,), jnp.int32)
            walk_s = lambda n: [index] * n + [dma((n, slots * LANES // SEGMENT))]
            slot_s = [pltpu.SMEM((2 * halo,), jnp.int32), dma((2 * side,))]
            local, local_back = (
                call(functools.partial(local_kernel, chunk_l, back), "local_edges", tab_f, walk + [VMEM], walk_s(2) + four)
                for back in (False, True)
            )
            part = local(counts, flat, flat_dst, w, tab_one)
            hid, tab_two, to_p, to_n, back = call(
                functools.partial(hidden_kernel, chunk_h), "hidden",
                [sds((rows, 2 * LANES), BF16), tab_f, pack_b, pack_b, sds((2 * side, LANES), jnp.int32)],
                walk + [VMEM] * 5, [tab, wide_b, w2_pad, half] + list_s + walk_s(2) + four,
            )(counts, flat, flat_dst, w, send, from_prev, from_next, part, w2)
            from_prev = lax.ppermute(to_n, AXIS, to_next)
            from_next = lax.ppermute(to_p, AXIS, to_prev)
            back = back.reshape(-1)
            part = local(counts, flat, flat_dst, w, tab_two)
            loss, grad, to_p, to_n = call(
                functools.partial(loss_kernel, limit, 4, chunk_h, classes), "loss", [one, tab_f, pack_f, pack_f],
                walk + [ANY] + [VMEM] * 7, [tab] + walk_s(3) + four,
            )(counts, flat, flat_dst, w, flat_back, lists, count, from_prev, from_next, part, labels, mask)
            got_prev = lax.ppermute(to_p, AXIS, to_prev)
            got_next = lax.ppermute(to_n, AXIS, to_next)
            part = local_back(counts, flat, flat_dst, w, grad)
            grad_two, grad, to_p, to_n, slot, n_back = call(
                functools.partial(middle_kernel, limit, chunk_h), "middle",
                [sds(w2_pad, F32), tab_f, half_f, half_f, sds((2 * side, LANES), jnp.int32), sds((2,), jnp.int32)],
                walk + [SMEM] + [VMEM] * 5, [(4 * limit, LANES), w2_pad] + slot_s + walk_s(2) + four, out_specs=[VMEM] * 5 + [SMEM],
            )(counts, flat_back, flat_dst, w, back, got_prev, got_next, part, hid, w2)
            got_prev = lax.ppermute(to_p, AXIS, to_prev)
            got_next = lax.ppermute(to_n, AXIS, to_next)
            part = local_back(counts, flat, flat_dst, w, grad)
            grad_one = call(
                last_kernel, "last", sds((x.shape[1], 2 * LANES), F32), [SMEM, SMEM, ANY] + [VMEM] * 4, slot_s + four
            )(back, n_back, slot, got_prev, got_next, part, x)
            return grad_one, grad_two, loss

        few = halo // 32 * 19
        grad_one, grad_two, loss = lax.cond(need.reshape(()) > few, lambda: run(halo), lambda: run(few))
        unit = SUB * num_dev
        lines = 2 * (x.shape[1] + -(-classes // SUB) * SUB) + SUB
        lines = -(-lines // unit) * unit
        grad_one, grad_two, mean = call(
            functools.partial(reduce_kernel, num_dev), "reduce", [sds(grad_one.shape, F32), sds((classes, 2 * LANES), F32), sds((1, 1), F32)],
            [VMEM] * 4, [(lines, LANES), (lines, LANES), (lines // 2, LANES), (num_dev // 2 - 1, lines // num_dev, LANES), dma((2, 2 * num_dev))],
            collective=1, vmem=8,
        )(grad_one, grad_two, loss, count)
        return mean.reshape(()), grad_one, grad_two.T

    row = P(AXIS)
    return jax.shard_map(
        step, mesh=mesh, in_specs=(row, P(), P(), row, row, row, row, row, row), out_specs=(P(), P(), P()), check_vma=False
    )
```

```python
import functools

import jax
import jax.numpy as jnp
from jax import lax
from jax.experimental import pallas as pl
from jax.experimental.pallas import tpu as pltpu
from jax.sharding import PartitionSpec as P

AXIS = "graph"
LANES = 128
ROWS_A = (((0,), (0,)), ((), ()))
COLS_A = (((1,), (1,)), ((), ()))
F32, BF16 = jnp.float32, jnp.bfloat16
VMEM = pl.BlockSpec(memory_space=pltpu.VMEM)
SMEM = pl.BlockSpec(memory_space=pltpu.SMEM)
ANY = pl.BlockSpec(memory_space=pl.ANY)
STEP = 512
BLOCK = 256
BYTE = BLOCK
SUB = 8
TILE = (SUB, LANES)
SQUARE = (LANES, LANES)
PREP_CHUNK = 64
SMALL = PREP_CHUNK
SEGMENT = 1024
MESH = pl.DeviceIdType.MESH


def dot(a, b, dims=(((1,), (0,)), ((), ()))):
    return lax.dot_general(a, b, dims, preferred_element_type=F32)


def fill_zero(ref):
    step = BLOCK if ref.shape[0] % BLOCK == 0 else SMALL
    zero = jnp.zeros((step, LANES), F32)

    @pl.loop(0, ref.shape[0], step=step)
    def _(i):
        ref[pl.ds(i, step), :] = zero


def copy_in(dst, src):
    @pl.loop(0, dst.shape[0], step=STEP)
    def _(i):
        dst[pl.ds(i, STEP), :] = src[pl.ds(i, STEP), :].astype(F32)


class Edges:
    def __init__(self, first, last, w, arrays, smem, sems):
        self.first, self.last, self.w = first, last, w
        self.pairs = tuple(zip(arrays, smem))
        self.sems = sems

    def copies(self, seg):
        part = pl.ds(pl.multiple_of(seg * SEGMENT, SEGMENT), SEGMENT)
        return [pltpu.make_async_copy(a.at[part], b.at[part], self.sems.at[i, seg]) for i, (a, b) in enumerate(self.pairs)]

    def fetch(self):
        per = SEGMENT // PREP_CHUNK
        for seg in range(self.pairs[0][1].shape[0] // SEGMENT):

            @pl.when(jnp.logical_and(seg * per < self.last, (seg + 1) * per > self.first))
            def _():
                for c in self.copies(seg):
                    c.start()

    def walk(self, chunk, from_idx, to_idx, table, accs, wait):
        group, per, ratio = len(accs), SEGMENT // chunk, PREP_CHUNK // chunk
        first, last = self.first * ratio, self.last * ratio

        def body(c, _):
            base = c * chunk
            w_chunk = self.w.at[pl.ds(pl.multiple_of(base, chunk), chunk)]
            for g in range(0, chunk, group):
                pend = []
                for u in range(group):
                    k = base + g + u
                    s = pl.multiple_of(from_idx[k], 2)
                    d = pl.multiple_of(to_idx[k], 2)
                    pend.append((d, accs[u][pl.ds(d, 2), :] + table[pl.ds(s, 2), :] * w_chunk[g + u : g + u + 1, :]))
                for u in range(group):
                    accs[u][pl.ds(pend[u][0], 2), :] = pend[u][1]
            return 0

        if not wait:
            lax.fori_loop(first, last, body, 0)
            return

        def segment(seg, _):
            for c in self.copies(seg):
                c.wait()
            lax.fori_loop(jnp.maximum(first, seg * per), jnp.minimum(last, (seg + 1) * per), body, 0)
            return 0

        lax.fori_loop(first // per, (last + per - 1) // per, segment, 0)


def one_hot_rows(idx, which, start, table):
    lane = across(SQUARE)
    hot = []
    for q in range(2):
        want = spread(idx[which : which + 1, pl.ds(pl.multiple_of(start + q * LANES, LANES), LANES)])
        hot.append(
            stack_lanes([jnp.where(want == lane + LANES * j, 1.0, 0.0).astype(BF16) for j in range(table.shape[0] // LANES)])
        )
    return dot(stack_rows(hot), table[...])


def low_lanes(rows):
    return across((rows, LANES)) < LANES // 2


def swap_lanes(v):
    return pltpu.roll(v, LANES // 2, 1)


def fetch_index(send, idx, sems):
    parts = [pl.ds(i, LANES) for i in range(0, send.shape[1], LANES)]
    return [pltpu.make_async_copy(send.at[1, p], idx.at[p], sems.at[i]) for i, p in enumerate(parts)]


def gather_block(send, idx, i, table_b, table, buf):
    got = one_hot_rows(send, 0, i, table_b)
    out = buf.at[pl.ds(pl.multiple_of(2 * i, 512), 512)]
    for u in range(BLOCK):
        s = pl.multiple_of(idx[i + u] * 2, 2)
        out[2 * u : 2 * u + 2, :] = table[pl.ds(s, 2), :]
    return got


def gather_rows(send, idx, table_b, table, buf, to_prev, to_next, also):
    @pl.loop(0, to_prev.shape[0], step=BLOCK)
    def _(i):
        i = pl.multiple_of(i, BLOCK)
        to_prev[pl.ds(i, BLOCK), :] = gather_block(send, idx, i, table_b, table, buf).astype(BF16)
        also(i)

    @pl.loop(0, to_next.shape[0], step=BLOCK)
    def _(i):
        to_next[pl.ds(pl.multiple_of(i, BLOCK), BLOCK), :] = stack_lanes(halves([buf], i, BLOCK)).astype(BF16)


def pack_rows(out, i, half, a_even, a_odd, b_even, b_odd):
    n = a_even.shape[0]
    out[pl.ds(i, n), :] = a_even.astype(out.dtype)
    out[pl.ds(half + i, n), :] = b_even.astype(out.dtype)
    out[pl.ds(2 * half + i, n), :] = jnp.where(low_lanes(n), a_odd, swap_lanes(b_odd)).astype(out.dtype)


def gather_packed(send, idx, table_b, table, buf, to_prev, to_next):
    half = to_prev.shape[0] // 3

    @pl.loop(0, half, step=BLOCK)
    def _(i):
        i = pl.multiple_of(i, BLOCK)
        a = gather_block(send, idx, i, table_b, table, buf)
        b = gather_block(send, idx, half + i, table_b, table, buf)
        pack_rows(to_prev, i, half, a[:, :LANES], a[:, LANES:], b[:, :LANES], b[:, LANES:])

    @pl.loop(0, half, step=BLOCK)
    def _(i):
        i = pl.multiple_of(i, BLOCK)
        pack_rows(to_next, i, half, *halves([buf], i, BLOCK), *halves([buf], half + i, BLOCK))


def unpack_rows(got, table, start, half=None):
    half = got.shape[0] // 3 if half is None else half
    n = half // 2

    @pl.loop(0, half, step=n)
    def _(i):
        i = pl.multiple_of(i, n)
        a, b, both = (got[pl.ds(k + i, n), :].astype(F32) for k in (0, half, 2 * half))
        put_halves(table, start + i, n, a, jnp.where(low_lanes(n), both, 0.0))
        put_halves(table, start + half + i, n, b, jnp.where(low_lanes(n), swap_lanes(both), 0.0))


def unpack_plain(got, table, start):
    @pl.loop(0, got.shape[0], step=BLOCK)
    def _(i):
        t = got[pl.ds(i, BLOCK), :].astype(F32)
        put_halves(table, start + i, BLOCK, t[:, :LANES], t[:, LANES:])


def spread(row):
    return jnp.transpose(jnp.broadcast_to(row, SQUARE))


def return_rows(back, slots, start, count, vals, accs, chunk=32):
    group = len(accs)

    def body(c, _):
        block = vals.at[pl.ds(pl.multiple_of(c * 2 * chunk, 2 * chunk), 2 * chunk)]
        for g in range(0, chunk, group):
            pend = []
            for u in range(group):
                d = pl.multiple_of(back[slots[start + c * chunk + g + u]], 2)
                pend.append((d, accs[u][pl.ds(d, 2), :] + block[2 * (g + u) : 2 * (g + u) + 2, :]))
            for u in range(group):
                accs[u][pl.ds(pend[u][0], 2), :] = pend[u][1]
        return 0

    lax.fori_loop(0, (count + chunk - 1) // chunk, body, 0)


def group(i, n, which):
    return pl.ds(2 * i + which, n, stride=2), slice(None)


def halves(accs, i, n):
    return [functools.reduce(jnp.add, [a[group(i, n, k)] for a in accs]) for k in range(2)]


def put_halves(table, i, n, *parts):
    for k, part in enumerate(parts):
        table[group(i, n, k)] = part


def stack_rows(parts):
    return jnp.concatenate(parts, axis=0)


def stack_lanes(parts):
    return jnp.concatenate(parts, axis=1)


def down(shape):
    return lax.broadcasted_iota(jnp.int32, shape, 0)


def across(shape):
    return lax.broadcasted_iota(jnp.int32, shape, 1)


def prefix(mask, above):
    m = mask.astype(BF16)
    before = (down(SQUARE) < across(SQUARE)).astype(BF16)
    return dot(m, before) + dot(above, dot(m, jnp.ones(SQUARE, BF16)).astype(BF16))


def rank_halo(halo, counts, src, used, src_back, lists):
    lines = used.shape[0]
    side = lines // 2
    i, j = down((lines, lines)), across((lines, lines))
    above = jnp.logical_and(j < i, (j >= side) == (i >= side)).astype(F32).astype(BF16)
    rank = prefix(used[...], above).astype(jnp.int32)
    low, high = rank & (LANES - 1), rank >> 7
    table = stack_rows([low.astype(F32), high.astype(F32)]).astype(BF16)

    quad = 4

    def four(c, _):
        slot = [src[pl.ds(c * quad + q, 1), :] >> 1 for q in range(quad)]
        spots = stack_lanes([(down(SQUARE) == (t & (LANES - 1))).astype(F32) for t in slot]).astype(BF16)
        got = dot(table, spots)
        h = stack_lanes(slot) >> 7
        got = jnp.where(down(got[:lines].shape) == h, got[:lines] + LANES * got[lines:], 0.0)
        got = (jnp.sum(got, axis=0, keepdims=True).astype(jnp.int32) + jnp.where(h >= side, halo, 0)) * 2
        for q in range(quad):
            src_back[pl.ds(c * quad + q, 1), :] = got[:, q * LANES : (q + 1) * LANES]
        return 0

    ratio = quad * LANES // PREP_CHUNK
    lax.fori_loop(counts[0] // ratio, (counts[1] + ratio - 1) // ratio, four, 0)
    for k in range(2):
        acc = jnp.zeros((24, LANES), F32)
        for hh in range(side):
            q = k * side + hh
            pick = jnp.where(down(TILE) == high[q : q + 1, :], used[q : q + 1, :], 0.0)
            lhs = stack_rows([pick * across(TILE).astype(F32), pick * hh, pick]).astype(BF16)
            acc += dot(lhs, (down(SQUARE) == low[q : q + 1, :]).astype(F32).astype(BF16), COLS_A)
        slots = acc[:8] + LANES * acc[8:16]
        lists[k * side : (k + 1) * side, :] = jnp.where(acc[16:24] > 0.0, slots[:side], -1.0)


def first_kernel(compact, halo, tab, tab_b, send, counts, src, w, used, to_prev, to_next, w_out, src_back, lists, buf, idx, sems):
    fetch = fetch_index(send, idx, sems)
    for c in fetch:
        c.start()
    src_back[...] = src[...]
    if compact:
        rank_halo(halo, counts, src, used, src_back, lists)
    else:
        line = down(lists.shape)
        line = jnp.where(line >= lists.shape[0] // 2, line - lists.shape[0] // 2, line)
        lists[...] = (line * LANES + across(lists.shape)).astype(F32)
    for c in fetch:
        c.wait()
    share = w.shape[0] * BLOCK // halo

    def widen(i):
        for q in range(share):
            r = i // BLOCK * share + q
            w_out[pl.ds(pl.multiple_of(r * LANES, LANES), LANES), :] = spread(w[pl.ds(r, 1), :])

    gather_rows(send, idx, tab_b, tab, buf, to_prev, to_next, widen)


def greet(n):
    me = lax.axis_index(AXIS)
    barrier = pltpu.get_barrier_semaphore()
    for o in range(1, n):
        pl.semaphore_signal(barrier, inc=1, device_id=(lax.rem(me + o, n),), device_id_type=MESH)
    return me, lambda: pl.semaphore_wait(barrier, n - 1)


def remote(src, dst, send_sem, recv_sem, peer):
    return pltpu.make_async_remote_copy(
        src_ref=src, dst_ref=dst, send_sem=send_sem, recv_sem=recv_sem, device_id=(peer,), device_id_type=MESH
    )


def reduce_kernel(n, one, two, loss, count, one_out, two_out, mean, work, full, got_pair, got_rest, sems):
    me = lax.axis_index(AXIS)
    chips, core = n // 2, lax.rem(me, 2)
    chip = lax.div(me, 2)
    pair = me + 1 - 2 * core
    others = [lax.rem(chip + o, chips) for o in range(1, chips)]
    barrier = pltpu.get_barrier_semaphore()
    for p in [pair] + [2 * c + core for c in others]:
        pl.semaphore_signal(barrier, inc=1, device_id=(p,), device_id_type=MESH)
    classes = two_out.shape[0]
    lines = -(-classes // SUB) * SUB
    top, wide = one.shape
    work[:top, :] = one[:, :LANES]
    work[top : 2 * top, :] = one[:, LANES:]
    work[2 * top : 2 * top + lines, :] = two[:lines, :LANES]
    work[2 * top + lines : 2 * top + 2 * lines, :] = two[:lines, LANES:]
    tail = 2 * top + 2 * lines
    work[tail : tail + SUB, :] = loss[...]
    work[tail + SUB :, :] = jnp.zeros((work.shape[0] - tail - SUB, LANES), F32)
    pl.semaphore_wait(barrier, chips)

    half = work.shape[0] // 2
    piece = half // chips
    spot = lambda c, k: pl.ds(pl.multiple_of(k * half + c * piece, SUB), piece)
    link = lambda kind, o, src, dst, peer: remote(src, dst, sems.at[0, kind * chips + o], sems.at[1, kind * chips + o], peer)
    order = list(enumerate(others + [chip]))
    swap = [link(0, o, work.at[spot(c, 1 - core)], got_pair.at[pl.ds(o * piece, piece)], pair) for o, c in order]
    for c in swap:
        c.start()
    scatter = [link(1, o, work.at[spot(c, core)], got_rest.at[o], 2 * c + core) for o, c in order[:-1]]
    for o, c in order:
        swap[o].wait_recv()
        work[spot(c, core), :] += got_pair[o * piece : (o + 1) * piece, :]
        if o:
            scatter[o - 1].start()
    for c in scatter:
        c.wait_recv()
    own = spot(chip, core)
    work[own, :] += jnp.sum(got_rest[...], axis=0)
    full[own, :] = work[own, :]
    for c in swap + scatter:
        c.wait_send()
    gather = [link(2, o, work.at[own], full.at[own], 2 * c + core) for o, c in order[:-1]]
    for c in gather:
        c.start()
    forward = [link(3, chips - 1, work.at[own], full.at[own], pair)]
    forward[0].start()
    for o, _ in order[:-1]:
        gather[o].wait_recv()
        came = spot(lax.rem(chip + chips - 1 - o, chips), core)
        forward.append(link(3, o, full.at[came], full.at[came], pair))
        forward[-1].start()
    for c in gather:
        c.wait_send()
    for c in forward:
        c.wait()
    one_out[:, :LANES] = full[:top, :]
    one_out[:, LANES:] = full[top : 2 * top, :]
    two_out[:, :LANES] = full[2 * top : 2 * top + classes, :]
    two_out[:, LANES:] = full[2 * top + lines : 2 * top + lines + classes, :]
    mean[...] = jnp.sum(full[tail : tail + SUB, :], keepdims=True) / count[:1, :1]


def prep_kernel(n, chunk, rows, src_in, dst_in, w_in, mask, x, w1, tab, tab_b, src_out, dst_out, w_out, used, counts, count, need, total, values, places, hits, mine, theirs, send_sem, recv_sem):
    me, met = greet(n)
    lines, slots = src_in.shape[0], src_out.shape[0]
    src, d, half_w = src_in[...], dst_in[...], w_in[...] * 0.5
    live = w_in[...] != 0.0
    halo = src >= rows
    above = (across((lines, lines)) < down((lines, lines))).astype(F32).astype(BF16)
    is_local, is_halo = jnp.logical_and(live, jnp.logical_not(halo)), jnp.logical_and(live, halo)
    rank = lambda m: prefix(m.astype(F32), above).astype(jnp.int32)
    n_local = jnp.sum(is_local.astype(F32)).astype(jnp.int32)
    n_halo = jnp.sum(is_halo.astype(F32)).astype(jnp.int32)
    local_chunks = (n_local + chunk - 1) // chunk
    counts[0] = local_chunks
    counts[1] = local_chunks + (n_halo + chunk - 1) // chunk
    pos = jnp.where(is_local, rank(is_local), jnp.where(is_halo, rank(is_halo) + local_chunks * chunk, -1))
    s = jnp.where(halo, src - rows, src)
    w_a = half_w.astype(BF16).astype(F32)
    w_b = (half_w - w_a).astype(BF16).astype(F32)
    w_c = half_w - w_a - w_b
    high = ((s >> 8) * 8 + (d >> 8)).astype(F32)
    planes = [(s % BYTE).astype(F32), (d % BYTE).astype(F32), high, w_a, w_b, w_c]
    for i, p in enumerate(planes):
        values[i * lines : (i + 1) * lines, :] = p
    for i, p in enumerate((pos >> 7, pos & (LANES - 1), jnp.where(is_halo, s >> 7, -1), s & (LANES - 1))):
        places[i * lines : (i + 1) * lines, :] = p
    row = lambda i, q: pl.ds(i * lines + q, 1)
    spot = lambda size, i, q: (down((size, LANES)) == places[row(i, q), :]).astype(F32)
    hits[...] = jnp.zeros_like(hits)

    @pl.loop(0, lines, step=SUB)
    def _(base):
        acc = None
        for r in range(0, SUB, 2):
            lhs = stack_lanes([spot(hits.shape[0], 2, base + q) for q in (r, r + 1)]).astype(BF16)
            rhs = stack_lanes([spot(LANES, 3, base + q) for q in (r, r + 1)]).astype(BF16)
            part = dot(lhs, rhs, COLS_A)
            acc = part if acc is None else acc + part
        hits[...] += acc

    flags = (hits[...] > 0.0).astype(F32)
    used[...] = flags
    side = hits.shape[0] // 2
    most = jnp.maximum(jnp.sum(flags[:side], keepdims=True), jnp.sum(flags[side:], keepdims=True))
    mine[:1, :] = jnp.sum(mask[...].astype(F32), axis=0, keepdims=True)
    mine[1:, :] = jnp.broadcast_to(most, (1, LANES))
    met()
    copies = [remote(mine, theirs.at[o - 1], send_sem.at[o - 1], recv_sem.at[o - 1], lax.rem(me + o, n)) for o in range(1, n)]
    for c in copies:
        c.start()
    total[...] = jnp.zeros_like(total)

    @pl.loop(0, lines, step=SUB)
    def _(base):
        acc = None
        for r in range(0, SUB, 2):
            lhs, rhs = [], []
            for q in (base + r, base + r + 1):
                pick = down((slots, LANES)) == places[row(0, q), :]
                lhs.append(stack_rows([jnp.where(pick, values[row(i, q), :], 0.0) for i in range(len(planes))]))
                rhs.append(spot(LANES, 1, q))
            part = dot(stack_lanes(lhs).astype(BF16), stack_lanes(rhs).astype(BF16), COLS_A)
            acc = part if acc is None else acc + part
        total[...] += acc

    plane = lambda i: total[i * slots : (i + 1) * slots, :]
    high = plane(2).astype(jnp.int32)
    w1_b = w1[...].astype(BF16)

    @pl.loop(0, rows, step=STEP)
    def _(i):
        t = dot(x[pl.ds(i, STEP), :], w1_b).astype(BF16)
        tab_b[pl.ds(i, STEP), :] = t
        t = t.astype(F32)
        put_halves(tab, i, STEP, t[:, :LANES], t[:, LANES:])

    src_out[...] = ((high >> 3) * BYTE + plane(0).astype(jnp.int32)) * 2
    dst_out[...] = ((high & 7) * BYTE + plane(1).astype(jnp.int32)) * 2
    w_out[...] = (plane(3) + plane(4) + plane(5)) * 2.0
    for c in copies:
        c.wait()
    every = jnp.sum(mine[:1, :] + jnp.sum(theirs[:, :1, :], axis=0), keepdims=True)
    count[...] = jnp.maximum(jnp.broadcast_to(every, count.shape), 1.0)
    need[0] = jnp.max(jnp.maximum(mine[1:, :], jnp.max(theirs[:, 1:, :], axis=0))).astype(jnp.int32)


def local_kernel(chunk, backward, counts, src, dst, w, table, out, src_s, dst_s, sems, *accs):
    edges = Edges(0, counts[0], w, (src, dst), (src_s, dst_s), sems)
    edges.fetch()
    for a in accs:
        fill_zero(a)
    edges.walk(chunk, *((dst_s, src_s) if backward else (src_s, dst_s)), table, accs, True)

    @pl.loop(0, out.shape[0], step=STEP)
    def _(i):
        out[pl.ds(i, STEP), :] = functools.reduce(jnp.add, [a[pl.ds(i, STEP), :] for a in accs])


def forward_halo(chunk, edges, src_s, dst_s, from_prev, from_next, part, htab, accs, unpack):
    edges.fetch()
    unpack(from_prev, htab, 0)
    unpack(from_next, htab, htab.shape[0] // 4)
    copy_in(accs[0], part)
    for a in accs[1:]:
        fill_zero(a)
    edges.walk(chunk, src_s, dst_s, htab, accs, True)


def backward_halo(limit, chunk, edges, src_s, dst_s, grad, back_prev, back_next, accs, wait, lists=None):
    split = accs[0].shape[0] // 2
    for a in accs:
        for start in (0, split):
            fill_zero(a.at[pl.ds(start, limit * 2)])
    edges.walk(chunk, dst_s, src_s, grad, accs, wait)
    if lists is None:

        @pl.loop(0, back_prev.shape[0], step=SMALL)
        def _(i):
            back_prev[pl.ds(i, SMALL), :] = functools.reduce(jnp.add, [a[pl.ds(i, SMALL), :] for a in accs])
            back_next[pl.ds(i, SMALL), :] = functools.reduce(jnp.add, [a[pl.ds(split + i, SMALL), :] for a in accs])
        return
    side = lists.shape[0] // 2
    half = (back_prev.shape[0] - side) // 3
    n = half // 2
    for k, out in enumerate((back_prev, back_next)):
        start = k * (split // 2)

        @pl.loop(0, half, step=n)
        def _(i):
            i = pl.multiple_of(i, n)
            pack_rows(out, i, half, *halves(accs, start + i, n), *halves(accs, start + half + i, n))

        out[3 * half : 3 * half + side, :] = lists[k * side : (k + 1) * side, :]


def padded(w, buf):
    low = w.shape[0] // SUB * SUB
    buf[low:, :] = jnp.zeros((buf.shape[0] - low, buf.shape[1]), F32)
    buf[:w.shape[0], :] = w[...]
    return buf[...].astype(BF16)


def hidden_kernel(chunk, counts, src, dst, w, send, from_prev, from_next, part, w2, hid, tab, to_prev, to_next, back, htab, tab_b, w2_pad, buf, idx, idx_sems, src_s, dst_s, sems, *accs):
    fetch = fetch_index(send, idx, idx_sems)
    for c in fetch:
        c.start()
    edges = Edges(counts[0], counts[1], w, (src, dst), (src_s, dst_s), sems)
    w2_b = padded(w2, w2_pad)
    per = send.shape[1] // LANES
    for i in range(2 * per):
        back[i : i + 1, :] = send[i // per : i // per + 1, (i % per) * LANES : (i % per + 1) * LANES] * 2
    forward_halo(chunk, edges, src_s, dst_s, from_prev, from_next, part, htab, accs, unpack_plain)

    @pl.loop(0, hid.shape[0], step=STEP)
    def _(i):
        even, odd = halves(accs, i, STEP)
        h = stack_lanes([jnp.maximum(even, 0.0), jnp.maximum(odd, 0.0)]).astype(BF16)
        hid[pl.ds(i, STEP), :] = h
        t = dot(h, w2_b, COLS_A).astype(BF16)
        tab_b[pl.ds(i, STEP), :] = t
        t = t.astype(F32)
        put_halves(tab, i, STEP, t[:, :LANES], t[:, LANES:])

    for c in fetch:
        c.wait()
    gather_packed(send, idx, tab_b, tab, buf, to_prev, to_next)


def loss_kernel(limit, quad, chunk, classes, counts, src, dst, w, src_back, lists, count, from_prev, from_next, part, labels, mask, loss, grad, back_prev, back_next, htab, src_s, dst_s, back_s, sems, *accs):
    edges = Edges(counts[0], counts[1], w, (src, dst, src_back), (src_s, dst_s, back_s), sems)
    forward_halo(chunk, edges, src_s, dst_s, from_prev, from_next, part, htab, accs, unpack_rows)
    lane = across(SQUARE)
    live = lane < classes - LANES
    scale = 1.0 / count[:1, :]
    loss[...] = jnp.zeros_like(loss)

    @pl.loop(0, labels.shape[0], step=quad)
    def _(first):
        for b in [first + q for q in range(quad)]:
            even, odd = halves(accs, b * LANES, LANES)
            odd = jnp.where(live, odd, -jnp.inf)
            keep = spread(mask[pl.ds(b, 1), :])
            label = jnp.where(keep > 0, spread(labels[pl.ds(b, 1), :]), -1)
            hit_even, hit_odd = lane == label, lane + LANES == label
            top = jnp.max(jnp.maximum(even, odd), axis=1, keepdims=True)
            exp_even, exp_odd = jnp.exp(even - top), jnp.exp(odd - top)
            total = jnp.sum(exp_even + exp_odd, axis=1, keepdims=True)
            norm = jnp.where(jnp.logical_and(lane == 0, keep > 0), top + jnp.log(total), 0.0)
            per_row = norm - jnp.where(hit_even, even, jnp.where(hit_odd, odd, 0.0))
            loss[...] += jnp.sum(per_row.reshape(LANES // SUB, *TILE), axis=0)
            share = keep.astype(F32) * scale * (1.0 / total)
            put_halves(
                grad, b * LANES, LANES, *(e * share - jnp.where(hit, scale, 0.0) for e, hit in ((exp_even, hit_even), (exp_odd, hit_odd)))
            )

    backward_halo(limit, chunk, edges, back_s, dst_s, grad, back_prev, back_next, accs, False, lists)


def take_returns(back, slots, counts, part, got_prev, got_next, accs):
    return_rows(back, slots, 0, counts[0], got_prev, accs)
    return_rows(back, slots, slots.shape[0] // 2, counts[1], got_next, accs)


def fetch_lines(lines, smem, sems):
    return [pltpu.make_async_copy(lines.at[i], smem.at[pl.ds(i * LANES, LANES)], sems.at[i]) for i in range(lines.shape[0])]


def middle_kernel(limit, chunk, counts, src, dst, w, back, got_prev, got_next, part, hid, w2, grad_two, grad, back_prev, back_next, slots, n_back, returned, w2_pad, slot_s, slot_sems, src_s, dst_s, sems, *accs):
    edges = Edges(counts[0], counts[1], w, (src, dst), (src_s, dst_s), sems)
    edges.fetch()
    side = slots.shape[0] // 2
    half = (got_prev.shape[0] - side) // 3
    for k, got in enumerate((got_prev, got_next)):
        slot = got[3 * half :, :].astype(jnp.int32)
        slots[k * side : (k + 1) * side, :] = jnp.maximum(slot, 0) + (1 - k) * side * LANES
        n_back[k] = jnp.sum((slot >= 0).astype(F32)).astype(jnp.int32)
    w2_b = padded(w2, w2_pad)
    unpack_rows(got_prev, returned, 0, half)
    unpack_rows(got_next, returned, 2 * half, half)
    fetch = fetch_lines(slots, slot_s, slot_sems)
    for c in fetch:
        c.start()
    copy_in(accs[0], part)
    for a in accs[1:]:
        fill_zero(a)
    for c in fetch:
        c.wait()
    take_returns(back, slot_s, n_back, part, returned.at[pl.ds(0, 4 * half)], returned.at[pl.ds(4 * half, 4 * half)], accs)
    grad_two[...] = jnp.zeros_like(grad_two)

    @pl.loop(0, hid.shape[0], step=STEP)
    def _(i):
        even, odd = halves(accs, i, STEP)
        d_tab = stack_lanes([even, odd]).astype(BF16)
        h = hid[pl.ds(i, STEP), :]
        grad_two[...] += dot(d_tab, h, ROWS_A)
        d_hid = dot(d_tab, w2_b)
        d_pre = jnp.where(h > 0, d_hid, 0.0)
        put_halves(grad, i, STEP, d_pre[:, :LANES], d_pre[:, LANES:])

    backward_halo(limit, chunk, edges, src_s, dst_s, grad, back_prev, back_next, accs, True)


def last_kernel(back, n_back, slots, got_prev, got_next, part, x, grad_one, slot_s, slot_sems, *accs):
    fetch = fetch_lines(slots, slot_s, slot_sems)
    for c in fetch:
        c.start()
    copy_in(accs[0], part)
    for a in accs[1:]:
        fill_zero(a)
    for c in fetch:
        c.wait()
    take_returns(back, slot_s, n_back, part, got_prev, got_next, accs)
    grad_one[...] = jnp.zeros_like(grad_one)

    @pl.loop(0, x.shape[0], step=STEP)
    def _(i):
        even, odd = halves(accs, i, STEP)
        d_tab = stack_lanes([even, odd]).astype(BF16)
        grad_one[...] += dot(x[pl.ds(i, STEP), :], d_tab, ROWS_A)


def call(body, name, outs, ins, scratch, out_specs=None, collective=None, vmem=14):
    extra = {} if collective is None else dict(collective_id=collective, has_side_effects=True)
    return pl.pallas_call(
        body, name=name, out_shape=outs, in_specs=ins, out_specs=out_specs or jax.tree.map(lambda _: VMEM, outs),
        scratch_shapes=[pltpu.VMEM(s, F32) if isinstance(s, tuple) else s for s in scratch],
        compiler_params=pltpu.CompilerParams(vmem_limit_bytes=vmem * 2**20, **extra),
        cost_estimate=pl.CostEstimate(flops=10**10, bytes_accessed=10**7, transcendentals=0),
    )


def solution(mesh):
    num_dev = mesh.shape[AXIS]
    to_next = [(d, (d + 1) % num_dev) for d in range(num_dev)]
    to_prev = [(d, (d - 1) % num_dev) for d in range(num_dev)]

    def step(x, w_one, w_two, send, edge_src, edge_dst, edge_w, labels, mask):
        rows, halo, edges, classes = x.shape[0], send.shape[1], edge_src.shape[0], w_two.shape[1]
        tab, half, w2_pad = (2 * rows, LANES), (2 * halo, LANES), (2 * LANES, 2 * LANES)
        sds = jax.ShapeDtypeStruct
        tab_f = sds(tab, F32)
        half_b, pack_b = sds((halo, 2 * LANES), BF16), sds((3 * halo // 2, LANES), BF16)
        wide_b = pltpu.VMEM((rows, 2 * LANES), BF16)
        one = sds(TILE, F32)
        dma = pltpu.SemaphoreType.DMA
        chunk_l, chunk_h = 64, 32
        lines = edges // LANES
        slots = lines + 8
        side = halo // LANES
        w2 = w_two.T
        mask = mask.reshape(-1, LANES)
        labels = labels.reshape(-1, LANES)
        lined = [a.reshape(lines, LANES) for a in (edge_src, edge_dst, edge_w)]
        ints = sds((slots, LANES), jnp.int32)
        sided = sds((2 * side, LANES), F32)
        tab_one, tab_b, src, dst, w_lines, used, counts, count, need = call(
            functools.partial(prep_kernel, num_dev, PREP_CHUNK, rows), "prep",
            [tab_f, sds((rows, 2 * LANES), BF16), ints, ints, sds((slots, LANES), F32), sided, sds((2,), jnp.int32), one, sds((1,), jnp.int32)],
            [VMEM] * 6,
            [(6 * slots, LANES), (6 * lines, LANES), pltpu.VMEM((4 * lines, LANES), jnp.int32), sided.shape, (2, LANES), (num_dev - 1, 2, LANES)]
            + [dma((num_dev - 1,))] * 2,
            out_specs=[VMEM] * 6 + [SMEM, VMEM, SMEM], vmem=60, collective=0,
        )(*lined, mask, x, w_one)

        def run(limit):
            compact = limit < halo
            pack_f, half_f = sds((3 * limit // 2 + side, LANES), F32), sds((2 * limit, LANES), F32)
            list_s = [pltpu.SMEM((halo,), jnp.int32), dma((side,))]
            to_p, to_n, w, src_back, lists = call(
                functools.partial(first_kernel, compact, halo), "first", [half_b, half_b, sds((slots * LANES, LANES), F32), ints, sided],
                [VMEM] * 3 + [SMEM] + [VMEM] * 3, [half] + list_s, vmem=8,
            )(tab_one, tab_b, send, counts, src, w_lines, used)
            from_prev = lax.ppermute(to_n, AXIS, to_next)
            from_next = lax.ppermute(to_p, AXIS, to_prev)
            flat, flat_dst, flat_back = src.reshape(-1), dst.reshape(-1), src_back.reshape(-1)

            four = [tab] * 4
            walk = [SMEM, ANY, ANY, VMEM]
            index = pltpu.SMEM((slots * LANES,), jnp.int32)
            walk_s = lambda n: [index] * n + [dma((n, slots * LANES // SEGMENT))]
            slot_s = [pltpu.SMEM((2 * halo,), jnp.int32), dma((2 * side,))]
            local, local_back = (
                call(functools.partial(local_kernel, chunk_l, back), "local_edges", tab_f, walk + [VMEM], walk_s(2) + four)
                for back in (False, True)
            )
            part = local(counts, flat, flat_dst, w, tab_one)
            hid, tab_two, to_p, to_n, back = call(
                functools.partial(hidden_kernel, chunk_h), "hidden",
                [sds((rows, 2 * LANES), BF16), tab_f, pack_b, pack_b, sds((2 * side, LANES), jnp.int32)],
                walk + [VMEM] * 5, [tab, wide_b, w2_pad, half] + list_s + walk_s(2) + four,
            )(counts, flat, flat_dst, w, send, from_prev, from_next, part, w2)
            from_prev = lax.ppermute(to_n, AXIS, to_next)
            from_next = lax.ppermute(to_p, AXIS, to_prev)
            back = back.reshape(-1)
            part = local(counts, flat, flat_dst, w, tab_two)
            loss, grad, to_p, to_n = call(
                functools.partial(loss_kernel, limit, 4, chunk_h, classes), "loss", [one, tab_f, pack_f, pack_f],
                walk + [ANY] + [VMEM] * 7, [tab] + walk_s(3) + four,
            )(counts, flat, flat_dst, w, flat_back, lists, count, from_prev, from_next, part, labels, mask)
            got_prev = lax.ppermute(to_p, AXIS, to_prev)
            got_next = lax.ppermute(to_n, AXIS, to_next)
            part = local_back(counts, flat, flat_dst, w, grad)
            grad_two, grad, to_p, to_n, slot, n_back = call(
                functools.partial(middle_kernel, limit, chunk_h), "middle",
                [sds(w2_pad, F32), tab_f, half_f, half_f, sds((2 * side, LANES), jnp.int32), sds((2,), jnp.int32)],
                walk + [SMEM] + [VMEM] * 5, [(4 * limit, LANES), w2_pad] + slot_s + walk_s(2) + four, out_specs=[VMEM] * 5 + [SMEM],
            )(counts, flat_back, flat_dst, w, back, got_prev, got_next, part, hid, w2)
            got_prev = lax.ppermute(to_p, AXIS, to_prev)
            got_next = lax.ppermute(to_n, AXIS, to_next)
            part = local_back(counts, flat, flat_dst, w, grad)
            grad_one = call(
                last_kernel, "last", sds((x.shape[1], 2 * LANES), F32), [SMEM, SMEM, ANY] + [VMEM] * 4, slot_s + four
            )(back, n_back, slot, got_prev, got_next, part, x)
            return grad_one, grad_two, loss

        limits = [halo // 32 * part for part in (16, 19, 32)]
        need = need.reshape(())
        choice = sum((need > limit).astype(jnp.int32) for limit in limits[:-1])
        grad_one, grad_two, loss = lax.switch(choice, [functools.partial(run, limit) for limit in limits])
        unit = SUB * num_dev
        lines = 2 * (x.shape[1] + -(-classes // SUB) * SUB) + SUB
        lines = -(-lines // unit) * unit
        grad_one, grad_two, mean = call(
            functools.partial(reduce_kernel, num_dev), "reduce", [sds(grad_one.shape, F32), sds((classes, 2 * LANES), F32), sds((1, 1), F32)],
            [VMEM] * 4, [(lines, LANES), (lines, LANES), (lines // 2, LANES), (num_dev // 2 - 1, lines // num_dev, LANES), dma((2, 2 * num_dev))],
            collective=1, vmem=8,
        )(grad_one, grad_two, loss, count)
        return mean.reshape(()), grad_one, grad_two.T

    row = P(AXIS)
    return jax.shard_map(
        step, mesh=mesh, in_specs=(row, P(), P(), row, row, row, row, row, row), out_specs=(P(), P(), P()), check_vma=False
    )
```

```python
import functools

import jax
import jax.numpy as jnp
from jax import lax
from jax.experimental import pallas as pl
from jax.experimental.pallas import tpu as pltpu
from jax.sharding import PartitionSpec as P

AXIS = "graph"
LANES = 128
ROWS_A = (((0,), (0,)), ((), ()))
COLS_A = (((1,), (1,)), ((), ()))
F32, BF16 = jnp.float32, jnp.bfloat16
VMEM = pl.BlockSpec(memory_space=pltpu.VMEM)
SMEM = pl.BlockSpec(memory_space=pltpu.SMEM)
ANY = pl.BlockSpec(memory_space=pl.ANY)
STEP = 512
BLOCK = 256
BYTE = BLOCK
SUB = 8
TILE = (SUB, LANES)
SQUARE = (LANES, LANES)
PREP_CHUNK = 64
SMALL = PREP_CHUNK
SEGMENT = 1024
MESH = pl.DeviceIdType.MESH


def dot(a, b, dims=(((1,), (0,)), ((), ()))):
    return lax.dot_general(a, b, dims, preferred_element_type=F32)


def fill_zero(ref):
    step = BLOCK if ref.shape[0] % BLOCK == 0 else SMALL
    zero = jnp.zeros((step, LANES), F32)

    @pl.loop(0, ref.shape[0], step=step)
    def _(i):
        ref[pl.ds(i, step), :] = zero


def copy_in(dst, src):
    @pl.loop(0, dst.shape[0], step=STEP)
    def _(i):
        dst[pl.ds(i, STEP), :] = src[pl.ds(i, STEP), :].astype(F32)


class Edges:
    def __init__(self, first, last, w, arrays, smem, sems):
        self.first, self.last, self.w = first, last, w
        self.pairs = tuple(zip(arrays, smem))
        self.sems = sems

    def copies(self, seg):
        part = pl.ds(pl.multiple_of(seg * SEGMENT, SEGMENT), SEGMENT)
        return [pltpu.make_async_copy(a.at[part], b.at[part], self.sems.at[i, seg]) for i, (a, b) in enumerate(self.pairs)]

    def fetch(self):
        per = SEGMENT // PREP_CHUNK
        for seg in range(self.pairs[0][1].shape[0] // SEGMENT):

            @pl.when(jnp.logical_and(seg * per < self.last, (seg + 1) * per > self.first))
            def _():
                for c in self.copies(seg):
                    c.start()

    def walk(self, chunk, from_idx, to_idx, table, accs, wait):
        group, per, ratio = len(accs), SEGMENT // chunk, PREP_CHUNK // chunk
        first, last = self.first * ratio, self.last * ratio

        def body(c, _):
            base = c * chunk
            w_chunk = self.w.at[pl.ds(pl.multiple_of(base, chunk), chunk)]
            for g in range(0, chunk, group):
                pend = []
                for u in range(group):
                    k = base + g + u
                    s = pl.multiple_of(from_idx[k], 2)
                    d = pl.multiple_of(to_idx[k], 2)
                    pend.append((d, accs[u][pl.ds(d, 2), :] + table[pl.ds(s, 2), :] * w_chunk[g + u : g + u + 1, :]))
                for u in range(group):
                    accs[u][pl.ds(pend[u][0], 2), :] = pend[u][1]
            return 0

        if not wait:
            lax.fori_loop(first, last, body, 0)
            return

        def segment(seg, _):
            for c in self.copies(seg):
                c.wait()
            lax.fori_loop(jnp.maximum(first, seg * per), jnp.minimum(last, (seg + 1) * per), body, 0)
            return 0

        lax.fori_loop(first // per, (last + per - 1) // per, segment, 0)


def one_hot_rows(idx, which, start, table):
    lane = across(SQUARE)
    hot = []
    for q in range(2):
        want = spread(idx[which : which + 1, pl.ds(pl.multiple_of(start + q * LANES, LANES), LANES)])
        hot.append(
            stack_lanes([jnp.where(want == lane + LANES * j, 1.0, 0.0).astype(BF16) for j in range(table.shape[0] // LANES)])
        )
    return dot(stack_rows(hot), table[...])


def low_lanes(rows):
    return across((rows, LANES)) < LANES // 2


def swap_lanes(v):
    return pltpu.roll(v, LANES // 2, 1)


def fetch_index(send, idx, sems):
    parts = [pl.ds(i, LANES) for i in range(0, send.shape[1], LANES)]
    return [pltpu.make_async_copy(send.at[1, p], idx.at[p], sems.at[i]) for i, p in enumerate(parts)]


def gather_block(send, idx, i, table_b, table, buf):
    got = one_hot_rows(send, 0, i, table_b)
    out = buf.at[pl.ds(pl.multiple_of(2 * i, 512), 512)]
    for u in range(BLOCK):
        s = pl.multiple_of(idx[i + u] * 2, 2)
        out[2 * u : 2 * u + 2, :] = table[pl.ds(s, 2), :]
    return got


def gather_rows(send, idx, table_b, table, buf, to_prev, to_next, also):
    @pl.loop(0, to_prev.shape[0], step=BLOCK)
    def _(i):
        i = pl.multiple_of(i, BLOCK)
        to_prev[pl.ds(i, BLOCK), :] = gather_block(send, idx, i, table_b, table, buf).astype(BF16)
        also(i)

    @pl.loop(0, to_next.shape[0], step=BLOCK)
    def _(i):
        to_next[pl.ds(pl.multiple_of(i, BLOCK), BLOCK), :] = stack_lanes(halves([buf], i, BLOCK)).astype(BF16)


def pack_rows(out, i, half, a_even, a_odd, b_even, b_odd):
    n = a_even.shape[0]
    out[pl.ds(i, n), :] = a_even.astype(out.dtype)
    out[pl.ds(half + i, n), :] = b_even.astype(out.dtype)
    out[pl.ds(2 * half + i, n), :] = jnp.where(low_lanes(n), a_odd, swap_lanes(b_odd)).astype(out.dtype)


def gather_packed(send, idx, table_b, table, buf, to_prev, to_next):
    half = to_prev.shape[0] // 3

    @pl.loop(0, half, step=BLOCK)
    def _(i):
        i = pl.multiple_of(i, BLOCK)
        a = gather_block(send, idx, i, table_b, table, buf)
        b = gather_block(send, idx, half + i, table_b, table, buf)
        pack_rows(to_prev, i, half, a[:, :LANES], a[:, LANES:], b[:, :LANES], b[:, LANES:])

    @pl.loop(0, half, step=BLOCK)
    def _(i):
        i = pl.multiple_of(i, BLOCK)
        pack_rows(to_next, i, half, *halves([buf], i, BLOCK), *halves([buf], half + i, BLOCK))


def unpack_rows(got, table, start, half=None):
    half = got.shape[0] // 3 if half is None else half
    n = half // 2

    @pl.loop(0, half, step=n)
    def _(i):
        i = pl.multiple_of(i, n)
        a, b, both = (got[pl.ds(k + i, n), :].astype(F32) for k in (0, half, 2 * half))
        put_halves(table, start + i, n, a, jnp.where(low_lanes(n), both, 0.0))
        put_halves(table, start + half + i, n, b, jnp.where(low_lanes(n), swap_lanes(both), 0.0))


def unpack_plain(got, table, start):
    @pl.loop(0, got.shape[0], step=BLOCK)
    def _(i):
        t = got[pl.ds(i, BLOCK), :].astype(F32)
        put_halves(table, start + i, BLOCK, t[:, :LANES], t[:, LANES:])


def spread(row):
    return jnp.transpose(jnp.broadcast_to(row, SQUARE))


def return_rows(back, slots, start, count, vals, accs, chunk=32):
    group = len(accs)

    def body(c, _):
        block = vals.at[pl.ds(pl.multiple_of(c * 2 * chunk, 2 * chunk), 2 * chunk)]
        for g in range(0, chunk, group):
            pend = []
            for u in range(group):
                d = pl.multiple_of(back[slots[start + c * chunk + g + u]], 2)
                pend.append((d, accs[u][pl.ds(d, 2), :] + block[2 * (g + u) : 2 * (g + u) + 2, :]))
            for u in range(group):
                accs[u][pl.ds(pend[u][0], 2), :] = pend[u][1]
        return 0

    lax.fori_loop(0, (count + chunk - 1) // chunk, body, 0)


def group(i, n, which):
    return pl.ds(2 * i + which, n, stride=2), slice(None)


def halves(accs, i, n):
    return [functools.reduce(jnp.add, [a[group(i, n, k)] for a in accs]) for k in range(2)]


def put_halves(table, i, n, *parts):
    for k, part in enumerate(parts):
        table[group(i, n, k)] = part


def stack_rows(parts):
    return jnp.concatenate(parts, axis=0)


def stack_lanes(parts):
    return jnp.concatenate(parts, axis=1)


def down(shape):
    return lax.broadcasted_iota(jnp.int32, shape, 0)


def across(shape):
    return lax.broadcasted_iota(jnp.int32, shape, 1)


def prefix(mask, above):
    m = mask.astype(BF16)
    before = (down(SQUARE) < across(SQUARE)).astype(BF16)
    return dot(m, before) + dot(above, dot(m, jnp.ones(SQUARE, BF16)).astype(BF16))


def rank_halo(halo, counts, src, used, src_back, lists):
    lines = used.shape[0]
    side = lines // 2
    i, j = down((lines, lines)), across((lines, lines))
    above = jnp.logical_and(j < i, (j >= side) == (i >= side)).astype(F32).astype(BF16)
    rank = prefix(used[...], above).astype(jnp.int32)
    low, high = rank & (LANES - 1), rank >> 7
    table = stack_rows([low.astype(F32), high.astype(F32)]).astype(BF16)

    quad = 4

    def four(c, _):
        slot = [src[pl.ds(c * quad + q, 1), :] >> 1 for q in range(quad)]
        spots = stack_lanes([(down(SQUARE) == (t & (LANES - 1))).astype(F32) for t in slot]).astype(BF16)
        got = dot(table, spots)
        h = stack_lanes(slot) >> 7
        got = jnp.where(down(got[:lines].shape) == h, got[:lines] + LANES * got[lines:], 0.0)
        got = (jnp.sum(got, axis=0, keepdims=True).astype(jnp.int32) + jnp.where(h >= side, halo, 0)) * 2
        for q in range(quad):
            src_back[pl.ds(c * quad + q, 1), :] = got[:, q * LANES : (q + 1) * LANES]
        return 0

    ratio = quad * LANES // PREP_CHUNK
    lax.fori_loop(counts[0] // ratio, (counts[1] + ratio - 1) // ratio, four, 0)
    for k in range(2):
        acc = jnp.zeros((24, LANES), F32)
        for hh in range(side):
            q = k * side + hh
            pick = jnp.where(down(TILE) == high[q : q + 1, :], used[q : q + 1, :], 0.0)
            lhs = stack_rows([pick * across(TILE).astype(F32), pick * hh, pick]).astype(BF16)
            acc += dot(lhs, (down(SQUARE) == low[q : q + 1, :]).astype(F32).astype(BF16), COLS_A)
        slots = acc[:8] + LANES * acc[8:16]
        lists[k * side : (k + 1) * side, :] = jnp.where(acc[16:24] > 0.0, slots[:side], -1.0)


def first_kernel(compact, halo, tab, tab_b, send, counts, src, w, used, to_prev, to_next, w_out, src_back, lists, buf, idx, sems):
    fetch = fetch_index(send, idx, sems)
    for c in fetch:
        c.start()
    src_back[...] = src[...]
    if compact:
        rank_halo(halo, counts, src, used, src_back, lists)
    else:
        line = down(lists.shape)
        line = jnp.where(line >= lists.shape[0] // 2, line - lists.shape[0] // 2, line)
        lists[...] = (line * LANES + across(lists.shape)).astype(F32)
    for c in fetch:
        c.wait()
    share = w.shape[0] * BLOCK // halo

    def widen(i):
        for q in range(share):
            r = i // BLOCK * share + q
            w_out[pl.ds(pl.multiple_of(r * LANES, LANES), LANES), :] = spread(w[pl.ds(r, 1), :])

    gather_rows(send, idx, tab_b, tab, buf, to_prev, to_next, widen)


def greet(n):
    me = lax.axis_index(AXIS)
    barrier = pltpu.get_barrier_semaphore()
    for o in range(1, n):
        pl.semaphore_signal(barrier, inc=1, device_id=(lax.rem(me + o, n),), device_id_type=MESH)
    return me, lambda: pl.semaphore_wait(barrier, n - 1)


def remote(src, dst, send_sem, recv_sem, peer):
    return pltpu.make_async_remote_copy(
        src_ref=src, dst_ref=dst, send_sem=send_sem, recv_sem=recv_sem, device_id=(peer,), device_id_type=MESH
    )


def reduce_kernel(n, one, two, loss, count, one_out, two_out, mean, work, full, got_pair, got_rest, sems):
    me = lax.axis_index(AXIS)
    chips, core = n // 2, lax.rem(me, 2)
    chip = lax.div(me, 2)
    pair = me + 1 - 2 * core
    others = [lax.rem(chip + o, chips) for o in range(1, chips)]
    barrier = pltpu.get_barrier_semaphore()
    for p in [pair] + [2 * c + core for c in others]:
        pl.semaphore_signal(barrier, inc=1, device_id=(p,), device_id_type=MESH)
    classes = two_out.shape[0]
    lines = -(-classes // SUB) * SUB
    top, wide = one.shape
    work[:top, :] = one[:, :LANES]
    work[top : 2 * top, :] = one[:, LANES:]
    work[2 * top : 2 * top + lines, :] = two[:lines, :LANES]
    work[2 * top + lines : 2 * top + 2 * lines, :] = two[:lines, LANES:]
    tail = 2 * top + 2 * lines
    work[tail : tail + SUB, :] = loss[...]
    work[tail + SUB :, :] = jnp.zeros((work.shape[0] - tail - SUB, LANES), F32)
    pl.semaphore_wait(barrier, chips)

    half = work.shape[0] // 2
    piece = half // chips
    spot = lambda c, k: pl.ds(pl.multiple_of(k * half + c * piece, SUB), piece)
    link = lambda kind, o, src, dst, peer: remote(src, dst, sems.at[0, kind * chips + o], sems.at[1, kind * chips + o], peer)
    order = list(enumerate(others + [chip]))
    swap = [link(0, o, work.at[spot(c, 1 - core)], got_pair.at[pl.ds(o * piece, piece)], pair) for o, c in order]
    for c in swap:
        c.start()
    scatter = [link(1, o, work.at[spot(c, core)], got_rest.at[o], 2 * c + core) for o, c in order[:-1]]
    for o, c in order:
        swap[o].wait_recv()
        work[spot(c, core), :] += got_pair[o * piece : (o + 1) * piece, :]
        if o:
            scatter[o - 1].start()
    for c in scatter:
        c.wait_recv()
    own = spot(chip, core)
    work[own, :] += jnp.sum(got_rest[...], axis=0)
    full[own, :] = work[own, :]
    for c in swap + scatter:
        c.wait_send()
    gather = [link(2, o, work.at[own], full.at[own], 2 * c + core) for o, c in order[:-1]]
    for c in gather:
        c.start()
    forward = [link(3, chips - 1, work.at[own], full.at[own], pair)]
    forward[0].start()
    for o, _ in order[:-1]:
        gather[o].wait_recv()
        came = spot(lax.rem(chip + chips - 1 - o, chips), core)
        forward.append(link(3, o, full.at[came], full.at[came], pair))
        forward[-1].start()
    for c in gather:
        c.wait_send()
    for c in forward:
        c.wait()
    one_out[:, :LANES] = full[:top, :]
    one_out[:, LANES:] = full[top : 2 * top, :]
    two_out[:, :LANES] = full[2 * top : 2 * top + classes, :]
    two_out[:, LANES:] = full[2 * top + lines : 2 * top + lines + classes, :]
    mean[...] = jnp.sum(full[tail : tail + SUB, :], keepdims=True) / count[:1, :1]


def prep_kernel(n, chunk, rows, src_in, dst_in, w_in, mask, x, w1, tab, tab_b, src_out, dst_out, w_out, used, counts, count, need, total, values, places, hits, mine, theirs, send_sem, recv_sem):
    me, met = greet(n)
    lines, slots = src_in.shape[0], src_out.shape[0]
    src, d, half_w = src_in[...], dst_in[...], w_in[...] * 0.5
    live = w_in[...] != 0.0
    halo = src >= rows
    above = (across((lines, lines)) < down((lines, lines))).astype(F32).astype(BF16)
    is_local, is_halo = jnp.logical_and(live, jnp.logical_not(halo)), jnp.logical_and(live, halo)
    rank = lambda m: prefix(m.astype(F32), above).astype(jnp.int32)
    n_local = jnp.sum(is_local.astype(F32)).astype(jnp.int32)
    n_halo = jnp.sum(is_halo.astype(F32)).astype(jnp.int32)
    local_chunks = (n_local + chunk - 1) // chunk
    counts[0] = local_chunks
    counts[1] = local_chunks + (n_halo + chunk - 1) // chunk
    pos = jnp.where(is_local, rank(is_local), jnp.where(is_halo, rank(is_halo) + local_chunks * chunk, -1))
    s = jnp.where(halo, src - rows, src)
    w_a = half_w.astype(BF16).astype(F32)
    w_b = (half_w - w_a).astype(BF16).astype(F32)
    w_c = half_w - w_a - w_b
    high = ((s >> 8) * 8 + (d >> 8)).astype(F32)
    planes = [(s % BYTE).astype(F32), (d % BYTE).astype(F32), high, w_a, w_b, w_c]
    for i, p in enumerate(planes):
        values[i * lines : (i + 1) * lines, :] = p
    for i, p in enumerate((pos >> 7, pos & (LANES - 1), jnp.where(is_halo, s >> 7, -1), s & (LANES - 1))):
        places[i * lines : (i + 1) * lines, :] = p
    row = lambda i, q: pl.ds(i * lines + q, 1)
    spot = lambda size, i, q: (down((size, LANES)) == places[row(i, q), :]).astype(F32)
    hits[...] = jnp.zeros_like(hits)

    @pl.loop(0, lines, step=SUB)
    def _(base):
        acc = None
        for r in range(0, SUB, 2):
            lhs = stack_lanes([spot(hits.shape[0], 2, base + q) for q in (r, r + 1)]).astype(BF16)
            rhs = stack_lanes([spot(LANES, 3, base + q) for q in (r, r + 1)]).astype(BF16)
            part = dot(lhs, rhs, COLS_A)
            acc = part if acc is None else acc + part
        hits[...] += acc

    flags = (hits[...] > 0.0).astype(F32)
    used[...] = flags
    side = hits.shape[0] // 2
    most = jnp.maximum(jnp.sum(flags[:side], keepdims=True), jnp.sum(flags[side:], keepdims=True))
    mine[:1, :] = jnp.sum(mask[...].astype(F32), axis=0, keepdims=True)
    mine[1:, :] = jnp.broadcast_to(most, (1, LANES))
    met()
    copies = [remote(mine, theirs.at[o - 1], send_sem.at[o - 1], recv_sem.at[o - 1], lax.rem(me + o, n)) for o in range(1, n)]
    for c in copies:
        c.start()
    total[...] = jnp.zeros_like(total)

    @pl.loop(0, lines, step=SUB)
    def _(base):
        acc = None
        for r in range(0, SUB, 2):
            lhs, rhs = [], []
            for q in (base + r, base + r + 1):
                pick = down((slots, LANES)) == places[row(0, q), :]
                lhs.append(stack_rows([jnp.where(pick, values[row(i, q), :], 0.0) for i in range(len(planes))]))
                rhs.append(spot(LANES, 1, q))
            part = dot(stack_lanes(lhs).astype(BF16), stack_lanes(rhs).astype(BF16), COLS_A)
            acc = part if acc is None else acc + part
        total[...] += acc

    plane = lambda i: total[i * slots : (i + 1) * slots, :]
    high = plane(2).astype(jnp.int32)
    w1_b = w1[...].astype(BF16)

    @pl.loop(0, rows, step=STEP)
    def _(i):
        t = dot(x[pl.ds(i, STEP), :], w1_b).astype(BF16)
        tab_b[pl.ds(i, STEP), :] = t
        t = t.astype(F32)
        put_halves(tab, i, STEP, t[:, :LANES], t[:, LANES:])

    src_out[...] = ((high >> 3) * BYTE + plane(0).astype(jnp.int32)) * 2
    dst_out[...] = ((high & 7) * BYTE + plane(1).astype(jnp.int32)) * 2
    w_out[...] = (plane(3) + plane(4) + plane(5)) * 2.0
    for c in copies:
        c.wait()
    every = jnp.sum(mine[:1, :] + jnp.sum(theirs[:, :1, :], axis=0), keepdims=True)
    count[...] = jnp.maximum(jnp.broadcast_to(every, count.shape), 1.0)
    need[0] = jnp.max(jnp.maximum(mine[1:, :], jnp.max(theirs[:, 1:, :], axis=0))).astype(jnp.int32)


def local_kernel(chunk, backward, counts, src, dst, w, table, out, src_s, dst_s, sems, *accs):
    edges = Edges(0, counts[0], w, (src, dst), (src_s, dst_s), sems)
    edges.fetch()
    for a in accs:
        fill_zero(a)
    edges.walk(chunk, *((dst_s, src_s) if backward else (src_s, dst_s)), table, accs, True)

    @pl.loop(0, out.shape[0], step=STEP)
    def _(i):
        out[pl.ds(i, STEP), :] = functools.reduce(jnp.add, [a[pl.ds(i, STEP), :] for a in accs])


def forward_halo(chunk, edges, src_s, dst_s, from_prev, from_next, part, htab, accs, unpack):
    edges.fetch()
    unpack(from_prev, htab, 0)
    unpack(from_next, htab, htab.shape[0] // 4)
    copy_in(accs[0], part)
    for a in accs[1:]:
        fill_zero(a)
    edges.walk(chunk, src_s, dst_s, htab, accs, True)


def backward_halo(limit, chunk, edges, src_s, dst_s, grad, back_prev, back_next, accs, wait, lists=None):
    split = accs[0].shape[0] // 2
    for a in accs:
        for start in (0, split):
            fill_zero(a.at[pl.ds(start, limit * 2)])
    edges.walk(chunk, dst_s, src_s, grad, accs, wait)
    if lists is None:

        @pl.loop(0, back_prev.shape[0], step=SMALL)
        def _(i):
            back_prev[pl.ds(i, SMALL), :] = functools.reduce(jnp.add, [a[pl.ds(i, SMALL), :] for a in accs])
            back_next[pl.ds(i, SMALL), :] = functools.reduce(jnp.add, [a[pl.ds(split + i, SMALL), :] for a in accs])
        return
    side = lists.shape[0] // 2
    half = (back_prev.shape[0] - side) // 3
    n = half // 2
    for k, out in enumerate((back_prev, back_next)):
        start = k * (split // 2)

        @pl.loop(0, half, step=n)
        def _(i):
            i = pl.multiple_of(i, n)
            pack_rows(out, i, half, *halves(accs, start + i, n), *halves(accs, start + half + i, n))

        out[3 * half : 3 * half + side, :] = lists[k * side : (k + 1) * side, :]


def padded(w, buf):
    low = w.shape[0] // SUB * SUB
    buf[low:, :] = jnp.zeros((buf.shape[0] - low, buf.shape[1]), F32)
    buf[:w.shape[0], :] = w[...]
    return buf[...].astype(BF16)


def hidden_kernel(chunk, counts, src, dst, w, send, from_prev, from_next, part, w2, hid, tab, to_prev, to_next, back, htab, tab_b, w2_pad, buf, idx, idx_sems, src_s, dst_s, sems, *accs):
    fetch = fetch_index(send, idx, idx_sems)
    for c in fetch:
        c.start()
    edges = Edges(counts[0], counts[1], w, (src, dst), (src_s, dst_s), sems)
    w2_b = padded(w2, w2_pad)
    per = send.shape[1] // LANES
    for i in range(2 * per):
        back[i : i + 1, :] = send[i // per : i // per + 1, (i % per) * LANES : (i % per + 1) * LANES] * 2
    forward_halo(chunk, edges, src_s, dst_s, from_prev, from_next, part, htab, accs, unpack_plain)

    @pl.loop(0, hid.shape[0], step=STEP)
    def _(i):
        even, odd = halves(accs, i, STEP)
        h = stack_lanes([jnp.maximum(even, 0.0), jnp.maximum(odd, 0.0)]).astype(BF16)
        hid[pl.ds(i, STEP), :] = h
        t = dot(h, w2_b, COLS_A).astype(BF16)
        tab_b[pl.ds(i, STEP), :] = t
        t = t.astype(F32)
        put_halves(tab, i, STEP, t[:, :LANES], t[:, LANES:])

    for c in fetch:
        c.wait()
    gather_packed(send, idx, tab_b, tab, buf, to_prev, to_next)


def loss_kernel(limit, quad, chunk, classes, counts, src, dst, w, src_back, lists, count, from_prev, from_next, part, labels, mask, loss, grad, back_prev, back_next, htab, src_s, dst_s, back_s, sems, *accs):
    edges = Edges(counts[0], counts[1], w, (src, dst, src_back), (src_s, dst_s, back_s), sems)
    forward_halo(chunk, edges, src_s, dst_s, from_prev, from_next, part, htab, accs, unpack_rows)
    lane = across(SQUARE)
    live = lane < classes - LANES
    scale = 1.0 / count[:1, :]
    loss[...] = jnp.zeros_like(loss)

    @pl.loop(0, labels.shape[0], step=quad)
    def _(first):
        for b in [first + q for q in range(quad)]:
            even, odd = halves(accs, b * LANES, LANES)
            odd = jnp.where(live, odd, -jnp.inf)
            keep = spread(mask[pl.ds(b, 1), :])
            label = jnp.where(keep > 0, spread(labels[pl.ds(b, 1), :]), -1)
            hit_even, hit_odd = lane == label, lane + LANES == label
            top = jnp.max(jnp.maximum(even, odd), axis=1, keepdims=True)
            exp_even, exp_odd = jnp.exp(even - top), jnp.exp(odd - top)
            total = jnp.sum(exp_even + exp_odd, axis=1, keepdims=True)
            norm = jnp.where(jnp.logical_and(lane == 0, keep > 0), top + jnp.log(total), 0.0)
            per_row = norm - jnp.where(hit_even, even, jnp.where(hit_odd, odd, 0.0))
            loss[...] += jnp.sum(per_row.reshape(LANES // SUB, *TILE), axis=0)
            share = keep.astype(F32) * scale * (1.0 / total)
            put_halves(
                grad, b * LANES, LANES, *(e * share - jnp.where(hit, scale, 0.0) for e, hit in ((exp_even, hit_even), (exp_odd, hit_odd)))
            )

    backward_halo(limit, chunk, edges, back_s, dst_s, grad, back_prev, back_next, accs, False, lists)


def take_returns(back, slots, counts, part, got_prev, got_next, accs):
    return_rows(back, slots, 0, counts[0], got_prev, accs)
    return_rows(back, slots, slots.shape[0] // 2, counts[1], got_next, accs)


def fetch_lines(lines, smem, sems):
    return [pltpu.make_async_copy(lines.at[i], smem.at[pl.ds(i * LANES, LANES)], sems.at[i]) for i in range(lines.shape[0])]


def middle_kernel(limit, chunk, counts, src, dst, w, back, got_prev, got_next, part, hid, w2, grad_two, grad, back_prev, back_next, slots, n_back, returned, w2_pad, slot_s, slot_sems, src_s, dst_s, sems, *accs):
    edges = Edges(counts[0], counts[1], w, (src, dst), (src_s, dst_s), sems)
    edges.fetch()
    side = slots.shape[0] // 2
    half = (got_prev.shape[0] - side) // 3
    for k, got in enumerate((got_prev, got_next)):
        slot = got[3 * half :, :].astype(jnp.int32)
        slots[k * side : (k + 1) * side, :] = jnp.maximum(slot, 0) + (1 - k) * side * LANES
        n_back[k] = jnp.sum((slot >= 0).astype(F32)).astype(jnp.int32)
    w2_b = padded(w2, w2_pad)
    unpack_rows(got_prev, returned, 0, half)
    unpack_rows(got_next, returned, 2 * half, half)
    fetch = fetch_lines(slots, slot_s, slot_sems)
    for c in fetch:
        c.start()
    copy_in(accs[0], part)
    for a in accs[1:]:
        fill_zero(a)
    for c in fetch:
        c.wait()
    take_returns(back, slot_s, n_back, part, returned.at[pl.ds(0, 4 * half)], returned.at[pl.ds(4 * half, 4 * half)], accs)
    grad_two[...] = jnp.zeros_like(grad_two)

    @pl.loop(0, hid.shape[0], step=STEP)
    def _(i):
        even, odd = halves(accs, i, STEP)
        d_tab = stack_lanes([even, odd]).astype(BF16)
        h = hid[pl.ds(i, STEP), :]
        grad_two[...] += dot(d_tab, h, ROWS_A)
        d_hid = dot(d_tab, w2_b)
        d_pre = jnp.where(h > 0, d_hid, 0.0)
        put_halves(grad, i, STEP, d_pre[:, :LANES], d_pre[:, LANES:])

    backward_halo(limit, chunk, edges, src_s, dst_s, grad, back_prev, back_next, accs, True)


def last_kernel(back, n_back, slots, got_prev, got_next, part, x, grad_one, slot_s, slot_sems, *accs):
    fetch = fetch_lines(slots, slot_s, slot_sems)
    for c in fetch:
        c.start()
    copy_in(accs[0], part)
    for a in accs[1:]:
        fill_zero(a)
    for c in fetch:
        c.wait()
    take_returns(back, slot_s, n_back, part, got_prev, got_next, accs)
    grad_one[...] = jnp.zeros_like(grad_one)

    @pl.loop(0, x.shape[0], step=STEP)
    def _(i):
        even, odd = halves(accs, i, STEP)
        d_tab = stack_lanes([even, odd]).astype(BF16)
        grad_one[...] += dot(x[pl.ds(i, STEP), :], d_tab, ROWS_A)


def call(body, name, outs, ins, scratch, out_specs=None, collective=None, vmem=14):
    extra = {} if collective is None else dict(collective_id=collective, has_side_effects=True)
    return pl.pallas_call(
        body, name=name, out_shape=outs, in_specs=ins, out_specs=out_specs or jax.tree.map(lambda _: VMEM, outs),
        scratch_shapes=[pltpu.VMEM(s, F32) if isinstance(s, tuple) else s for s in scratch],
        compiler_params=pltpu.CompilerParams(vmem_limit_bytes=vmem * 2**20, **extra),
        cost_estimate=pl.CostEstimate(flops=10**10, bytes_accessed=10**7, transcendentals=0),
    )


def solution(mesh):
    num_dev = mesh.shape[AXIS]
    to_next = [(d, (d + 1) % num_dev) for d in range(num_dev)]
    to_prev = [(d, (d - 1) % num_dev) for d in range(num_dev)]

    def step(x, w_one, w_two, send, edge_src, edge_dst, edge_w, labels, mask):
        rows, halo, edges, classes = x.shape[0], send.shape[1], edge_src.shape[0], w_two.shape[1]
        tab, half, w2_pad = (2 * rows, LANES), (2 * halo, LANES), (2 * LANES, 2 * LANES)
        sds = jax.ShapeDtypeStruct
        tab_f = sds(tab, F32)
        half_b, pack_b = sds((halo, 2 * LANES), BF16), sds((3 * halo // 2, LANES), BF16)
        wide_b = pltpu.VMEM((rows, 2 * LANES), BF16)
        one = sds(TILE, F32)
        dma = pltpu.SemaphoreType.DMA
        chunk_l, chunk_h = 64, 32
        lines = edges // LANES
        slots = lines + 8
        side = halo // LANES
        w2 = w_two.T
        mask = mask.reshape(-1, LANES)
        labels = labels.reshape(-1, LANES)
        lined = [a.reshape(lines, LANES) for a in (edge_src, edge_dst, edge_w)]
        ints = sds((slots, LANES), jnp.int32)
        sided = sds((2 * side, LANES), F32)
        tab_one, tab_b, src, dst, w_lines, used, counts, count, need = call(
            functools.partial(prep_kernel, num_dev, PREP_CHUNK, rows), "prep",
            [tab_f, sds((rows, 2 * LANES), BF16), ints, ints, sds((slots, LANES), F32), sided, sds((2,), jnp.int32), one, sds((1,), jnp.int32)],
            [VMEM] * 6,
            [(6 * slots, LANES), (6 * lines, LANES), pltpu.VMEM((4 * lines, LANES), jnp.int32), sided.shape, (2, LANES), (num_dev - 1, 2, LANES)]
            + [dma((num_dev - 1,))] * 2,
            out_specs=[VMEM] * 6 + [SMEM, VMEM, SMEM], vmem=60, collective=0,
        )(*lined, mask, x, w_one)

        def run(limit):
            compact = limit < halo
            pack_f, half_f = sds((3 * limit // 2 + side, LANES), F32), sds((2 * limit, LANES), F32)
            list_s = [pltpu.SMEM((halo,), jnp.int32), dma((side,))]
            to_p, to_n, w, src_back, lists = call(
                functools.partial(first_kernel, compact, halo), "first", [half_b, half_b, sds((slots * LANES, LANES), F32), ints, sided],
                [VMEM] * 3 + [SMEM] + [VMEM] * 3, [half] + list_s, vmem=8,
            )(tab_one, tab_b, send, counts, src, w_lines, used)
            from_prev = lax.ppermute(to_n, AXIS, to_next)
            from_next = lax.ppermute(to_p, AXIS, to_prev)
            flat, flat_dst, flat_back = src.reshape(-1), dst.reshape(-1), src_back.reshape(-1)

            four = [tab] * 4
            walk = [SMEM, ANY, ANY, VMEM]
            index = pltpu.SMEM((slots * LANES,), jnp.int32)
            walk_s = lambda n: [index] * n + [dma((n, slots * LANES // SEGMENT))]
            slot_s = [pltpu.SMEM((2 * halo,), jnp.int32), dma((2 * side,))]
            local, local_back = (
                call(functools.partial(local_kernel, chunk_l, back), "local_edges", tab_f, walk + [VMEM], walk_s(2) + four)
                for back in (False, True)
            )
            part = local(counts, flat, flat_dst, w, tab_one)
            hid, tab_two, to_p, to_n, back = call(
                functools.partial(hidden_kernel, chunk_h), "hidden",
                [sds((rows, 2 * LANES), BF16), tab_f, pack_b, pack_b, sds((2 * side, LANES), jnp.int32)],
                walk + [VMEM] * 5, [tab, wide_b, w2_pad, half] + list_s + walk_s(2) + four,
            )(counts, flat, flat_dst, w, send, from_prev, from_next, part, w2)
            from_prev = lax.ppermute(to_n, AXIS, to_next)
            from_next = lax.ppermute(to_p, AXIS, to_prev)
            back = back.reshape(-1)
            part = local(counts, flat, flat_dst, w, tab_two)
            loss, grad, to_p, to_n = call(
                functools.partial(loss_kernel, limit, 4, chunk_h, classes), "loss", [one, tab_f, pack_f, pack_f],
                walk + [ANY] + [VMEM] * 7, [tab] + walk_s(3) + four,
            )(counts, flat, flat_dst, w, flat_back, lists, count, from_prev, from_next, part, labels, mask)
            got_prev = lax.ppermute(to_p, AXIS, to_prev)
            got_next = lax.ppermute(to_n, AXIS, to_next)
            part = local_back(counts, flat, flat_dst, w, grad)
            grad_two, grad, to_p, to_n, slot, n_back = call(
                functools.partial(middle_kernel, limit, chunk_h), "middle",
                [sds(w2_pad, F32), tab_f, half_f, half_f, sds((2 * side, LANES), jnp.int32), sds((2,), jnp.int32)],
                walk + [SMEM] + [VMEM] * 5, [(4 * limit, LANES), w2_pad] + slot_s + walk_s(2) + four, out_specs=[VMEM] * 5 + [SMEM],
            )(counts, flat_back, flat_dst, w, back, got_prev, got_next, part, hid, w2)
            got_prev = lax.ppermute(to_p, AXIS, to_prev)
            got_next = lax.ppermute(to_n, AXIS, to_next)
            part = local_back(counts, flat, flat_dst, w, grad)
            grad_one = call(
                last_kernel, "last", sds((x.shape[1], 2 * LANES), F32), [SMEM, SMEM, ANY] + [VMEM] * 4, slot_s + four
            )(back, n_back, slot, got_prev, got_next, part, x)
            return grad_one, grad_two, loss

        limits = [halo // 32 * part for part in (15, 17, 19, 32)]
        need = need.reshape(())
        choice = sum((need > limit).astype(jnp.int32) for limit in limits[:-1])
        grad_one, grad_two, loss = lax.switch(choice, [functools.partial(run, limit) for limit in limits])
        unit = SUB * num_dev
        lines = 2 * (x.shape[1] + -(-classes // SUB) * SUB) + SUB
        lines = -(-lines // unit) * unit
        grad_one, grad_two, mean = call(
            functools.partial(reduce_kernel, num_dev), "reduce", [sds(grad_one.shape, F32), sds((classes, 2 * LANES), F32), sds((1, 1), F32)],
            [VMEM] * 4, [(lines, LANES), (lines, LANES), (lines // 2, LANES), (num_dev // 2 - 1, lines // num_dev, LANES), dma((2, 2 * num_dev))],
            collective=1, vmem=8,
        )(grad_one, grad_two, loss, count)
        return mean.reshape(()), grad_one, grad_two.T

    row = P(AXIS)
    return jax.shard_map(
        step, mesh=mesh, in_specs=(row, P(), P(), row, row, row, row, row, row), out_specs=(P(), P(), P()), check_vma=False
    )
```

```python
import functools

import jax
import jax.numpy as jnp
from jax import lax
from jax.experimental import pallas as pl
from jax.experimental.pallas import tpu as pltpu
from jax.sharding import PartitionSpec as P

AXIS = "graph"
LANES = 128
ROWS_A = (((0,), (0,)), ((), ()))
COLS_A = (((1,), (1,)), ((), ()))
F32, BF16 = jnp.float32, jnp.bfloat16
VMEM = pl.BlockSpec(memory_space=pltpu.VMEM)
SMEM = pl.BlockSpec(memory_space=pltpu.SMEM)
ANY = pl.BlockSpec(memory_space=pl.ANY)
STEP = 512
BLOCK = 256
BYTE = BLOCK
SUB = 8
TWICE = 2 * SUB
TILE = (SUB, LANES)
SQUARE = (LANES, LANES)
PREP_CHUNK = 64
SMALL = PREP_CHUNK
SEGMENT = 1024
MESH = pl.DeviceIdType.MESH


def dot(a, b, dims=(((1,), (0,)), ((), ()))):
    return lax.dot_general(a, b, dims, preferred_element_type=F32)


def fill_zero(ref):
    step = BLOCK if ref.shape[0] % BLOCK == 0 else SMALL
    zero = jnp.zeros((step, LANES), F32)

    @pl.loop(0, ref.shape[0], step=step)
    def _(i):
        ref[pl.ds(i, step), :] = zero


def copy_in(dst, src):
    @pl.loop(0, dst.shape[0], step=STEP)
    def _(i):
        dst[pl.ds(i, STEP), :] = src[pl.ds(i, STEP), :].astype(F32)


class Edges:
    def __init__(self, first, last, w, arrays, smem, sems):
        self.first, self.last, self.w = first, last, w
        self.pairs = tuple(zip(arrays, smem))
        self.sems = sems

    def copies(self, seg):
        part = pl.ds(pl.multiple_of(seg * SEGMENT, SEGMENT), SEGMENT)
        return [pltpu.make_async_copy(a.at[part], b.at[part], self.sems.at[i, seg]) for i, (a, b) in enumerate(self.pairs)]

    def fetch(self):
        per = SEGMENT // PREP_CHUNK
        for seg in range(self.pairs[0][1].shape[0] // SEGMENT):

            @pl.when(jnp.logical_and(seg * per < self.last, (seg + 1) * per > self.first))
            def _():
                for c in self.copies(seg):
                    c.start()

    def walk(self, chunk, from_idx, to_idx, table, accs, wait):
        group, per, ratio = len(accs), SEGMENT // chunk, PREP_CHUNK // chunk
        first, last = self.first * ratio, self.last * ratio

        def body(c, _):
            base = c * chunk
            w_chunk = self.w.at[pl.ds(pl.multiple_of(base, chunk), chunk)]
            for g in range(0, chunk, group):
                pend = []
                for u in range(group):
                    k = base + g + u
                    s = pl.multiple_of(from_idx[k], 2)
                    d = pl.multiple_of(to_idx[k], 2)
                    pend.append((d, accs[u][pl.ds(d, 2), :] + table[pl.ds(s, 2), :] * w_chunk[g + u : g + u + 1, :]))
                for u in range(group):
                    accs[u][pl.ds(pend[u][0], 2), :] = pend[u][1]
            return 0

        if not wait:
            lax.fori_loop(first, last, body, 0)
            return

        def segment(seg, _):
            for c in self.copies(seg):
                c.wait()
            lax.fori_loop(jnp.maximum(first, seg * per), jnp.minimum(last, (seg + 1) * per), body, 0)
            return 0

        lax.fori_loop(first // per, (last + per - 1) // per, segment, 0)


def one_hot_rows(idx, which, start, table):
    lane = across(SQUARE)
    hot = []
    for q in range(2):
        want = spread(idx[which : which + 1, pl.ds(pl.multiple_of(start + q * LANES, LANES), LANES)])
        hot.append(
            stack_lanes([jnp.where(want == lane + LANES * j, 1.0, 0.0).astype(BF16) for j in range(table.shape[0] // LANES)])
        )
    return dot(stack_rows(hot), table[...])


def low_lanes(rows):
    return across((rows, LANES)) < LANES // 2


def swap_lanes(v):
    return pltpu.roll(v, LANES // 2, 1)


def fetch_index(send, idx, sems):
    parts = [pl.ds(i, LANES) for i in range(0, send.shape[1], LANES)]
    return [pltpu.make_async_copy(send.at[1, p], idx.at[p], sems.at[i]) for i, p in enumerate(parts)]


def gather_block(send, idx, i, table_b, table, buf):
    got = one_hot_rows(send, 0, i, table_b)
    out = buf.at[pl.ds(pl.multiple_of(2 * i, 512), 512)]
    for u in range(BLOCK):
        s = pl.multiple_of(idx[i + u] * 2, 2)
        out[2 * u : 2 * u + 2, :] = table[pl.ds(s, 2), :]
    return got


def gather_rows(send, idx, table_b, table, buf, to_prev, to_next, also):
    @pl.loop(0, to_prev.shape[0], step=BLOCK)
    def _(i):
        i = pl.multiple_of(i, BLOCK)
        to_prev[pl.ds(i, BLOCK), :] = gather_block(send, idx, i, table_b, table, buf).astype(BF16)
        also(i)

    @pl.loop(0, to_next.shape[0], step=BLOCK)
    def _(i):
        to_next[pl.ds(pl.multiple_of(i, BLOCK), BLOCK), :] = stack_lanes(halves([buf], i, BLOCK)).astype(BF16)


def pack_rows(out, i, half, a_even, a_odd, b_even, b_odd):
    n = a_even.shape[0]
    out[pl.ds(i, n), :] = a_even.astype(out.dtype)
    out[pl.ds(half + i, n), :] = b_even.astype(out.dtype)
    out[pl.ds(2 * half + i, n), :] = jnp.where(low_lanes(n), a_odd, swap_lanes(b_odd)).astype(out.dtype)


def gather_packed(send, idx, table_b, table, buf, to_prev, to_next):
    half = to_prev.shape[0] // 3

    @pl.loop(0, half, step=BLOCK)
    def _(i):
        i = pl.multiple_of(i, BLOCK)
        a = gather_block(send, idx, i, table_b, table, buf)
        b = gather_block(send, idx, half + i, table_b, table, buf)
        pack_rows(to_prev, i, half, a[:, :LANES], a[:, LANES:], b[:, :LANES], b[:, LANES:])

    @pl.loop(0, half, step=BLOCK)
    def _(i):
        i = pl.multiple_of(i, BLOCK)
        pack_rows(to_next, i, half, *halves([buf], i, BLOCK), *halves([buf], half + i, BLOCK))


def unpack_rows(got, table, start, half=None):
    half = got.shape[0] // 3 if half is None else half
    n = half // 2

    @pl.loop(0, half, step=n)
    def _(i):
        i = pl.multiple_of(i, n)
        a, b, both = (got[pl.ds(k + i, n), :].astype(F32) for k in (0, half, 2 * half))
        put_halves(table, start + i, n, a, jnp.where(low_lanes(n), both, 0.0))
        put_halves(table, start + half + i, n, b, jnp.where(low_lanes(n), swap_lanes(both), 0.0))


def unpack_plain(got, table, start):
    @pl.loop(0, got.shape[0], step=BLOCK)
    def _(i):
        t = got[pl.ds(i, BLOCK), :].astype(F32)
        put_halves(table, start + i, BLOCK, t[:, :LANES], t[:, LANES:])


def spread(row):
    return jnp.transpose(jnp.broadcast_to(row, SQUARE))


def return_rows(back, slots, start, count, vals, accs, chunk=32):
    group = len(accs)

    def body(c, _):
        block = vals.at[pl.ds(pl.multiple_of(c * 2 * chunk, 2 * chunk), 2 * chunk)]
        for g in range(0, chunk, group):
            pend = []
            for u in range(group):
                d = pl.multiple_of(back[slots[start + c * chunk + g + u]], 2)
                pend.append((d, accs[u][pl.ds(d, 2), :] + block[2 * (g + u) : 2 * (g + u) + 2, :]))
            for u in range(group):
                accs[u][pl.ds(pend[u][0], 2), :] = pend[u][1]
        return 0

    lax.fori_loop(0, (count + chunk - 1) // chunk, body, 0)


def group(i, n, which):
    return pl.ds(2 * i + which, n, stride=2), slice(None)


def halves(accs, i, n):
    return [functools.reduce(jnp.add, [a[group(i, n, k)] for a in accs]) for k in range(2)]


def put_halves(table, i, n, *parts):
    for k, part in enumerate(parts):
        table[group(i, n, k)] = part


def stack_rows(parts):
    return jnp.concatenate(parts, axis=0)


def stack_lanes(parts):
    return jnp.concatenate(parts, axis=1)


def down(shape):
    return lax.broadcasted_iota(jnp.int32, shape, 0)


def across(shape):
    return lax.broadcasted_iota(jnp.int32, shape, 1)


def prefix(mask, above):
    m = mask.astype(BF16)
    before = (down(SQUARE) < across(SQUARE)).astype(BF16)
    return dot(m, before) + dot(above, dot(m, jnp.ones(SQUARE, BF16)).astype(BF16))


def rank_halo(halo, counts, src, used, src_back, lists):
    lines = used.shape[0]
    side = lines // 2
    i, j = down((lines, lines)), across((lines, lines))
    above = jnp.logical_and(j < i, (j >= side) == (i >= side)).astype(F32).astype(BF16)
    rank = prefix(used[...], above).astype(jnp.int32)
    low, high = rank & (LANES - 1), rank >> 7
    table = stack_rows([low.astype(F32), high.astype(F32)]).astype(BF16)

    quad = 4

    def four(c, _):
        slot = [src[pl.ds(c * quad + q, 1), :] >> 1 for q in range(quad)]
        spots = stack_lanes([(down(SQUARE) == (t & (LANES - 1))).astype(F32) for t in slot]).astype(BF16)
        got = dot(table, spots)
        h = stack_lanes(slot) >> 7
        got = jnp.where(down(got[:lines].shape) == h, got[:lines] + LANES * got[lines:], 0.0)
        got = (jnp.sum(got, axis=0, keepdims=True).astype(jnp.int32) + jnp.where(h >= side, halo, 0)) * 2
        for q in range(quad):
            src_back[pl.ds(c * quad + q, 1), :] = got[:, q * LANES : (q + 1) * LANES]
        return 0

    ratio = quad * LANES // PREP_CHUNK
    lax.fori_loop(counts[0] // ratio, (counts[1] + ratio - 1) // ratio, four, 0)
    for k in range(2):
        acc = jnp.zeros((24, LANES), F32)
        for hh in range(side):
            q = k * side + hh
            pick = jnp.where(down(TILE) == high[q : q + 1, :], used[q : q + 1, :], 0.0)
            lhs = stack_rows([pick * across(TILE).astype(F32), pick * hh, pick]).astype(BF16)
            acc += dot(lhs, (down(SQUARE) == low[q : q + 1, :]).astype(F32).astype(BF16), COLS_A)
        slots = acc[:8] + LANES * acc[8:16]
        lists[k * side : (k + 1) * side, :] = jnp.where(acc[16:24] > 0.0, slots[:side], -1.0)


def first_kernel(compact, halo, tab, tab_b, send, counts, src, w, used, to_prev, to_next, w_out, src_back, lists, buf, idx, sems):
    fetch = fetch_index(send, idx, sems)
    for c in fetch:
        c.start()
    src_back[...] = src[...]
    if compact:
        rank_halo(halo, counts, src, used, src_back, lists)
    else:
        line = down(lists.shape)
        line = jnp.where(line >= lists.shape[0] // 2, line - lists.shape[0] // 2, line)
        lists[...] = (line * LANES + across(lists.shape)).astype(F32)
    for c in fetch:
        c.wait()
    share = w.shape[0] * BLOCK // halo

    def widen(i):
        for q in range(share):
            r = i // BLOCK * share + q
            w_out[pl.ds(pl.multiple_of(r * LANES, LANES), LANES), :] = spread(w[pl.ds(r, 1), :])

    gather_rows(send, idx, tab_b, tab, buf, to_prev, to_next, widen)


def greet(n):
    me = lax.axis_index(AXIS)
    barrier = pltpu.get_barrier_semaphore()
    for o in range(1, n):
        pl.semaphore_signal(barrier, inc=1, device_id=(lax.rem(me + o, n),), device_id_type=MESH)
    return me, lambda: pl.semaphore_wait(barrier, n - 1)


def remote(src, dst, send_sem, recv_sem, peer):
    return pltpu.make_async_remote_copy(
        src_ref=src, dst_ref=dst, send_sem=send_sem, recv_sem=recv_sem, device_id=(peer,), device_id_type=MESH
    )


def reduce_kernel(n, one, two, loss, count, one_out, two_out, mean, work, full, got_pair, got_rest, sems):
    me = lax.axis_index(AXIS)
    chips, core = n // 2, lax.rem(me, 2)
    chip = lax.div(me, 2)
    pair = me + 1 - 2 * core
    others = [lax.rem(chip + o, chips) for o in range(1, chips)]
    barrier = pltpu.get_barrier_semaphore()
    for p in [pair] + [2 * c + core for c in others]:
        pl.semaphore_signal(barrier, inc=1, device_id=(p,), device_id_type=MESH)
    classes = two_out.shape[0]
    lines = -(-classes // SUB) * SUB
    top, wide = one.shape
    work[:top, :] = one[:, :LANES]
    work[top : 2 * top, :] = one[:, LANES:]
    work[2 * top : 2 * top + lines, :] = two[:lines, :LANES]
    work[2 * top + lines : 2 * top + 2 * lines, :] = two[:lines, LANES:]
    tail = 2 * top + 2 * lines
    work[tail : tail + SUB, :] = loss[...]
    work[tail + SUB :, :] = jnp.zeros((work.shape[0] - tail - SUB, LANES), F32)
    pl.semaphore_wait(barrier, chips)

    half = work.shape[0] // 2
    piece = half // chips
    spot = lambda c, k: pl.ds(pl.multiple_of(k * half + c * piece, SUB), piece)
    link = lambda kind, o, src, dst, peer: remote(src, dst, sems.at[0, kind * chips + o], sems.at[1, kind * chips + o], peer)
    order = list(enumerate(others + [chip]))
    swap = [link(0, o, work.at[spot(c, 1 - core)], got_pair.at[pl.ds(o * piece, piece)], pair) for o, c in order]
    for c in swap:
        c.start()
    scatter = [link(1, o, work.at[spot(c, core)], got_rest.at[o], 2 * c + core) for o, c in order[:-1]]
    for o, c in order:
        swap[o].wait_recv()
        work[spot(c, core), :] += got_pair[o * piece : (o + 1) * piece, :]
        if o:
            scatter[o - 1].start()
    for c in scatter:
        c.wait_recv()
    own = spot(chip, core)
    work[own, :] += jnp.sum(got_rest[...], axis=0)
    full[own, :] = work[own, :]
    for c in swap + scatter:
        c.wait_send()
    gather = [link(2, o, work.at[own], full.at[own], 2 * c + core) for o, c in order[:-1]]
    for c in gather:
        c.start()
    forward = [link(3, chips - 1, work.at[own], full.at[own], pair)]
    forward[0].start()
    for o, _ in order[:-1]:
        gather[o].wait_recv()
        came = spot(lax.rem(chip + chips - 1 - o, chips), core)
        forward.append(link(3, o, full.at[came], full.at[came], pair))
        forward[-1].start()
    for c in gather:
        c.wait_send()
    for c in forward:
        c.wait()
    one_out[:, :LANES] = full[:top, :]
    one_out[:, LANES:] = full[top : 2 * top, :]
    two_out[:, :LANES] = full[2 * top : 2 * top + classes, :]
    two_out[:, LANES:] = full[2 * top + lines : 2 * top + lines + classes, :]
    mean[...] = jnp.sum(full[tail : tail + SUB, :], keepdims=True) / count[:1, :1]


def prep_kernel(n, chunk, rows, src_in, dst_in, w_in, mask, x, w1, tab, tab_b, src_out, dst_out, w_out, used, counts, count, need, total, values, places, hits, mine, theirs, send_sem, recv_sem):
    me, met = greet(n)
    lines, slots = src_in.shape[0], src_out.shape[0]
    src, d, half_w = src_in[...], dst_in[...], w_in[...] * 0.5
    live = w_in[...] != 0.0
    halo = src >= rows
    above = (across((lines, lines)) < down((lines, lines))).astype(F32).astype(BF16)
    is_local, is_halo = jnp.logical_and(live, jnp.logical_not(halo)), jnp.logical_and(live, halo)
    rank = lambda m: prefix(m.astype(F32), above).astype(jnp.int32)
    n_local = jnp.sum(is_local.astype(F32)).astype(jnp.int32)
    n_halo = jnp.sum(is_halo.astype(F32)).astype(jnp.int32)
    local_chunks = (n_local + chunk - 1) // chunk
    counts[0] = local_chunks
    counts[1] = local_chunks + (n_halo + chunk - 1) // chunk
    pos = jnp.where(is_local, rank(is_local), jnp.where(is_halo, rank(is_halo) + local_chunks * chunk, -1))
    s = jnp.where(halo, src - rows, src)
    w_a = half_w.astype(BF16).astype(F32)
    w_b = (half_w - w_a).astype(BF16).astype(F32)
    w_c = half_w - w_a - w_b
    high = ((s >> 8) * 8 + (d >> 8)).astype(F32)
    planes = [(s % BYTE).astype(F32), (d % BYTE).astype(F32), high, w_a, w_b, w_c]
    for i, p in enumerate(planes):
        values[i * lines : (i + 1) * lines, :] = p
    for i, p in enumerate((pos >> 7, pos & (LANES - 1), jnp.where(is_halo, s >> 7, -1), s & (LANES - 1))):
        places[i * lines : (i + 1) * lines, :] = p
    row = lambda i, q: pl.ds(i * lines + q, 1)
    spot = lambda size, i, q: (down((size, LANES)) == places[row(i, q), :]).astype(F32)
    hits[...] = jnp.zeros_like(hits)

    @pl.loop(0, lines, step=TWICE)
    def _(base):
        acc = None
        for r in range(0, TWICE, 2):
            lhs = stack_lanes([spot(hits.shape[0], 2, base + q) for q in (r, r + 1)]).astype(BF16)
            rhs = stack_lanes([spot(LANES, 3, base + q) for q in (r, r + 1)]).astype(BF16)
            part = dot(lhs, rhs, COLS_A)
            acc = part if acc is None else acc + part
        hits[...] += acc

    flags = (hits[...] > 0.0).astype(F32)
    used[...] = flags
    side = hits.shape[0] // 2
    most = jnp.maximum(jnp.sum(flags[:side], keepdims=True), jnp.sum(flags[side:], keepdims=True))
    mine[:1, :] = jnp.sum(mask[...].astype(F32), axis=0, keepdims=True)
    mine[1:, :] = jnp.broadcast_to(most, (1, LANES))
    met()
    copies = [remote(mine, theirs.at[o - 1], send_sem.at[o - 1], recv_sem.at[o - 1], lax.rem(me + o, n)) for o in range(1, n)]
    for c in copies:
        c.start()
    total[...] = jnp.zeros_like(total)

    @pl.loop(0, lines, step=TWICE)
    def _(base):
        acc = None
        for r in range(0, TWICE, 2):
            lhs, rhs = [], []
            for q in (base + r, base + r + 1):
                pick = down((slots, LANES)) == places[row(0, q), :]
                lhs.append(stack_rows([jnp.where(pick, values[row(i, q), :], 0.0) for i in range(len(planes))]))
                rhs.append(spot(LANES, 1, q))
            part = dot(stack_lanes(lhs).astype(BF16), stack_lanes(rhs).astype(BF16), COLS_A)
            acc = part if acc is None else acc + part
        total[...] += acc

    plane = lambda i: total[i * slots : (i + 1) * slots, :]
    high = plane(2).astype(jnp.int32)
    w1_b = w1[...].astype(BF16)

    @pl.loop(0, rows, step=STEP)
    def _(i):
        t = dot(x[pl.ds(i, STEP), :], w1_b).astype(BF16)
        tab_b[pl.ds(i, STEP), :] = t
        t = t.astype(F32)
        put_halves(tab, i, STEP, t[:, :LANES], t[:, LANES:])

    src_out[...] = ((high >> 3) * BYTE + plane(0).astype(jnp.int32)) * 2
    dst_out[...] = ((high & 7) * BYTE + plane(1).astype(jnp.int32)) * 2
    w_out[...] = (plane(3) + plane(4) + plane(5)) * 2.0
    for c in copies:
        c.wait()
    every = jnp.sum(mine[:1, :] + jnp.sum(theirs[:, :1, :], axis=0), keepdims=True)
    count[...] = jnp.maximum(jnp.broadcast_to(every, count.shape), 1.0)
    need[0] = jnp.max(jnp.maximum(mine[1:, :], jnp.max(theirs[:, 1:, :], axis=0))).astype(jnp.int32)


def local_kernel(chunk, backward, counts, src, dst, w, table, out, src_s, dst_s, sems, *accs):
    edges = Edges(0, counts[0], w, (src, dst), (src_s, dst_s), sems)
    edges.fetch()
    for a in accs:
        fill_zero(a)
    edges.walk(chunk, *((dst_s, src_s) if backward else (src_s, dst_s)), table, accs, True)

    @pl.loop(0, out.shape[0], step=STEP)
    def _(i):
        out[pl.ds(i, STEP), :] = functools.reduce(jnp.add, [a[pl.ds(i, STEP), :] for a in accs])


def forward_halo(chunk, edges, src_s, dst_s, from_prev, from_next, part, htab, accs, unpack):
    edges.fetch()
    unpack(from_prev, htab, 0)
    unpack(from_next, htab, htab.shape[0] // 4)
    copy_in(accs[0], part)
    for a in accs[1:]:
        fill_zero(a)
    edges.walk(chunk, src_s, dst_s, htab, accs, True)


def backward_halo(limit, chunk, edges, src_s, dst_s, grad, back_prev, back_next, accs, wait, lists=None):
    split = accs[0].shape[0] // 2
    for a in accs:
        for start in (0, split):
            fill_zero(a.at[pl.ds(start, limit * 2)])
    edges.walk(chunk, dst_s, src_s, grad, accs, wait)
    if lists is None:

        @pl.loop(0, back_prev.shape[0], step=SMALL)
        def _(i):
            back_prev[pl.ds(i, SMALL), :] = functools.reduce(jnp.add, [a[pl.ds(i, SMALL), :] for a in accs])
            back_next[pl.ds(i, SMALL), :] = functools.reduce(jnp.add, [a[pl.ds(split + i, SMALL), :] for a in accs])
        return
    side = lists.shape[0] // 2
    half = (back_prev.shape[0] - side) // 3
    n = half // 2
    for k, out in enumerate((back_prev, back_next)):
        start = k * (split // 2)

        @pl.loop(0, half, step=n)
        def _(i):
            i = pl.multiple_of(i, n)
            pack_rows(out, i, half, *halves(accs, start + i, n), *halves(accs, start + half + i, n))

        out[3 * half : 3 * half + side, :] = lists[k * side : (k + 1) * side, :]


def padded(w, buf):
    low = w.shape[0] // SUB * SUB
    buf[low:, :] = jnp.zeros((buf.shape[0] - low, buf.shape[1]), F32)
    buf[:w.shape[0], :] = w[...]
    return buf[...].astype(BF16)


def hidden_kernel(chunk, counts, src, dst, w, send, from_prev, from_next, part, w2, hid, tab, to_prev, to_next, back, htab, tab_b, w2_pad, buf, idx, idx_sems, src_s, dst_s, sems, *accs):
    fetch = fetch_index(send, idx, idx_sems)
    for c in fetch:
        c.start()
    edges = Edges(counts[0], counts[1], w, (src, dst), (src_s, dst_s), sems)
    w2_b = padded(w2, w2_pad)
    per = send.shape[1] // LANES
    for i in range(2 * per):
        back[i : i + 1, :] = send[i // per : i // per + 1, (i % per) * LANES : (i % per + 1) * LANES] * 2
    forward_halo(chunk, edges, src_s, dst_s, from_prev, from_next, part, htab, accs, unpack_plain)

    @pl.loop(0, hid.shape[0], step=STEP)
    def _(i):
        even, odd = halves(accs, i, STEP)
        h = stack_lanes([jnp.maximum(even, 0.0), jnp.maximum(odd, 0.0)]).astype(BF16)
        hid[pl.ds(i, STEP), :] = h
        t = dot(h, w2_b, COLS_A).astype(BF16)
        tab_b[pl.ds(i, STEP), :] = t
        t = t.astype(F32)
        put_halves(tab, i, STEP, t[:, :LANES], t[:, LANES:])

    for c in fetch:
        c.wait()
    gather_packed(send, idx, tab_b, tab, buf, to_prev, to_next)


def loss_kernel(limit, quad, chunk, classes, counts, src, dst, w, src_back, lists, count, from_prev, from_next, part, labels, mask, loss, grad, back_prev, back_next, htab, src_s, dst_s, back_s, sems, *accs):
    edges = Edges(counts[0], counts[1], w, (src, dst, src_back), (src_s, dst_s, back_s), sems)
    forward_halo(chunk, edges, src_s, dst_s, from_prev, from_next, part, htab, accs, unpack_rows)
    lane = across(SQUARE)
    live = lane < classes - LANES
    scale = 1.0 / count[:1, :]
    loss[...] = jnp.zeros_like(loss)

    @pl.loop(0, labels.shape[0], step=quad)
    def _(first):
        for b in [first + q for q in range(quad)]:
            even, odd = halves(accs, b * LANES, LANES)
            odd = jnp.where(live, odd, -jnp.inf)
            keep = spread(mask[pl.ds(b, 1), :])
            label = jnp.where(keep > 0, spread(labels[pl.ds(b, 1), :]), -1)
            hit_even, hit_odd = lane == label, lane + LANES == label
            top = jnp.max(jnp.maximum(even, odd), axis=1, keepdims=True)
            exp_even, exp_odd = jnp.exp(even - top), jnp.exp(odd - top)
            total = jnp.sum(exp_even + exp_odd, axis=1, keepdims=True)
            norm = jnp.where(jnp.logical_and(lane == 0, keep > 0), top + jnp.log(total), 0.0)
            per_row = norm - jnp.where(hit_even, even, jnp.where(hit_odd, odd, 0.0))
            loss[...] += jnp.sum(per_row.reshape(LANES // SUB, *TILE), axis=0)
            share = keep.astype(F32) * scale * (1.0 / total)
            put_halves(
                grad, b * LANES, LANES, *(e * share - jnp.where(hit, scale, 0.0) for e, hit in ((exp_even, hit_even), (exp_odd, hit_odd)))
            )

    backward_halo(limit, chunk, edges, back_s, dst_s, grad, back_prev, back_next, accs, False, lists)


def take_returns(back, slots, counts, part, got_prev, got_next, accs):
    return_rows(back, slots, 0, counts[0], got_prev, accs)
    return_rows(back, slots, slots.shape[0] // 2, counts[1], got_next, accs)


def fetch_lines(lines, smem, sems):
    return [pltpu.make_async_copy(lines.at[i], smem.at[pl.ds(i * LANES, LANES)], sems.at[i]) for i in range(lines.shape[0])]


def middle_kernel(limit, chunk, counts, src, dst, w, back, got_prev, got_next, part, hid, w2, grad_two, grad, back_prev, back_next, slots, n_back, returned, w2_pad, slot_s, slot_sems, src_s, dst_s, sems, *accs):
    edges = Edges(counts[0], counts[1], w, (src, dst), (src_s, dst_s), sems)
    edges.fetch()
    side = slots.shape[0] // 2
    half = (got_prev.shape[0] - side) // 3
    for k, got in enumerate((got_prev, got_next)):
        slot = got[3 * half :, :].astype(jnp.int32)
        slots[k * side : (k + 1) * side, :] = jnp.maximum(slot, 0) + (1 - k) * side * LANES
        n_back[k] = jnp.sum((slot >= 0).astype(F32)).astype(jnp.int32)
    w2_b = padded(w2, w2_pad)
    unpack_rows(got_prev, returned, 0, half)
    unpack_rows(got_next, returned, 2 * half, half)
    fetch = fetch_lines(slots, slot_s, slot_sems)
    for c in fetch:
        c.start()
    copy_in(accs[0], part)
    for a in accs[1:]:
        fill_zero(a)
    for c in fetch:
        c.wait()
    take_returns(back, slot_s, n_back, part, returned.at[pl.ds(0, 4 * half)], returned.at[pl.ds(4 * half, 4 * half)], accs)
    grad_two[...] = jnp.zeros_like(grad_two)

    @pl.loop(0, hid.shape[0], step=STEP)
    def _(i):
        even, odd = halves(accs, i, STEP)
        d_tab = stack_lanes([even, odd]).astype(BF16)
        h = hid[pl.ds(i, STEP), :]
        grad_two[...] += dot(d_tab, h, ROWS_A)
        d_hid = dot(d_tab, w2_b)
        d_pre = jnp.where(h > 0, d_hid, 0.0)
        put_halves(grad, i, STEP, d_pre[:, :LANES], d_pre[:, LANES:])

    backward_halo(limit, chunk, edges, src_s, dst_s, grad, back_prev, back_next, accs, True)


def last_kernel(back, n_back, slots, got_prev, got_next, part, x, grad_one, slot_s, slot_sems, *accs):
    fetch = fetch_lines(slots, slot_s, slot_sems)
    for c in fetch:
        c.start()
    copy_in(accs[0], part)
    for a in accs[1:]:
        fill_zero(a)
    for c in fetch:
        c.wait()
    take_returns(back, slot_s, n_back, part, got_prev, got_next, accs)
    grad_one[...] = jnp.zeros_like(grad_one)

    @pl.loop(0, x.shape[0], step=STEP)
    def _(i):
        even, odd = halves(accs, i, STEP)
        d_tab = stack_lanes([even, odd]).astype(BF16)
        grad_one[...] += dot(x[pl.ds(i, STEP), :], d_tab, ROWS_A)


def call(body, name, outs, ins, scratch, out_specs=None, collective=None, vmem=14):
    extra = {} if collective is None else dict(collective_id=collective, has_side_effects=True)
    return pl.pallas_call(
        body, name=name, out_shape=outs, in_specs=ins, out_specs=out_specs or jax.tree.map(lambda _: VMEM, outs),
        scratch_shapes=[pltpu.VMEM(s, F32) if isinstance(s, tuple) else s for s in scratch],
        compiler_params=pltpu.CompilerParams(vmem_limit_bytes=vmem * 2**20, **extra),
        cost_estimate=pl.CostEstimate(flops=10**10, bytes_accessed=10**7, transcendentals=0),
    )


def solution(mesh):
    num_dev = mesh.shape[AXIS]
    to_next = [(d, (d + 1) % num_dev) for d in range(num_dev)]
    to_prev = [(d, (d - 1) % num_dev) for d in range(num_dev)]

    def step(x, w_one, w_two, send, edge_src, edge_dst, edge_w, labels, mask):
        rows, halo, edges, classes = x.shape[0], send.shape[1], edge_src.shape[0], w_two.shape[1]
        tab, half, w2_pad = (2 * rows, LANES), (2 * halo, LANES), (2 * LANES, 2 * LANES)
        sds = jax.ShapeDtypeStruct
        tab_f = sds(tab, F32)
        half_b, pack_b = sds((halo, 2 * LANES), BF16), sds((3 * halo // 2, LANES), BF16)
        wide_b = pltpu.VMEM((rows, 2 * LANES), BF16)
        one = sds(TILE, F32)
        dma = pltpu.SemaphoreType.DMA
        chunk_l, chunk_h = 64, 32
        lines = edges // LANES
        slots = lines + 8
        side = halo // LANES
        w2 = w_two.T
        mask = mask.reshape(-1, LANES)
        labels = labels.reshape(-1, LANES)
        lined = [a.reshape(lines, LANES) for a in (edge_src, edge_dst, edge_w)]
        ints = sds((slots, LANES), jnp.int32)
        sided = sds((2 * side, LANES), F32)
        tab_one, tab_b, src, dst, w_lines, used, counts, count, need = call(
            functools.partial(prep_kernel, num_dev, PREP_CHUNK, rows), "prep",
            [tab_f, sds((rows, 2 * LANES), BF16), ints, ints, sds((slots, LANES), F32), sided, sds((2,), jnp.int32), one, sds((1,), jnp.int32)],
            [VMEM] * 6,
            [(6 * slots, LANES), (6 * lines, LANES), pltpu.VMEM((4 * lines, LANES), jnp.int32), sided.shape, (2, LANES), (num_dev - 1, 2, LANES)]
            + [dma((num_dev - 1,))] * 2,
            out_specs=[VMEM] * 6 + [SMEM, VMEM, SMEM], vmem=60, collective=0,
        )(*lined, mask, x, w_one)

        def run(limit):
            compact = limit < halo
            pack_f, half_f = sds((3 * limit // 2 + side, LANES), F32), sds((2 * limit, LANES), F32)
            list_s = [pltpu.SMEM((halo,), jnp.int32), dma((side,))]
            to_p, to_n, w, src_back, lists = call(
                functools.partial(first_kernel, compact, halo), "first", [half_b, half_b, sds((slots * LANES, LANES), F32), ints, sided],
                [VMEM] * 3 + [SMEM] + [VMEM] * 3, [half] + list_s, vmem=8,
            )(tab_one, tab_b, send, counts, src, w_lines, used)
            from_prev = lax.ppermute(to_n, AXIS, to_next)
            from_next = lax.ppermute(to_p, AXIS, to_prev)
            flat, flat_dst, flat_back = src.reshape(-1), dst.reshape(-1), src_back.reshape(-1)

            four = [tab] * 4
            walk = [SMEM, ANY, ANY, VMEM]
            index = pltpu.SMEM((slots * LANES,), jnp.int32)
            walk_s = lambda n: [index] * n + [dma((n, slots * LANES // SEGMENT))]
            slot_s = [pltpu.SMEM((2 * halo,), jnp.int32), dma((2 * side,))]
            local, local_back = (
                call(functools.partial(local_kernel, chunk_l, back), "local_edges", tab_f, walk + [VMEM], walk_s(2) + four)
                for back in (False, True)
            )
            part = local(counts, flat, flat_dst, w, tab_one)
            hid, tab_two, to_p, to_n, back = call(
                functools.partial(hidden_kernel, chunk_h), "hidden",
                [sds((rows, 2 * LANES), BF16), tab_f, pack_b, pack_b, sds((2 * side, LANES), jnp.int32)],
                walk + [VMEM] * 5, [tab, wide_b, w2_pad, half] + list_s + walk_s(2) + four,
            )(counts, flat, flat_dst, w, send, from_prev, from_next, part, w2)
            from_prev = lax.ppermute(to_n, AXIS, to_next)
            from_next = lax.ppermute(to_p, AXIS, to_prev)
            back = back.reshape(-1)
            part = local(counts, flat, flat_dst, w, tab_two)
            loss, grad, to_p, to_n = call(
                functools.partial(loss_kernel, limit, 4, chunk_h, classes), "loss", [one, tab_f, pack_f, pack_f],
                walk + [ANY] + [VMEM] * 7, [tab] + walk_s(3) + four,
            )(counts, flat, flat_dst, w, flat_back, lists, count, from_prev, from_next, part, labels, mask)
            got_prev = lax.ppermute(to_p, AXIS, to_prev)
            got_next = lax.ppermute(to_n, AXIS, to_next)
            part = local_back(counts, flat, flat_dst, w, grad)
            grad_two, grad, to_p, to_n, slot, n_back = call(
                functools.partial(middle_kernel, limit, chunk_h), "middle",
                [sds(w2_pad, F32), tab_f, half_f, half_f, sds((2 * side, LANES), jnp.int32), sds((2,), jnp.int32)],
                walk + [SMEM] + [VMEM] * 5, [(4 * limit, LANES), w2_pad] + slot_s + walk_s(2) + four, out_specs=[VMEM] * 5 + [SMEM],
            )(counts, flat_back, flat_dst, w, back, got_prev, got_next, part, hid, w2)
            got_prev = lax.ppermute(to_p, AXIS, to_prev)
            got_next = lax.ppermute(to_n, AXIS, to_next)
            part = local_back(counts, flat, flat_dst, w, grad)
            grad_one = call(
                last_kernel, "last", sds((x.shape[1], 2 * LANES), F32), [SMEM, SMEM, ANY] + [VMEM] * 4, slot_s + four
            )(back, n_back, slot, got_prev, got_next, part, x)
            return grad_one, grad_two, loss

        limits = [halo // 32 * part for part in (15, 17, 19, 32)]
        need = need.reshape(())
        choice = sum((need > limit).astype(jnp.int32) for limit in limits[:-1])
        grad_one, grad_two, loss = lax.switch(choice, [functools.partial(run, limit) for limit in limits])
        unit = SUB * num_dev
        lines = 2 * (x.shape[1] + -(-classes // SUB) * SUB) + SUB
        lines = -(-lines // unit) * unit
        grad_one, grad_two, mean = call(
            functools.partial(reduce_kernel, num_dev), "reduce", [sds(grad_one.shape, F32), sds((classes, 2 * LANES), F32), sds((1, 1), F32)],
            [VMEM] * 4, [(lines, LANES), (lines, LANES), (lines // 2, LANES), (num_dev // 2 - 1, lines // num_dev, LANES), dma((2, 2 * num_dev))],
            collective=1, vmem=8,
        )(grad_one, grad_two, loss, count)
        return mean.reshape(()), grad_one, grad_two.T

    row = P(AXIS)
    return jax.shard_map(
        step, mesh=mesh, in_specs=(row, P(), P(), row, row, row, row, row, row), out_specs=(P(), P(), P()), check_vma=False
    )
```
